16 devices in a mesh: dp: 2 (over y, z), tp: 8 (over x, core).
Axes of the slice: x: 4, y: 2, z: 1, core: 2. Of those that a mesh axis runs over, the one named last changes fastest.
The devices are a block of a 4x4x8 slice.
Arguments:
- y_one: float32 [16, 1024, 1024], P('dp', 'tp'), parts along dimension 0
- y_two: float32 [16, 1024, 1024], P('dp', 'tp'), parts along dimension 0
- dy_one: float32 [16, 1024, 1024], P('dp', 'tp'), parts along dimension 0
- dy_two: float32 [16, 1024, 1024], P('dp', 'tp'), parts along dimension 0
- w_qkv: bfloat16 [1, 1024, 8, 3, 128], P(None, None, 'tp')
- w_out: bfloat16 [1, 8, 128, 1024], P(None, 'tp')
- w_up: bfloat16 [1, 1024, 4096], P(None, None, 'tp')
- w_down: bfloat16 [1, 4096, 1024], P(None, 'tp')
Outputs:
- output 1: float32 [16, 1024, 1024], P('dp', 'tp'), parts along dimension 0
- output 2: float32 [16, 1024, 1024], P('dp', 'tp'), parts along dimension 0
- output 3: float32 [16, 1024, 1024], P('dp', 'tp'), parts along dimension 0
- output 4: float32 [16, 1024, 1024], P('dp', 'tp'), parts along dimension 0
- output 5: float32 [2, 1024, 8, 3, 128], P('dp', None, 'tp'), parts along dimension 0
- output 6: float32 [2, 8, 128, 1024], P('dp', 'tp'), parts along dimension 0
- output 7: float32 [2, 1024, 4096], P('dp', None, 'tp'), parts along dimension 0
- output 8: float32 [2, 4096, 1024], P('dp', 'tp'), parts along dimension 0
There are 2 independent parts. The reference program is written for one: setup_inputs(seed, part) draws one part's arguments, and reference() takes and returns one part's arrays. A program takes and returns all parts, laid end to end along the dimension named above; an argument that names none is the same for every part.
All inputs are finite; a program needn't handle non-finite values.
Results may differ from the reference program's by a relative error of at most 0.00836604.
Values are sent between devices in bfloat16 or wider.
A program may use at most 768 MiB of HBM per device.

```python
import jax
import jax.numpy as jnp
from jax import lax

SEQ_COUNT = 8
SEQ_LEN = 1024
HIDDEN = 1024
N_HEADS = 8
FFN_DIM = 4096
N_LAYERS = 1

HEAD_DIM = HIDDEN // N_HEADS
TOKENS = SEQ_COUNT * SEQ_LEN
STATE_SHAPE = (SEQ_COUNT, SEQ_LEN, HIDDEN)
RMS_EPS = 1e-6
ATTN_SCALE = HEAD_DIM ** -0.5
Q_GAIN = 2.5
OUT_GAIN = 0.6
DOWN_GAIN = 0.5


def setup_inputs(seed: int = 0, part: int = 0) -> dict:
    base_key = jax.random.key(seed)
    act_keys = jax.random.split(jax.random.fold_in(base_key, part), 4)
    w_keys = jax.random.split(jax.random.fold_in(base_key, 100003), 4)
    y_one = jax.random.normal(act_keys[0], STATE_SHAPE, jnp.float32)
    y_two = jax.random.normal(act_keys[1], STATE_SHAPE, jnp.float32)
    dy_one = jax.random.normal(act_keys[2], STATE_SHAPE, jnp.float32)
    dy_two = jax.random.normal(act_keys[3], STATE_SHAPE, jnp.float32)
    qkv_gain = jnp.array([Q_GAIN, 1.0, 1.0], jnp.float32).reshape(1, 1, 1, 3, 1)
    w_qkv = (jax.random.normal(w_keys[0], (N_LAYERS, HIDDEN, N_HEADS, 3, HEAD_DIM), jnp.float32) * qkv_gain * HIDDEN ** -0.5).astype(jnp.bfloat16)
    w_out = (jax.random.normal(w_keys[1], (N_LAYERS, N_HEADS, HEAD_DIM, HIDDEN), jnp.float32) * (OUT_GAIN * HIDDEN ** -0.5)).astype(jnp.bfloat16)
    w_up = (jax.random.normal(w_keys[2], (N_LAYERS, HIDDEN, FFN_DIM), jnp.float32) * HIDDEN ** -0.5).astype(jnp.bfloat16)
    w_down = (jax.random.normal(w_keys[3], (N_LAYERS, FFN_DIM, HIDDEN), jnp.float32) * (DOWN_GAIN * FFN_DIM ** -0.5)).astype(jnp.bfloat16)
    return {"y_one": y_one, "y_two": y_two, "dy_one": dy_one, "dy_two": dy_two, "w_qkv": w_qkv, "w_out": w_out, "w_up": w_up, "w_down": w_down}


def rms_norm(tensor):
    return tensor * lax.rsqrt(jnp.mean(tensor * tensor, axis=-1, keepdims=True) + RMS_EPS)


def rms_back(tensor, grad_in):
    inv_rms = lax.rsqrt(jnp.mean(tensor * tensor, axis=-1, keepdims=True) + RMS_EPS)
    return inv_rms * grad_in - tensor * (inv_rms * inv_rms * inv_rms) * jnp.mean(grad_in * tensor, axis=-1, keepdims=True)


def gelu_tanh(tensor):
    return jax.nn.gelu(tensor, approximate=True)


def mixed_dot(left, right):
    return jnp.dot(left, right, preferred_element_type=jnp.float32)


def as_wide(tensor):
    return tensor.astype(jnp.float32)


def attn_forward(qkv_seq):
    q_heads = as_wide(qkv_seq[0])
    k_heads = as_wide(qkv_seq[1])
    v_heads = as_wide(qkv_seq[2])
    scores = jnp.einsum("nqd,nkd->nqk", q_heads, k_heads) * ATTN_SCALE
    attn_prob = jax.nn.softmax(scores, axis=-1)
    context = jnp.einsum("nqk,nkd->nqd", as_wide(attn_prob.astype(jnp.bfloat16)), v_heads)
    return context.astype(jnp.bfloat16)


def attn_backward(operands):
    qkv_seq, d_context = operands
    q_heads = as_wide(qkv_seq[0])
    k_heads = as_wide(qkv_seq[1])
    v_heads = as_wide(qkv_seq[2])
    scores = jnp.einsum("nqd,nkd->nqk", q_heads, k_heads) * ATTN_SCALE
    attn_prob = jax.nn.softmax(scores, axis=-1)
    d_ctx = as_wide(d_context)
    d_prob = jnp.einsum("nqd,nkd->nqk", d_ctx, v_heads)
    d_value = jnp.einsum("nqk,nqd->nkd", as_wide(attn_prob.astype(jnp.bfloat16)), d_ctx)
    d_scores = attn_prob * (d_prob - jnp.sum(d_prob * attn_prob, axis=-1, keepdims=True)) * ATTN_SCALE
    d_scores = as_wide(d_scores.astype(jnp.bfloat16))
    d_query = jnp.einsum("nqk,nkd->nqd", d_scores, k_heads)
    d_key = jnp.einsum("nqk,nqd->nkd", d_scores, q_heads)
    return jnp.stack([d_query, d_key, d_value]).astype(jnp.bfloat16)


def block_backward(state_in, layer_weights):
    y_one, y_two, dy_one, dy_two = state_in
    w_qkv, w_out, w_up, w_down = layer_weights
    w_qkv_flat = w_qkv.reshape(HIDDEN, 3 * HIDDEN)
    w_out_flat = w_out.reshape(HIDDEN, HIDDEN)
    u_mlp = rms_norm(y_one).astype(jnp.bfloat16).reshape(TOKENS, HIDDEN)
    pre_act = mixed_dot(u_mlp, w_up)
    hidden, gelu_pull = jax.vjp(gelu_tanh, pre_act)
    hidden_b = hidden.astype(jnp.bfloat16)
    x_two = y_two - mixed_dot(hidden_b, w_down).reshape(STATE_SHAPE)
    cot_mlp = dy_two.astype(jnp.bfloat16).reshape(TOKENS, HIDDEN)
    dw_down = mixed_dot(hidden_b.T, cot_mlp)
    d_pre = gelu_pull(mixed_dot(cot_mlp, w_down.T))[0].astype(jnp.bfloat16)
    dw_up = mixed_dot(u_mlp.T, d_pre)
    dy_one = dy_one + rms_back(y_one, mixed_dot(d_pre, w_up.T).reshape(STATE_SHAPE))
    u_att = rms_norm(x_two).astype(jnp.bfloat16).reshape(TOKENS, HIDDEN)
    qkv_seqs = mixed_dot(u_att, w_qkv_flat).astype(jnp.bfloat16).reshape(SEQ_COUNT, SEQ_LEN, N_HEADS, 3, HEAD_DIM).transpose(0, 3, 2, 1, 4)
    context = lax.map(attn_forward, qkv_seqs)
    context_flat = context.transpose(0, 2, 1, 3).reshape(TOKENS, HIDDEN)
    x_one = y_one - mixed_dot(context_flat, w_out_flat).reshape(STATE_SHAPE)
    cot_att = dy_one.astype(jnp.bfloat16).reshape(TOKENS, HIDDEN)
    dw_out = mixed_dot(context_flat.T, cot_att)
    d_context = mixed_dot(cot_att, w_out_flat.T).astype(jnp.bfloat16).reshape(SEQ_COUNT, SEQ_LEN, N_HEADS, HEAD_DIM).transpose(0, 2, 1, 3)
    d_qkv = lax.map(attn_backward, (qkv_seqs, d_context))
    d_qkv_flat = d_qkv.transpose(0, 3, 2, 1, 4).reshape(TOKENS, 3 * HIDDEN)
    dw_qkv = mixed_dot(u_att.T, d_qkv_flat)
    dx_two = dy_two + rms_back(x_two, mixed_dot(d_qkv_flat, w_qkv_flat.T).reshape(STATE_SHAPE))
    grads = (dw_qkv.reshape(HIDDEN, N_HEADS, 3, HEAD_DIM), dw_out.reshape(N_HEADS, HEAD_DIM, HIDDEN), dw_up, dw_down)
    return (x_one, x_two, dy_one, dx_two), grads


def reference(y_one, y_two, dy_one, dy_two, w_qkv, w_out, w_up, w_down):
    final_state, grad_stack = lax.scan(block_backward, (y_one, y_two, dy_one, dy_two), (w_qkv, w_out, w_up, w_down), reverse=True)
    x_one, x_two, dx_one, dx_two = final_state
    dw_qkv, dw_out, dw_up, dw_down = grad_stack
    return (x_one, x_two, dx_one, dx_two, dw_qkv, dw_out, dw_up, dw_down)
```

```python
import jax
import jax.numpy as jnp
from jax import lax
from jax.sharding import PartitionSpec as P

RMS_EPS = 1e-6


def inv_rms(tensor):
    return lax.rsqrt(jnp.mean(tensor * tensor, axis=-1, keepdims=True) + RMS_EPS)


def rms_norm(tensor):
    return tensor * inv_rms(tensor)


def rms_back(tensor, grad_in):
    scale = inv_rms(tensor)
    return scale * grad_in - tensor * (scale * scale * scale) * jnp.mean(grad_in * tensor, axis=-1, keepdims=True)


def gelu_tanh(tensor):
    return jax.nn.gelu(tensor, approximate=True)


def to_sequences(tensor):
    return lax.all_to_all(tensor, "tp", split_axis=0, concat_axis=1, tiled=True)


def to_positions(tensor):
    return lax.all_to_all(tensor, "tp", split_axis=1, concat_axis=0, tiled=True)


def dot32(spec, left, right):
    return jnp.einsum(spec, left, right, preferred_element_type=jnp.float32)


def local_backward(y_one, y_two, dy_one, dy_two, w_qkv, w_out, w_up, w_down):
    bf16 = jnp.bfloat16
    attn_scale = w_qkv.shape[4] ** -0.5
    up_full = lax.all_gather(w_up[0], "tp", axis=1, tiled=True)
    down_full = lax.all_gather(w_down[0], "tp", axis=0, tiled=True)
    qkv_full = lax.all_gather(w_qkv[0], "tp", axis=1, tiled=True)
    out_full = lax.all_gather(w_out[0], "tp", axis=0, tiled=True)

    u_mlp = rms_norm(y_one).astype(bf16)
    hidden, gelu_pull = jax.vjp(gelu_tanh, dot32("bsh,hf->bsf", u_mlp, up_full))
    hidden_b = hidden.astype(bf16)
    x_two = y_two - dot32("bsf,fh->bsh", hidden_b, down_full)
    cot_mlp = dy_two.astype(bf16)
    d_pre = gelu_pull(dot32("bsh,fh->bsf", cot_mlp, down_full))[0].astype(bf16)
    dy_one = dy_one + rms_back(y_one, dot32("bsf,hf->bsh", d_pre, up_full))

    u_att = to_sequences(rms_norm(x_two).astype(bf16))
    cot_att = to_sequences(dy_one.astype(bf16))

    dw_down = lax.psum_scatter(dot32("bsf,bsh->fh", hidden_b, cot_mlp), "tp", scatter_dimension=0, tiled=True)
    dw_up = lax.psum_scatter(dot32("bsh,bsf->fh", u_mlp, d_pre), "tp", scatter_dimension=0, tiled=True).T

    qkv_all = dot32("bsh,hnjd->jbnsd", u_att, qkv_full).astype(bf16)
    q_heads, k_heads, v_heads = qkv_all[0], qkv_all[1], qkv_all[2]
    scores = dot32("bnqd,bnkd->bnqk", q_heads, k_heads) * attn_scale
    attn_prob = jax.nn.softmax(scores, axis=-1)
    prob_b = attn_prob.astype(bf16)
    context = dot32("bnqk,bnkd->bnqd", prob_b, v_heads).astype(bf16)
    context_pos = to_positions(jnp.swapaxes(context, 1, 2).reshape(u_att.shape))
    x_one = y_one - dot32("bsm,mh->bsh", context_pos, out_full.reshape(-1, out_full.shape[-1]))
    dw_out = lax.psum_scatter(dot32("bnqd,bqh->ndh", context, cot_att), "tp", scatter_dimension=0, tiled=True)
    d_context = dot32("bqh,ndh->bnqd", cot_att, out_full).astype(bf16)
    d_prob = dot32("bnqd,bnkd->bnqk", d_context, v_heads)
    d_value = dot32("bnqk,bnqd->bnkd", prob_b, d_context)
    d_scores = (attn_prob * (d_prob - jnp.sum(d_prob * attn_prob, axis=-1, keepdims=True)) * attn_scale).astype(bf16)
    d_query = dot32("bnqk,bnkd->bnqd", d_scores, k_heads)
    d_key = dot32("bnqk,bnqd->bnkd", d_scores, q_heads)
    d_qkv = jnp.stack([d_query.astype(bf16), d_key.astype(bf16), d_value.astype(bf16)])
    dw_qkv_rows = dot32("jbnsd,bsh->njdh", d_qkv, u_att)
    dw_qkv = lax.psum_scatter(dw_qkv_rows.reshape(-1, dw_qkv_rows.shape[-1]), "tp", scatter_dimension=0, tiled=True)
    dw_qkv = jnp.moveaxis(dw_qkv.reshape(-1, *dw_qkv_rows.shape[1:]), 3, 0)
    du_att = to_positions(dot32("jbnsd,hnjd->bsh", d_qkv, qkv_full))
    dx_two = dy_two + rms_back(x_two, du_att)
    return (x_one, x_two, dy_one, dx_two, dw_qkv[None], dw_out[None], dw_up[None], dw_down[None])


def solution(mesh):
    state_spec = P("dp", "tp", None)
    in_specs = (state_spec, state_spec, state_spec, state_spec, P(None, None, "tp", None, None), P(None, "tp", None, None), P(None, None, "tp"), P(None, "tp", None))
    out_specs = (state_spec, state_spec, state_spec, state_spec, P("dp", None, "tp", None, None), P("dp", "tp", None, None), P("dp", None, "tp"), P("dp", "tp", None))
    return jax.shard_map(local_backward, mesh=mesh, in_specs=in_specs, out_specs=out_specs, check_vma=False)
```

```python
import functools

import jax
import jax.numpy as jnp
from jax import lax
from jax.experimental import pallas as pl
from jax.experimental.pallas import tpu as pltpu
from jax.sharding import PartitionSpec as P

RMS_EPS = 1e-6
MESH = pl.DeviceIdType.MESH
BF16, F32 = jnp.bfloat16, jnp.float32
VMEM_LIMIT = 64 * 1024 * 1024 - 65536


def inv_rms(tensor):
    return lax.rsqrt(jnp.mean(tensor * tensor, axis=-1, keepdims=True) + RMS_EPS)


def rms_norm(tensor):
    return tensor * inv_rms(tensor)


def rms_back(tensor, grad_in):
    scale = inv_rms(tensor)
    return scale * grad_in - tensor * (scale * scale * scale) * jnp.mean(grad_in * tensor, axis=-1, keepdims=True)


def gelu_and_slope(tensor):
    root = (2.0 / jnp.pi) ** 0.5
    squared = tensor * tensor
    tanh = jnp.tanh(root * (tensor + 0.044715 * (tensor * squared)))
    cdf = 0.5 * (1.0 + tanh)
    slope = cdf + (0.5 * root) * tensor * ((1.0 - tanh * tanh) * (1.0 + (3 * 0.044715) * squared))
    return tensor * cdf, slope


def dot_nn(left, right):
    return lax.dot_general(left, right, (((1,), (0,)), ((), ())), preferred_element_type=F32)


def dot_nt(left, right):
    return lax.dot_general(left, right, (((1,), (1,)), ((), ())), preferred_element_type=F32)


def dot_tn(left, right):
    return lax.dot_general(left, right, (((0,), (0,)), ((), ())), preferred_element_type=F32)


class Ring:
    def __init__(self):
        me = lax.axis_index("tp")
        chip, core = me // 2, me % 2
        self.me, self.chip, self.core = me, chip, core
        self.chips = (chip, chip + 1 - 2 * (chip % 2), 3 - chip, (chip + 2) % 4)

    def at(self, slot):
        core = self.core if slot % 2 == 0 else 1 - self.core
        return self.chips[slot // 2] * 2 + core

    def at_traced(self, slot):
        relation, other = slot // 2, slot % 2
        own, near_t, near_f, opposite = self.chips
        chip = jnp.where(relation == 0, own, jnp.where(relation == 1, near_t, jnp.where(relation == 2, near_f, opposite)))
        return chip * 2 + (self.core + other) % 2

    def barrier(self):
        barrier = pltpu.get_barrier_semaphore()
        for slot in (1, 2, 3, 4, 5):
            pl.semaphore_signal(barrier, inc=1, device_id={"tp": self.at(slot)}, device_id_type=MESH)
        pl.semaphore_wait(barrier, 5)

    def copy(self, src, dst, send_sem, recv_sem, slot):
        return pltpu.make_async_remote_copy(src_ref=src, dst_ref=dst, send_sem=send_sem, recv_sem=recv_sem, device_id={"tp": self.at(slot)}, device_id_type=MESH)


PARTNER, SAME_T, OTHER_T, SAME_F, OTHER_F, SAME_O, OTHER_O = 1, 2, 3, 4, 5, 6, 7


def mlp_kernel(
    y_one, y_two, dy_one, dy_two, w_up, w_down, w_att,
    x_two, dx_one, uc_seq, att_full, part_own, part_near,
    u_all, c_all, up_all, down_all, acc, uc_own, relay, y_buf, x_buf,
    load_sem, y_sem, x_sem, w_send, w_recv, uc_send, uc_recv, att_send, att_recv, a2a_send, a2a_recv, relay_recv,
):
    ring = Ring()
    half = 512
    slab = 128

    def weight(which, src_slot, dst_slot, to, index):
        buf = (up_all, down_all)[which]
        return ring.copy(buf.at[src_slot], buf.at[dst_slot], w_send.at[index], w_recv.at[dst_slot, which], to)

    def weight_pair(src_slot, dst_slot, to, index):
        return [weight(which, src_slot, dst_slot, to, index + which) for which in (0, 1)]

    w_own = weight_pair(0, 1, PARTNER, 0) + weight_pair(0, 2, SAME_T, 2) + weight_pair(0, 4, SAME_F, 4)
    w_near_t = weight_pair(2, 6, SAME_F, 6) + weight_pair(2, 3, PARTNER, 8)
    w_near_f = weight_pair(4, 5, PARTNER, 10)
    w_far = weight_pair(6, 7, PARTNER, 12)

    def uc_pair(src_slot, dst_slot, to, index):
        return [ring.copy(buf.at[src_slot], buf.at[dst_slot], uc_send.at[index + which], uc_recv.at[dst_slot, which], to) for which, buf in enumerate((u_all, c_all))]

    uc_out = uc_pair(0, 2, SAME_T, 0) + uc_pair(0, 1, PARTNER, 2)
    uc_pass = uc_pair(2, 3, PARTNER, 4)

    def att(src, dst_slot, to, index):
        return ring.copy(src, att_full.at[dst_slot], att_send.at[index], att_recv.at[dst_slot], to)

    att_out = [att(w_att, 4, SAME_F, 0), att(w_att, 2, SAME_T, 1), att(w_att, 1, PARTNER, 2)]
    att_near_t = [att(att_full.at[2], 6, SAME_F, 3), att(att_full.at[2], 3, PARTNER, 4)]
    att_near_f = [att(att_full.at[4], 5, PARTNER, 5)]
    att_far = [att(att_full.at[6], 7, PARTNER, 6)]

    a2a_out = {slot: ring.copy(uc_own.at[slot], uc_seq.at[slot], a2a_send.at[slot], a2a_recv.at[slot], slot) for slot in (1, 2, 3, 4, 5)}
    a2a_out[SAME_O] = ring.copy(uc_own.at[SAME_O], relay.at[0], a2a_send.at[SAME_O], relay_recv.at[0], SAME_T)
    a2a_out[OTHER_O] = ring.copy(uc_own.at[OTHER_O], relay.at[1], a2a_send.at[OTHER_O], relay_recv.at[1], SAME_F)
    a2a_pass = [
        ring.copy(relay.at[0], uc_seq.at[SAME_O], a2a_send.at[8], a2a_recv.at[SAME_O], SAME_F),
        ring.copy(relay.at[1], uc_seq.at[OTHER_O], a2a_send.at[9], a2a_recv.at[OTHER_O], OTHER_T),
    ]
    uc_keep = pltpu.make_async_copy(uc_own.at[0], uc_seq.at[0], load_sem.at[4])

    def start(copies):
        for copy in copies:
            copy.start()

    loads = [
        pltpu.make_async_copy(w_up, up_all.at[0], load_sem.at[0]),
        pltpu.make_async_copy(w_down, down_all.at[0], load_sem.at[1]),
        pltpu.make_async_copy(y_one, acc.at[0], load_sem.at[2]),
        pltpu.make_async_copy(dy_two, acc.at[1], load_sem.at[3]),
    ]
    start(loads)
    ring.barrier()
    loads[0].wait()
    loads[1].wait()
    start(w_own)
    loads[2].wait()
    loads[3].wait()

    def normalize(step, carry):
        rows = pl.ds(pl.multiple_of(step * slab, slab), slab)
        u_all[0, rows, :] = rms_norm(acc[0, rows, :]).astype(BF16)
        c_all[0, rows, :] = acc[1, rows, :].astype(BF16)
        acc[0, rows, :] = jnp.zeros((slab, acc.shape[2]), F32)
        acc[1, rows, :] = jnp.zeros((slab, acc.shape[2]), F32)
        return carry

    lax.fori_loop(0, acc.shape[1] // slab, normalize, 0)
    start(uc_out)

    def y_loads(step, buf):
        seq = ring.at_traced(7 - step)
        rows = pl.ds(pl.multiple_of(seq * slab, slab), slab)
        return [pltpu.make_async_copy(src.at[rows], y_buf.at[buf, which], y_sem.at[buf, which]) for which, src in enumerate((y_one, y_two, dy_one))]

    def x_stores(step, buf):
        seq = ring.at_traced(7 - step)
        rows = pl.ds(pl.multiple_of(seq * slab, slab), slab)
        return [pltpu.make_async_copy(x_buf.at[buf, which], dst.at[rows], x_sem.at[buf, which]) for which, dst in enumerate((x_two, dx_one))]

    def feed_forward(step, carry):
        slot = jnp.where(step == 3, 4, jnp.where(step == 4, 3, step))

        @pl.when(step >= 1)
        def _():
            for which, buf in enumerate((up_all, down_all)):
                ring.copy(buf.at[slot], buf.at[slot], w_send.at[0], w_recv.at[slot, which], PARTNER).wait_recv()

        @pl.when(step == 2)
        def _():
            start(w_near_t)
            start(att_out)

        @pl.when(step == 3)
        def _():
            start(w_near_f)

        @pl.when(step == 6)
        def _():
            start(w_far)

        @pl.when(step == 7)
        def _():
            start(y_loads(0, 0))

        def rows_step(part, carry):
            rows = pl.ds(pl.multiple_of(part * half, half), half)
            hidden, slope = gelu_and_slope(dot_nt(u_all[0, rows, :], up_all[slot]))
            d_pre = (slope * dot_nt(c_all[0, rows, :], down_all[slot])).astype(BF16)
            acc[0, rows, :] += dot_nn(hidden.astype(BF16), down_all[slot])
            acc[1, rows, :] += dot_nn(d_pre, up_all[slot])
            return carry

        lax.fori_loop(0, acc.shape[1] // half, rows_step, 0)
        return carry

    lax.fori_loop(0, 8, feed_forward, 0)

    def finish(step, carry):
        slot = 7 - step
        buf = step % 2
        seq = ring.at_traced(slot)
        rows = pl.ds(pl.multiple_of(seq * slab, slab), slab)
        for copy in y_loads(step, buf):
            copy.wait()

        @pl.when(step < 7)
        def _():
            start(y_loads(step + 1, 1 - buf))

        @pl.when(step >= 2)
        def _():
            for copy in x_stores(step - 2, buf):
                copy.wait()

        y_first = y_buf[buf, 0]
        x_second = y_buf[buf, 1] - acc[0, rows, :]
        dy_first = y_buf[buf, 2] + rms_back(y_first, acc[1, rows, :])
        x_buf[buf, 0] = x_second
        x_buf[buf, 1] = dy_first
        uc_own[slot, 0] = rms_norm(x_second).astype(BF16)
        uc_own[slot, 1] = dy_first.astype(BF16)
        acc[0, rows, :] = jnp.zeros((slab, acc.shape[2]), F32)
        acc[1, rows, :] = jnp.zeros((slab, acc.shape[2]), F32)
        start(x_stores(step, buf))
        return carry

    lax.fori_loop(0, 8, finish, 0)
    for slot in (7, 6, 5, 4, 3, 2, 1):
        a2a_out[slot].start()
    uc_keep.start()
    for step in (6, 7):
        for copy in x_stores(step, step % 2):
            copy.wait()

    def gradients(step, carry):
        first = step // 8
        tokens = (step % 8) // 2
        slot = 4 - 4 * first

        @pl.when((step == 2) | (step == 4) | (step == 6))
        def _():
            for which, buf in enumerate((u_all, c_all)):
                ring.copy(buf.at[tokens], buf.at[tokens], uc_send.at[0], uc_recv.at[tokens, which], PARTNER).wait_recv()

        @pl.when(step == 4)
        def _():
            start(uc_pass)

        @pl.when(step == 5)
        def _():
            ring.copy(w_att, att_full.at[2], att_send.at[0], att_recv.at[2], PARTNER).wait_recv()
            start(att_near_t)
            ring.copy(w_att, att_full.at[4], att_send.at[0], att_recv.at[4], PARTNER).wait_recv()
            start(att_near_f)

        @pl.when(step == 10)
        def _():
            for index in (0, 1):
                ring.copy(relay.at[index], relay.at[index], a2a_send.at[0], relay_recv.at[index], PARTNER).wait_recv()
            start(a2a_pass)

        rows = pl.ds(pl.multiple_of((step % 2) * half, half), half)
        u_part, c_part = u_all[tokens, rows, :], c_all[tokens, rows, :]
        hidden, slope = gelu_and_slope(dot_nt(up_all[slot], u_part))
        d_pre = (slope * dot_nt(down_all[slot], c_part)).astype(BF16)
        acc[first, pl.ds(0, half), :] += dot_nn(d_pre, u_part)
        acc[first, pl.ds(half, half), :] += dot_nn(hidden.astype(BF16), c_part)
        return carry

    lax.fori_loop(0, 16, gradients, 0)
    out_near = pltpu.make_async_copy(acc.at[0], part_near, load_sem.at[0])
    out_own = pltpu.make_async_copy(acc.at[1], part_own, load_sem.at[1])
    out_near.start()
    out_own.start()

    ring.copy(w_att, att_full.at[6], att_send.at[0], att_recv.at[6], PARTNER).wait_recv()
    start(att_far)
    for slot in (1, 3, 5, 7):
        ring.copy(w_att, att_full.at[slot], att_send.at[0], att_recv.at[slot], PARTNER).wait_recv()
    for slot in range(1, 8):
        ring.copy(uc_own.at[slot], uc_seq.at[slot], a2a_send.at[0], a2a_recv.at[slot], PARTNER).wait_recv()
    for copy in w_own + w_near_t + w_near_f + w_far + uc_out + uc_pass + att_out + att_near_t + att_near_f + att_far + list(a2a_out.values()) + a2a_pass:
        copy.wait_send()
    uc_keep.wait()
    out_near.wait()
    out_own.wait()


def mlp_call(y_one, y_two, dy_one, dy_two, w_up, w_down, w_att):
    tokens, hidden = y_one.shape
    ffn = w_up.shape[0]
    any_spec = pl.BlockSpec(memory_space=pl.ANY)
    dma, vmem = pltpu.SemaphoreType.DMA, pltpu.VMEM
    out_shape = (
        jax.ShapeDtypeStruct((tokens, hidden), F32),
        jax.ShapeDtypeStruct((tokens, hidden), F32),
        jax.ShapeDtypeStruct((8, 2, tokens // 8, hidden), BF16),
        jax.ShapeDtypeStruct((8, *w_att.shape), BF16),
        jax.ShapeDtypeStruct((2 * ffn, hidden), F32),
        jax.ShapeDtypeStruct((2 * ffn, hidden), F32),
    )
    scratch = [
        vmem((4, tokens, hidden), BF16), vmem((4, tokens, hidden), BF16),
        vmem((8, ffn, hidden), BF16), vmem((8, ffn, hidden), BF16),
        vmem((2, tokens, hidden), F32),
        vmem((8, 2, tokens // 8, hidden), BF16), vmem((2, 2, tokens // 8, hidden), BF16),
        vmem((2, 3, tokens // 8, hidden), F32), vmem((2, 2, tokens // 8, hidden), F32),
        dma((5,)), dma((2, 3)), dma((2, 2)), dma((14,)), dma((8, 2)), dma((6,)), dma((4, 2)), dma((7,)), dma((8,)), dma((10,)), dma((8,)), dma((2,)),
    ]
    return pl.pallas_call(
        mlp_kernel,
        out_shape=out_shape,
        in_specs=[any_spec] * 7,
        out_specs=(any_spec,) * 6,
        scratch_shapes=scratch,
        compiler_params=pltpu.CompilerParams(collective_id=0, has_side_effects=True, vmem_limit_bytes=VMEM_LIMIT),
        cost_estimate=pl.CostEstimate(flops=70 * 10**9, bytes_accessed=64 * 2**20, transcendentals=0),
        name="feed_forward",
    )(y_one, y_two, dy_one, dy_two, w_up, w_down, w_att)


def attention_kernel(
    scale, uc_seq, w_att, att_full, part_near,
    near_recv, d_att, o_pos, du_pos, wo_full,
    uc_all, w_buf, qkv, d_ctx, d_qkv, o_all, du_all, part_send, part_keep, part_core, part_t, part_f, o_relay, du_relay,
    load_sem, w_sem, wo_sem, near_sem, core_send, core_recv, t_send, t_recv, f_sem, o_send, o_recv, du_send, du_recv, o_relay_recv, du_relay_recv,
):
    ring = Ring()
    slab, hidden = uc_seq.shape[2], uc_seq.shape[3]
    seq_len = 8 * slab
    dim = w_att.shape[0] // 4
    tile = 256

    def head_slot(step):
        pair = step // 2
        relation = jnp.where(pair == 0, 1, jnp.where(pair == 1, 3, jnp.where(pair == 2, 2, 0)))
        return relation * 2 + 1 - step % 2

    def w_load(step, buf):
        return pltpu.make_async_copy(att_full.at[head_slot(step)], w_buf.at[buf], w_sem.at[buf])

    w_load_own = pltpu.make_async_copy(w_att, w_buf.at[1], w_sem.at[1])
    near = ring.copy(part_near, near_recv, near_sem.at[0], near_sem.at[1], SAME_F)

    def core_copy(step, buf):
        relation = head_slot(step) // 2
        return ring.copy(part_send.at[buf], part_core.at[relation], core_send.at[buf], core_recv.at[relation], PARTNER)

    t_copies = [
        ring.copy(part_keep.at[1], part_t.at[0], t_send.at[0], t_recv.at[0], SAME_T),
        ring.copy(part_keep.at[3], part_t.at[1], t_send.at[1], t_recv.at[1], SAME_T),
    ]
    f_copy = ring.copy(part_keep.at[2], part_f, f_sem.at[0], f_sem.at[1], SAME_F)

    def rows_of(slot):
        return pl.ds(slot * slab, slab)

    def to_positions(src, dst, relay, send_sem, recv_sem, relay_sem):
        near_t, near_f = ring.at(SAME_T), ring.at(SAME_F)
        out = [
            ring.copy(src.at[rows_of(SAME_O)], relay.at[0], send_sem.at[6], relay_sem.at[0], SAME_T),
            ring.copy(src.at[rows_of(OTHER_O)], relay.at[1], send_sem.at[7], relay_sem.at[1], SAME_F),
        ] + [ring.copy(src.at[rows_of(slot)], dst.at[ring.me], send_sem.at[slot], recv_sem.at[slot], slot) for slot in (5, 4, 3, 2, 1)]
        onward = [
            ring.copy(relay.at[0], dst.at[near_t], send_sem.at[8], recv_sem.at[SAME_O], SAME_F),
            ring.copy(relay.at[1], dst.at[near_f], send_sem.at[9], recv_sem.at[OTHER_O], OTHER_T),
        ]
        keep = pltpu.make_async_copy(src.at[rows_of(0)], dst.at[ring.me], send_sem.at[0])
        return out, onward, keep

    o_out, o_pass, o_keep = to_positions(o_all, o_pos, o_relay, o_send, o_recv, o_relay_recv)
    du_out, du_pass, du_keep = to_positions(du_all, du_pos, du_relay, du_send, du_recv, du_relay_recv)

    def start(copies):
        for copy in copies:
            copy.start()

    loads = [pltpu.make_async_copy(uc_seq.at[slot, which], uc_all.at[which, rows_of(slot)], load_sem.at[slot, which]) for slot in range(8) for which in (0, 1)]
    start(loads)
    w_load(0, 0).start()
    ring.barrier()
    near.start()
    du_all[...] = jnp.zeros_like(du_all)
    for copy in loads:
        copy.wait()

    def head_step(step, carry):
        buf = step % 2
        slot = head_slot(step)
        relation = slot // 2
        w_load(step, buf).wait()

        @pl.when(step < 6)
        def _():
            w_load(step + 1, 1 - buf).start()

        @pl.when(step == 6)
        def _():
            w_load_own.start()

        head = ring.at_traced(slot)
        columns = pl.ds(pl.multiple_of(head * dim, dim), dim)
        wo_copy = pltpu.make_async_copy(w_buf.at[buf, pl.ds(3 * dim, dim)], wo_full.at[head], wo_sem.at[0])
        wo_copy.start()
        qkv[...] = dot_nt(uc_all[0], w_buf[buf, pl.ds(0, 3 * dim), :]).astype(BF16)
        d_ctx[...] = dot_nt(uc_all[1], w_buf[buf, pl.ds(3 * dim, dim), :]).astype(BF16)

        def query_tile(part, carry):
            d_key, d_value = carry
            rows = pl.ds(pl.multiple_of(part * tile, tile), tile)
            query, key, value = qkv[rows, pl.ds(0, dim)], qkv[:, pl.ds(dim, dim)], qkv[:, pl.ds(2 * dim, dim)]
            scores = dot_nt(query, key) * scale
            grown = jnp.exp(scores - jnp.max(scores, axis=-1, keepdims=True))
            prob = grown / jnp.sum(grown, axis=-1, keepdims=True)
            prob_b = prob.astype(BF16)
            o_all[rows, columns] = dot_nn(prob_b, value).astype(BF16)
            d_out = d_ctx[rows, :]
            d_prob = dot_nt(d_out, value)
            d_score = (prob * (d_prob - jnp.sum(d_prob * prob, axis=-1, keepdims=True)) * scale).astype(BF16)
            d_qkv[rows, pl.ds(0, dim)] = dot_nn(d_score, key).astype(BF16)
            return d_key + dot_tn(d_score, query), d_value + dot_tn(prob_b, d_out)

        zeros = jnp.zeros((seq_len, dim), F32)
        d_key, d_value = lax.fori_loop(0, seq_len // tile, query_tile, (zeros, zeros))
        d_qkv[:, pl.ds(dim, dim)] = d_key.astype(BF16)
        d_qkv[:, pl.ds(2 * dim, dim)] = d_value.astype(BF16)

        def du_tile(part, carry):
            rows = pl.ds(pl.multiple_of(part * tile, tile), tile)
            du_all[rows, :] += dot_nn(d_qkv[rows, :], w_buf[buf, pl.ds(0, 3 * dim), :])
            return carry

        lax.fori_loop(0, seq_len // tile, du_tile, 0)

        def write_part(dst, index):
            dst[index, pl.ds(0, 3 * dim), :] = dot_tn(d_qkv[...], uc_all[0])
            dst[index, pl.ds(3 * dim, dim), :] = dot_tn(o_all[:, columns], uc_all[1])

        @pl.when(step % 2 == 0)
        def _():
            send = (step // 2) % 2

            @pl.when(step >= 4)
            def _():
                core_copy(step - 4, send).wait_send()

            write_part(part_send, send)
            core_copy(step, send).start()

        @pl.when(step % 2 == 1)
        def _():
            write_part(part_keep, relation)
            core_copy(step - 1, 0).wait_recv()
            part_keep[relation] += part_core[relation]

        @pl.when(step == 1)
        def _():
            t_copies[0].start()

        @pl.when(step == 3)
        def _():
            t_copies[1].start()

        @pl.when(step == 5)
        def _():
            t_copies[1].wait_recv()
            part_keep[2] += part_t[1]
            f_copy.start()

        wo_copy.wait()
        return carry

    lax.fori_loop(0, 8, head_step, 0)
    start(o_out)
    start(du_out)
    o_keep.start()
    du_keep.start()
    for copy in o_out[:2]:
        copy.wait_recv()
    start(o_pass)
    t_copies[0].wait_recv()
    part_keep[0] += part_t[0]
    f_copy.wait_recv()
    part_keep[0] += part_f[...]
    d_att_copy = pltpu.make_async_copy(part_keep.at[0], d_att, load_sem.at[0, 0])
    d_att_copy.start()
    for copy in du_out[:2]:
        copy.wait_recv()
    start(du_pass)

    for dst, recv_sem in ((o_pos, o_recv), (du_pos, du_recv)):
        for slot in range(1, 8):
            ring.copy(dst.at[0], dst.at[ring.at(slot)], near_sem.at[0], recv_sem.at[slot], PARTNER).wait_recv()
    for copy in o_out + du_out + o_pass + du_pass + t_copies + [f_copy, near, core_copy(4, 0), core_copy(6, 1)]:
        copy.wait_send()
    near.wait_recv()
    o_keep.wait()
    du_keep.wait()
    d_att_copy.wait()


def attention_call(uc_seq, w_att, att_full, part_near):
    slab, hidden = uc_seq.shape[2:]
    rows = w_att.shape[0]
    dim = rows // 4
    seq_len = 8 * slab
    any_spec = pl.BlockSpec(memory_space=pl.ANY)
    dma, vmem = pltpu.SemaphoreType.DMA, pltpu.VMEM
    out_shape = (
        jax.ShapeDtypeStruct(part_near.shape, F32),
        jax.ShapeDtypeStruct(w_att.shape, F32),
        jax.ShapeDtypeStruct((8, slab, hidden), BF16),
        jax.ShapeDtypeStruct((8, slab, hidden), F32),
        jax.ShapeDtypeStruct((8, dim, hidden), BF16),
    )
    scratch = [
        vmem((2, seq_len, hidden), BF16), vmem((2, rows, hidden), BF16), vmem((seq_len, 3 * dim), BF16), vmem((seq_len, dim), BF16), vmem((seq_len, 3 * dim), BF16),
        vmem((seq_len, hidden), BF16), vmem((seq_len, hidden), F32),
        vmem((2, rows, hidden), F32), vmem((4, rows, hidden), F32), vmem((4, rows, hidden), F32), vmem((2, rows, hidden), F32), vmem((rows, hidden), F32),
        vmem((2, slab, hidden), BF16), vmem((2, slab, hidden), F32),
        dma((8, 2)), dma((2,)), dma((1,)), dma((2,)), dma((2,)), dma((4,)), dma((2,)), dma((2,)), dma((2,)), dma((10,)), dma((8,)), dma((10,)), dma((8,)), dma((2,)), dma((2,)),
    ]
    return pl.pallas_call(
        functools.partial(attention_kernel, dim ** -0.5),
        out_shape=out_shape,
        in_specs=[any_spec] * 4,
        out_specs=(any_spec,) * 5,
        scratch_shapes=scratch,
        compiler_params=pltpu.CompilerParams(collective_id=1, has_side_effects=True, vmem_limit_bytes=VMEM_LIMIT),
        cost_estimate=pl.CostEstimate(flops=40 * 10**9, bytes_accessed=64 * 2**20, transcendentals=0),
        name="attention",
    )(uc_seq, w_att, att_full, part_near)


def local_backward(y_one, y_two, dy_one, dy_two, w_qkv, w_out, w_up, w_down):
    shape = y_one.shape
    hidden = shape[2]
    _, _, _, parts, dim = w_qkv.shape
    flat = [tensor.reshape(-1, hidden) for tensor in (y_one, y_two, dy_one, dy_two)]
    w_att = jnp.concatenate([w_qkv.reshape(hidden, parts * dim).T, w_out.reshape(dim, hidden)])
    x_two, dx_one, uc_seq, att_full, part_own, part_near = mlp_call(*flat, w_up[0].T, w_down[0], w_att)
    near_recv, d_att, o_pos, du_pos, wo_full = attention_call(uc_seq, w_att, att_full, part_near)
    grads = part_own + near_recv
    ffn = w_down.shape[1]
    x_one = y_one - jnp.einsum("bsm,mh->bsh", o_pos, wo_full.reshape(-1, hidden), preferred_element_type=F32)
    x_two = x_two.reshape(shape)
    dx_two = dy_two + rms_back(x_two, du_pos)
    dw_qkv = d_att[: parts * dim].T.reshape(1, hidden, 1, parts, dim)
    dw_out = d_att[parts * dim :].reshape(1, 1, dim, hidden)
    return (x_one, x_two, dx_one.reshape(shape), dx_two, dw_qkv, dw_out, grads[:ffn].T[None], grads[ffn:][None])


def solution(mesh):
    state_spec = P("dp", "tp", None)
    in_specs = (state_spec, state_spec, state_spec, state_spec, P(None, None, "tp", None, None), P(None, "tp", None, None), P(None, None, "tp"), P(None, "tp", None))
    out_specs = (state_spec, state_spec, state_spec, state_spec, P("dp", None, "tp", None, None), P("dp", "tp", None, None), P("dp", None, "tp"), P("dp", "tp", None))
    return jax.shard_map(local_backward, mesh=mesh, in_specs=in_specs, out_specs=out_specs, check_vma=False)
```

```python
import functools

import jax
import jax.numpy as jnp
from jax import lax
from jax.experimental import pallas as pl
from jax.experimental.pallas import tpu as pltpu
from jax.sharding import PartitionSpec as P

RMS_EPS = 1e-6
MESH = pl.DeviceIdType.MESH
BF16, F32 = jnp.bfloat16, jnp.float32
VMEM_LIMIT = 64 * 1024 * 1024 - 65536


def inv_rms(tensor):
    return lax.rsqrt(jnp.mean(tensor * tensor, axis=-1, keepdims=True) + RMS_EPS)


def rms_norm(tensor):
    return tensor * inv_rms(tensor)


def rms_back(tensor, grad_in):
    scale = inv_rms(tensor)
    return scale * grad_in - tensor * (scale * scale * scale) * jnp.mean(grad_in * tensor, axis=-1, keepdims=True)


def gelu_and_slope(tensor):
    root = (2.0 / jnp.pi) ** 0.5
    squared = tensor * tensor
    tanh = jnp.tanh(root * (tensor + 0.044715 * (tensor * squared)))
    cdf = 0.5 * (1.0 + tanh)
    slope = cdf + (0.5 * root) * tensor * ((1.0 - tanh * tanh) * (1.0 + (3 * 0.044715) * squared))
    return tensor * cdf, slope


def dot_nn(left, right):
    return lax.dot_general(left, right, (((1,), (0,)), ((), ())), preferred_element_type=F32)


def dot_nt(left, right):
    return lax.dot_general(left, right, (((1,), (1,)), ((), ())), preferred_element_type=F32)


def dot_tn(left, right):
    return lax.dot_general(left, right, (((0,), (0,)), ((), ())), preferred_element_type=F32)


class Ring:
    def __init__(self):
        me = lax.axis_index("tp")
        chip, core = me // 2, me % 2
        self.me, self.chip, self.core = me, chip, core
        self.chips = (chip, chip + 1 - 2 * (chip % 2), 3 - chip, (chip + 2) % 4)

    def at(self, slot):
        core = self.core if slot % 2 == 0 else 1 - self.core
        return self.chips[slot // 2] * 2 + core

    def at_traced(self, slot):
        relation, other = slot // 2, slot % 2
        own, near_t, near_f, opposite = self.chips
        chip = jnp.where(relation == 0, own, jnp.where(relation == 1, near_t, jnp.where(relation == 2, near_f, opposite)))
        return chip * 2 + (self.core + other) % 2

    def barrier(self):
        barrier = pltpu.get_barrier_semaphore()
        for slot in (1, 2, 3, 4, 5):
            pl.semaphore_signal(barrier, inc=1, device_id={"tp": self.at(slot)}, device_id_type=MESH)
        pl.semaphore_wait(barrier, 5)

    def copy(self, src, dst, send_sem, recv_sem, slot):
        return pltpu.make_async_remote_copy(src_ref=src, dst_ref=dst, send_sem=send_sem, recv_sem=recv_sem, device_id={"tp": self.at(slot)}, device_id_type=MESH)


PARTNER, SAME_T, OTHER_T, SAME_F, OTHER_F, SAME_O, OTHER_O = 1, 2, 3, 4, 5, 6, 7


def mlp_kernel(
    y_one, y_two, dy_one, dy_two, w_up, w_down, w_qkv, w_out,
    x_two, dx_one, uc_seq, att_full, part_own, part_near, near_recv,
    u_all, c_all, up_all, down_all, acc, uc_own, relay, y_buf, x_buf, up_raw, qkv_raw, att_own,
    load_sem, y_sem, x_sem, w_send, w_recv, uc_send, uc_recv, att_send, att_recv, a2a_send, a2a_recv, relay_recv, near_sem,
):
    ring = Ring()
    half = 512
    slab = 128

    def weight(which, src_slot, dst_slot, to, index):
        buf = (up_all, down_all)[which]
        return ring.copy(buf.at[src_slot], buf.at[dst_slot], w_send.at[index], w_recv.at[dst_slot, which], to)

    def weight_pair(src_slot, dst_slot, to, index):
        return [weight(which, src_slot, dst_slot, to, index + which) for which in (0, 1)]

    w_own = weight_pair(0, 1, PARTNER, 0) + weight_pair(0, 2, SAME_T, 2) + weight_pair(0, 4, SAME_F, 4)
    w_near_t = weight_pair(2, 6, SAME_F, 6) + weight_pair(2, 3, PARTNER, 8)
    w_near_f = weight_pair(4, 5, PARTNER, 10)
    w_far = weight_pair(6, 7, PARTNER, 12)

    def uc_pair(src_slot, dst_slot, to, index):
        return [ring.copy(buf.at[src_slot], buf.at[dst_slot], uc_send.at[index + which], uc_recv.at[dst_slot, which], to) for which, buf in enumerate((u_all, c_all))]

    uc_out = uc_pair(0, 2, SAME_T, 0) + uc_pair(0, 1, PARTNER, 2)
    uc_pass = uc_pair(2, 3, PARTNER, 4)

    def att(src, dst_slot, to, index):
        return ring.copy(src, att_full.at[dst_slot], att_send.at[index], att_recv.at[dst_slot], to)

    att_out = [att(att_own, 4, SAME_F, 0), att(att_own, 2, SAME_T, 1), att(att_own, 1, PARTNER, 2)]
    att_keep = pltpu.make_async_copy(att_own, att_full.at[0], load_sem.at[6])
    att_near_t = [att(att_full.at[2], 6, SAME_F, 3), att(att_full.at[2], 3, PARTNER, 4)]
    att_near_f = [att(att_full.at[4], 5, PARTNER, 5)]
    att_far = [att(att_full.at[6], 7, PARTNER, 6)]

    a2a_out = {slot: ring.copy(uc_own.at[slot], uc_seq.at[slot], a2a_send.at[slot], a2a_recv.at[slot], slot) for slot in (1, 2, 3, 4, 5)}
    a2a_out[SAME_O] = ring.copy(uc_own.at[SAME_O], relay.at[0], a2a_send.at[SAME_O], relay_recv.at[0], SAME_T)
    a2a_out[OTHER_O] = ring.copy(uc_own.at[OTHER_O], relay.at[1], a2a_send.at[OTHER_O], relay_recv.at[1], SAME_F)
    a2a_pass = [
        ring.copy(relay.at[0], uc_seq.at[SAME_O], a2a_send.at[8], a2a_recv.at[SAME_O], SAME_F),
        ring.copy(relay.at[1], uc_seq.at[OTHER_O], a2a_send.at[9], a2a_recv.at[OTHER_O], OTHER_T),
    ]
    uc_keep = pltpu.make_async_copy(uc_own.at[0], uc_seq.at[0], load_sem.at[4])

    def start(copies):
        for copy in copies:
            copy.start()

    dim = w_out.shape[0]
    near_rows = near_recv.shape[0]
    near = ring.copy(acc.at[0, pl.ds(0, near_rows)], near_recv, near_sem.at[0], near_sem.at[1], SAME_F)

    loads = [
        pltpu.make_async_copy(w_down, down_all.at[0], load_sem.at[0]),
        pltpu.make_async_copy(w_up, up_raw, load_sem.at[1]),
        pltpu.make_async_copy(y_one, acc.at[0], load_sem.at[2]),
        pltpu.make_async_copy(dy_two, acc.at[1], load_sem.at[3]),
        pltpu.make_async_copy(w_qkv, qkv_raw, load_sem.at[5]),
        pltpu.make_async_copy(w_out, att_own.at[pl.ds(3 * dim, dim)], load_sem.at[7]),
    ]
    start(loads)
    ring.barrier()
    loads[0].wait()
    start(w_own[1::2])
    loads[1].wait()
    for part in range(up_raw.shape[1] // dim):
        up_all[0, pl.ds(part * dim, dim), :] = up_raw[:, pl.ds(part * dim, dim)].T
    start(w_own[0::2])
    loads[2].wait()
    loads[3].wait()

    def normalize(step, carry):
        rows = pl.ds(pl.multiple_of(step * slab, slab), slab)
        u_all[0, rows, :] = rms_norm(acc[0, rows, :]).astype(BF16)
        c_all[0, rows, :] = acc[1, rows, :].astype(BF16)
        acc[0, rows, :] = jnp.zeros((slab, acc.shape[2]), F32)
        acc[1, rows, :] = jnp.zeros((slab, acc.shape[2]), F32)
        return carry

    lax.fori_loop(0, acc.shape[1] // slab, normalize, 0)
    start(uc_out)
    loads[4].wait()
    for part in range(3):
        att_own[pl.ds(part * dim, dim), :] = qkv_raw[part].T
    loads[5].wait()
    att_keep.start()

    def y_loads(step, buf):
        seq = ring.at_traced(7 - step)
        rows = pl.ds(pl.multiple_of(seq * slab, slab), slab)
        return [pltpu.make_async_copy(src.at[rows], y_buf.at[buf, which], y_sem.at[buf, which]) for which, src in enumerate((y_one, y_two, dy_one))]

    def x_stores(step, buf):
        seq = ring.at_traced(7 - step)
        rows = pl.ds(pl.multiple_of(seq * slab, slab), slab)
        return [pltpu.make_async_copy(x_buf.at[buf, which], dst.at[rows], x_sem.at[buf, which]) for which, dst in enumerate((x_two, dx_one))]

    def feed_forward(step, carry):
        slot = jnp.where(step == 3, 4, jnp.where(step == 4, 3, step))

        @pl.when(step >= 1)
        def _():
            for which, buf in enumerate((up_all, down_all)):
                ring.copy(buf.at[slot], buf.at[slot], w_send.at[0], w_recv.at[slot, which], PARTNER).wait_recv()

        @pl.when(step == 2)
        def _():
            start(w_near_t)
            start(att_out)

        @pl.when(step == 3)
        def _():
            start(w_near_f)

        @pl.when(step == 6)
        def _():
            start(w_far)

        @pl.when(step == 7)
        def _():
            start(y_loads(0, 0))

        def rows_step(part, carry):
            rows = pl.ds(pl.multiple_of(part * half, half), half)
            hidden, slope = gelu_and_slope(dot_nt(u_all[0, rows, :], up_all[slot]))
            d_pre = (slope * dot_nt(c_all[0, rows, :], down_all[slot])).astype(BF16)
            acc[0, rows, :] += dot_nn(hidden.astype(BF16), down_all[slot])
            acc[1, rows, :] += dot_nn(d_pre, up_all[slot])
            return carry

        lax.fori_loop(0, acc.shape[1] // half, rows_step, 0)
        return carry

    lax.fori_loop(0, 8, feed_forward, 0)

    def finish(step, carry):
        slot = 7 - step
        buf = step % 2
        seq = ring.at_traced(slot)
        rows = pl.ds(pl.multiple_of(seq * slab, slab), slab)
        for copy in y_loads(step, buf):
            copy.wait()

        @pl.when(step < 7)
        def _():
            start(y_loads(step + 1, 1 - buf))

        @pl.when(step >= 2)
        def _():
            for copy in x_stores(step - 2, buf):
                copy.wait()

        y_first = y_buf[buf, 0]
        x_second = y_buf[buf, 1] - acc[0, rows, :]
        dy_first = y_buf[buf, 2] + rms_back(y_first, acc[1, rows, :])
        x_buf[buf, 0] = x_second
        x_buf[buf, 1] = dy_first
        uc_own[slot, 0] = rms_norm(x_second).astype(BF16)
        uc_own[slot, 1] = dy_first.astype(BF16)
        acc[0, rows, :] = jnp.zeros((slab, acc.shape[2]), F32)
        acc[1, rows, :] = jnp.zeros((slab, acc.shape[2]), F32)
        start(x_stores(step, buf))
        return carry

    lax.fori_loop(0, 8, finish, 0)
    for slot in (7, 6, 5, 4, 3, 2, 1):
        a2a_out[slot].start()
    uc_keep.start()
    for step in (6, 7):
        for copy in x_stores(step, step % 2):
            copy.wait()

    def gradients(step, carry):
        first = step // 8
        tokens = (step % 8) // 2
        slot = 4 - 4 * first

        @pl.when((step == 2) | (step == 4) | (step == 6))
        def _():
            for which, buf in enumerate((u_all, c_all)):
                ring.copy(buf.at[tokens], buf.at[tokens], uc_send.at[0], uc_recv.at[tokens, which], PARTNER).wait_recv()

        @pl.when(step == 4)
        def _():
            start(uc_pass)

        @pl.when(step == 5)
        def _():
            ring.copy(att_own, att_full.at[2], att_send.at[0], att_recv.at[2], PARTNER).wait_recv()
            start(att_near_t)
            ring.copy(att_own, att_full.at[4], att_send.at[0], att_recv.at[4], PARTNER).wait_recv()
            start(att_near_f)

        @pl.when(step == 8)
        def _():
            near.start()

        @pl.when(step == 10)
        def _():
            for index in (0, 1):
                ring.copy(relay.at[index], relay.at[index], a2a_send.at[0], relay_recv.at[index], PARTNER).wait_recv()
            start(a2a_pass)

        rows = pl.ds(pl.multiple_of((step % 2) * half, half), half)
        u_part, c_part = u_all[tokens, rows, :], c_all[tokens, rows, :]
        hidden, slope = gelu_and_slope(dot_nt(up_all[slot], u_part))
        d_pre = (slope * dot_nt(down_all[slot], c_part)).astype(BF16)
        acc[first, pl.ds(0, half), :] += dot_nn(d_pre, u_part)
        acc[first, pl.ds(half, half), :] += dot_nn(hidden.astype(BF16), c_part)
        return carry

    lax.fori_loop(0, 16, gradients, 0)
    out_near = pltpu.make_async_copy(acc.at[0, pl.ds(near_rows, acc.shape[1] - near_rows)], part_near, load_sem.at[0])
    out_own = pltpu.make_async_copy(acc.at[1], part_own, load_sem.at[1])
    out_near.start()
    out_own.start()

    ring.copy(att_own, att_full.at[6], att_send.at[0], att_recv.at[6], PARTNER).wait_recv()
    start(att_far)
    for slot in (1, 3, 5, 7):
        ring.copy(att_own, att_full.at[slot], att_send.at[0], att_recv.at[slot], PARTNER).wait_recv()
    for slot in range(1, 8):
        ring.copy(uc_own.at[slot], uc_seq.at[slot], a2a_send.at[0], a2a_recv.at[slot], PARTNER).wait_recv()
    for copy in w_own + w_near_t + w_near_f + w_far + uc_out + uc_pass + att_out + att_near_t + att_near_f + att_far + list(a2a_out.values()) + a2a_pass:
        copy.wait_send()
    near.wait()
    uc_keep.wait()
    att_keep.wait()
    out_near.wait()
    out_own.wait()


def mlp_call(y_one, y_two, dy_one, dy_two, w_up, w_down, w_qkv, w_out):
    tokens, hidden = y_one.shape
    ffn = w_down.shape[0]
    dim = w_out.shape[0]
    near_rows = ffn // 2
    any_spec = pl.BlockSpec(memory_space=pl.ANY)
    dma, vmem = pltpu.SemaphoreType.DMA, pltpu.VMEM
    out_shape = (
        jax.ShapeDtypeStruct((tokens, hidden), F32),
        jax.ShapeDtypeStruct((tokens, hidden), F32),
        jax.ShapeDtypeStruct((8, 2, tokens // 8, hidden), BF16),
        jax.ShapeDtypeStruct((8, 4 * dim, hidden), BF16),
        jax.ShapeDtypeStruct((2 * ffn, hidden), F32),
        jax.ShapeDtypeStruct((2 * ffn - near_rows, hidden), F32),
        jax.ShapeDtypeStruct((near_rows, hidden), F32),
    )
    scratch = [
        vmem((4, tokens, hidden), BF16), vmem((4, tokens, hidden), BF16),
        vmem((8, ffn, hidden), BF16), vmem((8, ffn, hidden), BF16),
        vmem((2, tokens, hidden), F32),
        vmem((8, 2, tokens // 8, hidden), BF16), vmem((2, 2, tokens // 8, hidden), BF16),
        vmem((2, 3, tokens // 8, hidden), F32), vmem((2, 2, tokens // 8, hidden), F32),
        vmem((hidden, ffn), BF16), vmem((3, hidden, dim), BF16), vmem((4 * dim, hidden), BF16),
        dma((8,)), dma((2, 3)), dma((2, 2)), dma((14,)), dma((8, 2)), dma((6,)), dma((4, 2)), dma((7,)), dma((8,)), dma((10,)), dma((8,)), dma((2,)), dma((2,)),
    ]
    return pl.pallas_call(
        mlp_kernel,
        out_shape=out_shape,
        in_specs=[any_spec] * 8,
        out_specs=(any_spec,) * 7,
        scratch_shapes=scratch,
        compiler_params=pltpu.CompilerParams(collective_id=0, has_side_effects=True, vmem_limit_bytes=VMEM_LIMIT),
        cost_estimate=pl.CostEstimate(flops=70 * 10**9, bytes_accessed=64 * 2**20, transcendentals=0),
        name="feed_forward",
    )(y_one, y_two, dy_one, dy_two, w_up, w_down, w_qkv, w_out)


def attention_kernel(
    scale, uc_seq, att_full, part_near,
    near_recv, d_att, o_pos, du_pos, wo_full,
    uc_all, w_buf, qkv, d_ctx, d_qkv, o_all, du_all, part_send, part_keep, part_core, part_t, part_f, o_relay, du_relay, near_buf,
    load_sem, w_sem, wo_sem, near_sem, core_send, core_recv, t_send, t_recv, f_sem, o_send, o_recv, du_send, du_recv, o_relay_recv, du_relay_recv,
):
    ring = Ring()
    slab, hidden = uc_seq.shape[2], uc_seq.shape[3]
    seq_len = 8 * slab
    dim = att_full.shape[1] // 4
    tile = 256

    def head_slot(step):
        pair = step // 2
        relation = jnp.where(pair == 0, 1, jnp.where(pair == 1, 3, jnp.where(pair == 2, 2, 0)))
        return relation * 2 + 1 - step % 2

    def w_load(step, buf):
        return pltpu.make_async_copy(att_full.at[head_slot(step)], w_buf.at[buf], w_sem.at[buf])

    near_load = pltpu.make_async_copy(part_near, near_buf, near_sem.at[2])
    near = ring.copy(near_buf, near_recv, near_sem.at[0], near_sem.at[1], SAME_F)

    def core_copy(step, buf):
        relation = head_slot(step) // 2
        return ring.copy(part_send.at[buf], part_core.at[relation], core_send.at[buf], core_recv.at[relation], PARTNER)

    t_copies = [
        ring.copy(part_keep.at[1], part_t.at[0], t_send.at[0], t_recv.at[0], SAME_T),
        ring.copy(part_keep.at[3], part_t.at[1], t_send.at[1], t_recv.at[1], SAME_T),
    ]
    f_copy = ring.copy(part_keep.at[2], part_f, f_sem.at[0], f_sem.at[1], SAME_F)

    def rows_of(slot):
        return pl.ds(slot * slab, slab)

    def to_positions(src, dst, relay, send_sem, recv_sem, relay_sem):
        near_t, near_f = ring.at(SAME_T), ring.at(SAME_F)
        out = [
            ring.copy(src.at[rows_of(SAME_O)], relay.at[0], send_sem.at[6], relay_sem.at[0], SAME_T),
            ring.copy(src.at[rows_of(OTHER_O)], relay.at[1], send_sem.at[7], relay_sem.at[1], SAME_F),
        ] + [ring.copy(src.at[rows_of(slot)], dst.at[ring.me], send_sem.at[slot], recv_sem.at[slot], slot) for slot in (5, 4, 3, 2, 1)]
        onward = [
            ring.copy(relay.at[0], dst.at[near_t], send_sem.at[8], recv_sem.at[SAME_O], SAME_F),
            ring.copy(relay.at[1], dst.at[near_f], send_sem.at[9], recv_sem.at[OTHER_O], OTHER_T),
        ]
        keep = pltpu.make_async_copy(src.at[rows_of(0)], dst.at[ring.me], send_sem.at[0])
        return out, onward, keep

    o_out, o_pass, o_keep = to_positions(o_all, o_pos, o_relay, o_send, o_recv, o_relay_recv)
    du_out, du_pass, du_keep = to_positions(du_all, du_pos, du_relay, du_send, du_recv, du_relay_recv)

    def start(copies):
        for copy in copies:
            copy.start()

    loads = [pltpu.make_async_copy(uc_seq.at[slot, which], uc_all.at[which, rows_of(slot)], load_sem.at[slot, which]) for slot in range(8) for which in (0, 1)]
    near_load.start()
    start(loads)
    w_load(0, 0).start()
    ring.barrier()
    near_load.wait()
    near.start()
    du_all[...] = jnp.zeros_like(du_all)
    for copy in loads:
        copy.wait()

    def head_step(step, carry):
        buf = step % 2
        slot = head_slot(step)
        relation = slot // 2
        w_load(step, buf).wait()

        @pl.when(step < 7)
        def _():
            w_load(step + 1, 1 - buf).start()

        head = ring.at_traced(slot)
        columns = pl.ds(pl.multiple_of(head * dim, dim), dim)
        wo_copy = pltpu.make_async_copy(w_buf.at[buf, pl.ds(3 * dim, dim)], wo_full.at[head], wo_sem.at[0])
        wo_copy.start()
        qkv[...] = dot_nt(uc_all[0], w_buf[buf, pl.ds(0, 3 * dim), :]).astype(BF16)
        d_ctx[...] = dot_nt(uc_all[1], w_buf[buf, pl.ds(3 * dim, dim), :]).astype(BF16)

        def query_tile(part, carry):
            d_key, d_value = carry
            rows = pl.ds(pl.multiple_of(part * tile, tile), tile)
            query, key, value = qkv[rows, pl.ds(0, dim)], qkv[:, pl.ds(dim, dim)], qkv[:, pl.ds(2 * dim, dim)]
            scores = dot_nt(query, key) * scale
            grown = jnp.exp(scores - jnp.max(scores, axis=-1, keepdims=True))
            prob = grown / jnp.sum(grown, axis=-1, keepdims=True)
            prob_b = prob.astype(BF16)
            o_all[rows, columns] = dot_nn(prob_b, value).astype(BF16)
            d_out = d_ctx[rows, :]
            d_prob = dot_nt(d_out, value)
            d_score = (prob * (d_prob - jnp.sum(d_prob * prob, axis=-1, keepdims=True)) * scale).astype(BF16)
            d_qkv[rows, pl.ds(0, dim)] = dot_nn(d_score, key).astype(BF16)
            return d_key + dot_tn(d_score, query), d_value + dot_tn(prob_b, d_out)

        zeros = jnp.zeros((seq_len, dim), F32)
        d_key, d_value = lax.fori_loop(0, seq_len // tile, query_tile, (zeros, zeros))
        d_qkv[:, pl.ds(dim, dim)] = d_key.astype(BF16)
        d_qkv[:, pl.ds(2 * dim, dim)] = d_value.astype(BF16)

        def du_tile(part, carry):
            rows = pl.ds(pl.multiple_of(part * tile, tile), tile)
            du_all[rows, :] += dot_nn(d_qkv[rows, :], w_buf[buf, pl.ds(0, 3 * dim), :])
            return carry

        lax.fori_loop(0, seq_len // tile, du_tile, 0)

        def write_part(dst, index):
            dst[index, pl.ds(0, 3 * dim), :] = dot_tn(d_qkv[...], uc_all[0])
            dst[index, pl.ds(3 * dim, dim), :] = dot_tn(o_all[:, columns], uc_all[1])

        @pl.when(step % 2 == 0)
        def _():
            send = (step // 2) % 2

            @pl.when(step >= 4)
            def _():
                core_copy(step - 4, send).wait_send()

            write_part(part_send, send)
            core_copy(step, send).start()

        @pl.when(step % 2 == 1)
        def _():
            write_part(part_keep, relation)
            core_copy(step - 1, 0).wait_recv()
            part_keep[relation] += part_core[relation]

        @pl.when(step == 1)
        def _():
            t_copies[0].start()

        @pl.when(step == 3)
        def _():
            t_copies[1].start()

        @pl.when(step == 5)
        def _():
            t_copies[1].wait_recv()
            part_keep[2] += part_t[1]
            f_copy.start()

        wo_copy.wait()
        return carry

    lax.fori_loop(0, 8, head_step, 0)
    start(o_out)
    start(du_out)
    o_keep.start()
    du_keep.start()
    for copy in o_out[:2]:
        copy.wait_recv()
    start(o_pass)
    t_copies[0].wait_recv()
    part_keep[0] += part_t[0]
    f_copy.wait_recv()
    part_keep[0] += part_f[...]
    d_att_copy = pltpu.make_async_copy(part_keep.at[0], d_att, load_sem.at[0, 0])
    d_att_copy.start()
    for copy in du_out[:2]:
        copy.wait_recv()
    start(du_pass)

    for dst, recv_sem in ((o_pos, o_recv), (du_pos, du_recv)):
        for slot in range(1, 8):
            ring.copy(dst.at[0], dst.at[ring.at(slot)], near_sem.at[0], recv_sem.at[slot], PARTNER).wait_recv()
    for copy in o_out + du_out + o_pass + du_pass + t_copies + [f_copy, near, core_copy(4, 0), core_copy(6, 1)]:
        copy.wait_send()
    near.wait_recv()
    o_keep.wait()
    du_keep.wait()
    d_att_copy.wait()


def attention_call(uc_seq, att_full, part_near):
    slab, hidden = uc_seq.shape[2:]
    rows = att_full.shape[1]
    dim = rows // 4
    seq_len = 8 * slab
    any_spec = pl.BlockSpec(memory_space=pl.ANY)
    dma, vmem = pltpu.SemaphoreType.DMA, pltpu.VMEM
    out_shape = (
        jax.ShapeDtypeStruct(part_near.shape, F32),
        jax.ShapeDtypeStruct((rows, hidden), F32),
        jax.ShapeDtypeStruct((8, slab, hidden), BF16),
        jax.ShapeDtypeStruct((8, slab, hidden), F32),
        jax.ShapeDtypeStruct((8, dim, hidden), BF16),
    )
    scratch = [
        vmem((2, seq_len, hidden), BF16), vmem((2, rows, hidden), BF16), vmem((seq_len, 3 * dim), BF16), vmem((seq_len, dim), BF16), vmem((seq_len, 3 * dim), BF16),
        vmem((seq_len, hidden), BF16), vmem((seq_len, hidden), F32),
        vmem((2, rows, hidden), F32), vmem((4, rows, hidden), F32), vmem((4, rows, hidden), F32), vmem((2, rows, hidden), F32), vmem((rows, hidden), F32),
        vmem((2, slab, hidden), BF16), vmem((2, slab, hidden), F32), vmem(part_near.shape, F32),
        dma((8, 2)), dma((2,)), dma((1,)), dma((3,)), dma((2,)), dma((4,)), dma((2,)), dma((2,)), dma((2,)), dma((10,)), dma((8,)), dma((10,)), dma((8,)), dma((2,)), dma((2,)),
    ]
    return pl.pallas_call(
        functools.partial(attention_kernel, dim ** -0.5),
        out_shape=out_shape,
        in_specs=[any_spec] * 3,
        out_specs=(any_spec,) * 5,
        scratch_shapes=scratch,
        compiler_params=pltpu.CompilerParams(collective_id=1, has_side_effects=True, vmem_limit_bytes=VMEM_LIMIT),
        cost_estimate=pl.CostEstimate(flops=40 * 10**9, bytes_accessed=64 * 2**20, transcendentals=0),
        name="attention",
    )(uc_seq, att_full, part_near)


def finish_kernel(
    y_one, o_pos, wo_full, x_two, dx_one, dy_two, du_pos, up_own, up_near, up_rest, down_own, down_rest, d_qkv, d_out,
    x_one_out, x_two_out, dx_one_out, dx_two_out, dw_up, dw_down, dw_qkv, dw_out,
):
    x_one_out[0] = y_one[0] - dot_nn(o_pos[0], wo_full[...])
    x_two_out[0] = x_two[...]
    dx_one_out[0] = dx_one[...]
    dx_two_out[0] = dy_two[0] + rms_back(x_two[...], du_pos[0])
    half = up_near.shape[0]
    dw_up[:, pl.ds(0, half)] = (up_own[pl.ds(0, half), :] + up_near[...]).T
    dw_up[:, pl.ds(half, half)] = (up_own[pl.ds(half, half), :] + up_rest[...]).T
    dw_down[...] = down_own[...] + down_rest[...]
    dim = dw_qkv.shape[2]
    for part in range(3):
        dw_qkv[pl.ds(part, dw_qkv.shape[0] // 3, stride=3), 0, :] = d_qkv[pl.ds(part * dim, dim), :].T
    dw_out[...] = d_out[...]


def finish_call(y_one, o_pos, wo_full, x_two, dx_one, dy_two, du_pos, part_own, near_first, near_rest, d_att):
    seqs, slab, hidden = y_one.shape
    ffn = part_own.shape[0] // 2
    dim = d_att.shape[0] // 4
    half = near_first.shape[0]
    state = pl.BlockSpec((1, slab, hidden), lambda step: (step, 0, 0))
    flat = pl.BlockSpec((slab, hidden), lambda step: (step, 0))
    up_first = pl.BlockSpec((half, slab), lambda step: (0, step))
    rows = ffn // seqs
    in_specs = [
        state, state, pl.BlockSpec((hidden, hidden), lambda step: (0, 0)), flat, flat, state, state,
        pl.BlockSpec((ffn, slab), lambda step: (0, step)), up_first, up_first,
        pl.BlockSpec((rows, hidden), lambda step: (seqs + step, 0)), pl.BlockSpec((rows, hidden), lambda step: (half // rows + step, 0)),
        pl.BlockSpec((3 * dim, slab), lambda step: (0, step)), pl.BlockSpec((dim // seqs, hidden), lambda step: (3 * seqs + step, 0)),
    ]
    out_specs = [state] * 4 + [
        pl.BlockSpec((slab, ffn), lambda step: (step, 0)), pl.BlockSpec((rows, hidden), lambda step: (step, 0)),
        pl.BlockSpec((3 * slab, 1, dim), lambda step: (step, 0, 0)), pl.BlockSpec((dim // seqs, hidden), lambda step: (step, 0)),
    ]
    out_shape = [jax.ShapeDtypeStruct(y_one.shape, F32)] * 4 + [jax.ShapeDtypeStruct(shape, F32) for shape in ((hidden, ffn), (ffn, hidden), (3 * hidden, 1, dim), (dim, hidden))]
    return pl.pallas_call(
        finish_kernel,
        out_shape=out_shape,
        grid=(seqs,),
        in_specs=in_specs,
        out_specs=out_specs,
        compiler_params=pltpu.CompilerParams(dimension_semantics=("arbitrary",), vmem_limit_bytes=VMEM_LIMIT),
        cost_estimate=pl.CostEstimate(flops=2 * 10**9, bytes_accessed=60 * 2**20, transcendentals=0),
        name="finish",
    )(y_one, o_pos, wo_full, x_two, dx_one, dy_two, du_pos, part_own, near_first, near_rest, part_own, near_rest, d_att, d_att)


def local_backward(y_one, y_two, dy_one, dy_two, w_qkv, w_out, w_up, w_down):
    hidden = y_one.shape[2]
    _, _, _, parts, dim = w_qkv.shape
    flat = [tensor.reshape(-1, hidden) for tensor in (y_one, y_two, dy_one, dy_two)]
    qkv_parts = jnp.swapaxes(w_qkv[0, :, 0], 0, 1)
    x_two, dx_one, uc_seq, att_full, part_own, part_near, near_first = mlp_call(*flat, w_up[0], w_down[0], qkv_parts, w_out[0, 0])
    near_rest, d_att, o_pos, du_pos, wo_full = attention_call(uc_seq, att_full, part_near)
    x_one, x_two, dx_one, dx_two, dw_up, dw_down, dw_qkv, dw_out = finish_call(
        y_one, o_pos, wo_full.reshape(-1, hidden), x_two, dx_one, dy_two, du_pos, part_own, near_first, near_rest, d_att
    )
    return (x_one, x_two, dx_one, dx_two, dw_qkv.reshape(1, hidden, 1, parts, dim), dw_out[None, None], dw_up[None], dw_down[None])


def solution(mesh):
    state_spec = P("dp", "tp", None)
    in_specs = (state_spec, state_spec, state_spec, state_spec, P(None, None, "tp", None, None), P(None, "tp", None, None), P(None, None, "tp"), P(None, "tp", None))
    out_specs = (state_spec, state_spec, state_spec, state_spec, P("dp", None, "tp", None, None), P("dp", "tp", None, None), P("dp", None, "tp"), P("dp", "tp", None))
    return jax.shard_map(local_backward, mesh=mesh, in_specs=in_specs, out_specs=out_specs, check_vma=False)
```

```python
import functools

import jax
import jax.numpy as jnp
from jax import lax
from jax.experimental import pallas as pl
from jax.experimental.pallas import tpu as pltpu
from jax.sharding import PartitionSpec as P

RMS_EPS = 1e-6
MESH = pl.DeviceIdType.MESH
BF16, F32 = jnp.bfloat16, jnp.float32
VMEM_LIMIT = 64 * 1024 * 1024 - 65536


def inv_rms(tensor):
    return lax.rsqrt(jnp.mean(tensor * tensor, axis=-1, keepdims=True) + RMS_EPS)


def rms_norm(tensor):
    return tensor * inv_rms(tensor)


def rms_back(tensor, grad_in):
    scale = inv_rms(tensor)
    return scale * grad_in - tensor * (scale * scale * scale) * jnp.mean(grad_in * tensor, axis=-1, keepdims=True)


def gelu_and_slope(tensor):
    root = (2.0 / jnp.pi) ** 0.5
    squared = tensor * tensor
    tanh = jnp.tanh(root * (tensor + 0.044715 * (tensor * squared)))
    cdf = 0.5 * (1.0 + tanh)
    slope = cdf + (0.5 * root) * tensor * ((1.0 - tanh * tanh) * (1.0 + (3 * 0.044715) * squared))
    return tensor * cdf, slope


def dot_nn(left, right):
    return lax.dot_general(left, right, (((1,), (0,)), ((), ())), preferred_element_type=F32)


def dot_nt(left, right):
    return lax.dot_general(left, right, (((1,), (1,)), ((), ())), preferred_element_type=F32)


def dot_tn(left, right):
    return lax.dot_general(left, right, (((0,), (0,)), ((), ())), preferred_element_type=F32)


class Ring:
    def __init__(self):
        me = lax.axis_index("tp")
        chip, core = me // 2, me % 2
        self.me, self.chip, self.core = me, chip, core
        self.chips = (chip, chip + 1 - 2 * (chip % 2), 3 - chip, (chip + 2) % 4)

    def at(self, slot):
        core = self.core if slot % 2 == 0 else 1 - self.core
        return self.chips[slot // 2] * 2 + core

    def at_traced(self, slot):
        relation, other = slot // 2, slot % 2
        own, near_t, near_f, opposite = self.chips
        chip = jnp.where(relation == 0, own, jnp.where(relation == 1, near_t, jnp.where(relation == 2, near_f, opposite)))
        return chip * 2 + (self.core + other) % 2

    def barrier(self):
        barrier = pltpu.get_barrier_semaphore()
        for slot in (1, 2, 3, 4, 5):
            pl.semaphore_signal(barrier, inc=1, device_id={"tp": self.at(slot)}, device_id_type=MESH)
        pl.semaphore_wait(barrier, 5)

    def copy(self, src, dst, send_sem, recv_sem, slot):
        return pltpu.make_async_remote_copy(src_ref=src, dst_ref=dst, send_sem=send_sem, recv_sem=recv_sem, device_id={"tp": self.at(slot)}, device_id_type=MESH)


PARTNER, SAME_T, OTHER_T, SAME_F, OTHER_F, SAME_O, OTHER_O = 1, 2, 3, 4, 5, 6, 7


def mlp_kernel(
    y_one, y_two, dy_one, dy_two, w_up, w_down, w_qkv, w_out,
    x_two, dx_one, uc_seq, att_full, part_own, part_near, near_recv,
    u_all, c_all, up_all, down_all, acc, uc_own, relay, y_buf, x_buf, up_raw, qkv_raw, att_own,
    load_sem, y_sem, x_sem, w_send, w_recv, uc_send, uc_recv, att_send, att_recv, a2a_send, a2a_recv, relay_recv, near_sem,
):
    ring = Ring()
    half = 512
    slab = 128

    def weight(which, src_slot, dst_slot, to, index):
        buf = (up_all, down_all)[which]
        return ring.copy(buf.at[src_slot], buf.at[dst_slot], w_send.at[index], w_recv.at[dst_slot, which], to)

    def weight_pair(src_slot, dst_slot, to, index):
        return [weight(which, src_slot, dst_slot, to, index + which) for which in (0, 1)]

    w_own = weight_pair(0, 1, PARTNER, 0) + weight_pair(0, 2, SAME_T, 2) + weight_pair(0, 4, SAME_F, 4)
    w_near_t = weight_pair(2, 6, SAME_F, 6) + weight_pair(2, 3, PARTNER, 8)
    w_near_f = weight_pair(4, 5, PARTNER, 10)
    w_far = weight_pair(6, 7, PARTNER, 12)

    def uc_pair(src_slot, dst_slot, to, index):
        return [ring.copy(buf.at[src_slot], buf.at[dst_slot], uc_send.at[index + which], uc_recv.at[dst_slot, which], to) for which, buf in enumerate((u_all, c_all))]

    uc_out = uc_pair(0, 2, SAME_T, 0) + uc_pair(0, 1, PARTNER, 2)
    uc_pass = uc_pair(2, 3, PARTNER, 4)

    def att(src, dst_slot, to, index):
        return ring.copy(src, att_full.at[dst_slot], att_send.at[index], att_recv.at[dst_slot], to)

    att_out = [att(att_own, 4, SAME_F, 0), att(att_own, 2, SAME_T, 1), att(att_own, 1, PARTNER, 2)]
    att_keep = pltpu.make_async_copy(att_own, att_full.at[0], load_sem.at[6])
    att_near_f = [att(att_full.at[4], 5, PARTNER, 3)]
    att_near_t = [att(att_full.at[2], 3, PARTNER, 4)]

    a2a_out = {slot: ring.copy(uc_own.at[slot], uc_seq.at[slot], a2a_send.at[slot], a2a_recv.at[slot], slot) for slot in (1, 2, 3, 4, 5)}
    a2a_out[SAME_O] = ring.copy(uc_own.at[SAME_O], relay.at[0], a2a_send.at[SAME_O], relay_recv.at[0], SAME_T)
    a2a_out[OTHER_O] = ring.copy(uc_own.at[OTHER_O], relay.at[1], a2a_send.at[OTHER_O], relay_recv.at[1], SAME_F)
    a2a_pass = [
        ring.copy(relay.at[0], uc_seq.at[SAME_O], a2a_send.at[8], a2a_recv.at[SAME_O], SAME_F),
        ring.copy(relay.at[1], uc_seq.at[OTHER_O], a2a_send.at[9], a2a_recv.at[OTHER_O], OTHER_T),
    ]
    uc_keep = pltpu.make_async_copy(uc_own.at[0], uc_seq.at[0], load_sem.at[4])

    def start(copies):
        for copy in copies:
            copy.start()

    dim = w_out.shape[0]
    near_rows = near_recv.shape[0]
    near = ring.copy(acc.at[0, pl.ds(0, near_rows)], near_recv, near_sem.at[0], near_sem.at[1], SAME_F)

    loads = [
        pltpu.make_async_copy(w_down, down_all.at[0], load_sem.at[0]),
        pltpu.make_async_copy(w_up, up_raw, load_sem.at[1]),
        pltpu.make_async_copy(y_one, acc.at[0], load_sem.at[2]),
        pltpu.make_async_copy(dy_two, acc.at[1], load_sem.at[3]),
        pltpu.make_async_copy(w_qkv, qkv_raw, load_sem.at[5]),
        pltpu.make_async_copy(w_out, att_own.at[pl.ds(3 * dim, dim)], load_sem.at[7]),
    ]
    start(loads)
    ring.barrier()
    loads[0].wait()
    start(w_own[1::2])
    loads[1].wait()
    for part in range(up_raw.shape[1] // dim):
        up_all[0, pl.ds(part * dim, dim), :] = up_raw[:, pl.ds(part * dim, dim)].T
    start(w_own[0::2])
    loads[2].wait()
    loads[3].wait()

    def normalize(step, carry):
        rows = pl.ds(pl.multiple_of(step * slab, slab), slab)
        u_all[0, rows, :] = rms_norm(acc[0, rows, :]).astype(BF16)
        c_all[0, rows, :] = acc[1, rows, :].astype(BF16)
        acc[0, rows, :] = jnp.zeros((slab, acc.shape[2]), F32)
        acc[1, rows, :] = jnp.zeros((slab, acc.shape[2]), F32)
        return carry

    lax.fori_loop(0, acc.shape[1] // slab, normalize, 0)
    start(uc_out)
    loads[4].wait()
    for part in range(3):
        att_own[pl.ds(part * dim, dim), :] = qkv_raw[part].T
    loads[5].wait()
    att_keep.start()

    def y_loads(step, buf):
        seq = ring.at_traced(7 - step)
        rows = pl.ds(pl.multiple_of(seq * slab, slab), slab)
        return [pltpu.make_async_copy(src.at[rows], y_buf.at[buf, which], y_sem.at[buf, which]) for which, src in enumerate((y_one, y_two, dy_one))]

    def x_stores(step, buf):
        seq = ring.at_traced(7 - step)
        rows = pl.ds(pl.multiple_of(seq * slab, slab), slab)
        return [pltpu.make_async_copy(x_buf.at[buf, which], dst.at[rows], x_sem.at[buf, which]) for which, dst in enumerate((x_two, dx_one))]

    def feed_forward(step, carry):
        slot = jnp.where(step == 3, 4, jnp.where(step == 4, 3, step))

        @pl.when(step >= 1)
        def _():
            for which, buf in enumerate((up_all, down_all)):
                ring.copy(buf.at[slot], buf.at[slot], w_send.at[0], w_recv.at[slot, which], PARTNER).wait_recv()

        @pl.when(step == 2)
        def _():
            start(w_near_t)
            start(att_out)

        @pl.when(step == 3)
        def _():
            start(w_near_f)

        @pl.when(step == 6)
        def _():
            start(w_far)

        @pl.when(step == 7)
        def _():
            start(y_loads(0, 0))

        def rows_step(part, carry):
            rows = pl.ds(pl.multiple_of(part * half, half), half)
            hidden, slope = gelu_and_slope(dot_nt(u_all[0, rows, :], up_all[slot]))
            d_pre = (slope * dot_nt(c_all[0, rows, :], down_all[slot])).astype(BF16)
            acc[0, rows, :] += dot_nn(hidden.astype(BF16), down_all[slot])
            acc[1, rows, :] += dot_nn(d_pre, up_all[slot])
            return carry

        lax.fori_loop(0, acc.shape[1] // half, rows_step, 0)
        return carry

    lax.fori_loop(0, 8, feed_forward, 0)

    def finish(step, carry):
        slot = 7 - step
        buf = step % 2
        seq = ring.at_traced(slot)
        rows = pl.ds(pl.multiple_of(seq * slab, slab), slab)
        for copy in y_loads(step, buf):
            copy.wait()

        @pl.when(step < 7)
        def _():
            start(y_loads(step + 1, 1 - buf))

        @pl.when(step >= 2)
        def _():
            for copy in x_stores(step - 2, buf):
                copy.wait()

        y_first = y_buf[buf, 0]
        x_second = y_buf[buf, 1] - acc[0, rows, :]
        dy_first = y_buf[buf, 2] + rms_back(y_first, acc[1, rows, :])
        x_buf[buf, 0] = x_second
        x_buf[buf, 1] = dy_first
        uc_own[slot, 0] = rms_norm(x_second).astype(BF16)
        uc_own[slot, 1] = dy_first.astype(BF16)
        acc[0, rows, :] = jnp.zeros((slab, acc.shape[2]), F32)
        acc[1, rows, :] = jnp.zeros((slab, acc.shape[2]), F32)
        start(x_stores(step, buf))
        return carry

    lax.fori_loop(0, 8, finish, 0)
    for slot in (7, 6, 5, 4, 3, 2, 1):
        a2a_out[slot].start()
    uc_keep.start()
    for step in (6, 7):
        for copy in x_stores(step, step % 2):
            copy.wait()

    def gradients(step, carry):
        first = step // 8
        tokens = (step % 8) // 2
        slot = 4 - 4 * first

        @pl.when((step == 2) | (step == 4) | (step == 6))
        def _():
            for which, buf in enumerate((u_all, c_all)):
                ring.copy(buf.at[tokens], buf.at[tokens], uc_send.at[0], uc_recv.at[tokens, which], PARTNER).wait_recv()

        @pl.when(step == 4)
        def _():
            start(uc_pass)

        @pl.when(step == 8)
        def _():
            near.start()
            ring.copy(att_own, att_full.at[4], att_send.at[0], att_recv.at[4], PARTNER).wait_recv()
            start(att_near_f)
            ring.copy(att_own, att_full.at[2], att_send.at[0], att_recv.at[2], PARTNER).wait_recv()
            start(att_near_t)

        @pl.when(step == 9)
        def _():
            for index in (0, 1):
                ring.copy(relay.at[index], relay.at[index], a2a_send.at[0], relay_recv.at[index], PARTNER).wait_recv()
            start(a2a_pass)

        rows = pl.ds(pl.multiple_of((step % 2) * half, half), half)
        u_part, c_part = u_all[tokens, rows, :], c_all[tokens, rows, :]
        hidden, slope = gelu_and_slope(dot_nt(up_all[slot], u_part))
        d_pre = (slope * dot_nt(down_all[slot], c_part)).astype(BF16)
        acc[first, pl.ds(0, half), :] += dot_nn(d_pre, u_part)
        acc[first, pl.ds(half, half), :] += dot_nn(hidden.astype(BF16), c_part)
        return carry

    lax.fori_loop(0, 16, gradients, 0)
    out_near = pltpu.make_async_copy(acc.at[0, pl.ds(near_rows, acc.shape[1] - near_rows)], part_near, load_sem.at[0])
    out_own = pltpu.make_async_copy(acc.at[1], part_own, load_sem.at[1])
    out_near.start()
    out_own.start()

    for slot in (1, 3, 5):
        ring.copy(att_own, att_full.at[slot], att_send.at[0], att_recv.at[slot], PARTNER).wait_recv()
    for slot in range(1, 8):
        ring.copy(uc_own.at[slot], uc_seq.at[slot], a2a_send.at[0], a2a_recv.at[slot], PARTNER).wait_recv()
    for copy in w_own + w_near_t + w_near_f + w_far + uc_out + uc_pass + att_out + att_near_t + att_near_f + list(a2a_out.values()) + a2a_pass:
        copy.wait_send()
    near.wait()
    uc_keep.wait()
    att_keep.wait()
    out_near.wait()
    out_own.wait()


def mlp_call(y_one, y_two, dy_one, dy_two, w_up, w_down, w_qkv, w_out):
    tokens, hidden = y_one.shape
    ffn = w_down.shape[0]
    dim = w_out.shape[0]
    near_rows = ffn
    any_spec = pl.BlockSpec(memory_space=pl.ANY)
    dma, vmem = pltpu.SemaphoreType.DMA, pltpu.VMEM
    out_shape = (
        jax.ShapeDtypeStruct((tokens, hidden), F32),
        jax.ShapeDtypeStruct((tokens, hidden), F32),
        jax.ShapeDtypeStruct((8, 2, tokens // 8, hidden), BF16),
        jax.ShapeDtypeStruct((6, 4 * dim, hidden), BF16),
        jax.ShapeDtypeStruct((2 * ffn, hidden), F32),
        jax.ShapeDtypeStruct((2 * ffn - near_rows, hidden), F32),
        jax.ShapeDtypeStruct((near_rows, hidden), F32),
    )
    scratch = [
        vmem((4, tokens, hidden), BF16), vmem((4, tokens, hidden), BF16),
        vmem((8, ffn, hidden), BF16), vmem((8, ffn, hidden), BF16),
        vmem((2, tokens, hidden), F32),
        vmem((8, 2, tokens // 8, hidden), BF16), vmem((2, 2, tokens // 8, hidden), BF16),
        vmem((2, 3, tokens // 8, hidden), F32), vmem((2, 2, tokens // 8, hidden), F32),
        vmem((hidden, ffn), BF16), vmem((3, hidden, dim), BF16), vmem((4 * dim, hidden), BF16),
        dma((8,)), dma((2, 3)), dma((2, 2)), dma((14,)), dma((8, 2)), dma((6,)), dma((4, 2)), dma((5,)), dma((6,)), dma((10,)), dma((8,)), dma((2,)), dma((2,)),
    ]
    return pl.pallas_call(
        mlp_kernel,
        out_shape=out_shape,
        in_specs=[any_spec] * 8,
        out_specs=(any_spec,) * 7,
        scratch_shapes=scratch,
        compiler_params=pltpu.CompilerParams(collective_id=0, has_side_effects=True, vmem_limit_bytes=VMEM_LIMIT),
        cost_estimate=pl.CostEstimate(flops=70 * 10**9, bytes_accessed=64 * 2**20, transcendentals=0),
        name="feed_forward",
    )(y_one, y_two, dy_one, dy_two, w_up, w_down, w_qkv, w_out)


def attention_kernel(
    scale, uc_seq, att_full, part_near,
    near_recv, d_att, o_pos, du_pos, wo_full, att_far,
    uc_all, w_buf, qkv, d_ctx, d_qkv, o_all, du_all, part_send, part_keep, part_core, own_t, far_t, own_f, far_f, o_relay, du_relay, near_buf,
    load_sem, w_sem, wo_sem, near_sem, core_send, core_recv, part_out, part_in, far_sem, o_send, o_recv, du_send, du_recv, o_relay_recv, du_relay_recv,
):
    ring = Ring()
    slab, hidden = uc_seq.shape[2], uc_seq.shape[3]
    seq_len = 8 * slab
    dim = att_full.shape[1] // 4
    tile = 256

    def head_slot(step):
        return (step // 2 + 1) % 4 * 2 + 1 - step % 2

    def w_load(step, buf):
        return pltpu.make_async_copy(att_full.at[head_slot(step)], w_buf.at[buf], w_sem.at[buf])

    def w_load_far(step, buf):
        return pltpu.make_async_copy(att_far.at[1 - step % 2], w_buf.at[buf], w_sem.at[buf])

    far_from_t = ring.copy(att_full.at[SAME_F], att_far.at[0], far_sem.at[0], far_sem.at[1], SAME_T)
    far_from_core = ring.copy(att_far.at[0], att_far.at[1], far_sem.at[2], far_sem.at[3], PARTNER)

    near_load = pltpu.make_async_copy(part_near, near_buf, near_sem.at[2])
    near = ring.copy(near_buf, near_recv, near_sem.at[0], near_sem.at[1], SAME_F)

    def core_copy(step, buf):
        relation = head_slot(step) // 2
        return ring.copy(part_send.at[buf], part_core.at[relation], core_send.at[buf], core_recv.at[relation], PARTNER)

    rows_a, rows_b = pl.ds(0, 3 * dim), pl.ds(3 * dim, dim)

    def part(src, dst, index, slot):
        return ring.copy(src, dst, part_out.at[index], part_in.at[index], slot)

    t_own_a = part(part_keep.at[1, rows_a], own_t.at[rows_a], 0, SAME_T)
    t_far_a = part(part_keep.at[3, rows_a], far_t, 1, SAME_T)
    t_own_b = part(part_keep.at[1, rows_b], own_t.at[rows_b], 2, SAME_T)
    f_own_b = part(part_keep.at[2, rows_b], own_f.at[rows_b], 3, SAME_F)
    f_far_b = part(part_keep.at[3, rows_b], far_f, 4, SAME_F)
    f_own_a = part(part_keep.at[2, rows_a], own_f.at[rows_a], 5, SAME_F)

    def rows_of(slot):
        return pl.ds(slot * slab, slab)

    def to_positions(src, dst, relay, send_sem, recv_sem, relay_sem):
        near_t, near_f = ring.at(SAME_T), ring.at(SAME_F)
        out = [
            ring.copy(src.at[rows_of(SAME_O)], relay.at[0], send_sem.at[6], relay_sem.at[0], SAME_T),
            ring.copy(src.at[rows_of(OTHER_O)], relay.at[1], send_sem.at[7], relay_sem.at[1], SAME_F),
        ] + [ring.copy(src.at[rows_of(slot)], dst.at[ring.me], send_sem.at[slot], recv_sem.at[slot], slot) for slot in (5, 4, 3, 2, 1)]
        onward = [
            ring.copy(relay.at[0], dst.at[near_t], send_sem.at[8], recv_sem.at[SAME_O], SAME_F),
            ring.copy(relay.at[1], dst.at[near_f], send_sem.at[9], recv_sem.at[OTHER_O], OTHER_T),
        ]
        keep = pltpu.make_async_copy(src.at[rows_of(0)], dst.at[ring.me], send_sem.at[0])
        return out, onward, keep

    o_out, o_pass, o_keep = to_positions(o_all, o_pos, o_relay, o_send, o_recv, o_relay_recv)
    du_out, du_pass, du_keep = to_positions(du_all, du_pos, du_relay, du_send, du_recv, du_relay_recv)

    def start(copies):
        for copy in copies:
            copy.start()

    loads = [pltpu.make_async_copy(uc_seq.at[slot, which], uc_all.at[which, rows_of(slot)], load_sem.at[slot, which]) for slot in range(8) for which in (0, 1)]
    near_load.start()
    start(loads)
    w_load(0, 0).start()
    ring.barrier()
    far_from_t.start()
    near_load.wait()
    near.start()
    du_all[...] = jnp.zeros_like(du_all)
    for copy in loads:
        copy.wait()

    def head_step(step, carry):
        buf = step % 2
        slot = head_slot(step)
        relation = slot // 2
        pltpu.make_async_copy(att_full.at[0], w_buf.at[buf], w_sem.at[buf]).wait()

        @pl.when(step == 3)
        def _():
            far_from_core.wait_recv()

        @pl.when((step < 3) | (step == 5) | (step == 6))
        def _():
            w_load(step + 1, 1 - buf).start()

        @pl.when((step == 3) | (step == 4))
        def _():
            w_load_far(step + 1, 1 - buf).start()

        head = ring.at_traced(slot)
        columns = pl.ds(pl.multiple_of(head * dim, dim), dim)
        wo_copy = pltpu.make_async_copy(w_buf.at[buf, pl.ds(3 * dim, dim)], wo_full.at[head], wo_sem.at[0])
        wo_copy.start()
        qkv[...] = dot_nt(uc_all[0], w_buf[buf, pl.ds(0, 3 * dim), :]).astype(BF16)
        d_ctx[...] = dot_nt(uc_all[1], w_buf[buf, pl.ds(3 * dim, dim), :]).astype(BF16)

        def query_tile(part, carry):
            d_key, d_value = carry
            rows = pl.ds(pl.multiple_of(part * tile, tile), tile)
            query, key, value = qkv[rows, pl.ds(0, dim)], qkv[:, pl.ds(dim, dim)], qkv[:, pl.ds(2 * dim, dim)]
            scores = dot_nt(query, key) * scale
            grown = jnp.exp(scores - jnp.max(scores, axis=-1, keepdims=True))
            prob = grown / jnp.sum(grown, axis=-1, keepdims=True)
            prob_b = prob.astype(BF16)
            o_all[rows, columns] = dot_nn(prob_b, value).astype(BF16)
            d_out = d_ctx[rows, :]
            d_prob = dot_nt(d_out, value)
            d_score = (prob * (d_prob - jnp.sum(d_prob * prob, axis=-1, keepdims=True)) * scale).astype(BF16)
            d_qkv[rows, pl.ds(0, dim)] = dot_nn(d_score, key).astype(BF16)
            return d_key + dot_tn(d_score, query), d_value + dot_tn(prob_b, d_out)

        zeros = jnp.zeros((seq_len, dim), F32)
        d_key, d_value = lax.fori_loop(0, seq_len // tile, query_tile, (zeros, zeros))
        d_qkv[:, pl.ds(dim, dim)] = d_key.astype(BF16)
        d_qkv[:, pl.ds(2 * dim, dim)] = d_value.astype(BF16)

        def du_tile(part, carry):
            rows = pl.ds(pl.multiple_of(part * tile, tile), tile)
            du_all[rows, :] += dot_nn(d_qkv[rows, :], w_buf[buf, pl.ds(0, 3 * dim), :])
            return carry

        lax.fori_loop(0, seq_len // tile, du_tile, 0)

        def write_part(dst, index):
            dst[index, pl.ds(0, 3 * dim), :] = dot_tn(d_qkv[...], uc_all[0])
            dst[index, pl.ds(3 * dim, dim), :] = dot_tn(o_all[:, columns], uc_all[1])

        @pl.when(step % 2 == 0)
        def _():
            send = (step // 2) % 2

            @pl.when(step >= 4)
            def _():
                core_copy(step - 4, send).wait_send()

            write_part(part_send, send)
            core_copy(step, send).start()

        @pl.when(step % 2 == 1)
        def _():
            write_part(part_keep, relation)
            core_copy(step - 1, 0).wait_recv()
            part_keep[relation] += part_core[relation]

        @pl.when(step == 1)
        def _():
            t_own_a.start()

        @pl.when(step == 2)
        def _():
            far_from_t.wait_recv()
            far_from_core.start()

        @pl.when(step == 3)
        def _():
            f_own_b.start()

        @pl.when(step == 5)
        def _():
            t_far_a.start()
            f_far_b.start()

        wo_copy.wait()
        return carry

    lax.fori_loop(0, 8, head_step, 0)
    start(o_out)
    start(du_out)
    o_keep.start()
    du_keep.start()
    f_far_b.wait_recv()
    part_keep[1, rows_b] += far_f[...]
    t_own_b.start()
    t_far_a.wait_recv()
    part_keep[2, rows_a] += far_t[...]
    f_own_a.start()
    for copy in o_out[:2]:
        copy.wait_recv()
    start(o_pass)
    for copy in du_out[:2]:
        copy.wait_recv()
    start(du_pass)
    t_own_a.wait_recv()
    t_own_b.wait_recv()
    part_keep[0] += own_t[...]
    f_own_a.wait_recv()
    f_own_b.wait_recv()
    part_keep[0] += own_f[...]
    d_att_copy = pltpu.make_async_copy(part_keep.at[0], d_att, load_sem.at[0, 0])
    d_att_copy.start()

    for dst, recv_sem in ((o_pos, o_recv), (du_pos, du_recv)):
        for slot in range(1, 8):
            ring.copy(dst.at[0], dst.at[ring.at(slot)], near_sem.at[0], recv_sem.at[slot], PARTNER).wait_recv()
    for copy in o_out + du_out + o_pass + du_pass + [t_own_a, t_far_a, t_own_b, f_own_b, f_far_b, f_own_a, far_from_t, far_from_core, near, core_copy(4, 0), core_copy(6, 1)]:
        copy.wait_send()
    near.wait_recv()
    o_keep.wait()
    du_keep.wait()
    d_att_copy.wait()


def attention_call(uc_seq, att_full, part_near):
    slab, hidden = uc_seq.shape[2:]
    rows = att_full.shape[1]
    dim = rows // 4
    seq_len = 8 * slab
    any_spec = pl.BlockSpec(memory_space=pl.ANY)
    dma, vmem = pltpu.SemaphoreType.DMA, pltpu.VMEM
    out_shape = (
        jax.ShapeDtypeStruct(part_near.shape, F32),
        jax.ShapeDtypeStruct((rows, hidden), F32),
        jax.ShapeDtypeStruct((8, slab, hidden), BF16),
        jax.ShapeDtypeStruct((8, slab, hidden), F32),
        jax.ShapeDtypeStruct((8, dim, hidden), BF16),
        jax.ShapeDtypeStruct((2, rows, hidden), BF16),
    )
    scratch = [
        vmem((2, seq_len, hidden), BF16), vmem((2, rows, hidden), BF16), vmem((seq_len, 3 * dim), BF16), vmem((seq_len, dim), BF16), vmem((seq_len, 3 * dim), BF16),
        vmem((seq_len, hidden), BF16), vmem((seq_len, hidden), F32),
        vmem((2, rows, hidden), F32), vmem((4, rows, hidden), F32), vmem((4, rows, hidden), F32),
        vmem((rows, hidden), F32), vmem((3 * dim, hidden), F32), vmem((rows, hidden), F32), vmem((dim, hidden), F32),
        vmem((2, slab, hidden), BF16), vmem((2, slab, hidden), F32), vmem(part_near.shape, F32),
        dma((8, 2)), dma((2,)), dma((1,)), dma((3,)), dma((2,)), dma((4,)), dma((6,)), dma((6,)), dma((4,)), dma((10,)), dma((8,)), dma((10,)), dma((8,)), dma((2,)), dma((2,)),
    ]
    return pl.pallas_call(
        functools.partial(attention_kernel, dim ** -0.5),
        out_shape=out_shape,
        in_specs=[any_spec] * 3,
        out_specs=(any_spec,) * 6,
        scratch_shapes=scratch,
        compiler_params=pltpu.CompilerParams(collective_id=1, has_side_effects=True, vmem_limit_bytes=VMEM_LIMIT),
        cost_estimate=pl.CostEstimate(flops=40 * 10**9, bytes_accessed=64 * 2**20, transcendentals=0),
        name="attention",
    )(uc_seq, att_full, part_near)


def finish_kernel(
    y_one, o_pos, wo_full, x_two, dx_one, dy_two, du_pos, up_own, up_near, down_own, down_near, d_qkv, d_out,
    x_one_out, x_two_out, dx_one_out, dx_two_out, dw_up, dw_down, dw_qkv, dw_out,
):
    x_one_out[0] = y_one[0] - dot_nn(o_pos[0], wo_full[...])
    x_two_out[0] = x_two[...]
    dx_one_out[0] = dx_one[...]
    dx_two_out[0] = dy_two[0] + rms_back(x_two[...], du_pos[0])
    dw_up[...] = (up_own[...] + up_near[...]).T
    dw_down[...] = down_own[...] + down_near[...]
    dim = dw_qkv.shape[2]
    for part in range(3):
        dw_qkv[pl.ds(part, dw_qkv.shape[0] // 3, stride=3), 0, :] = d_qkv[pl.ds(part * dim, dim), :].T
    dw_out[...] = d_out[...]


def finish_call(y_one, o_pos, wo_full, x_two, dx_one, dy_two, du_pos, part_own, up_near, down_near, d_att):
    seqs, slab, hidden = y_one.shape
    ffn = part_own.shape[0] // 2
    dim = d_att.shape[0] // 4
    state = pl.BlockSpec((1, slab, hidden), lambda step: (step, 0, 0))
    flat = pl.BlockSpec((slab, hidden), lambda step: (step, 0))
    up = pl.BlockSpec((ffn, slab), lambda step: (0, step))
    rows = ffn // seqs
    in_specs = [
        state, state, pl.BlockSpec((hidden, hidden), lambda step: (0, 0)), flat, flat, state, state,
        up, up, pl.BlockSpec((rows, hidden), lambda step: (seqs + step, 0)), pl.BlockSpec((rows, hidden), lambda step: (step, 0)),
        pl.BlockSpec((3 * dim, slab), lambda step: (0, step)), pl.BlockSpec((dim // seqs, hidden), lambda step: (3 * seqs + step, 0)),
    ]
    out_specs = [state] * 4 + [
        pl.BlockSpec((slab, ffn), lambda step: (step, 0)), pl.BlockSpec((rows, hidden), lambda step: (step, 0)),
        pl.BlockSpec((3 * slab, 1, dim), lambda step: (step, 0, 0)), pl.BlockSpec((dim // seqs, hidden), lambda step: (step, 0)),
    ]
    out_shape = [jax.ShapeDtypeStruct(y_one.shape, F32)] * 4 + [jax.ShapeDtypeStruct(shape, F32) for shape in ((hidden, ffn), (ffn, hidden), (3 * hidden, 1, dim), (dim, hidden))]
    return pl.pallas_call(
        finish_kernel,
        out_shape=out_shape,
        grid=(seqs,),
        in_specs=in_specs,
        out_specs=out_specs,
        compiler_params=pltpu.CompilerParams(dimension_semantics=("arbitrary",), vmem_limit_bytes=VMEM_LIMIT),
        cost_estimate=pl.CostEstimate(flops=2 * 10**9, bytes_accessed=60 * 2**20, transcendentals=0),
        name="finish",
    )(y_one, o_pos, wo_full, x_two, dx_one, dy_two, du_pos, part_own, up_near, part_own, down_near, d_att, d_att)


def local_backward(y_one, y_two, dy_one, dy_two, w_qkv, w_out, w_up, w_down):
    hidden = y_one.shape[2]
    _, _, _, parts, dim = w_qkv.shape
    flat = [tensor.reshape(-1, hidden) for tensor in (y_one, y_two, dy_one, dy_two)]
    qkv_parts = jnp.swapaxes(w_qkv[0, :, 0], 0, 1)
    x_two, dx_one, uc_seq, att_full, part_own, part_near, up_near = mlp_call(*flat, w_up[0], w_down[0], qkv_parts, w_out[0, 0])
    down_near, d_att, o_pos, du_pos, wo_full, _ = attention_call(uc_seq, att_full, part_near)
    x_one, x_two, dx_one, dx_two, dw_up, dw_down, dw_qkv, dw_out = finish_call(
        y_one, o_pos, wo_full.reshape(-1, hidden), x_two, dx_one, dy_two, du_pos, part_own, up_near, down_near, d_att
    )
    return (x_one, x_two, dx_one, dx_two, dw_qkv.reshape(1, hidden, 1, parts, dim), dw_out[None, None], dw_up[None], dw_down[None])


def solution(mesh):
    state_spec = P("dp", "tp", None)
    in_specs = (state_spec, state_spec, state_spec, state_spec, P(None, None, "tp", None, None), P(None, "tp", None, None), P(None, None, "tp"), P(None, "tp", None))
    out_specs = (state_spec, state_spec, state_spec, state_spec, P("dp", None, "tp", None, None), P("dp", "tp", None, None), P("dp", None, "tp"), P("dp", "tp", None))
    return jax.shard_map(local_backward, mesh=mesh, in_specs=in_specs, out_specs=out_specs, check_vma=False)
```

```python
import functools

import jax
import jax.numpy as jnp
from jax import lax
from jax.experimental import pallas as pl
from jax.experimental.pallas import tpu as pltpu
from jax.sharding import PartitionSpec as P

RMS_EPS = 1e-6
LOG2_E = 1.4426950408889634
MESH = pl.DeviceIdType.MESH
BF16, F32 = jnp.bfloat16, jnp.float32
VMEM_LIMIT = 64 * 1024 * 1024 - 65536


def inv_rms(tensor):
    return lax.rsqrt(jnp.mean(tensor * tensor, axis=-1, keepdims=True) + RMS_EPS)


def rms_norm(tensor):
    return tensor * inv_rms(tensor)


def rms_back(tensor, grad_in):
    scale = inv_rms(tensor)
    return scale * grad_in - tensor * (scale * scale * scale) * jnp.mean(grad_in * tensor, axis=-1, keepdims=True)


def gelu_and_slope(tensor):
    root = (2.0 / jnp.pi) ** 0.5
    squared = tensor * tensor
    tanh = jnp.tanh(root * (tensor + 0.044715 * (tensor * squared)))
    cdf = 0.5 * (1.0 + tanh)
    slope = cdf + (0.5 * root) * tensor * ((1.0 - tanh * tanh) * (1.0 + (3 * 0.044715) * squared))
    return tensor * cdf, slope


def dot_nn(left, right):
    return lax.dot_general(left, right, (((1,), (0,)), ((), ())), preferred_element_type=F32)


def dot_nt(left, right):
    return lax.dot_general(left, right, (((1,), (1,)), ((), ())), preferred_element_type=F32)


def dot_tn(left, right):
    return lax.dot_general(left, right, (((0,), (0,)), ((), ())), preferred_element_type=F32)


class Ring:
    def __init__(self):
        me = lax.axis_index("tp")
        chip, core = me // 2, me % 2
        self.me, self.chip, self.core = me, chip, core
        self.chips = (chip, chip + 1 - 2 * (chip % 2), 3 - chip, (chip + 2) % 4)

    def at(self, slot):
        core = self.core if slot % 2 == 0 else 1 - self.core
        return self.chips[slot // 2] * 2 + core

    def at_traced(self, slot):
        relation, other = slot // 2, slot % 2
        own, near_t, near_f, opposite = self.chips
        chip = jnp.where(relation == 0, own, jnp.where(relation == 1, near_t, jnp.where(relation == 2, near_f, opposite)))
        return chip * 2 + (self.core + other) % 2

    def barrier(self):
        barrier = pltpu.get_barrier_semaphore()
        for slot in (1, 2, 3, 4, 5):
            pl.semaphore_signal(barrier, inc=1, device_id={"tp": self.at(slot)}, device_id_type=MESH)
        pl.semaphore_wait(barrier, 5)

    def copy(self, src, dst, send_sem, recv_sem, slot):
        return pltpu.make_async_remote_copy(src_ref=src, dst_ref=dst, send_sem=send_sem, recv_sem=recv_sem, device_id={"tp": self.at(slot)}, device_id_type=MESH)


PARTNER, SAME_T, OTHER_T, SAME_F, OTHER_F, SAME_O, OTHER_O = 1, 2, 3, 4, 5, 6, 7


def mlp_kernel(
    y_one, y_two, dy_one, dy_two, w_up, w_down, w_qkv, w_out,
    x_two, dx_one, uc_seq, att_full, part_own, part_near, near_recv,
    u_all, c_all, up_all, down_all, acc, uc_own, relay, y_buf, x_buf, up_raw, qkv_raw, att_own,
    load_sem, y_sem, x_sem, w_send, w_recv, uc_send, uc_recv, att_send, att_recv, a2a_send, a2a_recv, relay_recv, near_sem,
):
    ring = Ring()
    half = 512
    slab = 128

    def weight(which, src_slot, dst_slot, to, index):
        buf = (up_all, down_all)[which]
        return ring.copy(buf.at[src_slot], buf.at[dst_slot], w_send.at[index], w_recv.at[dst_slot, which], to)

    def weight_pair(src_slot, dst_slot, to, index):
        return [weight(which, src_slot, dst_slot, to, index + which) for which in (0, 1)]

    w_own = weight_pair(0, 1, PARTNER, 0) + weight_pair(0, 2, SAME_T, 2) + weight_pair(0, 4, SAME_F, 4)
    w_near_t = weight_pair(2, 6, SAME_F, 6) + weight_pair(2, 3, PARTNER, 8)
    w_near_f = weight_pair(4, 5, PARTNER, 10)
    w_far = weight_pair(6, 7, PARTNER, 12)

    def uc_pair(src_slot, dst_slot, to, index):
        return [ring.copy(buf.at[src_slot], buf.at[dst_slot], uc_send.at[index + which], uc_recv.at[dst_slot, which], to) for which, buf in enumerate((u_all, c_all))]

    uc_out = uc_pair(0, 2, SAME_T, 0) + uc_pair(0, 1, PARTNER, 2)
    uc_pass = uc_pair(2, 3, PARTNER, 4)

    def att(src, dst_slot, to, index):
        return ring.copy(src, att_full.at[dst_slot], att_send.at[index], att_recv.at[dst_slot], to)

    att_out = [att(att_own, 4, SAME_F, 0), att(att_own, 2, SAME_T, 1), att(att_own, 1, PARTNER, 2)]
    att_keep = pltpu.make_async_copy(att_own, att_full.at[0], load_sem.at[6])
    att_near_f = [att(att_full.at[4], 5, PARTNER, 3)]
    att_near_t = [att(att_full.at[2], 3, PARTNER, 4)]

    a2a_out = {slot: ring.copy(uc_own.at[slot], uc_seq.at[slot], a2a_send.at[slot], a2a_recv.at[slot], slot) for slot in (1, 2, 3, 4, 5)}
    a2a_out[SAME_O] = ring.copy(uc_own.at[SAME_O], relay.at[0], a2a_send.at[SAME_O], relay_recv.at[0], SAME_T)
    a2a_out[OTHER_O] = ring.copy(uc_own.at[OTHER_O], relay.at[1], a2a_send.at[OTHER_O], relay_recv.at[1], SAME_F)
    a2a_pass = [
        ring.copy(relay.at[0], uc_seq.at[SAME_O], a2a_send.at[8], a2a_recv.at[SAME_O], SAME_F),
        ring.copy(relay.at[1], uc_seq.at[OTHER_O], a2a_send.at[9], a2a_recv.at[OTHER_O], OTHER_T),
    ]
    uc_keep = pltpu.make_async_copy(uc_own.at[0], uc_seq.at[0], load_sem.at[4])

    def start(copies):
        for copy in copies:
            copy.start()

    dim = w_out.shape[0]
    near_rows = near_recv.shape[0]
    near = ring.copy(acc.at[0, pl.ds(0, near_rows)], near_recv, near_sem.at[0], near_sem.at[1], SAME_F)

    loads = [
        pltpu.make_async_copy(w_down, down_all.at[0], load_sem.at[0]),
        pltpu.make_async_copy(w_up, up_raw, load_sem.at[1]),
        pltpu.make_async_copy(y_one, acc.at[0], load_sem.at[2]),
        pltpu.make_async_copy(dy_two, acc.at[1], load_sem.at[3]),
        pltpu.make_async_copy(w_qkv, qkv_raw, load_sem.at[5]),
        pltpu.make_async_copy(w_out, att_own.at[pl.ds(3 * dim, dim)], load_sem.at[7]),
    ]
    start(loads)
    ring.barrier()
    loads[0].wait()
    start(w_own[1::2])
    loads[1].wait()
    for part in range(up_raw.shape[1] // dim):
        up_all[0, pl.ds(part * dim, dim), :] = up_raw[:, pl.ds(part * dim, dim)].T
    start(w_own[0::2])
    loads[2].wait()
    loads[3].wait()

    def normalize(step, carry):
        rows = pl.ds(pl.multiple_of(step * slab, slab), slab)
        u_all[0, rows, :] = rms_norm(acc[0, rows, :]).astype(BF16)
        c_all[0, rows, :] = acc[1, rows, :].astype(BF16)
        acc[0, rows, :] = jnp.zeros((slab, acc.shape[2]), F32)
        acc[1, rows, :] = jnp.zeros((slab, acc.shape[2]), F32)
        return carry

    lax.fori_loop(0, acc.shape[1] // slab, normalize, 0)
    start(uc_out)
    loads[4].wait()
    for part in range(3):
        att_own[pl.ds(part * dim, dim), :] = qkv_raw[part].T
    loads[5].wait()
    att_keep.start()

    def y_loads(step, buf):
        seq = ring.at_traced(7 - step)
        rows = pl.ds(pl.multiple_of(seq * slab, slab), slab)
        return [pltpu.make_async_copy(src.at[rows], y_buf.at[buf, which], y_sem.at[buf, which]) for which, src in enumerate((y_one, y_two, dy_one))]

    def x_stores(step, buf):
        seq = ring.at_traced(7 - step)
        rows = pl.ds(pl.multiple_of(seq * slab, slab), slab)
        return [pltpu.make_async_copy(x_buf.at[buf, which], dst.at[rows], x_sem.at[buf, which]) for which, dst in enumerate((x_two, dx_one))]

    def feed_forward(step, carry):
        slot = jnp.where(step == 3, 4, jnp.where(step == 4, 3, step))

        @pl.when(step >= 1)
        def _():
            for which, buf in enumerate((up_all, down_all)):
                ring.copy(buf.at[slot], buf.at[slot], w_send.at[0], w_recv.at[slot, which], PARTNER).wait_recv()

        @pl.when(step == 2)
        def _():
            start(w_near_t)
            start(att_out)

        @pl.when(step == 3)
        def _():
            start(w_near_f)

        @pl.when(step == 6)
        def _():
            start(w_far)

        @pl.when(step == 7)
        def _():
            start(y_loads(0, 0))

        def rows_step(part, carry):
            rows = pl.ds(pl.multiple_of(part * half, half), half)
            hidden, slope = gelu_and_slope(dot_nt(u_all[0, rows, :], up_all[slot]))
            d_pre = (slope * dot_nt(c_all[0, rows, :], down_all[slot])).astype(BF16)
            acc[0, rows, :] += dot_nn(hidden.astype(BF16), down_all[slot])
            acc[1, rows, :] += dot_nn(d_pre, up_all[slot])
            return carry

        lax.fori_loop(0, acc.shape[1] // half, rows_step, 0)
        return carry

    lax.fori_loop(0, 8, feed_forward, 0)

    def finish(step, carry):
        slot = 7 - step
        buf = step % 2
        seq = ring.at_traced(slot)
        rows = pl.ds(pl.multiple_of(seq * slab, slab), slab)
        for copy in y_loads(step, buf):
            copy.wait()

        @pl.when(step < 7)
        def _():
            start(y_loads(step + 1, 1 - buf))

        @pl.when(step >= 2)
        def _():
            for copy in x_stores(step - 2, buf):
                copy.wait()

        y_first = y_buf[buf, 0]
        x_second = y_buf[buf, 1] - acc[0, rows, :]
        dy_first = y_buf[buf, 2] + rms_back(y_first, acc[1, rows, :])
        x_buf[buf, 0] = x_second
        x_buf[buf, 1] = dy_first
        uc_own[slot, 0] = rms_norm(x_second).astype(BF16)
        uc_own[slot, 1] = dy_first.astype(BF16)
        acc[0, rows, :] = jnp.zeros((slab, acc.shape[2]), F32)
        acc[1, rows, :] = jnp.zeros((slab, acc.shape[2]), F32)
        start(x_stores(step, buf))
        return carry

    lax.fori_loop(0, 8, finish, 0)
    for slot in (7, 6, 5, 4, 3, 2, 1):
        a2a_out[slot].start()
    uc_keep.start()
    for step in (6, 7):
        for copy in x_stores(step, step % 2):
            copy.wait()

    def gradients(step, carry):
        first = step // 8
        tokens = (step % 8) // 2
        slot = 4 - 4 * first

        @pl.when((step == 2) | (step == 4) | (step == 6))
        def _():
            for which, buf in enumerate((u_all, c_all)):
                ring.copy(buf.at[tokens], buf.at[tokens], uc_send.at[0], uc_recv.at[tokens, which], PARTNER).wait_recv()

        @pl.when(step == 4)
        def _():
            start(uc_pass)

        @pl.when(step == 8)
        def _():
            near.start()
            ring.copy(att_own, att_full.at[4], att_send.at[0], att_recv.at[4], PARTNER).wait_recv()
            start(att_near_f)
            ring.copy(att_own, att_full.at[2], att_send.at[0], att_recv.at[2], PARTNER).wait_recv()
            start(att_near_t)

        @pl.when(step == 9)
        def _():
            for index in (0, 1):
                ring.copy(relay.at[index], relay.at[index], a2a_send.at[0], relay_recv.at[index], PARTNER).wait_recv()
            start(a2a_pass)

        rows = pl.ds(pl.multiple_of((step % 2) * half, half), half)
        u_part, c_part = u_all[tokens, rows, :], c_all[tokens, rows, :]
        hidden, slope = gelu_and_slope(dot_nt(up_all[slot], u_part))
        d_pre = (slope * dot_nt(down_all[slot], c_part)).astype(BF16)
        acc[first, pl.ds(0, half), :] += dot_nn(d_pre, u_part)
        acc[first, pl.ds(half, half), :] += dot_nn(hidden.astype(BF16), c_part)
        return carry

    lax.fori_loop(0, 16, gradients, 0)
    out_near = pltpu.make_async_copy(acc.at[0, pl.ds(near_rows, acc.shape[1] - near_rows)], part_near, load_sem.at[0])
    out_own = pltpu.make_async_copy(acc.at[1], part_own, load_sem.at[1])
    out_near.start()
    out_own.start()

    for slot in (1, 3, 5):
        ring.copy(att_own, att_full.at[slot], att_send.at[0], att_recv.at[slot], PARTNER).wait_recv()
    for slot in range(1, 8):
        ring.copy(uc_own.at[slot], uc_seq.at[slot], a2a_send.at[0], a2a_recv.at[slot], PARTNER).wait_recv()
    for copy in w_own + w_near_t + w_near_f + w_far + uc_out + uc_pass + att_out + att_near_t + att_near_f + list(a2a_out.values()) + a2a_pass:
        copy.wait_send()
    near.wait()
    uc_keep.wait()
    att_keep.wait()
    out_near.wait()
    out_own.wait()


def mlp_call(y_one, y_two, dy_one, dy_two, w_up, w_down, w_qkv, w_out):
    tokens, hidden = y_one.shape
    ffn = w_down.shape[0]
    dim = w_out.shape[0]
    near_rows = ffn
    any_spec = pl.BlockSpec(memory_space=pl.ANY)
    dma, vmem = pltpu.SemaphoreType.DMA, pltpu.VMEM
    out_shape = (
        jax.ShapeDtypeStruct((tokens, hidden), F32),
        jax.ShapeDtypeStruct((tokens, hidden), F32),
        jax.ShapeDtypeStruct((8, 2, tokens // 8, hidden), BF16),
        jax.ShapeDtypeStruct((6, 4 * dim, hidden), BF16),
        jax.ShapeDtypeStruct((2 * ffn, hidden), F32),
        jax.ShapeDtypeStruct((2 * ffn - near_rows, hidden), F32),
        jax.ShapeDtypeStruct((near_rows, hidden), F32),
    )
    scratch = [
        vmem((4, tokens, hidden), BF16), vmem((4, tokens, hidden), BF16),
        vmem((8, ffn, hidden), BF16), vmem((8, ffn, hidden), BF16),
        vmem((2, tokens, hidden), F32),
        vmem((8, 2, tokens // 8, hidden), BF16), vmem((2, 2, tokens // 8, hidden), BF16),
        vmem((2, 3, tokens // 8, hidden), F32), vmem((2, 2, tokens // 8, hidden), F32),
        vmem((hidden, ffn), BF16), vmem((3, hidden, dim), BF16), vmem((4 * dim, hidden), BF16),
        dma((8,)), dma((2, 3)), dma((2, 2)), dma((14,)), dma((8, 2)), dma((6,)), dma((4, 2)), dma((5,)), dma((6,)), dma((10,)), dma((8,)), dma((2,)), dma((2,)),
    ]
    return pl.pallas_call(
        mlp_kernel,
        out_shape=out_shape,
        in_specs=[any_spec] * 8,
        out_specs=(any_spec,) * 7,
        scratch_shapes=scratch,
        compiler_params=pltpu.CompilerParams(collective_id=0, has_side_effects=True, vmem_limit_bytes=VMEM_LIMIT),
        cost_estimate=pl.CostEstimate(flops=70 * 10**9, bytes_accessed=64 * 2**20, transcendentals=0),
        name="feed_forward",
    )(y_one, y_two, dy_one, dy_two, w_up, w_down, w_qkv, w_out)


def attention_kernel(
    scale, uc_seq, att_full, part_near,
    near_recv, d_att, o_pos, du_pos, wo_full, att_far,
    uc_all, w_buf, qkv, d_ctx, d_qkv, o_all, du_all, part_send, part_keep, part_core, own_t, far_t, own_f, far_f, o_relay, du_relay, near_buf,
    load_sem, w_sem, wo_sem, near_sem, core_send, core_recv, part_out, part_in, far_sem, o_send, o_recv, du_send, du_recv, o_relay_recv, du_relay_recv,
):
    ring = Ring()
    slab, hidden = uc_seq.shape[2], uc_seq.shape[3]
    seq_len = 8 * slab
    dim = att_full.shape[1] // 4
    tile = 512

    def head_slot(step):
        return (step // 2 + 1) % 4 * 2 + 1 - step % 2

    def w_load(step, buf):
        return pltpu.make_async_copy(att_full.at[head_slot(step)], w_buf.at[buf], w_sem.at[buf])

    def w_load_far(step, buf):
        return pltpu.make_async_copy(att_far.at[1 - step % 2], w_buf.at[buf], w_sem.at[buf])

    far_from_t = ring.copy(att_full.at[SAME_F], att_far.at[0], far_sem.at[0], far_sem.at[1], SAME_T)
    far_from_core = ring.copy(att_far.at[0], att_far.at[1], far_sem.at[2], far_sem.at[3], PARTNER)

    near_load = pltpu.make_async_copy(part_near, near_buf, near_sem.at[2])
    near = ring.copy(near_buf, near_recv, near_sem.at[0], near_sem.at[1], SAME_F)

    def core_copy(step, buf):
        relation = head_slot(step) // 2
        return ring.copy(part_send.at[buf], part_core.at[relation], core_send.at[buf], core_recv.at[relation], PARTNER)

    rows_a, rows_b = pl.ds(0, 3 * dim), pl.ds(3 * dim, dim)

    def part(src, dst, index, slot):
        return ring.copy(src, dst, part_out.at[index], part_in.at[index], slot)

    t_own_a = part(part_keep.at[1, rows_a], own_t.at[rows_a], 0, SAME_T)
    t_far_a = part(part_keep.at[3, rows_a], far_t, 1, SAME_T)
    t_own_b = part(part_keep.at[1, rows_b], own_t.at[rows_b], 2, SAME_T)
    f_own_b = part(part_keep.at[2, rows_b], own_f.at[rows_b], 3, SAME_F)
    f_far_b = part(part_keep.at[3, rows_b], far_f, 4, SAME_F)
    f_own_a = part(part_keep.at[2, rows_a], own_f.at[rows_a], 5, SAME_F)

    def rows_of(slot):
        return pl.ds(slot * slab, slab)

    def to_positions(src, dst, relay, send_sem, recv_sem, relay_sem):
        near_t, near_f = ring.at(SAME_T), ring.at(SAME_F)
        out = [
            ring.copy(src.at[rows_of(SAME_O)], relay.at[0], send_sem.at[6], relay_sem.at[0], SAME_T),
            ring.copy(src.at[rows_of(OTHER_O)], relay.at[1], send_sem.at[7], relay_sem.at[1], SAME_F),
        ] + [ring.copy(src.at[rows_of(slot)], dst.at[ring.me], send_sem.at[slot], recv_sem.at[slot], slot) for slot in (5, 4, 3, 2, 1)]
        onward = [
            ring.copy(relay.at[0], dst.at[near_t], send_sem.at[8], recv_sem.at[SAME_O], SAME_F),
            ring.copy(relay.at[1], dst.at[near_f], send_sem.at[9], recv_sem.at[OTHER_O], OTHER_T),
        ]
        keep = pltpu.make_async_copy(src.at[rows_of(0)], dst.at[ring.me], send_sem.at[0])
        return out, onward, keep

    o_out, o_pass, o_keep = to_positions(o_all, o_pos, o_relay, o_send, o_recv, o_relay_recv)
    du_out, du_pass, du_keep = to_positions(du_all, du_pos, du_relay, du_send, du_recv, du_relay_recv)

    def start(copies):
        for copy in copies:
            copy.start()

    loads = [pltpu.make_async_copy(uc_seq.at[slot, which], uc_all.at[which, rows_of(slot)], load_sem.at[slot, which]) for slot in range(8) for which in (0, 1)]
    near_load.start()
    start(loads)
    w_load(0, 0).start()
    ring.barrier()
    far_from_t.start()
    near_load.wait()
    near.start()
    du_all[...] = jnp.zeros_like(du_all)
    for copy in loads:
        copy.wait()

    def head_step(step, carry):
        buf = step % 2
        slot = head_slot(step)
        relation = slot // 2
        pltpu.make_async_copy(att_full.at[0], w_buf.at[buf], w_sem.at[buf]).wait()

        @pl.when(step == 3)
        def _():
            far_from_core.wait_recv()

        @pl.when((step < 3) | (step == 5) | (step == 6))
        def _():
            w_load(step + 1, 1 - buf).start()

        @pl.when((step == 3) | (step == 4))
        def _():
            w_load_far(step + 1, 1 - buf).start()

        head = ring.at_traced(slot)
        columns = pl.ds(pl.multiple_of(head * dim, dim), dim)
        wo_copy = pltpu.make_async_copy(w_buf.at[buf, pl.ds(3 * dim, dim)], wo_full.at[head], wo_sem.at[0])
        wo_copy.start()
        qkv[...] = dot_nt(uc_all[0], w_buf[buf, pl.ds(0, 3 * dim), :]).astype(BF16)
        d_ctx[...] = dot_nt(uc_all[1], w_buf[buf, pl.ds(3 * dim, dim), :]).astype(BF16)

        query, key, value = (qkv[:, pl.ds(part * dim, dim)] for part in range(3))
        d_out = d_ctx[...]
        scores = dot_nt(query, key) * (scale * LOG2_E)
        grown = jnp.exp2(scores - jnp.max(scores, axis=-1, keepdims=True))
        prob = grown * (1.0 / jnp.sum(grown, axis=-1, keepdims=True))
        prob_b = prob.astype(BF16)
        o_all[:, columns] = dot_nn(prob_b, value).astype(BF16)
        d_prob = dot_nt(d_out, value)
        d_score = (prob * (d_prob - jnp.sum(d_prob * prob, axis=-1, keepdims=True)) * scale).astype(BF16)
        d_qkv[:, pl.ds(0, dim)] = dot_nn(d_score, key).astype(BF16)
        d_qkv[:, pl.ds(dim, dim)] = dot_nn(query.T, d_score).T.astype(BF16)
        d_qkv[:, pl.ds(2 * dim, dim)] = dot_nn(d_out.T, prob_b).T.astype(BF16)

        def du_tile(part, carry):
            rows = pl.ds(pl.multiple_of(part * tile, tile), tile)
            du_all[rows, :] += dot_nn(d_qkv[rows, :], w_buf[buf, pl.ds(0, 3 * dim), :])
            return carry

        lax.fori_loop(0, seq_len // tile, du_tile, 0)

        def write_part(dst, index):
            dst[index, pl.ds(0, 3 * dim), :] = dot_tn(d_qkv[...], uc_all[0])
            dst[index, pl.ds(3 * dim, dim), :] = dot_tn(o_all[:, columns], uc_all[1])

        @pl.when(step % 2 == 0)
        def _():
            send = (step // 2) % 2

            @pl.when(step >= 4)
            def _():
                core_copy(step - 4, send).wait_send()

            write_part(part_send, send)
            core_copy(step, send).start()

        @pl.when(step % 2 == 1)
        def _():
            write_part(part_keep, relation)
            core_copy(step - 1, 0).wait_recv()
            part_keep[relation] += part_core[relation]

        @pl.when(step == 1)
        def _():
            t_own_a.start()

        @pl.when(step == 2)
        def _():
            far_from_t.wait_recv()
            far_from_core.start()

        @pl.when(step == 3)
        def _():
            f_own_b.start()

        @pl.when(step == 5)
        def _():
            t_far_a.start()
            f_far_b.start()

        wo_copy.wait()
        return carry

    lax.fori_loop(0, 8, head_step, 0)
    start(o_out)
    start(du_out)
    o_keep.start()
    du_keep.start()
    f_far_b.wait_recv()
    part_keep[1, rows_b] += far_f[...]
    t_own_b.start()
    t_far_a.wait_recv()
    part_keep[2, rows_a] += far_t[...]
    f_own_a.start()
    for copy in o_out[:2]:
        copy.wait_recv()
    start(o_pass)
    for copy in du_out[:2]:
        copy.wait_recv()
    start(du_pass)
    t_own_a.wait_recv()
    t_own_b.wait_recv()
    part_keep[0] += own_t[...]
    f_own_a.wait_recv()
    f_own_b.wait_recv()
    part_keep[0] += own_f[...]
    d_att_copy = pltpu.make_async_copy(part_keep.at[0], d_att, load_sem.at[0, 0])
    d_att_copy.start()

    for dst, recv_sem in ((o_pos, o_recv), (du_pos, du_recv)):
        for slot in range(1, 8):
            ring.copy(dst.at[0], dst.at[ring.at(slot)], near_sem.at[0], recv_sem.at[slot], PARTNER).wait_recv()
    for copy in o_out + du_out + o_pass + du_pass + [t_own_a, t_far_a, t_own_b, f_own_b, f_far_b, f_own_a, far_from_t, far_from_core, near, core_copy(4, 0), core_copy(6, 1)]:
        copy.wait_send()
    near.wait_recv()
    o_keep.wait()
    du_keep.wait()
    d_att_copy.wait()


def attention_call(uc_seq, att_full, part_near):
    slab, hidden = uc_seq.shape[2:]
    rows = att_full.shape[1]
    dim = rows // 4
    seq_len = 8 * slab
    any_spec = pl.BlockSpec(memory_space=pl.ANY)
    dma, vmem = pltpu.SemaphoreType.DMA, pltpu.VMEM
    out_shape = (
        jax.ShapeDtypeStruct(part_near.shape, F32),
        jax.ShapeDtypeStruct((rows, hidden), F32),
        jax.ShapeDtypeStruct((8, slab, hidden), BF16),
        jax.ShapeDtypeStruct((8, slab, hidden), F32),
        jax.ShapeDtypeStruct((8, dim, hidden), BF16),
        jax.ShapeDtypeStruct((2, rows, hidden), BF16),
    )
    scratch = [
        vmem((2, seq_len, hidden), BF16), vmem((2, rows, hidden), BF16), vmem((seq_len, 3 * dim), BF16), vmem((seq_len, dim), BF16), vmem((seq_len, 3 * dim), BF16),
        vmem((seq_len, hidden), BF16), vmem((seq_len, hidden), F32),
        vmem((2, rows, hidden), F32), vmem((4, rows, hidden), F32), vmem((4, rows, hidden), F32),
        vmem((rows, hidden), F32), vmem((3 * dim, hidden), F32), vmem((rows, hidden), F32), vmem((dim, hidden), F32),
        vmem((2, slab, hidden), BF16), vmem((2, slab, hidden), F32), vmem(part_near.shape, F32),
        dma((8, 2)), dma((2,)), dma((1,)), dma((3,)), dma((2,)), dma((4,)), dma((6,)), dma((6,)), dma((4,)), dma((10,)), dma((8,)), dma((10,)), dma((8,)), dma((2,)), dma((2,)),
    ]
    return pl.pallas_call(
        functools.partial(attention_kernel, dim ** -0.5),
        out_shape=out_shape,
        in_specs=[any_spec] * 3,
        out_specs=(any_spec,) * 6,
        scratch_shapes=scratch,
        compiler_params=pltpu.CompilerParams(collective_id=1, has_side_effects=True, vmem_limit_bytes=VMEM_LIMIT),
        cost_estimate=pl.CostEstimate(flops=40 * 10**9, bytes_accessed=64 * 2**20, transcendentals=0),
        name="attention",
    )(uc_seq, att_full, part_near)


def finish_kernel(
    y_one, o_pos, wo_full, x_two, dx_one, dy_two, du_pos, up_own, up_near, down_own, down_near, d_qkv, d_out,
    x_one_out, x_two_out, dx_one_out, dx_two_out, dw_up, dw_down, dw_qkv, dw_out,
):
    x_one_out[0] = y_one[0] - dot_nn(o_pos[0], wo_full[...])
    x_two_out[0] = x_two[...]
    dx_one_out[0] = dx_one[...]
    dx_two_out[0] = dy_two[0] + rms_back(x_two[...], du_pos[0])
    dw_up[...] = (up_own[...] + up_near[...]).T
    dw_down[...] = down_own[...] + down_near[...]
    dim = dw_qkv.shape[2]
    for part in range(3):
        dw_qkv[pl.ds(part, dw_qkv.shape[0] // 3, stride=3), 0, :] = d_qkv[pl.ds(part * dim, dim), :].T
    dw_out[...] = d_out[...]


def finish_call(y_one, o_pos, wo_full, x_two, dx_one, dy_two, du_pos, part_own, up_near, down_near, d_att):
    seqs, slab, hidden = y_one.shape
    ffn = part_own.shape[0] // 2
    dim = d_att.shape[0] // 4
    state = pl.BlockSpec((1, slab, hidden), lambda step: (step, 0, 0))
    flat = pl.BlockSpec((slab, hidden), lambda step: (step, 0))
    up = pl.BlockSpec((ffn, slab), lambda step: (0, step))
    rows = ffn // seqs
    in_specs = [
        state, state, pl.BlockSpec((hidden, hidden), lambda step: (0, 0)), flat, flat, state, state,
        up, up, pl.BlockSpec((rows, hidden), lambda step: (seqs + step, 0)), pl.BlockSpec((rows, hidden), lambda step: (step, 0)),
        pl.BlockSpec((3 * dim, slab), lambda step: (0, step)), pl.BlockSpec((dim // seqs, hidden), lambda step: (3 * seqs + step, 0)),
    ]
    out_specs = [state] * 4 + [
        pl.BlockSpec((slab, ffn), lambda step: (step, 0)), pl.BlockSpec((rows, hidden), lambda step: (step, 0)),
        pl.BlockSpec((3 * slab, 1, dim), lambda step: (step, 0, 0)), pl.BlockSpec((dim // seqs, hidden), lambda step: (step, 0)),
    ]
    out_shape = [jax.ShapeDtypeStruct(y_one.shape, F32)] * 4 + [jax.ShapeDtypeStruct(shape, F32) for shape in ((hidden, ffn), (ffn, hidden), (3 * hidden, 1, dim), (dim, hidden))]
    return pl.pallas_call(
        finish_kernel,
        out_shape=out_shape,
        grid=(seqs,),
        in_specs=in_specs,
        out_specs=out_specs,
        compiler_params=pltpu.CompilerParams(dimension_semantics=("arbitrary",), vmem_limit_bytes=VMEM_LIMIT),
        cost_estimate=pl.CostEstimate(flops=2 * 10**9, bytes_accessed=60 * 2**20, transcendentals=0),
        name="finish",
    )(y_one, o_pos, wo_full, x_two, dx_one, dy_two, du_pos, part_own, up_near, part_own, down_near, d_att, d_att)


def local_backward(y_one, y_two, dy_one, dy_two, w_qkv, w_out, w_up, w_down):
    hidden = y_one.shape[2]
    _, _, _, parts, dim = w_qkv.shape
    flat = [tensor.reshape(-1, hidden) for tensor in (y_one, y_two, dy_one, dy_two)]
    qkv_parts = jnp.swapaxes(w_qkv[0, :, 0], 0, 1)
    x_two, dx_one, uc_seq, att_full, part_own, part_near, up_near = mlp_call(*flat, w_up[0], w_down[0], qkv_parts, w_out[0, 0])
    down_near, d_att, o_pos, du_pos, wo_full, _ = attention_call(uc_seq, att_full, part_near)
    x_one, x_two, dx_one, dx_two, dw_up, dw_down, dw_qkv, dw_out = finish_call(
        y_one, o_pos, wo_full.reshape(-1, hidden), x_two, dx_one, dy_two, du_pos, part_own, up_near, down_near, d_att
    )
    return (x_one, x_two, dx_one, dx_two, dw_qkv.reshape(1, hidden, 1, parts, dim), dw_out[None, None], dw_up[None], dw_down[None])


def solution(mesh):
    state_spec = P("dp", "tp", None)
    in_specs = (state_spec, state_spec, state_spec, state_spec, P(None, None, "tp", None, None), P(None, "tp", None, None), P(None, None, "tp"), P(None, "tp", None))
    out_specs = (state_spec, state_spec, state_spec, state_spec, P("dp", None, "tp", None, None), P("dp", "tp", None, None), P("dp", None, "tp"), P("dp", "tp", None))
    return jax.shard_map(local_backward, mesh=mesh, in_specs=in_specs, out_specs=out_specs, check_vma=False)
```

```python
import functools

import jax
import jax.numpy as jnp
from jax import lax
from jax.experimental import pallas as pl
from jax.experimental.pallas import tpu as pltpu
from jax.sharding import PartitionSpec as P

RMS_EPS = 1e-6
LOG2_E = 1.4426950408889634
MESH = pl.DeviceIdType.MESH
BF16, F32 = jnp.bfloat16, jnp.float32
VMEM_LIMIT = 64 * 1024 * 1024 - 65536


def inv_rms(tensor):
    return lax.rsqrt(jnp.mean(tensor * tensor, axis=-1, keepdims=True) + RMS_EPS)


def rms_norm(tensor):
    return tensor * inv_rms(tensor)


def rms_back(tensor, grad_in):
    scale = inv_rms(tensor)
    return scale * grad_in - tensor * (scale * scale * scale) * jnp.mean(grad_in * tensor, axis=-1, keepdims=True)


def gelu_and_slope(tensor):
    root = (2.0 / jnp.pi) ** 0.5
    squared = tensor * tensor
    tanh = jnp.tanh(root * (tensor + 0.044715 * (tensor * squared)))
    cdf = 0.5 * (1.0 + tanh)
    slope = cdf + (0.5 * root) * tensor * ((1.0 - tanh * tanh) * (1.0 + (3 * 0.044715) * squared))
    return tensor * cdf, slope


def dot_nn(left, right):
    return lax.dot_general(left, right, (((1,), (0,)), ((), ())), preferred_element_type=F32)


def dot_nt(left, right):
    return lax.dot_general(left, right, (((1,), (1,)), ((), ())), preferred_element_type=F32)


def dot_tn(left, right):
    return lax.dot_general(left, right, (((0,), (0,)), ((), ())), preferred_element_type=F32)


class Ring:
    def __init__(self):
        me = lax.axis_index("tp")
        chip, core = me // 2, me % 2
        self.me, self.chip, self.core = me, chip, core
        self.chips = (chip, chip + 1 - 2 * (chip % 2), 3 - chip, (chip + 2) % 4)

    def at(self, slot):
        core = self.core if slot % 2 == 0 else 1 - self.core
        return self.chips[slot // 2] * 2 + core

    def at_traced(self, slot):
        relation, other = slot // 2, slot % 2
        own, near_t, near_f, opposite = self.chips
        chip = jnp.where(relation == 0, own, jnp.where(relation == 1, near_t, jnp.where(relation == 2, near_f, opposite)))
        return chip * 2 + (self.core + other) % 2

    def barrier(self):
        barrier = pltpu.get_barrier_semaphore()
        for slot in (1, 2, 3, 4, 5):
            pl.semaphore_signal(barrier, inc=1, device_id={"tp": self.at(slot)}, device_id_type=MESH)
        pl.semaphore_wait(barrier, 5)

    def copy(self, src, dst, send_sem, recv_sem, slot):
        return pltpu.make_async_remote_copy(src_ref=src, dst_ref=dst, send_sem=send_sem, recv_sem=recv_sem, device_id={"tp": self.at(slot)}, device_id_type=MESH)


PARTNER, SAME_T, OTHER_T, SAME_F, OTHER_F, SAME_O, OTHER_O = 1, 2, 3, 4, 5, 6, 7


def mlp_kernel(
    y_one, y_two, dy_one, dy_two, w_up, w_down, w_qkv, w_out,
    x_two, dx_one, uc_seq, att_full, part_own, part_near, near_recv,
    u_all, c_all, up_all, down_all, acc, uc_own, relay, y_buf, x_buf, up_raw, qkv_raw, att_own,
    load_sem, y_sem, x_sem, w_send, w_recv, uc_send, uc_recv, att_send, att_recv, a2a_send, a2a_recv, relay_recv, near_sem,
):
    ring = Ring()
    half = 512
    slab = 128

    def weight(which, src_slot, dst_slot, to, index):
        buf = (up_all, down_all)[which]
        return ring.copy(buf.at[src_slot], buf.at[dst_slot], w_send.at[index], w_recv.at[dst_slot, which], to)

    def weight_pair(src_slot, dst_slot, to, index):
        return [weight(which, src_slot, dst_slot, to, index + which) for which in (0, 1)]

    w_own = weight_pair(0, 1, PARTNER, 0) + weight_pair(0, 2, SAME_T, 2) + weight_pair(0, 4, SAME_F, 4)
    w_near_t = weight_pair(2, 6, SAME_F, 6) + weight_pair(2, 3, PARTNER, 8)
    w_near_f = weight_pair(4, 5, PARTNER, 10)
    w_far = weight_pair(6, 7, PARTNER, 12)

    def uc_pair(src_slot, dst_slot, to, index):
        return [ring.copy(buf.at[src_slot], buf.at[dst_slot], uc_send.at[index + which], uc_recv.at[dst_slot, which], to) for which, buf in enumerate((u_all, c_all))]

    uc_out = uc_pair(0, 2, SAME_T, 0) + uc_pair(0, 1, PARTNER, 2)
    uc_pass = uc_pair(2, 3, PARTNER, 4)

    def att(src, dst_slot, to, index):
        return ring.copy(src, att_full.at[dst_slot], att_send.at[index], att_recv.at[dst_slot], to)

    att_out = [att(att_own, 4, SAME_F, 0), att(att_own, 2, SAME_T, 1), att(att_own, 1, PARTNER, 2)]
    att_keep = pltpu.make_async_copy(att_own, att_full.at[0], load_sem.at[6])
    att_near_f = [att(att_full.at[4], 5, PARTNER, 3)]
    att_near_t = [att(att_full.at[2], 3, PARTNER, 4)]

    a2a_out = {slot: ring.copy(uc_own.at[slot], uc_seq.at[slot], a2a_send.at[slot], a2a_recv.at[slot], slot) for slot in (1, 2, 3, 4, 5)}
    a2a_out[SAME_O] = ring.copy(uc_own.at[SAME_O], relay.at[0], a2a_send.at[SAME_O], relay_recv.at[0], SAME_T)
    a2a_out[OTHER_O] = ring.copy(uc_own.at[OTHER_O], relay.at[1], a2a_send.at[OTHER_O], relay_recv.at[1], SAME_F)
    a2a_pass = [
        ring.copy(relay.at[0], uc_seq.at[SAME_O], a2a_send.at[8], a2a_recv.at[SAME_O], SAME_F),
        ring.copy(relay.at[1], uc_seq.at[OTHER_O], a2a_send.at[9], a2a_recv.at[OTHER_O], OTHER_T),
    ]
    uc_keep = pltpu.make_async_copy(uc_own.at[0], uc_seq.at[0], load_sem.at[4])

    def start(copies):
        for copy in copies:
            copy.start()

    dim = w_out.shape[0]
    near_rows = near_recv.shape[0]
    near = ring.copy(acc.at[0, pl.ds(0, near_rows)], near_recv, near_sem.at[0], near_sem.at[1], SAME_F)

    loads = [
        pltpu.make_async_copy(w_down, down_all.at[0], load_sem.at[0]),
        pltpu.make_async_copy(w_up, up_raw, load_sem.at[1]),
        pltpu.make_async_copy(y_one, acc.at[0], load_sem.at[2]),
        pltpu.make_async_copy(dy_two, acc.at[1], load_sem.at[3]),
        pltpu.make_async_copy(w_qkv, qkv_raw, load_sem.at[5]),
        pltpu.make_async_copy(w_out, att_own.at[pl.ds(3 * dim, dim)], load_sem.at[7]),
    ]
    start(loads)
    ring.barrier()
    loads[0].wait()
    start(w_own[1::2])
    loads[1].wait()
    for part in range(up_raw.shape[1] // dim):
        up_all[0, pl.ds(part * dim, dim), :] = up_raw[:, pl.ds(part * dim, dim)].T
    start(w_own[0::2])
    loads[2].wait()
    loads[3].wait()

    def normalize(step, carry):
        rows = pl.ds(pl.multiple_of(step * slab, slab), slab)
        u_all[0, rows, :] = rms_norm(acc[0, rows, :]).astype(BF16)
        c_all[0, rows, :] = acc[1, rows, :].astype(BF16)
        acc[0, rows, :] = jnp.zeros((slab, acc.shape[2]), F32)
        acc[1, rows, :] = jnp.zeros((slab, acc.shape[2]), F32)
        return carry

    lax.fori_loop(0, acc.shape[1] // slab, normalize, 0)
    start(uc_out)
    loads[4].wait()
    for part in range(3):
        att_own[pl.ds(part * dim, dim), :] = qkv_raw[part].T
    loads[5].wait()
    att_keep.start()

    def y_loads(step, buf):
        seq = ring.at_traced(7 - step)
        rows = pl.ds(pl.multiple_of(seq * slab, slab), slab)
        return [pltpu.make_async_copy(src.at[rows], y_buf.at[buf, which], y_sem.at[buf, which]) for which, src in enumerate((y_one, y_two, dy_one))]

    def x_stores(step, buf):
        seq = ring.at_traced(7 - step)
        rows = pl.ds(pl.multiple_of(seq * slab, slab), slab)
        return [pltpu.make_async_copy(x_buf.at[buf, which], dst.at[rows], x_sem.at[buf, which]) for which, dst in enumerate((x_two, dx_one))]

    def feed_forward(step, carry):
        slot = jnp.where(step == 3, 4, jnp.where(step == 4, 3, step))

        @pl.when(step >= 1)
        def _():
            for which, buf in enumerate((up_all, down_all)):
                ring.copy(buf.at[slot], buf.at[slot], w_send.at[0], w_recv.at[slot, which], PARTNER).wait_recv()

        @pl.when(step == 2)
        def _():
            start(w_near_t)
            start(att_out)

        @pl.when(step == 3)
        def _():
            start(w_near_f)

        @pl.when(step == 6)
        def _():
            start(w_far)

        @pl.when(step == 7)
        def _():
            start(y_loads(0, 0))

        def rows_step(part, carry):
            rows = pl.ds(pl.multiple_of(part * half, half), half)
            hidden, slope = gelu_and_slope(dot_nt(u_all[0, rows, :], up_all[slot]))
            d_pre = (slope * dot_nt(c_all[0, rows, :], down_all[slot])).astype(BF16)
            acc[0, rows, :] += dot_nn(hidden.astype(BF16), down_all[slot])
            acc[1, rows, :] += dot_nn(d_pre, up_all[slot])
            return carry

        lax.fori_loop(0, acc.shape[1] // half, rows_step, 0)
        return carry

    lax.fori_loop(0, 8, feed_forward, 0)

    def finish(step, carry):
        slot = 7 - step
        buf = step % 2
        seq = ring.at_traced(slot)
        rows = pl.ds(pl.multiple_of(seq * slab, slab), slab)
        for copy in y_loads(step, buf):
            copy.wait()

        @pl.when(step < 7)
        def _():
            start(y_loads(step + 1, 1 - buf))

        @pl.when(step >= 2)
        def _():
            for copy in x_stores(step - 2, buf):
                copy.wait()

        y_first = y_buf[buf, 0]
        x_second = y_buf[buf, 1] - acc[0, rows, :]
        dy_first = y_buf[buf, 2] + rms_back(y_first, acc[1, rows, :])
        x_buf[buf, 0] = x_second
        x_buf[buf, 1] = dy_first
        uc_own[slot, 0] = rms_norm(x_second).astype(BF16)
        uc_own[slot, 1] = dy_first.astype(BF16)
        acc[0, rows, :] = jnp.zeros((slab, acc.shape[2]), F32)
        acc[1, rows, :] = jnp.zeros((slab, acc.shape[2]), F32)
        start(x_stores(step, buf))
        return carry

    lax.fori_loop(0, 8, finish, 0)
    for slot in (7, 6, 5, 4, 3, 2, 1):
        a2a_out[slot].start()
    uc_keep.start()
    for step in (6, 7):
        for copy in x_stores(step, step % 2):
            copy.wait()

    def gradients(step, carry):
        first = step // 8
        tokens = (step % 8) // 2
        slot = 4 - 4 * first

        @pl.when((step == 2) | (step == 4) | (step == 6))
        def _():
            for which, buf in enumerate((u_all, c_all)):
                ring.copy(buf.at[tokens], buf.at[tokens], uc_send.at[0], uc_recv.at[tokens, which], PARTNER).wait_recv()

        @pl.when(step == 4)
        def _():
            start(uc_pass)

        @pl.when(step == 8)
        def _():
            near.start()
            ring.copy(att_own, att_full.at[4], att_send.at[0], att_recv.at[4], PARTNER).wait_recv()
            start(att_near_f)
            ring.copy(att_own, att_full.at[2], att_send.at[0], att_recv.at[2], PARTNER).wait_recv()
            start(att_near_t)

        @pl.when(step == 9)
        def _():
            for index in (0, 1):
                ring.copy(relay.at[index], relay.at[index], a2a_send.at[0], relay_recv.at[index], PARTNER).wait_recv()
            start(a2a_pass)

        rows = pl.ds(pl.multiple_of((step % 2) * half, half), half)
        u_part, c_part = u_all[tokens, rows, :], c_all[tokens, rows, :]
        hidden, slope = gelu_and_slope(dot_nt(up_all[slot], u_part))
        d_pre = (slope * dot_nt(down_all[slot], c_part)).astype(BF16)
        acc[first, pl.ds(0, half), :] += dot_nn(d_pre, u_part)
        acc[first, pl.ds(half, half), :] += dot_nn(hidden.astype(BF16), c_part)
        return carry

    lax.fori_loop(0, 16, gradients, 0)
    out_near = pltpu.make_async_copy(acc.at[0, pl.ds(near_rows, acc.shape[1] - near_rows)], part_near, load_sem.at[0])
    out_own = pltpu.make_async_copy(acc.at[1], part_own, load_sem.at[1])
    out_near.start()
    out_own.start()

    for slot in (1, 3, 5):
        ring.copy(att_own, att_full.at[slot], att_send.at[0], att_recv.at[slot], PARTNER).wait_recv()
    for slot in range(1, 8):
        ring.copy(uc_own.at[slot], uc_seq.at[slot], a2a_send.at[0], a2a_recv.at[slot], PARTNER).wait_recv()
    for copy in w_own + w_near_t + w_near_f + w_far + uc_out + uc_pass + att_out + att_near_t + att_near_f + list(a2a_out.values()) + a2a_pass:
        copy.wait_send()
    near.wait()
    uc_keep.wait()
    att_keep.wait()
    out_near.wait()
    out_own.wait()


def mlp_call(y_one, y_two, dy_one, dy_two, w_up, w_down, w_qkv, w_out):
    tokens, hidden = y_one.shape
    ffn = w_down.shape[0]
    dim = w_out.shape[0]
    near_rows = ffn
    any_spec = pl.BlockSpec(memory_space=pl.ANY)
    dma, vmem = pltpu.SemaphoreType.DMA, pltpu.VMEM
    out_shape = (
        jax.ShapeDtypeStruct((tokens, hidden), F32),
        jax.ShapeDtypeStruct((tokens, hidden), F32),
        jax.ShapeDtypeStruct((8, 2, tokens // 8, hidden), BF16),
        jax.ShapeDtypeStruct((6, 4 * dim, hidden), BF16),
        jax.ShapeDtypeStruct((2 * ffn, hidden), F32),
        jax.ShapeDtypeStruct((2 * ffn - near_rows, hidden), F32),
        jax.ShapeDtypeStruct((near_rows, hidden), F32),
    )
    scratch = [
        vmem((4, tokens, hidden), BF16), vmem((4, tokens, hidden), BF16),
        vmem((8, ffn, hidden), BF16), vmem((8, ffn, hidden), BF16),
        vmem((2, tokens, hidden), F32),
        vmem((8, 2, tokens // 8, hidden), BF16), vmem((2, 2, tokens // 8, hidden), BF16),
        vmem((2, 3, tokens // 8, hidden), F32), vmem((2, 2, tokens // 8, hidden), F32),
        vmem((hidden, ffn), BF16), vmem((3, hidden, dim), BF16), vmem((4 * dim, hidden), BF16),
        dma((8,)), dma((2, 3)), dma((2, 2)), dma((14,)), dma((8, 2)), dma((6,)), dma((4, 2)), dma((5,)), dma((6,)), dma((10,)), dma((8,)), dma((2,)), dma((2,)),
    ]
    return pl.pallas_call(
        mlp_kernel,
        out_shape=out_shape,
        in_specs=[any_spec] * 8,
        out_specs=(any_spec,) * 7,
        scratch_shapes=scratch,
        compiler_params=pltpu.CompilerParams(collective_id=0, has_side_effects=True, vmem_limit_bytes=VMEM_LIMIT),
        cost_estimate=pl.CostEstimate(flops=70 * 10**9, bytes_accessed=64 * 2**20, transcendentals=0),
        name="feed_forward",
    )(y_one, y_two, dy_one, dy_two, w_up, w_down, w_qkv, w_out)


def attention_kernel(
    scale, uc_seq, att_full, part_own, part_near, up_near,
    d_up, d_down, d_att, o_pos, du_pos, wo_full, att_far,
    uc_all, qkv_buf, wo_buf, qkv, d_ctx, d_qkv, o_all, du_all, part_send, part_keep, part_core, own_t, far_t, own_f, far_f, o_relay, du_relay, near_out, near_buf,
    load_sem, w_sem, wo_sem, near_sem, core_send, core_recv, part_out, part_in, far_sem, o_send, o_recv, du_send, du_recv, o_relay_recv, du_relay_recv,
):
    ring = Ring()
    slab, hidden = uc_seq.shape[2], uc_seq.shape[3]
    seq_len = 8 * slab
    dim = att_full.shape[1] // 4
    tile = 512

    def relation_of(step):
        return (step + 1) % 4

    def w_loads(heads, buf):
        copies = []
        for index, head in enumerate(heads):
            copies.append(pltpu.make_async_copy(head.at[pl.ds(0, 3 * dim)], qkv_buf.at[buf, pl.ds(index * 3 * dim, 3 * dim)], w_sem.at[buf, index, 0]))
            copies.append(pltpu.make_async_copy(head.at[pl.ds(3 * dim, dim)], wo_buf.at[buf, pl.ds(index * dim, dim)], w_sem.at[buf, index, 1]))
        return copies

    far_from_t = ring.copy(att_full.at[SAME_F], att_far.at[0], far_sem.at[0], far_sem.at[1], SAME_T)
    far_from_core = ring.copy(att_far.at[0], att_far.at[1], far_sem.at[2], far_sem.at[3], PARTNER)

    near_load = pltpu.make_async_copy(part_near, near_out, near_sem.at[2])
    near = ring.copy(near_out, near_buf, near_sem.at[0], near_sem.at[1], SAME_F)

    def core_copy(relation, buf):
        return ring.copy(part_send.at[buf], part_core.at[relation], core_send.at[buf], core_recv.at[relation], PARTNER)

    core_last = [core_copy(3, 0), core_copy(0, 1)]
    rows = part_keep.shape[1]
    ff_loads = [
        pltpu.make_async_copy(part_own.at[pl.ds(0, rows)], part_send.at[0], load_sem.at[1, 0]),
        pltpu.make_async_copy(part_own.at[pl.ds(rows, rows)], part_send.at[1], load_sem.at[1, 1]),
        pltpu.make_async_copy(up_near, part_core.at[1], load_sem.at[2, 0]),
    ]
    ff_stores = [pltpu.make_async_copy(part_send.at[index], dst, load_sem.at[3, index]) for index, dst in enumerate((d_up, d_down))]

    rows_a, rows_b = pl.ds(0, 3 * dim), pl.ds(3 * dim, dim)

    def part(src, dst, index, slot):
        return ring.copy(src, dst, part_out.at[index], part_in.at[index], slot)

    t_own_a = part(part_keep.at[1, rows_a], own_t.at[rows_a], 0, SAME_T)
    t_far_a = part(part_keep.at[3, rows_a], far_t, 1, SAME_T)
    t_own_b = part(part_keep.at[1, rows_b], own_t.at[rows_b], 2, SAME_T)
    f_own_b = part(part_keep.at[2, rows_b], own_f.at[rows_b], 3, SAME_F)
    f_far_b = part(part_keep.at[3, rows_b], far_f, 4, SAME_F)
    f_own_a = part(part_keep.at[2, rows_a], own_f.at[rows_a], 5, SAME_F)

    def rows_of(slot):
        return pl.ds(slot * slab, slab)

    def to_positions(src, dst, relay, send_sem, recv_sem, relay_sem):
        near_t, near_f = ring.at(SAME_T), ring.at(SAME_F)
        out = [
            ring.copy(src.at[rows_of(SAME_O)], relay.at[0], send_sem.at[6], relay_sem.at[0], SAME_T),
            ring.copy(src.at[rows_of(OTHER_O)], relay.at[1], send_sem.at[7], relay_sem.at[1], SAME_F),
        ] + [ring.copy(src.at[rows_of(slot)], dst.at[ring.me], send_sem.at[slot], recv_sem.at[slot], slot) for slot in (5, 4, 3, 2, 1)]
        onward = [
            ring.copy(relay.at[0], dst.at[near_t], send_sem.at[8], recv_sem.at[SAME_O], SAME_F),
            ring.copy(relay.at[1], dst.at[near_f], send_sem.at[9], recv_sem.at[OTHER_O], OTHER_T),
        ]
        keep = pltpu.make_async_copy(src.at[rows_of(0)], dst.at[ring.me], send_sem.at[0])
        return out, onward, keep

    o_out, o_pass, o_keep = to_positions(o_all, o_pos, o_relay, o_send, o_recv, o_relay_recv)
    du_out, du_pass, du_keep = to_positions(du_all, du_pos, du_relay, du_send, du_recv, du_relay_recv)

    def start(copies):
        for copy in copies:
            copy.start()

    loads = [pltpu.make_async_copy(uc_seq.at[slot, which], uc_all.at[which, rows_of(slot)], load_sem.at[slot, which]) for slot in range(8) for which in (0, 1)]
    near_load.start()
    start(loads)
    start(w_loads([att_full.at[3], att_full.at[2]], 0))
    ring.barrier()
    far_from_t.start()
    near_load.wait()
    near.start()
    du_all[...] = jnp.zeros_like(du_all)
    for copy in loads:
        copy.wait()

    def chip_step(step, carry):
        buf = step % 2
        relation = relation_of(step)
        for copy in w_loads([att_far.at[0], att_far.at[0]], buf):
            copy.wait()

        @pl.when(step == 0)
        def _():
            start(w_loads([att_full.at[5], att_full.at[4]], 1))

        @pl.when(step == 1)
        def _():
            far_from_core.wait_recv()
            start(w_loads([att_far.at[1], att_far.at[0]], 0))

        @pl.when(step == 2)
        def _():
            start(w_loads([att_full.at[1], att_full.at[0]], 1))

        heads = [ring.at_traced(relation * 2 + other) for other in (1, 0)]
        wo_copies = [pltpu.make_async_copy(wo_buf.at[buf, pl.ds(index * dim, dim)], wo_full.at[head], wo_sem.at[index]) for index, head in enumerate(heads)]
        start(wo_copies)
        qkv[...] = dot_nt(uc_all[0], qkv_buf[buf]).astype(BF16)
        d_ctx[...] = dot_nt(uc_all[1], wo_buf[buf]).astype(BF16)
        for index, head in enumerate(heads):
            columns = pl.ds(pl.multiple_of(head * dim, dim), dim)
            own = pl.ds(index * 3 * dim, 3 * dim)
            query, key, value = (qkv[:, pl.ds((index * 3 + part) * dim, dim)] for part in range(3))
            d_out = d_ctx[:, pl.ds(index * dim, dim)]
            scores = dot_nt(query, key) * (scale * LOG2_E)
            grown = jnp.exp2(scores - jnp.max(scores, axis=-1, keepdims=True))
            prob = grown * (1.0 / jnp.sum(grown, axis=-1, keepdims=True))
            prob_b = prob.astype(BF16)
            o_all[:, columns] = dot_nn(prob_b, value).astype(BF16)
            d_prob = dot_nt(d_out, value)
            d_score = (prob * (d_prob - jnp.sum(d_prob * prob, axis=-1, keepdims=True)) * scale).astype(BF16)
            d_qkv[:, pl.ds(index * 3 * dim, dim)] = dot_nn(d_score, key).astype(BF16)
            d_qkv[:, pl.ds((index * 3 + 1) * dim, dim)] = dot_nn(query.T, d_score).T.astype(BF16)
            d_qkv[:, pl.ds((index * 3 + 2) * dim, dim)] = dot_nn(d_out.T, prob_b).T.astype(BF16)
            if index == 0:
                @pl.when(step >= 2)
                def _():
                    core_copy(relation, buf).wait_send()

            dst = part_send.at[buf] if index == 0 else part_keep.at[relation]
            dst[pl.ds(0, 3 * dim), :] = dot_tn(d_qkv[:, own], uc_all[0])
            dst[pl.ds(3 * dim, dim), :] = dot_tn(o_all[:, columns], uc_all[1])
            if index == 0:
                core_copy(relation, buf).start()
        core_copy(relation, buf).wait_recv()
        part_keep[relation] += part_core[relation]

        @pl.when(step == 0)
        def _():
            t_own_a.start()

        @pl.when(step == 1)
        def _():
            f_own_b.start()

        @pl.when(step == 2)
        def _():
            t_far_a.start()
            f_far_b.start()

        def du_tile(part, carry):
            rows = pl.ds(pl.multiple_of(part * tile, tile), tile)
            du_all[rows, :] += dot_nn(d_qkv[rows, :], qkv_buf[buf])
            return carry

        lax.fori_loop(0, seq_len // tile, du_tile, 0)

        @pl.when(step == 0)
        def _():
            far_from_t.wait_recv()
            far_from_core.start()

        for copy in wo_copies:
            copy.wait()
        return carry

    lax.fori_loop(0, 4, chip_step, 0)
    start(o_out)
    start(du_out)
    o_keep.start()
    du_keep.start()
    for copy in core_last:
        copy.wait_send()
    start(ff_loads)
    f_far_b.wait_recv()
    part_keep[1, rows_b] += far_f[...]
    t_own_b.start()
    for copy in o_out[:2]:
        copy.wait_recv()
    start(o_pass)
    t_far_a.wait_recv()
    part_keep[2, rows_a] += far_t[...]
    f_own_a.start()
    for copy in ff_loads:
        copy.wait()
    part_send[0] += part_core[1]
    near.wait_recv()
    part_send[1] += near_buf[...]
    for copy in ff_stores:
        copy.start()
    for copy in du_out[:2]:
        copy.wait_recv()
    start(du_pass)
    t_own_a.wait_recv()
    t_own_b.wait_recv()
    part_keep[0] += own_t[...]
    f_own_a.wait_recv()
    f_own_b.wait_recv()
    part_keep[0] += own_f[...]
    d_att_copy = pltpu.make_async_copy(part_keep.at[0], d_att, load_sem.at[0, 0])
    d_att_copy.start()

    for dst, recv_sem in ((o_pos, o_recv), (du_pos, du_recv)):
        for slot in range(1, 8):
            ring.copy(dst.at[0], dst.at[ring.at(slot)], near_sem.at[0], recv_sem.at[slot], PARTNER).wait_recv()
    for copy in o_out + du_out + o_pass + du_pass + [t_own_a, t_far_a, t_own_b, f_own_b, f_far_b, f_own_a, far_from_t, far_from_core, near]:
        copy.wait_send()
    for copy in ff_stores:
        copy.wait()
    o_keep.wait()
    du_keep.wait()
    d_att_copy.wait()


def attention_call(uc_seq, att_full, part_own, part_near, up_near):
    slab, hidden = uc_seq.shape[2:]
    rows = att_full.shape[1]
    dim = rows // 4
    seq_len = 8 * slab
    any_spec = pl.BlockSpec(memory_space=pl.ANY)
    dma, vmem = pltpu.SemaphoreType.DMA, pltpu.VMEM
    out_shape = (
        jax.ShapeDtypeStruct(up_near.shape, F32),
        jax.ShapeDtypeStruct(part_near.shape, F32),
        jax.ShapeDtypeStruct((rows, hidden), F32),
        jax.ShapeDtypeStruct((8, slab, hidden), BF16),
        jax.ShapeDtypeStruct((8, slab, hidden), F32),
        jax.ShapeDtypeStruct((8, dim, hidden), BF16),
        jax.ShapeDtypeStruct((2, rows, hidden), BF16),
    )
    scratch = [
        vmem((2, seq_len, hidden), BF16), vmem((2, 6 * dim, hidden), BF16), vmem((2, 2 * dim, hidden), BF16),
        vmem((seq_len, 6 * dim), BF16), vmem((seq_len, 2 * dim), BF16), vmem((seq_len, 6 * dim), BF16),
        vmem((seq_len, hidden), BF16), vmem((seq_len, hidden), F32),
        vmem((2, rows, hidden), F32), vmem((4, rows, hidden), F32), vmem((4, rows, hidden), F32),
        vmem((rows, hidden), F32), vmem((3 * dim, hidden), F32), vmem((rows, hidden), F32), vmem((dim, hidden), F32),
        vmem((2, slab, hidden), BF16), vmem((2, slab, hidden), F32), vmem(part_near.shape, F32), vmem(part_near.shape, F32),
        dma((8, 2)), dma((2, 2, 2)), dma((2,)), dma((3,)), dma((2,)), dma((4,)), dma((6,)), dma((6,)), dma((4,)), dma((10,)), dma((8,)), dma((10,)), dma((8,)), dma((2,)), dma((2,)),
    ]
    return pl.pallas_call(
        functools.partial(attention_kernel, dim ** -0.5),
        out_shape=out_shape,
        in_specs=[any_spec] * 5,
        out_specs=(any_spec,) * 7,
        scratch_shapes=scratch,
        compiler_params=pltpu.CompilerParams(collective_id=1, has_side_effects=True, vmem_limit_bytes=VMEM_LIMIT),
        cost_estimate=pl.CostEstimate(flops=40 * 10**9, bytes_accessed=64 * 2**20, transcendentals=0),
        name="attention",
    )(uc_seq, att_full, part_own, part_near, up_near)


def finish_kernel(
    y_one, o_pos, wo_full, x_two, dx_one, dy_two, du_pos, d_up, d_down, d_qkv, d_out,
    x_one_out, x_two_out, dx_one_out, dx_two_out, dw_up, dw_down, dw_qkv, dw_out,
):
    x_one_out[0] = y_one[0] - dot_nn(o_pos[0], wo_full[...])
    x_two_out[0] = x_two[...]
    dx_one_out[0] = dx_one[...]
    dx_two_out[0] = dy_two[0] + rms_back(x_two[...], du_pos[0])
    dw_down[...] = d_down[...]
    dw_out[...] = d_out[...]

    @pl.when(pl.program_id(0) % 2 == 0)
    def _():
        dim = dw_qkv.shape[2]
        dw_up[...] = d_up[...].T
        for part in range(3):
            dw_qkv[pl.ds(part, dw_qkv.shape[0] // 3, stride=3), 0, :] = d_qkv[pl.ds(part * dim, dim), :].T


def finish_call(y_one, o_pos, wo_full, x_two, dx_one, dy_two, du_pos, d_up, d_down, d_att):
    seqs, slab, hidden = y_one.shape
    ffn = d_up.shape[0]
    dim = d_att.shape[0] // 4
    steps = 2 * seqs
    half = slab // 2
    state = pl.BlockSpec((1, half, hidden), lambda step: (step // 2, step % 2, 0))
    flat = pl.BlockSpec((half, hidden), lambda step: (step, 0))
    rows, out_rows = ffn // steps, dim // steps
    in_specs = [
        state, state, pl.BlockSpec((hidden, hidden), lambda step: (0, 0)), flat, flat, state, state,
        pl.BlockSpec((ffn, slab), lambda step: (0, step // 2)), pl.BlockSpec((rows, hidden), lambda step: (step, 0)),
        pl.BlockSpec((3 * dim, slab), lambda step: (0, step // 2)), pl.BlockSpec((out_rows, hidden), lambda step: (3 * steps + step, 0)),
    ]
    out_specs = [state] * 4 + [
        pl.BlockSpec((slab, ffn), lambda step: (step // 2, 0)), pl.BlockSpec((rows, hidden), lambda step: (step, 0)),
        pl.BlockSpec((3 * slab, 1, dim), lambda step: (step // 2, 0, 0)), pl.BlockSpec((out_rows, hidden), lambda step: (step, 0)),
    ]
    out_shape = [jax.ShapeDtypeStruct(y_one.shape, F32)] * 4 + [jax.ShapeDtypeStruct(shape, F32) for shape in ((hidden, ffn), (ffn, hidden), (3 * hidden, 1, dim), (dim, hidden))]
    return pl.pallas_call(
        finish_kernel,
        out_shape=out_shape,
        grid=(steps,),
        in_specs=in_specs,
        out_specs=out_specs,
        compiler_params=pltpu.CompilerParams(dimension_semantics=("arbitrary",), vmem_limit_bytes=VMEM_LIMIT),
        cost_estimate=pl.CostEstimate(flops=2 * 10**9, bytes_accessed=60 * 2**20, transcendentals=0),
        name="finish",
    )(y_one, o_pos, wo_full, x_two, dx_one, dy_two, du_pos, d_up, d_down, d_att, d_att)


def local_backward(y_one, y_two, dy_one, dy_two, w_qkv, w_out, w_up, w_down):
    hidden = y_one.shape[2]
    _, _, _, parts, dim = w_qkv.shape
    flat = [tensor.reshape(-1, hidden) for tensor in (y_one, y_two, dy_one, dy_two)]
    qkv_parts = jnp.swapaxes(w_qkv[0, :, 0], 0, 1)
    x_two, dx_one, uc_seq, att_full, part_own, part_near, up_near = mlp_call(*flat, w_up[0], w_down[0], qkv_parts, w_out[0, 0])
    d_up, d_down, d_att, o_pos, du_pos, wo_full, _ = attention_call(uc_seq, att_full, part_own, part_near, up_near)
    x_one, x_two, dx_one, dx_two, dw_up, dw_down, dw_qkv, dw_out = finish_call(
        y_one, o_pos, wo_full.reshape(-1, hidden), x_two, dx_one, dy_two, du_pos, d_up, d_down, d_att
    )
    return (x_one, x_two, dx_one, dx_two, dw_qkv.reshape(1, hidden, 1, parts, dim), dw_out[None, None], dw_up[None], dw_down[None])


def solution(mesh):
    state_spec = P("dp", "tp", None)
    in_specs = (state_spec, state_spec, state_spec, state_spec, P(None, None, "tp", None, None), P(None, "tp", None, None), P(None, None, "tp"), P(None, "tp", None))
    out_specs = (state_spec, state_spec, state_spec, state_spec, P("dp", None, "tp", None, None), P("dp", "tp", None, None), P("dp", None, "tp"), P("dp", "tp", None))
    return jax.shard_map(local_backward, mesh=mesh, in_specs=in_specs, out_specs=out_specs, check_vma=False)
```

```python
import functools

import jax
import jax.numpy as jnp
from jax import lax
from jax.experimental import pallas as pl
from jax.experimental.pallas import tpu as pltpu
from jax.sharding import PartitionSpec as P

RMS_EPS = 1e-6
LOG2_E = 1.4426950408889634
MESH = pl.DeviceIdType.MESH
BF16, F32 = jnp.bfloat16, jnp.float32
VMEM_LIMIT = 64 * 1024 * 1024 - 65536


def inv_rms(tensor):
    return lax.rsqrt(jnp.mean(tensor * tensor, axis=-1, keepdims=True) + RMS_EPS)


def rms_norm(tensor):
    return tensor * inv_rms(tensor)


def rms_back(tensor, grad_in):
    scale = inv_rms(tensor)
    return scale * grad_in - tensor * (scale * scale * scale) * jnp.mean(grad_in * tensor, axis=-1, keepdims=True)


def gelu_and_slope(tensor):
    root = (2.0 / jnp.pi) ** 0.5
    squared = tensor * tensor
    tanh = jnp.tanh(root * (tensor + 0.044715 * (tensor * squared)))
    cdf = 0.5 * (1.0 + tanh)
    slope = cdf + (0.5 * root) * tensor * ((1.0 - tanh * tanh) * (1.0 + (3 * 0.044715) * squared))
    return tensor * cdf, slope


def dot_nn(left, right):
    return lax.dot_general(left, right, (((1,), (0,)), ((), ())), preferred_element_type=F32)


def dot_nt(left, right):
    return lax.dot_general(left, right, (((1,), (1,)), ((), ())), preferred_element_type=F32)


def dot_tn(left, right):
    return lax.dot_general(left, right, (((0,), (0,)), ((), ())), preferred_element_type=F32)


class Ring:
    def __init__(self):
        me = lax.axis_index("tp")
        chip, core = me // 2, me % 2
        self.me, self.chip, self.core = me, chip, core
        self.chips = (chip, chip + 1 - 2 * (chip % 2), 3 - chip, (chip + 2) % 4)

    def at(self, slot):
        core = self.core if slot % 2 == 0 else 1 - self.core
        return self.chips[slot // 2] * 2 + core

    def at_traced(self, slot):
        relation, other = slot // 2, slot % 2
        own, near_t, near_f, opposite = self.chips
        chip = jnp.where(relation == 0, own, jnp.where(relation == 1, near_t, jnp.where(relation == 2, near_f, opposite)))
        return chip * 2 + (self.core + other) % 2

    def barrier(self):
        barrier = pltpu.get_barrier_semaphore()
        for slot in (1, 2, 3, 4, 5):
            pl.semaphore_signal(barrier, inc=1, device_id={"tp": self.at(slot)}, device_id_type=MESH)
        pl.semaphore_wait(barrier, 5)

    def copy(self, src, dst, send_sem, recv_sem, slot):
        return pltpu.make_async_remote_copy(src_ref=src, dst_ref=dst, send_sem=send_sem, recv_sem=recv_sem, device_id={"tp": self.at(slot)}, device_id_type=MESH)


PARTNER, SAME_T, OTHER_T, SAME_F, OTHER_F, SAME_O, OTHER_O = 1, 2, 3, 4, 5, 6, 7


def mlp_kernel(
    y_one, y_two, dy_one, dy_two, w_up, w_down, w_qkv, w_out,
    x_two, dx_one, uc_seq, att_full, part_own, part_near, near_recv,
    u_all, c_all, up_all, down_all, acc, uc_own, relay, y_buf, x_buf, up_raw, qkv_raw, att_own,
    load_sem, y_sem, x_sem, w_send, w_recv, uc_send, uc_recv, att_send, att_recv, a2a_send, a2a_recv, relay_recv, near_sem,
):
    ring = Ring()
    half = 512
    slab = 128

    def weight(which, src_slot, dst_slot, to, index):
        buf = (up_all, down_all)[which]
        return ring.copy(buf.at[src_slot], buf.at[dst_slot], w_send.at[index], w_recv.at[dst_slot, which], to)

    def weight_pair(src_slot, dst_slot, to, index):
        return [weight(which, src_slot, dst_slot, to, index + which) for which in (0, 1)]

    w_own = weight_pair(0, 1, PARTNER, 0) + weight_pair(0, 2, SAME_T, 2) + weight_pair(0, 4, SAME_F, 4)
    w_near_t = weight_pair(2, 6, SAME_F, 6) + weight_pair(2, 3, PARTNER, 8)
    w_near_f = weight_pair(4, 5, PARTNER, 10)
    w_far = weight_pair(6, 7, PARTNER, 12)

    def uc_pair(src_slot, dst_slot, to, index):
        return [ring.copy(buf.at[src_slot], buf.at[dst_slot], uc_send.at[index + which], uc_recv.at[dst_slot, which], to) for which, buf in enumerate((u_all, c_all))]

    uc_out = uc_pair(0, 2, SAME_T, 0) + uc_pair(0, 1, PARTNER, 2)
    uc_pass = uc_pair(2, 3, PARTNER, 4)

    def att(src, dst_slot, to, index):
        return ring.copy(src, att_full.at[dst_slot], att_send.at[index], att_recv.at[dst_slot], to)

    att_out = [att(att_own, 4, SAME_F, 0), att(att_own, 2, SAME_T, 1), att(att_own, 1, PARTNER, 2)]
    att_keep = pltpu.make_async_copy(att_own, att_full.at[0], load_sem.at[6])
    att_near_f = [att(att_full.at[4], 5, PARTNER, 3)]
    att_near_t = [att(att_full.at[2], 3, PARTNER, 4)]

    a2a_out = {slot: ring.copy(uc_own.at[slot], uc_seq.at[slot], a2a_send.at[slot], a2a_recv.at[slot], slot) for slot in (1, 2, 3, 4, 5)}
    a2a_out[SAME_O] = ring.copy(uc_own.at[SAME_O], relay.at[0], a2a_send.at[SAME_O], relay_recv.at[0], SAME_T)
    a2a_out[OTHER_O] = ring.copy(uc_own.at[OTHER_O], relay.at[1], a2a_send.at[OTHER_O], relay_recv.at[1], SAME_F)
    a2a_pass = [
        ring.copy(relay.at[0], uc_seq.at[SAME_O], a2a_send.at[8], a2a_recv.at[SAME_O], SAME_F),
        ring.copy(relay.at[1], uc_seq.at[OTHER_O], a2a_send.at[9], a2a_recv.at[OTHER_O], OTHER_T),
    ]
    uc_keep = pltpu.make_async_copy(uc_own.at[0], uc_seq.at[0], load_sem.at[4])

    def start(copies):
        for copy in copies:
            copy.start()

    dim = w_out.shape[0]
    near_rows = near_recv.shape[0]
    near = ring.copy(acc.at[0, pl.ds(0, near_rows)], near_recv, near_sem.at[0], near_sem.at[1], SAME_F)

    loads = [
        pltpu.make_async_copy(w_down, down_all.at[0], load_sem.at[0]),
        pltpu.make_async_copy(w_up, up_raw, load_sem.at[1]),
        pltpu.make_async_copy(y_one, acc.at[0], load_sem.at[2]),
        pltpu.make_async_copy(dy_two, acc.at[1], load_sem.at[3]),
        pltpu.make_async_copy(w_qkv, qkv_raw, load_sem.at[5]),
        pltpu.make_async_copy(w_out, att_own.at[pl.ds(3 * dim, dim)], load_sem.at[7]),
    ]
    start(loads)
    ring.barrier()
    loads[0].wait()
    start(w_own[1::2])
    loads[1].wait()
    for part in range(up_raw.shape[1] // dim):
        up_all[0, pl.ds(part * dim, dim), :] = up_raw[:, pl.ds(part * dim, dim)].T
    start(w_own[0::2])
    loads[2].wait()
    loads[3].wait()

    def normalize(step, carry):
        rows = pl.ds(pl.multiple_of(step * slab, slab), slab)
        u_all[0, rows, :] = rms_norm(acc[0, rows, :]).astype(BF16)
        c_all[0, rows, :] = acc[1, rows, :].astype(BF16)
        acc[0, rows, :] = jnp.zeros((slab, acc.shape[2]), F32)
        acc[1, rows, :] = jnp.zeros((slab, acc.shape[2]), F32)
        return carry

    lax.fori_loop(0, acc.shape[1] // slab, normalize, 0)
    start(uc_out)
    loads[4].wait()
    for part in range(3):
        att_own[pl.ds(part * dim, dim), :] = qkv_raw[part].T
    loads[5].wait()
    att_keep.start()

    def y_loads(step, buf):
        seq = ring.at_traced(7 - step)
        rows = pl.ds(pl.multiple_of(seq * slab, slab), slab)
        return [pltpu.make_async_copy(src.at[rows], y_buf.at[buf, which], y_sem.at[buf, which]) for which, src in enumerate((y_one, y_two, dy_one))]

    def x_stores(step, buf):
        seq = ring.at_traced(7 - step)
        rows = pl.ds(pl.multiple_of(seq * slab, slab), slab)
        return [pltpu.make_async_copy(x_buf.at[buf, which], dst.at[rows], x_sem.at[buf, which]) for which, dst in enumerate((x_two, dx_one))]

    def feed_forward(step, carry):
        slot = jnp.where(step == 3, 4, jnp.where(step == 4, 3, step))

        @pl.when(step >= 1)
        def _():
            for which, buf in enumerate((up_all, down_all)):
                ring.copy(buf.at[slot], buf.at[slot], w_send.at[0], w_recv.at[slot, which], PARTNER).wait_recv()

        @pl.when(step == 2)
        def _():
            start(w_near_t)
            start(att_out)

        @pl.when(step == 3)
        def _():
            start(w_near_f)

        @pl.when(step == 6)
        def _():
            start(w_far)

        @pl.when(step == 7)
        def _():
            start(y_loads(0, 0))

        def rows_step(part, carry):
            rows = pl.ds(pl.multiple_of(part * half, half), half)
            hidden, slope = gelu_and_slope(dot_nt(u_all[0, rows, :], up_all[slot]))
            d_pre = (slope * dot_nt(c_all[0, rows, :], down_all[slot])).astype(BF16)
            acc[0, rows, :] += dot_nn(hidden.astype(BF16), down_all[slot])
            acc[1, rows, :] += dot_nn(d_pre, up_all[slot])
            return carry

        lax.fori_loop(0, acc.shape[1] // half, rows_step, 0)
        return carry

    lax.fori_loop(0, 8, feed_forward, 0)

    def finish(step, carry):
        slot = 7 - step
        buf = step % 2
        seq = ring.at_traced(slot)
        rows = pl.ds(pl.multiple_of(seq * slab, slab), slab)
        for copy in y_loads(step, buf):
            copy.wait()

        @pl.when(step < 7)
        def _():
            start(y_loads(step + 1, 1 - buf))

        @pl.when(step >= 2)
        def _():
            for copy in x_stores(step - 2, buf):
                copy.wait()

        y_first = y_buf[buf, 0]
        x_second = y_buf[buf, 1] - acc[0, rows, :]
        dy_first = y_buf[buf, 2] + rms_back(y_first, acc[1, rows, :])
        x_buf[buf, 0] = x_second
        x_buf[buf, 1] = dy_first
        uc_own[slot, 0] = rms_norm(x_second).astype(BF16)
        uc_own[slot, 1] = dy_first.astype(BF16)
        acc[0, rows, :] = jnp.zeros((slab, acc.shape[2]), F32)
        acc[1, rows, :] = jnp.zeros((slab, acc.shape[2]), F32)
        start(x_stores(step, buf))
        return carry

    lax.fori_loop(0, 8, finish, 0)
    for slot in (7, 6, 5, 4, 3, 2, 1):
        a2a_out[slot].start()
    uc_keep.start()
    for step in (6, 7):
        for copy in x_stores(step, step % 2):
            copy.wait()

    def gradients(step, carry):
        first = step // 8
        tokens = (step % 8) // 2
        slot = 4 - 4 * first

        @pl.when((step == 2) | (step == 4) | (step == 6))
        def _():
            for which, buf in enumerate((u_all, c_all)):
                ring.copy(buf.at[tokens], buf.at[tokens], uc_send.at[0], uc_recv.at[tokens, which], PARTNER).wait_recv()

        @pl.when(step == 4)
        def _():
            start(uc_pass)

        @pl.when(step == 8)
        def _():
            near.start()
            ring.copy(att_own, att_full.at[4], att_send.at[0], att_recv.at[4], PARTNER).wait_recv()
            start(att_near_f)
            ring.copy(att_own, att_full.at[2], att_send.at[0], att_recv.at[2], PARTNER).wait_recv()
            start(att_near_t)

        @pl.when(step == 9)
        def _():
            for index in (0, 1):
                ring.copy(relay.at[index], relay.at[index], a2a_send.at[0], relay_recv.at[index], PARTNER).wait_recv()
            start(a2a_pass)

        rows = pl.ds(pl.multiple_of((step % 2) * half, half), half)
        u_part, c_part = u_all[tokens, rows, :], c_all[tokens, rows, :]
        hidden, slope = gelu_and_slope(dot_nt(up_all[slot], u_part))
        d_pre = (slope * dot_nt(down_all[slot], c_part)).astype(BF16)
        acc[first, pl.ds(0, half), :] += dot_nn(d_pre, u_part)
        acc[first, pl.ds(half, half), :] += dot_nn(hidden.astype(BF16), c_part)
        return carry

    lax.fori_loop(0, 16, gradients, 0)
    out_near = pltpu.make_async_copy(acc.at[0, pl.ds(near_rows, acc.shape[1] - near_rows)], part_near, load_sem.at[0])
    out_own = pltpu.make_async_copy(acc.at[1], part_own, load_sem.at[1])
    out_near.start()
    out_own.start()

    for slot in (1, 3, 5):
        ring.copy(att_own, att_full.at[slot], att_send.at[0], att_recv.at[slot], PARTNER).wait_recv()
    for slot in range(1, 8):
        ring.copy(uc_own.at[slot], uc_seq.at[slot], a2a_send.at[0], a2a_recv.at[slot], PARTNER).wait_recv()
    for copy in w_own + w_near_t + w_near_f + w_far + uc_out + uc_pass + att_out + att_near_t + att_near_f + list(a2a_out.values()) + a2a_pass:
        copy.wait_send()
    near.wait()
    uc_keep.wait()
    att_keep.wait()
    out_near.wait()
    out_own.wait()


def mlp_call(y_one, y_two, dy_one, dy_two, w_up, w_down, w_qkv, w_out):
    tokens, hidden = y_one.shape
    ffn = w_down.shape[0]
    dim = w_out.shape[0]
    near_rows = ffn
    any_spec = pl.BlockSpec(memory_space=pl.ANY)
    dma, vmem = pltpu.SemaphoreType.DMA, pltpu.VMEM
    out_shape = (
        jax.ShapeDtypeStruct((tokens, hidden), F32),
        jax.ShapeDtypeStruct((tokens, hidden), F32),
        jax.ShapeDtypeStruct((8, 2, tokens // 8, hidden), BF16),
        jax.ShapeDtypeStruct((6, 4 * dim, hidden), BF16),
        jax.ShapeDtypeStruct((2 * ffn, hidden), F32),
        jax.ShapeDtypeStruct((2 * ffn - near_rows, hidden), F32),
        jax.ShapeDtypeStruct((near_rows, hidden), F32),
    )
    scratch = [
        vmem((4, tokens, hidden), BF16), vmem((4, tokens, hidden), BF16),
        vmem((8, ffn, hidden), BF16), vmem((8, ffn, hidden), BF16),
        vmem((2, tokens, hidden), F32),
        vmem((8, 2, tokens // 8, hidden), BF16), vmem((2, 2, tokens // 8, hidden), BF16),
        vmem((2, 3, tokens // 8, hidden), F32), vmem((2, 2, tokens // 8, hidden), F32),
        vmem((hidden, ffn), BF16), vmem((3, hidden, dim), BF16), vmem((4 * dim, hidden), BF16),
        dma((8,)), dma((2, 3)), dma((2, 2)), dma((14,)), dma((8, 2)), dma((6,)), dma((4, 2)), dma((5,)), dma((6,)), dma((10,)), dma((8,)), dma((2,)), dma((2,)),
    ]
    return pl.pallas_call(
        mlp_kernel,
        out_shape=out_shape,
        in_specs=[any_spec] * 8,
        out_specs=(any_spec,) * 7,
        scratch_shapes=scratch,
        compiler_params=pltpu.CompilerParams(collective_id=0, has_side_effects=True, vmem_limit_bytes=VMEM_LIMIT),
        cost_estimate=pl.CostEstimate(flops=70 * 10**9, bytes_accessed=64 * 2**20, transcendentals=0),
        name="feed_forward",
    )(y_one, y_two, dy_one, dy_two, w_up, w_down, w_qkv, w_out)


def attention_kernel(
    scale, uc_seq, att_full, part_own, part_near, up_near,
    d_up, d_down, d_att, o_pos, du_pos, wo_full, att_far,
    uc_all, qkv_buf, wo_buf, qkv, d_ctx, d_qkv, o_all, du_all, part_send, part_keep, part_core, own_t, far_t, own_f, far_f, o_relay, du_relay, near_out, near_buf,
    load_sem, w_sem, wo_sem, near_sem, core_send, core_recv, part_out, part_in, far_sem, o_send, o_recv, du_send, du_recv, o_relay_recv, du_relay_recv,
):
    ring = Ring()
    slab, hidden = uc_seq.shape[2], uc_seq.shape[3]
    seq_len = 8 * slab
    dim = att_full.shape[1] // 4
    tile = 512

    def relation_of(step):
        return (step + 1) % 4

    def w_loads(heads, buf):
        copies = []
        for index, head in enumerate(heads):
            copies.append(pltpu.make_async_copy(head.at[pl.ds(0, 3 * dim)], qkv_buf.at[buf, pl.ds(index * 3 * dim, 3 * dim)], w_sem.at[buf, index, 0]))
            copies.append(pltpu.make_async_copy(head.at[pl.ds(3 * dim, dim)], wo_buf.at[buf, pl.ds(index * dim, dim)], w_sem.at[buf, index, 1]))
        return copies

    far_from_t = ring.copy(att_full.at[SAME_F], att_far.at[0], far_sem.at[0], far_sem.at[1], SAME_T)
    far_from_core = ring.copy(att_far.at[0], att_far.at[1], far_sem.at[2], far_sem.at[3], PARTNER)

    near_load = pltpu.make_async_copy(part_near, near_out, near_sem.at[2])
    near = ring.copy(near_out, near_buf, near_sem.at[0], near_sem.at[1], SAME_F)

    def core_copy(relation, buf):
        return ring.copy(part_send.at[buf], part_core.at[relation], core_send.at[buf], core_recv.at[relation], PARTNER)

    core_last = [core_copy(3, 0), core_copy(0, 1)]
    rows = part_keep.shape[1]
    ff_loads = [
        pltpu.make_async_copy(part_own.at[pl.ds(0, rows)], part_send.at[0], load_sem.at[1, 0]),
        pltpu.make_async_copy(part_own.at[pl.ds(rows, rows)], part_send.at[1], load_sem.at[1, 1]),
        pltpu.make_async_copy(up_near, part_core.at[1], load_sem.at[2, 0]),
    ]
    ff_stores = [pltpu.make_async_copy(part_send.at[index], dst, load_sem.at[3, index]) for index, dst in enumerate((d_up, d_down))]

    rows_a, rows_b = pl.ds(0, 3 * dim), pl.ds(3 * dim, dim)

    def part(src, dst, index, slot):
        return ring.copy(src, dst, part_out.at[index], part_in.at[index], slot)

    t_own_a = part(part_keep.at[1, rows_a], own_t.at[rows_a], 0, SAME_T)
    t_far_a = part(part_keep.at[3, rows_a], far_t, 1, SAME_T)
    t_own_b = part(part_keep.at[1, rows_b], own_t.at[rows_b], 2, SAME_T)
    f_own_b = part(part_keep.at[2, rows_b], own_f.at[rows_b], 3, SAME_F)
    f_far_b = part(part_keep.at[3, rows_b], far_f, 4, SAME_F)
    f_own_a = part(part_keep.at[2, rows_a], own_f.at[rows_a], 5, SAME_F)

    def rows_of(slot):
        return pl.ds(slot * slab, slab)

    def to_positions(src, dst, relay, send_sem, recv_sem, relay_sem):
        near_t, near_f = ring.at(SAME_T), ring.at(SAME_F)
        out = [
            ring.copy(src.at[rows_of(SAME_O)], relay.at[0], send_sem.at[6], relay_sem.at[0], SAME_T),
            ring.copy(src.at[rows_of(OTHER_O)], relay.at[1], send_sem.at[7], relay_sem.at[1], SAME_F),
        ] + [ring.copy(src.at[rows_of(slot)], dst.at[ring.me], send_sem.at[slot], recv_sem.at[slot], slot) for slot in (5, 4, 3, 2, 1)]
        onward = [
            ring.copy(relay.at[0], dst.at[near_t], send_sem.at[8], recv_sem.at[SAME_O], SAME_F),
            ring.copy(relay.at[1], dst.at[near_f], send_sem.at[9], recv_sem.at[OTHER_O], OTHER_T),
        ]
        keep = pltpu.make_async_copy(src.at[rows_of(0)], dst.at[ring.me], send_sem.at[0])
        return out, onward, keep

    o_out, o_pass, o_keep = to_positions(o_all, o_pos, o_relay, o_send, o_recv, o_relay_recv)
    du_out, du_pass, du_keep = to_positions(du_all, du_pos, du_relay, du_send, du_recv, du_relay_recv)

    def start(copies):
        for copy in copies:
            copy.start()

    loads = [pltpu.make_async_copy(uc_seq.at[slot, which], uc_all.at[which, rows_of(slot)], load_sem.at[slot, which]) for slot in range(8) for which in (0, 1)]
    near_load.start()
    start(loads)
    start(w_loads([att_full.at[3], att_full.at[2]], 0))
    ring.barrier()
    far_from_t.start()
    near_load.wait()
    near.start()
    du_all[...] = jnp.zeros_like(du_all)
    for copy in loads:
        copy.wait()

    def chip_step(step, carry):
        buf = step % 2
        relation = relation_of(step)
        for copy in w_loads([att_far.at[0], att_far.at[0]], buf):
            copy.wait()

        @pl.when(step == 0)
        def _():
            start(w_loads([att_full.at[5], att_full.at[4]], 1))

        @pl.when(step == 1)
        def _():
            far_from_core.wait_recv()
            start(w_loads([att_far.at[1], att_far.at[0]], 0))

        @pl.when(step == 2)
        def _():
            start(w_loads([att_full.at[1], att_full.at[0]], 1))

        heads = [ring.at_traced(relation * 2 + other) for other in (1, 0)]
        wo_copies = [pltpu.make_async_copy(wo_buf.at[buf, pl.ds(index * dim, dim)], wo_full.at[head], wo_sem.at[index]) for index, head in enumerate(heads)]
        start(wo_copies)
        qkv[...] = dot_nt(uc_all[0], qkv_buf[buf]).astype(BF16)
        d_ctx[...] = dot_nt(uc_all[1], wo_buf[buf]).astype(BF16)
        for index, head in enumerate(heads):
            columns = pl.ds(pl.multiple_of(head * dim, dim), dim)
            own = pl.ds(index * 3 * dim, 3 * dim)
            query, key, value = (qkv[:, pl.ds((index * 3 + part) * dim, dim)] for part in range(3))
            d_out = d_ctx[:, pl.ds(index * dim, dim)]
            scores = dot_nt(query, key) * (scale * LOG2_E)
            grown = jnp.exp2(scores - jnp.max(scores, axis=-1, keepdims=True))
            prob = grown * (1.0 / jnp.sum(grown, axis=-1, keepdims=True))
            prob_b = prob.astype(BF16)
            o_all[:, columns] = dot_nn(prob_b, value).astype(BF16)
            d_prob = dot_nt(d_out, value)
            d_score = (prob * (d_prob - jnp.sum(d_prob * prob, axis=-1, keepdims=True)) * scale).astype(BF16)
            d_qkv[:, pl.ds(index * 3 * dim, dim)] = dot_nn(d_score, key).astype(BF16)
            d_qkv[:, pl.ds((index * 3 + 1) * dim, dim)] = dot_nn(query.T, d_score).T.astype(BF16)
            d_qkv[:, pl.ds((index * 3 + 2) * dim, dim)] = dot_nn(d_out.T, prob_b).T.astype(BF16)
            if index == 0:
                @pl.when(step >= 2)
                def _():
                    core_copy(relation, buf).wait_send()

            dst = part_send.at[buf] if index == 0 else part_keep.at[relation]
            dst[pl.ds(0, 3 * dim), :] = dot_tn(d_qkv[:, own], uc_all[0])
            dst[pl.ds(3 * dim, dim), :] = dot_tn(o_all[:, columns], uc_all[1])
            if index == 0:
                core_copy(relation, buf).start()
        core_copy(relation, buf).wait_recv()
        part_keep[relation] += part_core[relation]

        @pl.when(step == 0)
        def _():
            t_own_a.start()

        @pl.when(step == 1)
        def _():
            f_own_b.start()

        @pl.when(step == 2)
        def _():
            t_far_a.start()
            f_far_b.start()

        def du_tile(part, carry):
            rows = pl.ds(pl.multiple_of(part * tile, tile), tile)
            du_all[rows, :] += dot_nn(d_qkv[rows, :], qkv_buf[buf])
            return carry

        lax.fori_loop(0, seq_len // tile, du_tile, 0)

        @pl.when(step == 0)
        def _():
            far_from_t.wait_recv()
            far_from_core.start()

        for copy in wo_copies:
            copy.wait()
        return carry

    lax.fori_loop(0, 4, chip_step, 0)
    start(o_out)
    start(du_out)
    o_keep.start()
    du_keep.start()
    for copy in core_last:
        copy.wait_send()
    start(ff_loads)
    f_far_b.wait_recv()
    part_keep[1, rows_b] += far_f[...]
    t_own_b.start()
    for copy in o_out[:2]:
        copy.wait_recv()
    start(o_pass)
    t_far_a.wait_recv()
    part_keep[2, rows_a] += far_t[...]
    f_own_a.start()
    for copy in ff_loads:
        copy.wait()
    part_send[0] += part_core[1]
    near.wait_recv()
    part_send[1] += near_buf[...]
    for copy in ff_stores:
        copy.start()
    for copy in du_out[:2]:
        copy.wait_recv()
    start(du_pass)
    t_own_a.wait_recv()
    t_own_b.wait_recv()
    part_keep[0] += own_t[...]
    f_own_a.wait_recv()
    f_own_b.wait_recv()
    part_keep[0] += own_f[...]
    d_att_copy = pltpu.make_async_copy(part_keep.at[0], d_att, load_sem.at[0, 0])
    d_att_copy.start()

    for dst, recv_sem in ((o_pos, o_recv), (du_pos, du_recv)):
        for slot in range(1, 8):
            ring.copy(dst.at[0], dst.at[ring.at(slot)], near_sem.at[0], recv_sem.at[slot], PARTNER).wait_recv()
    for copy in o_out + du_out + o_pass + du_pass + [t_own_a, t_far_a, t_own_b, f_own_b, f_far_b, f_own_a, far_from_t, far_from_core, near]:
        copy.wait_send()
    for copy in ff_stores:
        copy.wait()
    o_keep.wait()
    du_keep.wait()
    d_att_copy.wait()


def attention_call(uc_seq, att_full, part_own, part_near, up_near):
    slab, hidden = uc_seq.shape[2:]
    rows = att_full.shape[1]
    dim = rows // 4
    seq_len = 8 * slab
    any_spec = pl.BlockSpec(memory_space=pl.ANY)
    dma, vmem = pltpu.SemaphoreType.DMA, pltpu.VMEM
    out_shape = (
        jax.ShapeDtypeStruct(up_near.shape, F32),
        jax.ShapeDtypeStruct(part_near.shape, F32),
        jax.ShapeDtypeStruct((rows, hidden), F32),
        jax.ShapeDtypeStruct((8, slab, hidden), BF16),
        jax.ShapeDtypeStruct((8, slab, hidden), F32),
        jax.ShapeDtypeStruct((8, dim, hidden), BF16),
        jax.ShapeDtypeStruct((2, rows, hidden), BF16),
    )
    scratch = [
        vmem((2, seq_len, hidden), BF16), vmem((2, 6 * dim, hidden), BF16), vmem((2, 2 * dim, hidden), BF16),
        vmem((seq_len, 6 * dim), BF16), vmem((seq_len, 2 * dim), BF16), vmem((seq_len, 6 * dim), BF16),
        vmem((seq_len, hidden), BF16), vmem((seq_len, hidden), F32),
        vmem((2, rows, hidden), F32), vmem((4, rows, hidden), F32), vmem((4, rows, hidden), F32),
        vmem((rows, hidden), F32), vmem((3 * dim, hidden), F32), vmem((rows, hidden), F32), vmem((dim, hidden), F32),
        vmem((2, slab, hidden), BF16), vmem((2, slab, hidden), F32), vmem(part_near.shape, F32), vmem(part_near.shape, F32),
        dma((8, 2)), dma((2, 2, 2)), dma((2,)), dma((3,)), dma((2,)), dma((4,)), dma((6,)), dma((6,)), dma((4,)), dma((10,)), dma((8,)), dma((10,)), dma((8,)), dma((2,)), dma((2,)),
    ]
    return pl.pallas_call(
        functools.partial(attention_kernel, dim ** -0.5),
        out_shape=out_shape,
        in_specs=[any_spec] * 5,
        out_specs=(any_spec,) * 7,
        scratch_shapes=scratch,
        compiler_params=pltpu.CompilerParams(collective_id=1, has_side_effects=True, vmem_limit_bytes=VMEM_LIMIT),
        cost_estimate=pl.CostEstimate(flops=40 * 10**9, bytes_accessed=64 * 2**20, transcendentals=0),
        name="attention",
    )(uc_seq, att_full, part_own, part_near, up_near)


def finish_kernel(
    y_one, o_pos, wo_full, x_two, dx_one, dy_two, du_pos, d_up, d_down, d_att,
    x_one_out, x_two_out, dx_one_out, dx_two_out, dw_up, dw_down, dw_qkv, dw_out,
    y_buf, o_buf, wo_buf, x_buf, dx_buf, dy_buf, du_buf, up_buf, down_buf, att_buf, up_out, qkv_out, load_sem, store_sem,
):
    tokens = y_buf.shape[0]
    dim = wo_buf.shape[0] // 8
    chunk = 256
    chunks = [pl.ds(index * chunk, chunk) for index in range(tokens // chunk)]

    def pieces(src, dst, sem, row):
        return [pltpu.make_async_copy(src.at[rows], dst.at[rows], sem.at[row, index]) for index, rows in enumerate(chunks)]

    def whole(src, dst, sem, row):
        return pltpu.make_async_copy(src, dst, sem.at[row, 0])

    x_in, dy_in, du_in = pieces(x_two, x_buf, load_sem, 0), pieces(dy_two, dy_buf, load_sem, 1), pieces(du_pos, du_buf, load_sem, 2)
    y_in, o_in = pieces(y_one, y_buf, load_sem, 3), pieces(o_pos, o_buf, load_sem, 4)
    wo_in, dx_in = whole(wo_full, wo_buf, load_sem, 5), whole(dx_one, dx_buf, load_sem, 6)
    up_in, down_in, att_in = whole(d_up, up_buf, load_sem, 7), whole(d_down, down_buf, load_sem, 8), whole(d_att, att_buf, load_sem, 9)
    for group in zip(x_in, dy_in, du_in):
        for copy in group:
            copy.start()
    for copy in (dx_in, wo_in):
        copy.start()
    for group in zip(y_in, o_in):
        for copy in group:
            copy.start()
    for copy in (up_in, att_in, down_in):
        copy.start()

    x_store, dx2_store, x1_store = pieces(x_buf, x_two_out, store_sem, 0), pieces(dy_buf, dx_two_out, store_sem, 1), pieces(y_buf, x_one_out, store_sem, 2)
    for index, rows in enumerate(chunks):
        x_in[index].wait()
        x_store[index].start()
        dy_in[index].wait()
        du_in[index].wait()
        dy_buf[rows, :] += rms_back(x_buf[rows, :], du_buf[rows, :])
        dx2_store[index].start()
    dx_in.wait()
    dx_store = whole(dx_buf, dx_one_out, store_sem, 3)
    dx_store.start()
    wo_in.wait()
    for index, rows in enumerate(chunks):
        y_in[index].wait()
        o_in[index].wait()
        y_buf[rows, :] -= dot_nn(o_buf[rows, :], wo_buf[...])
        x1_store[index].start()
    up_in.wait()
    ffn = up_buf.shape[0]
    for part in range(up_out.shape[0] // ffn):
        up_out[pl.ds(part * ffn, ffn), :] = up_buf[:, pl.ds(part * ffn, ffn)].T
    up_store = whole(up_out, dw_up, store_sem, 4)
    up_store.start()
    att_in.wait()
    for part in range(3):
        qkv_out[pl.ds(part, tokens, stride=3), 0, :] = att_buf[pl.ds(part * dim, dim), :].T
    qkv_store = whole(qkv_out, dw_qkv, store_sem, 5)
    qkv_store.start()
    out_store = whole(att_buf.at[pl.ds(3 * dim, dim)], dw_out, store_sem, 6)
    out_store.start()
    down_in.wait()
    down_store = whole(down_buf, dw_down, store_sem, 7)
    down_store.start()
    for copy in x_store + dx2_store + x1_store + [dx_store, up_store, qkv_store, out_store, down_store]:
        copy.wait()


def finish_call(y_one, o_pos, wo_full, x_two, dx_one, dy_two, du_pos, d_up, d_down, d_att):
    tokens, hidden = y_one.shape
    ffn = d_up.shape[0]
    dim = d_att.shape[0] // 4
    any_spec = pl.BlockSpec(memory_space=pl.ANY)
    dma, vmem = pltpu.SemaphoreType.DMA, pltpu.VMEM
    state = (tokens, hidden)
    out_shape = [jax.ShapeDtypeStruct(shape, F32) for shape in (state, state, state, state, (hidden, ffn), (ffn, hidden), (3 * hidden, 1, dim), (dim, hidden))]
    scratch = [
        vmem(state, F32), vmem(state, BF16), vmem((hidden, hidden), BF16), vmem(state, F32), vmem(state, F32), vmem(state, F32), vmem(state, F32),
        vmem((ffn, hidden), F32), vmem((ffn, hidden), F32), vmem(d_att.shape, F32), vmem((hidden, ffn), F32), vmem((3 * hidden, 1, dim), F32),
        dma((10, 4)), dma((8, 4)),
    ]
    return pl.pallas_call(
        finish_kernel,
        out_shape=out_shape,
        in_specs=[any_spec] * 10,
        out_specs=[any_spec] * 8,
        scratch_shapes=scratch,
        compiler_params=pltpu.CompilerParams(vmem_limit_bytes=VMEM_LIMIT),
        cost_estimate=pl.CostEstimate(flops=2 * 10**9, bytes_accessed=52 * 2**20, transcendentals=0),
        name="finish",
    )(y_one, o_pos, wo_full, x_two, dx_one, dy_two, du_pos, d_up, d_down, d_att)


def local_backward(y_one, y_two, dy_one, dy_two, w_qkv, w_out, w_up, w_down):
    hidden = y_one.shape[2]
    _, _, _, parts, dim = w_qkv.shape
    flat = [tensor.reshape(-1, hidden) for tensor in (y_one, y_two, dy_one, dy_two)]
    qkv_parts = jnp.swapaxes(w_qkv[0, :, 0], 0, 1)
    x_two, dx_one, uc_seq, att_full, part_own, part_near, up_near = mlp_call(*flat, w_up[0], w_down[0], qkv_parts, w_out[0, 0])
    d_up, d_down, d_att, o_pos, du_pos, wo_full, _ = attention_call(uc_seq, att_full, part_own, part_near, up_near)
    tokens = flat[0].shape
    *states, dw_up, dw_down, dw_qkv, dw_out = finish_call(
        flat[0], o_pos.reshape(tokens), wo_full.reshape(-1, hidden), x_two, dx_one, flat[3], du_pos.reshape(tokens), d_up, d_down, d_att
    )
    states = [tensor.reshape(y_one.shape) for tensor in states]
    return (*states, dw_qkv.reshape(1, hidden, 1, parts, dim), dw_out[None, None], dw_up[None], dw_down[None])


def solution(mesh):
    state_spec = P("dp", "tp", None)
    in_specs = (state_spec, state_spec, state_spec, state_spec, P(None, None, "tp", None, None), P(None, "tp", None, None), P(None, None, "tp"), P(None, "tp", None))
    out_specs = (state_spec, state_spec, state_spec, state_spec, P("dp", None, "tp", None, None), P("dp", "tp", None, None), P("dp", None, "tp"), P("dp", "tp", None))
    return jax.shard_map(local_backward, mesh=mesh, in_specs=in_specs, out_specs=out_specs, check_vma=False)
```

```python
import functools

import jax
import jax.numpy as jnp
from jax import lax
from jax.experimental import pallas as pl
from jax.experimental.pallas import tpu as pltpu
from jax.sharding import PartitionSpec as P

RMS_EPS = 1e-6
LOG2_E = 1.4426950408889634
MESH = pl.DeviceIdType.MESH
BF16, F32 = jnp.bfloat16, jnp.float32
VMEM_LIMIT = 64 * 1024 * 1024 - 65536


def inv_rms(tensor):
    return lax.rsqrt(jnp.mean(tensor * tensor, axis=-1, keepdims=True) + RMS_EPS)


def rms_norm(tensor):
    return tensor * inv_rms(tensor)


def rms_back(tensor, grad_in):
    scale = inv_rms(tensor)
    return scale * grad_in - tensor * (scale * scale * scale) * jnp.mean(grad_in * tensor, axis=-1, keepdims=True)


def gelu_and_slope(tensor):
    root = (2.0 / jnp.pi) ** 0.5
    squared = tensor * tensor
    tanh = jnp.tanh(root * (tensor + 0.044715 * (tensor * squared)))
    cdf = 0.5 * (1.0 + tanh)
    slope = cdf + (0.5 * root) * tensor * ((1.0 - tanh * tanh) * (1.0 + (3 * 0.044715) * squared))
    return tensor * cdf, slope


def dot_nn(left, right):
    return lax.dot_general(left, right, (((1,), (0,)), ((), ())), preferred_element_type=F32)


def dot_nt(left, right):
    return lax.dot_general(left, right, (((1,), (1,)), ((), ())), preferred_element_type=F32)


def dot_tn(left, right):
    return lax.dot_general(left, right, (((0,), (0,)), ((), ())), preferred_element_type=F32)


class Ring:
    def __init__(self):
        me = lax.axis_index("tp")
        chip, core = me // 2, me % 2
        self.me, self.chip, self.core = me, chip, core
        self.chips = (chip, chip + 1 - 2 * (chip % 2), 3 - chip, (chip + 2) % 4)

    def at(self, slot):
        core = self.core if slot % 2 == 0 else 1 - self.core
        return self.chips[slot // 2] * 2 + core

    def at_traced(self, slot):
        relation, other = slot // 2, slot % 2
        own, near_t, near_f, opposite = self.chips
        chip = jnp.where(relation == 0, own, jnp.where(relation == 1, near_t, jnp.where(relation == 2, near_f, opposite)))
        return chip * 2 + (self.core + other) % 2

    def barrier(self):
        barrier = pltpu.get_barrier_semaphore()
        for slot in (1, 2, 3, 4, 5):
            pl.semaphore_signal(barrier, inc=1, device_id={"tp": self.at(slot)}, device_id_type=MESH)
        pl.semaphore_wait(barrier, 5)

    def copy(self, src, dst, send_sem, recv_sem, slot):
        return pltpu.make_async_remote_copy(src_ref=src, dst_ref=dst, send_sem=send_sem, recv_sem=recv_sem, device_id={"tp": self.at(slot)}, device_id_type=MESH)


PARTNER, SAME_T, OTHER_T, SAME_F, OTHER_F, SAME_O, OTHER_O = 1, 2, 3, 4, 5, 6, 7


def mlp_kernel(
    y_one, y_two, dy_one, dy_two, w_up, w_down, w_qkv, w_out,
    x_two, dx_one, uc_seq, att_full, part_own, part_near, near_recv,
    u_all, c_all, up_all, down_all, acc, uc_own, relay, y_buf, x_buf, up_raw, qkv_raw, att_own,
    load_sem, y_sem, x_sem, w_send, w_recv, uc_send, uc_recv, att_send, att_recv, a2a_send, a2a_recv, relay_recv, near_sem,
):
    ring = Ring()
    half = 512
    slab = 128

    def weight(which, src_slot, dst_slot, to, index):
        buf = (up_all, down_all)[which]
        return ring.copy(buf.at[src_slot], buf.at[dst_slot], w_send.at[index], w_recv.at[dst_slot, which], to)

    def weight_pair(src_slot, dst_slot, to, index):
        return [weight(which, src_slot, dst_slot, to, index + which) for which in (0, 1)]

    w_own = weight_pair(0, 1, PARTNER, 0) + weight_pair(0, 2, SAME_T, 2) + weight_pair(0, 4, SAME_F, 4)
    w_near_t = weight_pair(2, 6, SAME_F, 6) + weight_pair(2, 3, PARTNER, 8)
    w_near_f = weight_pair(4, 5, PARTNER, 10)
    w_far = weight_pair(6, 7, PARTNER, 12)

    def uc_pair(src_slot, dst_slot, to, index):
        return [ring.copy(buf.at[src_slot], buf.at[dst_slot], uc_send.at[index + which], uc_recv.at[dst_slot, which], to) for which, buf in enumerate((u_all, c_all))]

    uc_out = uc_pair(0, 2, SAME_T, 0) + uc_pair(0, 1, PARTNER, 2)
    uc_pass = uc_pair(2, 3, PARTNER, 4)

    def att(src, dst_slot, to, index):
        return ring.copy(src, att_full.at[dst_slot], att_send.at[index], att_recv.at[dst_slot], to)

    att_out = [att(att_own, 4, SAME_F, 0), att(att_own, 2, SAME_T, 1), att(att_own, 1, PARTNER, 2)]
    att_keep = pltpu.make_async_copy(att_own, att_full.at[0], load_sem.at[6])
    att_near_f = [att(att_full.at[4], 5, PARTNER, 3)]
    att_near_t = [att(att_full.at[2], 3, PARTNER, 4)]

    a2a_out = {slot: ring.copy(uc_own.at[slot], uc_seq.at[slot], a2a_send.at[slot], a2a_recv.at[slot], slot) for slot in (1, 2, 3, 4, 5)}
    a2a_out[SAME_O] = ring.copy(uc_own.at[SAME_O], relay.at[0], a2a_send.at[SAME_O], relay_recv.at[0], SAME_T)
    a2a_out[OTHER_O] = ring.copy(uc_own.at[OTHER_O], relay.at[1], a2a_send.at[OTHER_O], relay_recv.at[1], SAME_F)
    a2a_pass = [
        ring.copy(relay.at[0], uc_seq.at[SAME_O], a2a_send.at[8], a2a_recv.at[SAME_O], SAME_F),
        ring.copy(relay.at[1], uc_seq.at[OTHER_O], a2a_send.at[9], a2a_recv.at[OTHER_O], OTHER_T),
    ]
    uc_keep = pltpu.make_async_copy(uc_own.at[0], uc_seq.at[0], load_sem.at[4])

    def start(copies):
        for copy in copies:
            copy.start()

    dim = w_out.shape[0]
    near_rows = near_recv.shape[0]
    near = ring.copy(acc.at[0, pl.ds(0, near_rows)], near_recv, near_sem.at[0], near_sem.at[1], SAME_F)

    loads = [
        pltpu.make_async_copy(w_down, down_all.at[0], load_sem.at[0]),
        pltpu.make_async_copy(w_up, up_raw, load_sem.at[1]),
        pltpu.make_async_copy(y_one, acc.at[0], load_sem.at[2]),
        pltpu.make_async_copy(dy_two, acc.at[1], load_sem.at[3]),
        pltpu.make_async_copy(w_qkv, qkv_raw, load_sem.at[5]),
        pltpu.make_async_copy(w_out, att_own.at[pl.ds(3 * dim, dim)], load_sem.at[7]),
    ]
    start(loads)
    ring.barrier()
    loads[0].wait()
    start(w_own[1::2])
    loads[1].wait()
    for part in range(up_raw.shape[1] // dim):
        up_all[0, pl.ds(part * dim, dim), :] = up_raw[:, pl.ds(part * dim, dim)].T
    start(w_own[0::2])
    loads[2].wait()
    loads[3].wait()

    def normalize(step, carry):
        rows = pl.ds(pl.multiple_of(step * slab, slab), slab)
        u_all[0, rows, :] = rms_norm(acc[0, rows, :]).astype(BF16)
        c_all[0, rows, :] = acc[1, rows, :].astype(BF16)
        acc[0, rows, :] = jnp.zeros((slab, acc.shape[2]), F32)
        acc[1, rows, :] = jnp.zeros((slab, acc.shape[2]), F32)
        return carry

    lax.fori_loop(0, acc.shape[1] // slab, normalize, 0)
    start(uc_out)
    loads[4].wait()
    for part in range(3):
        att_own[pl.ds(part * dim, dim), :] = qkv_raw[part].T
    loads[5].wait()
    att_keep.start()

    def y_loads(step, buf):
        seq = ring.at_traced(7 - step)
        rows = pl.ds(pl.multiple_of(seq * slab, slab), slab)
        return [pltpu.make_async_copy(src.at[rows], y_buf.at[buf, which], y_sem.at[buf, which]) for which, src in enumerate((y_one, y_two, dy_one))]

    def x_stores(step, buf):
        seq = ring.at_traced(7 - step)
        rows = pl.ds(pl.multiple_of(seq * slab, slab), slab)
        return [pltpu.make_async_copy(x_buf.at[buf, which], dst.at[rows], x_sem.at[buf, which]) for which, dst in enumerate((x_two, dx_one))]

    def feed_forward(step, carry):
        slot = jnp.where(step == 3, 4, jnp.where(step == 4, 3, step))

        @pl.when(step >= 1)
        def _():
            for which, buf in enumerate((up_all, down_all)):
                ring.copy(buf.at[slot], buf.at[slot], w_send.at[0], w_recv.at[slot, which], PARTNER).wait_recv()

        @pl.when(step == 2)
        def _():
            start(w_near_t)
            start(att_out)

        @pl.when(step == 3)
        def _():
            start(w_near_f)

        @pl.when(step == 6)
        def _():
            start(w_far)

        @pl.when(step == 7)
        def _():
            start(y_loads(0, 0))

        def rows_step(part, carry):
            rows = pl.ds(pl.multiple_of(part * half, half), half)
            hidden, slope = gelu_and_slope(dot_nt(u_all[0, rows, :], up_all[slot]))
            d_pre = (slope * dot_nt(c_all[0, rows, :], down_all[slot])).astype(BF16)
            acc[0, rows, :] += dot_nn(hidden.astype(BF16), down_all[slot])
            acc[1, rows, :] += dot_nn(d_pre, up_all[slot])
            return carry

        lax.fori_loop(0, acc.shape[1] // half, rows_step, 0)
        return carry

    lax.fori_loop(0, 8, feed_forward, 0)

    def finish(step, carry):
        slot = 7 - step
        buf = step % 2
        seq = ring.at_traced(slot)
        rows = pl.ds(pl.multiple_of(seq * slab, slab), slab)
        for copy in y_loads(step, buf):
            copy.wait()

        @pl.when(step < 7)
        def _():
            start(y_loads(step + 1, 1 - buf))

        @pl.when(step >= 2)
        def _():
            for copy in x_stores(step - 2, buf):
                copy.wait()

        y_first = y_buf[buf, 0]
        x_second = y_buf[buf, 1] - acc[0, rows, :]
        dy_first = y_buf[buf, 2] + rms_back(y_first, acc[1, rows, :])
        x_buf[buf, 0] = x_second
        x_buf[buf, 1] = dy_first
        uc_own[slot, 0] = rms_norm(x_second).astype(BF16)
        uc_own[slot, 1] = dy_first.astype(BF16)
        acc[0, rows, :] = jnp.zeros((slab, acc.shape[2]), F32)
        acc[1, rows, :] = jnp.zeros((slab, acc.shape[2]), F32)
        start(x_stores(step, buf))
        return carry

    lax.fori_loop(0, 8, finish, 0)
    for slot in (7, 6, 5, 4, 3, 2, 1):
        a2a_out[slot].start()
    uc_keep.start()
    for step in (6, 7):
        for copy in x_stores(step, step % 2):
            copy.wait()

    def gradients(step, carry):
        first = step // 8
        tokens = (step % 8) // 2
        slot = 4 - 4 * first

        @pl.when((step == 2) | (step == 4) | (step == 6))
        def _():
            for which, buf in enumerate((u_all, c_all)):
                ring.copy(buf.at[tokens], buf.at[tokens], uc_send.at[0], uc_recv.at[tokens, which], PARTNER).wait_recv()

        @pl.when(step == 4)
        def _():
            start(uc_pass)

        @pl.when(step == 8)
        def _():
            near.start()
            ring.copy(att_own, att_full.at[4], att_send.at[0], att_recv.at[4], PARTNER).wait_recv()
            start(att_near_f)
            ring.copy(att_own, att_full.at[2], att_send.at[0], att_recv.at[2], PARTNER).wait_recv()
            start(att_near_t)

        @pl.when(step == 9)
        def _():
            for index in (0, 1):
                ring.copy(relay.at[index], relay.at[index], a2a_send.at[0], relay_recv.at[index], PARTNER).wait_recv()
            start(a2a_pass)

        rows = pl.ds(pl.multiple_of((step % 2) * half, half), half)
        u_part, c_part = u_all[tokens, rows, :], c_all[tokens, rows, :]
        hidden, slope = gelu_and_slope(dot_nt(up_all[slot], u_part))
        d_pre = (slope * dot_nt(down_all[slot], c_part)).astype(BF16)
        acc[first, pl.ds(0, half), :] += dot_nn(d_pre, u_part)
        acc[first, pl.ds(half, half), :] += dot_nn(hidden.astype(BF16), c_part)
        return carry

    lax.fori_loop(0, 16, gradients, 0)
    out_near = pltpu.make_async_copy(acc.at[0, pl.ds(near_rows, acc.shape[1] - near_rows)], part_near, load_sem.at[0])
    out_own = pltpu.make_async_copy(acc.at[1], part_own, load_sem.at[1])
    out_near.start()
    out_own.start()

    for slot in (1, 3, 5):
        ring.copy(att_own, att_full.at[slot], att_send.at[0], att_recv.at[slot], PARTNER).wait_recv()
    for slot in range(1, 8):
        ring.copy(uc_own.at[slot], uc_seq.at[slot], a2a_send.at[0], a2a_recv.at[slot], PARTNER).wait_recv()
    for copy in w_own + w_near_t + w_near_f + w_far + uc_out + uc_pass + att_out + att_near_t + att_near_f + list(a2a_out.values()) + a2a_pass:
        copy.wait_send()
    near.wait()
    uc_keep.wait()
    att_keep.wait()
    out_near.wait()
    out_own.wait()


def mlp_call(y_one, y_two, dy_one, dy_two, w_up, w_down, w_qkv, w_out):
    tokens, hidden = y_one.shape
    ffn = w_down.shape[0]
    dim = w_out.shape[0]
    near_rows = ffn
    any_spec = pl.BlockSpec(memory_space=pl.ANY)
    dma, vmem = pltpu.SemaphoreType.DMA, pltpu.VMEM
    out_shape = (
        jax.ShapeDtypeStruct((tokens, hidden), F32),
        jax.ShapeDtypeStruct((tokens, hidden), F32),
        jax.ShapeDtypeStruct((8, 2, tokens // 8, hidden), BF16),
        jax.ShapeDtypeStruct((6, 4 * dim, hidden), BF16),
        jax.ShapeDtypeStruct((2 * ffn, hidden), F32),
        jax.ShapeDtypeStruct((2 * ffn - near_rows, hidden), F32),
        jax.ShapeDtypeStruct((near_rows, hidden), F32),
    )
    scratch = [
        vmem((4, tokens, hidden), BF16), vmem((4, tokens, hidden), BF16),
        vmem((8, ffn, hidden), BF16), vmem((8, ffn, hidden), BF16),
        vmem((2, tokens, hidden), F32),
        vmem((8, 2, tokens // 8, hidden), BF16), vmem((2, 2, tokens // 8, hidden), BF16),
        vmem((2, 3, tokens // 8, hidden), F32), vmem((2, 2, tokens // 8, hidden), F32),
        vmem((hidden, ffn), BF16), vmem((3, hidden, dim), BF16), vmem((4 * dim, hidden), BF16),
        dma((8,)), dma((2, 3)), dma((2, 2)), dma((14,)), dma((8, 2)), dma((6,)), dma((4, 2)), dma((5,)), dma((6,)), dma((10,)), dma((8,)), dma((2,)), dma((2,)),
    ]
    return pl.pallas_call(
        mlp_kernel,
        out_shape=out_shape,
        in_specs=[any_spec] * 8,
        out_specs=(any_spec,) * 7,
        scratch_shapes=scratch,
        compiler_params=pltpu.CompilerParams(collective_id=0, has_side_effects=True, vmem_limit_bytes=VMEM_LIMIT),
        cost_estimate=pl.CostEstimate(flops=70 * 10**9, bytes_accessed=64 * 2**20, transcendentals=0),
        name="feed_forward",
    )(y_one, y_two, dy_one, dy_two, w_up, w_down, w_qkv, w_out)


def attention_kernel(
    scale, uc_seq, att_full, part_own, part_near, up_near,
    d_up, d_down, d_att, o_pos, du_pos, wo_full, att_far, du_relay,
    uc_all, qkv_buf, wo_buf, qkv, d_ctx, d_qkv, o_all, du_all, part_send, part_keep, part_core, own_t, far_t, own_f, far_f, o_relay, near_out, near_buf,
    load_sem, w_sem, wo_sem, near_sem, core_send, core_recv, part_out, part_in, far_sem, o_send, o_recv, du_send, du_recv, o_relay_recv, du_relay_recv,
):
    ring = Ring()
    slab, hidden = uc_seq.shape[2], uc_seq.shape[3]
    seq_len = 8 * slab
    dim = att_full.shape[1] // 4
    tile = 512

    def relation_of(step):
        return (step + 1) % 4

    def w_loads(heads, buf):
        copies = []
        for index, head in enumerate(heads):
            copies.append(pltpu.make_async_copy(head.at[pl.ds(0, 3 * dim)], qkv_buf.at[buf, pl.ds(index * 3 * dim, 3 * dim)], w_sem.at[buf, index, 0]))
            copies.append(pltpu.make_async_copy(head.at[pl.ds(3 * dim, dim)], wo_buf.at[buf, pl.ds(index * dim, dim)], w_sem.at[buf, index, 1]))
        return copies

    far_from_t = ring.copy(att_full.at[SAME_F], att_far.at[0], far_sem.at[0], far_sem.at[1], SAME_T)
    far_from_core = ring.copy(att_far.at[0], att_far.at[1], far_sem.at[2], far_sem.at[3], PARTNER)

    near_load = pltpu.make_async_copy(part_near, near_out, near_sem.at[2])
    near = ring.copy(near_out, near_buf, near_sem.at[0], near_sem.at[1], SAME_F)

    def core_copy(relation, buf):
        return ring.copy(part_send.at[buf], part_core.at[relation], core_send.at[buf], core_recv.at[relation], PARTNER)

    core_last = [core_copy(3, 0), core_copy(0, 1)]
    rows = part_keep.shape[1]
    ff_loads = [
        pltpu.make_async_copy(part_own.at[pl.ds(0, rows)], part_send.at[0], load_sem.at[1, 0]),
        pltpu.make_async_copy(part_own.at[pl.ds(rows, rows)], part_send.at[1], load_sem.at[1, 1]),
        pltpu.make_async_copy(up_near, part_core.at[1], load_sem.at[2, 0]),
    ]
    ff_stores = [pltpu.make_async_copy(part_send.at[index], dst, load_sem.at[3, index]) for index, dst in enumerate((d_up, d_down))]

    rows_a, rows_b = pl.ds(0, 3 * dim), pl.ds(3 * dim, dim)

    def part(src, dst, index, slot):
        return ring.copy(src, dst, part_out.at[index], part_in.at[index], slot)

    t_own_a = part(part_keep.at[1, rows_a], own_t.at[rows_a], 0, SAME_T)
    t_far_a = part(part_keep.at[3, rows_a], far_t, 1, SAME_T)
    t_own_b = part(part_keep.at[1, rows_b], own_t.at[rows_b], 2, SAME_T)
    f_own_b = part(part_keep.at[2, rows_b], own_f.at[rows_b], 3, SAME_F)
    f_far_b = part(part_keep.at[3, rows_b], far_f, 4, SAME_F)
    f_own_a = part(part_keep.at[2, rows_a], own_f.at[rows_a], 5, SAME_F)

    def rows_of(slot):
        return pl.ds(slot * slab, slab)

    def to_positions(src, dst, relay, send_sem, recv_sem, relay_sem):
        near_t, near_f = ring.at(SAME_T), ring.at(SAME_F)
        out = [
            ring.copy(src.at[rows_of(SAME_O)], relay.at[0], send_sem.at[6], relay_sem.at[0], SAME_T),
            ring.copy(src.at[rows_of(OTHER_O)], relay.at[1], send_sem.at[7], relay_sem.at[1], SAME_F),
        ] + [ring.copy(src.at[rows_of(slot)], dst.at[ring.me], send_sem.at[slot], recv_sem.at[slot], slot) for slot in (5, 4, 3, 2, 1)]
        onward = [
            ring.copy(relay.at[0], dst.at[near_t], send_sem.at[8], recv_sem.at[SAME_O], SAME_F),
            ring.copy(relay.at[1], dst.at[near_f], send_sem.at[9], recv_sem.at[OTHER_O], OTHER_T),
        ]
        keep = pltpu.make_async_copy(src.at[rows_of(0)], dst.at[ring.me], send_sem.at[0])
        return out, onward, keep

    o_out, o_pass, o_keep = to_positions(o_all, o_pos, o_relay, o_send, o_recv, o_relay_recv)
    du_out, _, du_keep = to_positions(du_all, du_pos, du_relay, du_send, du_recv, du_relay_recv)

    def start(copies):
        for copy in copies:
            copy.start()

    loads = [pltpu.make_async_copy(uc_seq.at[slot, which], uc_all.at[which, rows_of(slot)], load_sem.at[slot, which]) for slot in range(8) for which in (0, 1)]
    near_load.start()
    start(loads)
    start(w_loads([att_full.at[3], att_full.at[2]], 0))
    ring.barrier()
    far_from_t.start()
    near_load.wait()
    near.start()
    du_all[...] = jnp.zeros_like(du_all)
    for copy in loads:
        copy.wait()

    def chip_step(step, carry):
        buf = step % 2
        relation = relation_of(step)
        for copy in w_loads([att_far.at[0], att_far.at[0]], buf):
            copy.wait()

        @pl.when(step == 0)
        def _():
            start(w_loads([att_full.at[5], att_full.at[4]], 1))

        @pl.when(step == 1)
        def _():
            far_from_core.wait_recv()
            start(w_loads([att_far.at[1], att_far.at[0]], 0))

        @pl.when(step == 2)
        def _():
            start(w_loads([att_full.at[1], att_full.at[0]], 1))

        heads = [ring.at_traced(relation * 2 + other) for other in (1, 0)]
        wo_copies = [pltpu.make_async_copy(wo_buf.at[buf, pl.ds(index * dim, dim)], wo_full.at[head], wo_sem.at[index]) for index, head in enumerate(heads)]
        start(wo_copies)
        qkv[...] = dot_nt(uc_all[0], qkv_buf[buf]).astype(BF16)
        d_ctx[...] = dot_nt(uc_all[1], wo_buf[buf]).astype(BF16)
        for index, head in enumerate(heads):
            columns = pl.ds(pl.multiple_of(head * dim, dim), dim)
            own = pl.ds(index * 3 * dim, 3 * dim)
            query, key, value = (qkv[:, pl.ds((index * 3 + part) * dim, dim)] for part in range(3))
            d_out = d_ctx[:, pl.ds(index * dim, dim)]
            scores = dot_nt(query, key) * (scale * LOG2_E)
            grown = jnp.exp2(scores - jnp.max(scores, axis=-1, keepdims=True))
            prob = grown * (1.0 / jnp.sum(grown, axis=-1, keepdims=True))
            prob_b = prob.astype(BF16)
            o_all[:, columns] = dot_nn(prob_b, value).astype(BF16)
            d_prob = dot_nt(d_out, value)
            d_score = (prob * (d_prob - jnp.sum(d_prob * prob, axis=-1, keepdims=True)) * scale).astype(BF16)
            d_qkv[:, pl.ds(index * 3 * dim, dim)] = dot_nn(d_score, key).astype(BF16)
            d_qkv[:, pl.ds((index * 3 + 1) * dim, dim)] = dot_nn(query.T, d_score).T.astype(BF16)
            d_qkv[:, pl.ds((index * 3 + 2) * dim, dim)] = dot_nn(d_out.T, prob_b).T.astype(BF16)
            if index == 0:
                @pl.when(step >= 2)
                def _():
                    core_copy(relation, buf).wait_send()

            dst = part_send.at[buf] if index == 0 else part_keep.at[relation]
            dst[pl.ds(0, 3 * dim), :] = dot_tn(d_qkv[:, own], uc_all[0])
            dst[pl.ds(3 * dim, dim), :] = dot_tn(o_all[:, columns], uc_all[1])
            if index == 0:
                core_copy(relation, buf).start()
        core_copy(relation, buf).wait_recv()
        part_keep[relation] += part_core[relation]

        @pl.when(step == 0)
        def _():
            t_own_a.start()

        @pl.when(step == 1)
        def _():
            f_own_b.start()

        @pl.when(step == 2)
        def _():
            t_far_a.start()
            f_far_b.start()

        def du_tile(part, carry):
            rows = pl.ds(pl.multiple_of(part * tile, tile), tile)
            du_all[rows, :] += dot_nn(d_qkv[rows, :], qkv_buf[buf])
            return carry

        lax.fori_loop(0, seq_len // tile, du_tile, 0)

        @pl.when(step == 0)
        def _():
            far_from_t.wait_recv()
            far_from_core.start()

        for copy in wo_copies:
            copy.wait()
        return carry

    lax.fori_loop(0, 4, chip_step, 0)
    start(o_out)
    start(du_out)
    o_keep.start()
    du_keep.start()
    for copy in core_last:
        copy.wait_send()
    start(ff_loads)
    f_far_b.wait_recv()
    part_keep[1, rows_b] += far_f[...]
    t_own_b.start()
    for copy in o_out[:2]:
        copy.wait_recv()
    start(o_pass)
    t_far_a.wait_recv()
    part_keep[2, rows_a] += far_t[...]
    f_own_a.start()
    for copy in ff_loads:
        copy.wait()
    part_send[0] += part_core[1]
    near.wait_recv()
    part_send[1] += near_buf[...]
    for copy in ff_stores:
        copy.start()
    t_own_a.wait_recv()
    t_own_b.wait_recv()
    part_keep[0] += own_t[...]
    f_own_a.wait_recv()
    f_own_b.wait_recv()
    part_keep[0] += own_f[...]
    d_att_copy = pltpu.make_async_copy(part_keep.at[0], d_att, load_sem.at[0, 0])
    d_att_copy.start()

    for copy in du_out[:2]:
        copy.wait_recv()
    for dst, recv_sem, slots in ((o_pos, o_recv, range(1, 8)), (du_pos, du_recv, range(1, 6))):
        for slot in slots:
            ring.copy(dst.at[0], dst.at[ring.at(slot)], near_sem.at[0], recv_sem.at[slot], PARTNER).wait_recv()
    for copy in o_out + du_out + o_pass + [t_own_a, t_far_a, t_own_b, f_own_b, f_far_b, f_own_a, far_from_t, far_from_core, near]:
        copy.wait_send()
    for copy in ff_stores:
        copy.wait()
    o_keep.wait()
    du_keep.wait()
    d_att_copy.wait()


def attention_call(uc_seq, att_full, part_own, part_near, up_near):
    slab, hidden = uc_seq.shape[2:]
    rows = att_full.shape[1]
    dim = rows // 4
    seq_len = 8 * slab
    any_spec = pl.BlockSpec(memory_space=pl.ANY)
    dma, vmem = pltpu.SemaphoreType.DMA, pltpu.VMEM
    out_shape = (
        jax.ShapeDtypeStruct(up_near.shape, F32),
        jax.ShapeDtypeStruct(part_near.shape, F32),
        jax.ShapeDtypeStruct((rows, hidden), F32),
        jax.ShapeDtypeStruct((8, slab, hidden), BF16),
        jax.ShapeDtypeStruct((8, slab, hidden), F32),
        jax.ShapeDtypeStruct((8, dim, hidden), BF16),
        jax.ShapeDtypeStruct((2, rows, hidden), BF16),
        jax.ShapeDtypeStruct((2, slab, hidden), F32),
    )
    scratch = [
        vmem((2, seq_len, hidden), BF16), vmem((2, 6 * dim, hidden), BF16), vmem((2, 2 * dim, hidden), BF16),
        vmem((seq_len, 6 * dim), BF16), vmem((seq_len, 2 * dim), BF16), vmem((seq_len, 6 * dim), BF16),
        vmem((seq_len, hidden), BF16), vmem((seq_len, hidden), F32),
        vmem((2, rows, hidden), F32), vmem((4, rows, hidden), F32), vmem((4, rows, hidden), F32),
        vmem((rows, hidden), F32), vmem((3 * dim, hidden), F32), vmem((rows, hidden), F32), vmem((dim, hidden), F32),
        vmem((2, slab, hidden), BF16), vmem(part_near.shape, F32), vmem(part_near.shape, F32),
        dma((8, 2)), dma((2, 2, 2)), dma((2,)), dma((3,)), dma((2,)), dma((4,)), dma((6,)), dma((6,)), dma((4,)), dma((10,)), dma((8,)), dma((10,)), dma((8,)), dma((2,)), dma((2,)),
    ]
    return pl.pallas_call(
        functools.partial(attention_kernel, dim ** -0.5),
        out_shape=out_shape,
        in_specs=[any_spec] * 5,
        out_specs=(any_spec,) * 8,
        scratch_shapes=scratch,
        compiler_params=pltpu.CompilerParams(collective_id=1, has_side_effects=True, vmem_limit_bytes=VMEM_LIMIT),
        cost_estimate=pl.CostEstimate(flops=40 * 10**9, bytes_accessed=64 * 2**20, transcendentals=0),
        name="attention",
    )(uc_seq, att_full, part_own, part_near, up_near)


def finish_kernel(
    y_one, o_pos, wo_full, x_two, dx_one, dy_two, du_pos, d_up, d_down, d_att,
    x_one_out, x_two_out, dx_one_out, dx_two_out, dw_up, dw_down, dw_qkv, dw_out,
    y_buf, o_buf, wo_buf, x_buf, dx_buf, dy_buf, du_buf, up_buf, down_buf, att_buf, up_out, qkv_out, load_sem, store_sem,
):
    tokens = y_buf.shape[0]
    dim = wo_buf.shape[0] // 8
    chunk = 256
    chunks = [pl.ds(index * chunk, chunk) for index in range(tokens // chunk)]

    def pieces(src, dst, sem, row):
        return [pltpu.make_async_copy(src.at[rows], dst.at[rows], sem.at[row, index]) for index, rows in enumerate(chunks)]

    def whole(src, dst, sem, row):
        return pltpu.make_async_copy(src, dst, sem.at[row, 0])

    ring = Ring()
    slab = tokens // 8
    slots = [pl.ds(pl.multiple_of(ring.at(slot) * slab, slab), slab) for slot in range(6)]

    def slabs(src, dst, sem, row):
        return [pltpu.make_async_copy(src.at[rows], dst.at[rows], sem.at[row, index]) for index, rows in enumerate(slots)]

    x_in, dy_in, du_in = pieces(x_two, x_buf, load_sem, 0), slabs(dy_two, dy_buf, load_sem, 1), slabs(du_pos, du_buf, load_sem, 2)
    y_in, o_in = pieces(y_one, y_buf, load_sem, 3), pieces(o_pos, o_buf, load_sem, 4)
    wo_in, dx_in = whole(wo_full, wo_buf, load_sem, 5), whole(dx_one, dx_buf, load_sem, 6)
    up_in, down_in, att_in = whole(d_up, up_buf, load_sem, 7), whole(d_down, down_buf, load_sem, 8), whole(d_att, att_buf, load_sem, 9)
    for group in (x_in, *zip(dy_in, du_in)):
        for copy in group:
            copy.start()
    for copy in (dx_in, wo_in):
        copy.start()
    for group in zip(y_in, o_in):
        for copy in group:
            copy.start()
    for copy in (up_in, att_in, down_in):
        copy.start()

    x_store, dx2_store, x1_store = pieces(x_buf, x_two_out, store_sem, 0), slabs(dy_buf, dx_two_out, store_sem, 1), pieces(y_buf, x_one_out, store_sem, 2)
    for index in range(len(chunks)):
        x_in[index].wait()
        x_store[index].start()
    for index, rows in enumerate(slots):
        dy_in[index].wait()
        du_in[index].wait()
        dy_buf[rows, :] += rms_back(x_buf[rows, :], du_buf[rows, :])
        dx2_store[index].start()
    dx_in.wait()
    dx_store = whole(dx_buf, dx_one_out, store_sem, 3)
    dx_store.start()
    wo_in.wait()
    for index, rows in enumerate(chunks):
        y_in[index].wait()
        o_in[index].wait()
        y_buf[rows, :] -= dot_nn(o_buf[rows, :], wo_buf[...])
        x1_store[index].start()
    up_in.wait()
    ffn = up_buf.shape[0]
    for part in range(up_out.shape[0] // ffn):
        up_out[pl.ds(part * ffn, ffn), :] = up_buf[:, pl.ds(part * ffn, ffn)].T
    up_store = whole(up_out, dw_up, store_sem, 4)
    up_store.start()
    att_in.wait()
    for part in range(3):
        qkv_out[pl.ds(part, tokens, stride=3), 0, :] = att_buf[pl.ds(part * dim, dim), :].T
    qkv_store = whole(qkv_out, dw_qkv, store_sem, 5)
    qkv_store.start()
    out_store = whole(att_buf.at[pl.ds(3 * dim, dim)], dw_out, store_sem, 6)
    out_store.start()
    down_in.wait()
    down_store = whole(down_buf, dw_down, store_sem, 7)
    down_store.start()
    for copy in x_store + dx2_store + x1_store + [dx_store, up_store, qkv_store, out_store, down_store]:
        copy.wait()


def finish_call(y_one, o_pos, wo_full, x_two, dx_one, dy_two, du_pos, d_up, d_down, d_att):
    tokens, hidden = y_one.shape
    ffn = d_up.shape[0]
    dim = d_att.shape[0] // 4
    any_spec = pl.BlockSpec(memory_space=pl.ANY)
    dma, vmem = pltpu.SemaphoreType.DMA, pltpu.VMEM
    state = (tokens, hidden)
    out_shape = [jax.ShapeDtypeStruct(shape, F32) for shape in (state, state, state, state, (hidden, ffn), (ffn, hidden), (3 * hidden, 1, dim), (dim, hidden))]
    scratch = [
        vmem(state, F32), vmem(state, BF16), vmem((hidden, hidden), BF16), vmem(state, F32), vmem(state, F32), vmem(state, F32), vmem(state, F32),
        vmem((ffn, hidden), F32), vmem((ffn, hidden), F32), vmem(d_att.shape, F32), vmem((hidden, ffn), F32), vmem((3 * hidden, 1, dim), F32),
        dma((10, 6)), dma((8, 6)),
    ]
    return pl.pallas_call(
        finish_kernel,
        out_shape=out_shape,
        in_specs=[any_spec] * 10,
        out_specs=[any_spec] * 8,
        scratch_shapes=scratch,
        compiler_params=pltpu.CompilerParams(vmem_limit_bytes=VMEM_LIMIT),
        cost_estimate=pl.CostEstimate(flops=2 * 10**9, bytes_accessed=52 * 2**20, transcendentals=0),
        name="finish",
    )(y_one, o_pos, wo_full, x_two, dx_one, dy_two, du_pos, d_up, d_down, d_att)


def last_kernel(x_two, dy_two, du_far, du_far_other, dx_two_in, dx_two_out, x_buf, dy_buf, du_buf, load_sem, store_sem):
    ring = Ring()
    slab = du_far.shape[0]
    loads, stores = [], []
    for index, (slot, du) in enumerate(((SAME_O, du_far), (OTHER_O, du_far_other))):
        rows = pl.ds(pl.multiple_of(ring.at(slot) * slab, slab), slab)
        sources = ((x_two.at[rows], x_buf), (dy_two.at[rows], dy_buf), (du, du_buf))
        loads.append([pltpu.make_async_copy(src, dst.at[index], load_sem.at[index, which]) for which, (src, dst) in enumerate(sources)])
        stores.append(pltpu.make_async_copy(dy_buf.at[index], dx_two_out.at[rows], store_sem.at[index]))
    for copies in loads:
        for copy in copies:
            copy.start()
    for index, copies in enumerate(loads):
        for copy in copies:
            copy.wait()
        dy_buf[index] += rms_back(x_buf[index], du_buf[index])
        stores[index].start()
    for copy in stores:
        copy.wait()


def last_call(x_two, dy_two, du_far, du_far_other, dx_two):
    slab, hidden = du_far.shape
    any_spec = pl.BlockSpec(memory_space=pl.ANY)
    buf = pltpu.VMEM((2, slab, hidden), F32)
    return pl.pallas_call(
        last_kernel,
        out_shape=jax.ShapeDtypeStruct(dx_two.shape, F32),
        in_specs=[any_spec] * 5,
        out_specs=any_spec,
        input_output_aliases={4: 0},
        scratch_shapes=[buf, buf, buf, pltpu.SemaphoreType.DMA((2, 3)), pltpu.SemaphoreType.DMA((2,))],
        cost_estimate=pl.CostEstimate(flops=10**6, bytes_accessed=4 * 2**20, transcendentals=0),
        name="last",
    )(x_two, dy_two, du_far, du_far_other, dx_two)


def local_backward(y_one, y_two, dy_one, dy_two, w_qkv, w_out, w_up, w_down):
    hidden = y_one.shape[2]
    _, _, _, parts, dim = w_qkv.shape
    flat = [tensor.reshape(-1, hidden) for tensor in (y_one, y_two, dy_one, dy_two)]
    qkv_parts = jnp.swapaxes(w_qkv[0, :, 0], 0, 1)
    x_two, dx_one, uc_seq, att_full, part_own, part_near, up_near = mlp_call(*flat, w_up[0], w_down[0], qkv_parts, w_out[0, 0])
    d_up, d_down, d_att, o_pos, du_pos, wo_full, _, du_relay = attention_call(uc_seq, att_full, part_own, part_near, up_near)
    devices = range(lax.axis_size("tp"))
    to_f = [(device, (3 - device // 2) * 2 + device % 2) for device in devices]
    to_other_t = [(device, 4 * (device // 4) + 3 - device % 4) for device in devices]
    du_far, du_far_other = lax.ppermute(du_relay[0], "tp", to_f), lax.ppermute(du_relay[1], "tp", to_other_t)
    tokens = flat[0].shape
    *states, dw_up, dw_down, dw_qkv, dw_out = finish_call(
        flat[0], o_pos.reshape(tokens), wo_full.reshape(-1, hidden), x_two, dx_one, flat[3], du_pos.reshape(tokens), d_up, d_down, d_att
    )
    states[3] = last_call(x_two, flat[3], du_far, du_far_other, states[3])
    states = [tensor.reshape(y_one.shape) for tensor in states]
    return (*states, dw_qkv.reshape(1, hidden, 1, parts, dim), dw_out[None, None], dw_up[None], dw_down[None])


def solution(mesh):
    state_spec = P("dp", "tp", None)
    in_specs = (state_spec, state_spec, state_spec, state_spec, P(None, None, "tp", None, None), P(None, "tp", None, None), P(None, None, "tp"), P(None, "tp", None))
    out_specs = (state_spec, state_spec, state_spec, state_spec, P("dp", None, "tp", None, None), P("dp", "tp", None, None), P("dp", None, "tp"), P("dp", "tp", None))
    return jax.shard_map(local_backward, mesh=mesh, in_specs=in_specs, out_specs=out_specs, check_vma=False)
```

```python
import functools

import jax
import jax.numpy as jnp
from jax import lax
from jax.experimental import pallas as pl
from jax.experimental.pallas import tpu as pltpu
from jax.sharding import PartitionSpec as P

RMS_EPS = 1e-6
LOG2_E = 1.4426950408889634
MESH = pl.DeviceIdType.MESH
BF16, F32 = jnp.bfloat16, jnp.float32
VMEM_LIMIT = 64 * 1024 * 1024 - 65536


def inv_rms(tensor):
    return lax.rsqrt(jnp.mean(tensor * tensor, axis=-1, keepdims=True) + RMS_EPS)


def rms_norm(tensor):
    return tensor * inv_rms(tensor)


def rms_back(tensor, grad_in):
    scale = inv_rms(tensor)
    return scale * grad_in - tensor * (scale * scale * scale) * jnp.mean(grad_in * tensor, axis=-1, keepdims=True)


def gelu_and_slope(tensor):
    root = (2.0 / jnp.pi) ** 0.5
    squared = tensor * tensor
    tanh = jnp.tanh(root * (tensor + 0.044715 * (tensor * squared)))
    cdf = 0.5 * (1.0 + tanh)
    slope = cdf + (0.5 * root) * tensor * ((1.0 - tanh * tanh) * (1.0 + (3 * 0.044715) * squared))
    return tensor * cdf, slope


def dot_nn(left, right):
    return lax.dot_general(left, right, (((1,), (0,)), ((), ())), preferred_element_type=F32)


def dot_nt(left, right):
    return lax.dot_general(left, right, (((1,), (1,)), ((), ())), preferred_element_type=F32)


def dot_tn(left, right):
    return lax.dot_general(left, right, (((0,), (0,)), ((), ())), preferred_element_type=F32)


class Ring:
    def __init__(self):
        me = lax.axis_index("tp")
        chip, core = me // 2, me % 2
        self.me, self.chip, self.core = me, chip, core
        self.chips = (chip, chip + 1 - 2 * (chip % 2), 3 - chip, (chip + 2) % 4)

    def at(self, slot):
        core = self.core if slot % 2 == 0 else 1 - self.core
        return self.chips[slot // 2] * 2 + core

    def at_traced(self, slot):
        relation, other = slot // 2, slot % 2
        own, near_t, near_f, opposite = self.chips
        chip = jnp.where(relation == 0, own, jnp.where(relation == 1, near_t, jnp.where(relation == 2, near_f, opposite)))
        return chip * 2 + (self.core + other) % 2

    def barrier(self):
        barrier = pltpu.get_barrier_semaphore()
        for slot in (1, 2, 3, 4, 5):
            pl.semaphore_signal(barrier, inc=1, device_id={"tp": self.at(slot)}, device_id_type=MESH)
        pl.semaphore_wait(barrier, 5)

    def copy(self, src, dst, send_sem, recv_sem, slot):
        return pltpu.make_async_remote_copy(src_ref=src, dst_ref=dst, send_sem=send_sem, recv_sem=recv_sem, device_id={"tp": self.at(slot)}, device_id_type=MESH)


PARTNER, SAME_T, OTHER_T, SAME_F, OTHER_F, SAME_O, OTHER_O = 1, 2, 3, 4, 5, 6, 7


def mlp_kernel(
    y_one, y_two, dy_one, dy_two, w_up, w_down, w_qkv, w_out,
    x_two, dx_one, uc_seq, att_full, part_own, part_near, near_recv,
    u_all, c_all, up_all, down_all, acc, uc_own, relay, y_buf, x_buf, up_raw, qkv_raw, att_own,
    load_sem, y_sem, x_sem, w_send, w_recv, uc_send, uc_recv, att_send, att_recv, a2a_send, a2a_recv, relay_recv, near_sem,
):
    ring = Ring()
    half = 512
    slab = 128

    def weight(which, src_slot, dst_slot, to, index):
        buf = (up_all, down_all)[which]
        return ring.copy(buf.at[src_slot], buf.at[dst_slot], w_send.at[index], w_recv.at[dst_slot, which], to)

    def weight_pair(src_slot, dst_slot, to, index):
        return [weight(which, src_slot, dst_slot, to, index + which) for which in (0, 1)]

    w_own = weight_pair(0, 1, PARTNER, 0) + weight_pair(0, 2, SAME_T, 2) + weight_pair(0, 4, SAME_F, 4)
    w_near_t = weight_pair(2, 6, SAME_F, 6) + weight_pair(2, 3, PARTNER, 8)
    w_near_f = weight_pair(4, 5, PARTNER, 10)
    w_far = weight_pair(6, 7, PARTNER, 12)

    def uc_pair(src_slot, dst_slot, to, index):
        return [ring.copy(buf.at[src_slot], buf.at[dst_slot], uc_send.at[index + which], uc_recv.at[dst_slot, which], to) for which, buf in enumerate((u_all, c_all))]

    uc_out = uc_pair(0, 2, SAME_T, 0) + uc_pair(0, 1, PARTNER, 2)
    uc_pass = uc_pair(2, 3, PARTNER, 4)

    def att(src, dst_slot, to, index):
        return ring.copy(src, att_full.at[dst_slot], att_send.at[index], att_recv.at[dst_slot], to)

    att_out = [att(att_own, 4, SAME_F, 0), att(att_own, 2, SAME_T, 1), att(att_own, 1, PARTNER, 2)]
    att_keep = pltpu.make_async_copy(att_own, att_full.at[0], load_sem.at[6])
    att_near_f = [att(att_full.at[4], 5, PARTNER, 3)]
    att_near_t = [att(att_full.at[2], 3, PARTNER, 4)]

    a2a_out = {slot: ring.copy(uc_own.at[slot], uc_seq.at[slot], a2a_send.at[slot], a2a_recv.at[slot], slot) for slot in (1, 2, 3, 4, 5)}
    a2a_out[SAME_O] = ring.copy(uc_own.at[SAME_O], relay.at[0], a2a_send.at[SAME_O], relay_recv.at[0], SAME_T)
    a2a_out[OTHER_O] = ring.copy(uc_own.at[OTHER_O], relay.at[1], a2a_send.at[OTHER_O], relay_recv.at[1], SAME_F)
    a2a_pass = [
        ring.copy(relay.at[0], uc_seq.at[SAME_O], a2a_send.at[8], a2a_recv.at[SAME_O], SAME_F),
        ring.copy(relay.at[1], uc_seq.at[OTHER_O], a2a_send.at[9], a2a_recv.at[OTHER_O], OTHER_T),
    ]
    uc_keep = pltpu.make_async_copy(uc_own.at[0], uc_seq.at[0], load_sem.at[4])

    def start(copies):
        for copy in copies:
            copy.start()

    dim = w_out.shape[0]
    near_rows = near_recv.shape[0]
    near = ring.copy(acc.at[0, pl.ds(0, near_rows)], near_recv, near_sem.at[0], near_sem.at[1], SAME_F)

    loads = [
        pltpu.make_async_copy(w_down, down_all.at[0], load_sem.at[0]),
        pltpu.make_async_copy(w_up, up_raw, load_sem.at[1]),
        pltpu.make_async_copy(y_one, acc.at[0], load_sem.at[2]),
        pltpu.make_async_copy(dy_two, acc.at[1], load_sem.at[3]),
        pltpu.make_async_copy(w_qkv, qkv_raw, load_sem.at[5]),
        pltpu.make_async_copy(w_out, att_own.at[pl.ds(3 * dim, dim)], load_sem.at[7]),
    ]
    start(loads)
    ring.barrier()
    loads[0].wait()
    start(w_own[1::2])
    loads[1].wait()
    for part in range(up_raw.shape[1] // dim):
        up_all[0, pl.ds(part * dim, dim), :] = up_raw[:, pl.ds(part * dim, dim)].T
    start(w_own[0::2])
    loads[2].wait()
    loads[3].wait()

    def normalize(step, carry):
        rows = pl.ds(pl.multiple_of(step * slab, slab), slab)
        u_all[0, rows, :] = rms_norm(acc[0, rows, :]).astype(BF16)
        c_all[0, rows, :] = acc[1, rows, :].astype(BF16)
        acc[0, rows, :] = jnp.zeros((slab, acc.shape[2]), F32)
        acc[1, rows, :] = jnp.zeros((slab, acc.shape[2]), F32)
        return carry

    lax.fori_loop(0, acc.shape[1] // slab, normalize, 0)
    start(uc_out)
    loads[4].wait()
    for part in range(3):
        att_own[pl.ds(part * dim, dim), :] = qkv_raw[part].T
    loads[5].wait()
    att_keep.start()

    def y_loads(step, buf):
        seq = ring.at_traced(7 - step)
        rows = pl.ds(pl.multiple_of(seq * slab, slab), slab)
        return [pltpu.make_async_copy(src.at[rows], y_buf.at[buf, which], y_sem.at[buf, which]) for which, src in enumerate((y_one, y_two, dy_one))]

    def x_stores(step, buf):
        seq = ring.at_traced(7 - step)
        rows = pl.ds(pl.multiple_of(seq * slab, slab), slab)
        return [pltpu.make_async_copy(x_buf.at[buf, which], dst.at[rows], x_sem.at[buf, which]) for which, dst in enumerate((x_two, dx_one))]

    def feed_forward(step, carry):
        slot = jnp.where(step == 3, 4, jnp.where(step == 4, 3, step))

        @pl.when(step >= 1)
        def _():
            for which, buf in enumerate((up_all, down_all)):
                ring.copy(buf.at[slot], buf.at[slot], w_send.at[0], w_recv.at[slot, which], PARTNER).wait_recv()

        @pl.when(step == 2)
        def _():
            start(w_near_t)
            start(att_out)

        @pl.when(step == 3)
        def _():
            start(w_near_f)

        @pl.when(step == 6)
        def _():
            start(w_far)

        @pl.when(step == 7)
        def _():
            start(y_loads(0, 0))

        def rows_step(part, carry):
            rows = pl.ds(pl.multiple_of(part * half, half), half)
            hidden, slope = gelu_and_slope(dot_nt(u_all[0, rows, :], up_all[slot]))
            d_pre = (slope * dot_nt(c_all[0, rows, :], down_all[slot])).astype(BF16)
            acc[0, rows, :] += dot_nn(hidden.astype(BF16), down_all[slot])
            acc[1, rows, :] += dot_nn(d_pre, up_all[slot])
            return carry

        lax.fori_loop(0, acc.shape[1] // half, rows_step, 0)
        return carry

    lax.fori_loop(0, 8, feed_forward, 0)

    def finish(step, carry):
        slot = 7 - step
        buf = step % 2
        seq = ring.at_traced(slot)
        rows = pl.ds(pl.multiple_of(seq * slab, slab), slab)
        for copy in y_loads(step, buf):
            copy.wait()

        @pl.when(step < 7)
        def _():
            start(y_loads(step + 1, 1 - buf))

        @pl.when(step >= 2)
        def _():
            for copy in x_stores(step - 2, buf):
                copy.wait()

        y_first = y_buf[buf, 0]
        x_second = y_buf[buf, 1] - acc[0, rows, :]
        dy_first = y_buf[buf, 2] + rms_back(y_first, acc[1, rows, :])
        x_buf[buf, 0] = x_second
        x_buf[buf, 1] = dy_first
        uc_own[slot, 0] = rms_norm(x_second).astype(BF16)
        uc_own[slot, 1] = dy_first.astype(BF16)
        acc[0, rows, :] = jnp.zeros((slab, acc.shape[2]), F32)
        acc[1, rows, :] = jnp.zeros((slab, acc.shape[2]), F32)
        start(x_stores(step, buf))
        return carry

    lax.fori_loop(0, 8, finish, 0)
    for slot in (7, 6, 5, 4, 3, 2, 1):
        a2a_out[slot].start()
    uc_keep.start()
    for step in (6, 7):
        for copy in x_stores(step, step % 2):
            copy.wait()

    def gradients(step, carry):
        first = step // 8
        tokens = (step % 8) // 2
        slot = 4 - 4 * first

        @pl.when((step == 2) | (step == 4) | (step == 6))
        def _():
            for which, buf in enumerate((u_all, c_all)):
                ring.copy(buf.at[tokens], buf.at[tokens], uc_send.at[0], uc_recv.at[tokens, which], PARTNER).wait_recv()

        @pl.when(step == 4)
        def _():
            start(uc_pass)

        @pl.when(step == 8)
        def _():
            near.start()
            ring.copy(att_own, att_full.at[4], att_send.at[0], att_recv.at[4], PARTNER).wait_recv()
            start(att_near_f)
            ring.copy(att_own, att_full.at[2], att_send.at[0], att_recv.at[2], PARTNER).wait_recv()
            start(att_near_t)

        @pl.when(step == 9)
        def _():
            for index in (0, 1):
                ring.copy(relay.at[index], relay.at[index], a2a_send.at[0], relay_recv.at[index], PARTNER).wait_recv()
            start(a2a_pass)

        rows = pl.ds(pl.multiple_of((step % 2) * half, half), half)
        u_part, c_part = u_all[tokens, rows, :], c_all[tokens, rows, :]
        hidden, slope = gelu_and_slope(dot_nt(up_all[slot], u_part))
        d_pre = (slope * dot_nt(down_all[slot], c_part)).astype(BF16)
        acc[first, pl.ds(0, half), :] += dot_nn(d_pre, u_part)
        acc[first, pl.ds(half, half), :] += dot_nn(hidden.astype(BF16), c_part)
        return carry

    lax.fori_loop(0, 16, gradients, 0)
    out_near = pltpu.make_async_copy(acc.at[0, pl.ds(near_rows, acc.shape[1] - near_rows)], part_near, load_sem.at[0])
    out_own = pltpu.make_async_copy(acc.at[1], part_own, load_sem.at[1])
    out_near.start()
    out_own.start()

    for slot in (1, 3, 5):
        ring.copy(att_own, att_full.at[slot], att_send.at[0], att_recv.at[slot], PARTNER).wait_recv()
    for slot in range(1, 8):
        ring.copy(uc_own.at[slot], uc_seq.at[slot], a2a_send.at[0], a2a_recv.at[slot], PARTNER).wait_recv()
    for copy in w_own + w_near_t + w_near_f + w_far + uc_out + uc_pass + att_out + att_near_t + att_near_f + list(a2a_out.values()) + a2a_pass:
        copy.wait_send()
    near.wait()
    uc_keep.wait()
    att_keep.wait()
    out_near.wait()
    out_own.wait()


def mlp_call(y_one, y_two, dy_one, dy_two, w_up, w_down, w_qkv, w_out):
    tokens, hidden = y_one.shape
    ffn = w_down.shape[0]
    dim = w_out.shape[0]
    near_rows = ffn
    any_spec = pl.BlockSpec(memory_space=pl.ANY)
    dma, vmem = pltpu.SemaphoreType.DMA, pltpu.VMEM
    out_shape = (
        jax.ShapeDtypeStruct((tokens, hidden), F32),
        jax.ShapeDtypeStruct((tokens, hidden), F32),
        jax.ShapeDtypeStruct((8, 2, tokens // 8, hidden), BF16),
        jax.ShapeDtypeStruct((6, 4 * dim, hidden), BF16),
        jax.ShapeDtypeStruct((2 * ffn, hidden), F32),
        jax.ShapeDtypeStruct((2 * ffn - near_rows, hidden), F32),
        jax.ShapeDtypeStruct((near_rows, hidden), F32),
    )
    scratch = [
        vmem((4, tokens, hidden), BF16), vmem((4, tokens, hidden), BF16),
        vmem((8, ffn, hidden), BF16), vmem((8, ffn, hidden), BF16),
        vmem((2, tokens, hidden), F32),
        vmem((8, 2, tokens // 8, hidden), BF16), vmem((2, 2, tokens // 8, hidden), BF16),
        vmem((2, 3, tokens // 8, hidden), F32), vmem((2, 2, tokens // 8, hidden), F32),
        vmem((hidden, ffn), BF16), vmem((3, hidden, dim), BF16), vmem((4 * dim, hidden), BF16),
        dma((8,)), dma((2, 3)), dma((2, 2)), dma((14,)), dma((8, 2)), dma((6,)), dma((4, 2)), dma((5,)), dma((6,)), dma((10,)), dma((8,)), dma((2,)), dma((2,)),
    ]
    return pl.pallas_call(
        mlp_kernel,
        out_shape=out_shape,
        in_specs=[any_spec] * 8,
        out_specs=(any_spec,) * 7,
        scratch_shapes=scratch,
        compiler_params=pltpu.CompilerParams(collective_id=0, has_side_effects=True, vmem_limit_bytes=VMEM_LIMIT),
        cost_estimate=pl.CostEstimate(flops=70 * 10**9, bytes_accessed=64 * 2**20, transcendentals=0),
        name="feed_forward",
    )(y_one, y_two, dy_one, dy_two, w_up, w_down, w_qkv, w_out)


def attention_kernel(
    scale, uc_seq, att_full, part_own, part_near, up_near,
    d_up, d_down, d_att, o_pos, du_pos, wo_full, att_far, to_f, to_other_t,
    uc_all, qkv_buf, wo_buf, qkv, d_ctx, d_qkv, o_all, du_all, part_send, part_keep, part_core, own_t, far_t, own_f, far_f, o_relay, near_out, near_buf,
    load_sem, w_sem, wo_sem, near_sem, core_send, core_recv, part_out, part_in, far_sem, o_send, o_recv, du_send, du_recv, o_relay_recv, du_relay_recv,
):
    ring = Ring()
    slab, hidden = uc_seq.shape[2], uc_seq.shape[3]
    seq_len = 8 * slab
    dim = att_full.shape[1] // 4
    tile = 512

    def relation_of(step):
        return (step + 1) % 4

    def w_loads(heads, buf):
        copies = []
        for index, head in enumerate(heads):
            copies.append(pltpu.make_async_copy(head.at[pl.ds(0, 3 * dim)], qkv_buf.at[buf, pl.ds(index * 3 * dim, 3 * dim)], w_sem.at[buf, index, 0]))
            copies.append(pltpu.make_async_copy(head.at[pl.ds(3 * dim, dim)], wo_buf.at[buf, pl.ds(index * dim, dim)], w_sem.at[buf, index, 1]))
        return copies

    far_from_t = ring.copy(att_full.at[SAME_F], att_far.at[0], far_sem.at[0], far_sem.at[1], SAME_T)
    far_from_core = ring.copy(att_far.at[0], att_far.at[1], far_sem.at[2], far_sem.at[3], PARTNER)

    near_load = pltpu.make_async_copy(part_near, near_out, near_sem.at[2])
    near = ring.copy(near_out, near_buf, near_sem.at[0], near_sem.at[1], SAME_F)

    def core_copy(relation, buf):
        return ring.copy(part_send.at[buf], part_core.at[relation], core_send.at[buf], core_recv.at[relation], PARTNER)

    core_last = [core_copy(3, 0), core_copy(0, 1)]
    rows = part_keep.shape[1]
    ff_loads = [
        pltpu.make_async_copy(part_own.at[pl.ds(0, rows)], part_send.at[0], load_sem.at[1, 0]),
        pltpu.make_async_copy(part_own.at[pl.ds(rows, rows)], part_send.at[1], load_sem.at[1, 1]),
        pltpu.make_async_copy(up_near, part_core.at[1], load_sem.at[2, 0]),
    ]
    ff_stores = [pltpu.make_async_copy(part_send.at[index], dst, load_sem.at[3, index]) for index, dst in enumerate((d_up, d_down))]

    rows_a, rows_b = pl.ds(0, 3 * dim), pl.ds(3 * dim, dim)

    def part(src, dst, index, slot):
        return ring.copy(src, dst, part_out.at[index], part_in.at[index], slot)

    t_own_a = part(part_keep.at[1, rows_a], own_t.at[rows_a], 0, SAME_T)
    t_far_a = part(part_keep.at[3, rows_a], far_t, 1, SAME_T)
    t_own_b = part(part_keep.at[1, rows_b], own_t.at[rows_b], 2, SAME_T)
    f_own_b = part(part_keep.at[2, rows_b], own_f.at[rows_b], 3, SAME_F)
    f_far_b = part(part_keep.at[3, rows_b], far_f, 4, SAME_F)
    f_own_a = part(part_keep.at[2, rows_a], own_f.at[rows_a], 5, SAME_F)

    def rows_of(slot):
        return pl.ds(slot * slab, slab)

    def to_positions(src, dst, relay, send_sem, recv_sem, relay_sem):
        near_t, near_f = ring.at(SAME_T), ring.at(SAME_F)
        out = [
            ring.copy(src.at[rows_of(SAME_O)], relay.at[0], send_sem.at[6], relay_sem.at[0], SAME_T),
            ring.copy(src.at[rows_of(OTHER_O)], relay.at[1], send_sem.at[7], relay_sem.at[1], SAME_F),
        ] + [ring.copy(src.at[rows_of(slot)], dst.at[ring.me], send_sem.at[slot], recv_sem.at[slot], slot) for slot in (5, 4, 3, 2, 1)]
        onward = [
            ring.copy(relay.at[0], dst.at[near_t], send_sem.at[8], recv_sem.at[SAME_O], SAME_F),
            ring.copy(relay.at[1], dst.at[near_f], send_sem.at[9], recv_sem.at[OTHER_O], OTHER_T),
        ]
        keep = pltpu.make_async_copy(src.at[rows_of(0)], dst.at[ring.me], send_sem.at[0])
        return out, onward, keep

    o_out, o_pass, o_keep = to_positions(o_all, o_pos, o_relay, o_send, o_recv, o_relay_recv)
    late = slab - to_f.shape[0] % slab
    du_rows = {slot: rows_of(slot) for slot in range(1, 8)}
    du_rows[SAME_F], du_rows[OTHER_T] = pl.ds(SAME_F * slab, late), pl.ds(OTHER_T * slab, late)
    du_out = [
        ring.copy(du_all.at[rows_of(SAME_O)], to_f.at[pl.ds(0, slab)], du_send.at[6], du_relay_recv.at[0], SAME_T),
        ring.copy(du_all.at[rows_of(OTHER_O)], to_other_t.at[pl.ds(0, slab)], du_send.at[7], du_relay_recv.at[1], SAME_F),
    ] + [ring.copy(du_all.at[du_rows[slot]], du_pos.at[ring.me, pl.ds(0, du_rows[slot].size)], du_send.at[slot], du_recv.at[slot], slot) for slot in (5, 4, 3, 2, 1)]
    du_keep = pltpu.make_async_copy(du_all.at[rows_of(0)], du_pos.at[ring.me], du_send.at[0])
    du_late = [
        pltpu.make_async_copy(du_all.at[pl.ds(slot * slab + late, slab - late)], dst.at[pl.ds(slab, slab - late)], du_send.at[sem])
        for slot, dst, sem in ((SAME_F, to_f, 8), (OTHER_T, to_other_t, 9))
    ]

    def start(copies):
        for copy in copies:
            copy.start()

    loads = [pltpu.make_async_copy(uc_seq.at[slot, which], uc_all.at[which, rows_of(slot)], load_sem.at[slot, which]) for slot in range(8) for which in (0, 1)]
    near_load.start()
    start(loads)
    start(w_loads([att_full.at[3], att_full.at[2]], 0))
    ring.barrier()
    far_from_t.start()
    near_load.wait()
    near.start()
    du_all[...] = jnp.zeros_like(du_all)
    for copy in loads:
        copy.wait()

    def chip_step(step, carry):
        buf = step % 2
        relation = relation_of(step)
        for copy in w_loads([att_far.at[0], att_far.at[0]], buf):
            copy.wait()

        @pl.when(step == 0)
        def _():
            start(w_loads([att_full.at[5], att_full.at[4]], 1))

        @pl.when(step == 1)
        def _():
            far_from_core.wait_recv()
            start(w_loads([att_far.at[1], att_far.at[0]], 0))

        @pl.when(step == 2)
        def _():
            start(w_loads([att_full.at[1], att_full.at[0]], 1))

        heads = [ring.at_traced(relation * 2 + other) for other in (1, 0)]
        wo_copies = [pltpu.make_async_copy(wo_buf.at[buf, pl.ds(index * dim, dim)], wo_full.at[head], wo_sem.at[index]) for index, head in enumerate(heads)]
        start(wo_copies)
        qkv[...] = dot_nt(uc_all[0], qkv_buf[buf]).astype(BF16)
        d_ctx[...] = dot_nt(uc_all[1], wo_buf[buf]).astype(BF16)
        for index, head in enumerate(heads):
            columns = pl.ds(pl.multiple_of(head * dim, dim), dim)
            own = pl.ds(index * 3 * dim, 3 * dim)
            query, key, value = (qkv[:, pl.ds((index * 3 + part) * dim, dim)] for part in range(3))
            d_out = d_ctx[:, pl.ds(index * dim, dim)]
            scores = dot_nt(query, key) * (scale * LOG2_E)
            grown = jnp.exp2(scores - jnp.max(scores, axis=-1, keepdims=True))
            prob = grown * (1.0 / jnp.sum(grown, axis=-1, keepdims=True))
            prob_b = prob.astype(BF16)
            o_all[:, columns] = dot_nn(prob_b, value).astype(BF16)
            d_prob = dot_nt(d_out, value)
            d_score = (prob * (d_prob - jnp.sum(d_prob * prob, axis=-1, keepdims=True)) * scale).astype(BF16)
            d_qkv[:, pl.ds(index * 3 * dim, dim)] = dot_nn(d_score, key).astype(BF16)
            d_qkv[:, pl.ds((index * 3 + 1) * dim, dim)] = dot_nn(query.T, d_score).T.astype(BF16)
            d_qkv[:, pl.ds((index * 3 + 2) * dim, dim)] = dot_nn(d_out.T, prob_b).T.astype(BF16)
            if index == 0:
                @pl.when(step >= 2)
                def _():
                    core_copy(relation, buf).wait_send()

            dst = part_send.at[buf] if index == 0 else part_keep.at[relation]
            dst[pl.ds(0, 3 * dim), :] = dot_tn(d_qkv[:, own], uc_all[0])
            dst[pl.ds(3 * dim, dim), :] = dot_tn(o_all[:, columns], uc_all[1])
            if index == 0:
                core_copy(relation, buf).start()
        core_copy(relation, buf).wait_recv()
        part_keep[relation] += part_core[relation]

        @pl.when(step == 0)
        def _():
            t_own_a.start()

        @pl.when(step == 1)
        def _():
            f_own_b.start()

        @pl.when(step == 2)
        def _():
            t_far_a.start()
            f_far_b.start()

        def du_tile(part, carry):
            rows = pl.ds(pl.multiple_of(part * tile, tile), tile)
            du_all[rows, :] += dot_nn(d_qkv[rows, :], qkv_buf[buf])
            return carry

        lax.fori_loop(0, seq_len // tile, du_tile, 0)

        @pl.when(step == 0)
        def _():
            far_from_t.wait_recv()
            far_from_core.start()

        for copy in wo_copies:
            copy.wait()
        return carry

    lax.fori_loop(0, 4, chip_step, 0)
    start(o_out)
    start(du_out)
    start(du_late)
    o_keep.start()
    du_keep.start()
    for copy in core_last:
        copy.wait_send()
    start(ff_loads)
    f_far_b.wait_recv()
    part_keep[1, rows_b] += far_f[...]
    t_own_b.start()
    for copy in o_out[:2]:
        copy.wait_recv()
    start(o_pass)
    t_far_a.wait_recv()
    part_keep[2, rows_a] += far_t[...]
    f_own_a.start()
    for copy in ff_loads:
        copy.wait()
    part_send[0] += part_core[1]
    near.wait_recv()
    part_send[1] += near_buf[...]
    for copy in ff_stores:
        copy.start()
    t_own_a.wait_recv()
    t_own_b.wait_recv()
    part_keep[0] += own_t[...]
    f_own_a.wait_recv()
    f_own_b.wait_recv()
    part_keep[0] += own_f[...]
    d_att_copy = pltpu.make_async_copy(part_keep.at[0], d_att, load_sem.at[0, 0])
    d_att_copy.start()

    for copy in du_out[:2]:
        copy.wait_recv()
    for slot in range(1, 8):
        ring.copy(o_pos.at[0], o_pos.at[ring.at(slot)], near_sem.at[0], o_recv.at[slot], PARTNER).wait_recv()
    for copy in du_out[2:]:
        copy.wait_recv()
    for copy in du_late:
        copy.wait()
    for copy in o_out + du_out + o_pass + [t_own_a, t_far_a, t_own_b, f_own_b, f_far_b, f_own_a, far_from_t, far_from_core, near]:
        copy.wait_send()
    for copy in ff_stores:
        copy.wait()
    o_keep.wait()
    du_keep.wait()
    d_att_copy.wait()


def attention_call(uc_seq, att_full, part_own, part_near, up_near):
    slab, hidden = uc_seq.shape[2:]
    rows = att_full.shape[1]
    dim = rows // 4
    seq_len = 8 * slab
    any_spec = pl.BlockSpec(memory_space=pl.ANY)
    dma, vmem = pltpu.SemaphoreType.DMA, pltpu.VMEM
    out_shape = (
        jax.ShapeDtypeStruct(up_near.shape, F32),
        jax.ShapeDtypeStruct(part_near.shape, F32),
        jax.ShapeDtypeStruct((rows, hidden), F32),
        jax.ShapeDtypeStruct((8, slab, hidden), BF16),
        jax.ShapeDtypeStruct((8, slab, hidden), F32),
        jax.ShapeDtypeStruct((8, dim, hidden), BF16),
        jax.ShapeDtypeStruct((2, rows, hidden), BF16),
        jax.ShapeDtypeStruct((slab + slab // 2, hidden), F32),
        jax.ShapeDtypeStruct((slab + slab // 2, hidden), F32),
    )
    scratch = [
        vmem((2, seq_len, hidden), BF16), vmem((2, 6 * dim, hidden), BF16), vmem((2, 2 * dim, hidden), BF16),
        vmem((seq_len, 6 * dim), BF16), vmem((seq_len, 2 * dim), BF16), vmem((seq_len, 6 * dim), BF16),
        vmem((seq_len, hidden), BF16), vmem((seq_len, hidden), F32),
        vmem((2, rows, hidden), F32), vmem((4, rows, hidden), F32), vmem((4, rows, hidden), F32),
        vmem((rows, hidden), F32), vmem((3 * dim, hidden), F32), vmem((rows, hidden), F32), vmem((dim, hidden), F32),
        vmem((2, slab, hidden), BF16), vmem(part_near.shape, F32), vmem(part_near.shape, F32),
        dma((8, 2)), dma((2, 2, 2)), dma((2,)), dma((3,)), dma((2,)), dma((4,)), dma((6,)), dma((6,)), dma((4,)), dma((10,)), dma((8,)), dma((10,)), dma((8,)), dma((2,)), dma((2,)),
    ]
    return pl.pallas_call(
        functools.partial(attention_kernel, dim ** -0.5),
        out_shape=out_shape,
        in_specs=[any_spec] * 5,
        out_specs=(any_spec,) * 9,
        scratch_shapes=scratch,
        compiler_params=pltpu.CompilerParams(collective_id=1, has_side_effects=True, vmem_limit_bytes=VMEM_LIMIT),
        cost_estimate=pl.CostEstimate(flops=40 * 10**9, bytes_accessed=64 * 2**20, transcendentals=0),
        name="attention",
    )(uc_seq, att_full, part_own, part_near, up_near)


def finish_kernel(
    y_one, o_pos, wo_full, x_two, dx_one, dy_two, du_pos, d_up, d_down, d_att,
    x_one_out, x_two_out, dx_one_out, dx_two_out, dw_up, dw_down, dw_qkv, dw_out,
    y_buf, o_buf, wo_buf, x_buf, dx_buf, dy_buf, du_buf, up_buf, down_buf, att_buf, up_out, qkv_out, load_sem, store_sem,
):
    tokens = y_buf.shape[0]
    dim = wo_buf.shape[0] // 8
    chunk = 256
    chunks = [pl.ds(index * chunk, chunk) for index in range(tokens // chunk)]

    def pieces(src, dst, sem, row):
        return [pltpu.make_async_copy(src.at[rows], dst.at[rows], sem.at[row, index]) for index, rows in enumerate(chunks)]

    def whole(src, dst, sem, row):
        return pltpu.make_async_copy(src, dst, sem.at[row, 0])

    ring = Ring()
    slab = tokens // 8
    sizes = (slab, slab, slab, slab // 2, slab // 2, slab)
    slots = [pl.ds(pl.multiple_of(ring.at(slot) * slab, slab), size) for slot, size in enumerate(sizes)]

    def slabs(src, dst, sem, row):
        return [pltpu.make_async_copy(src.at[rows], dst.at[rows], sem.at[row, index]) for index, rows in enumerate(slots)]

    x_in, dy_in, du_in = pieces(x_two, x_buf, load_sem, 0), slabs(dy_two, dy_buf, load_sem, 1), slabs(du_pos, du_buf, load_sem, 2)
    y_in, o_in = pieces(y_one, y_buf, load_sem, 3), pieces(o_pos, o_buf, load_sem, 4)
    wo_in, dx_in = whole(wo_full, wo_buf, load_sem, 5), whole(dx_one, dx_buf, load_sem, 6)
    up_in, down_in, att_in = whole(d_up, up_buf, load_sem, 7), whole(d_down, down_buf, load_sem, 8), whole(d_att, att_buf, load_sem, 9)
    for group in (x_in, *zip(dy_in, du_in)):
        for copy in group:
            copy.start()
    for copy in (dx_in, wo_in):
        copy.start()
    for group in zip(y_in, o_in):
        for copy in group:
            copy.start()
    for copy in (up_in, att_in, down_in):
        copy.start()

    x_store, dx2_store, x1_store = pieces(x_buf, x_two_out, store_sem, 0), slabs(dy_buf, dx_two_out, store_sem, 1), pieces(y_buf, x_one_out, store_sem, 2)
    for index in range(len(chunks)):
        x_in[index].wait()
        x_store[index].start()
    for index, rows in enumerate(slots):
        dy_in[index].wait()
        du_in[index].wait()
        dy_buf[rows, :] += rms_back(x_buf[rows, :], du_buf[rows, :])
        dx2_store[index].start()
    dx_in.wait()
    dx_store = whole(dx_buf, dx_one_out, store_sem, 3)
    dx_store.start()
    wo_in.wait()
    for index, rows in enumerate(chunks):
        y_in[index].wait()
        o_in[index].wait()
        y_buf[rows, :] -= dot_nn(o_buf[rows, :], wo_buf[...])
        x1_store[index].start()
    up_in.wait()
    ffn = up_buf.shape[0]
    for part in range(up_out.shape[0] // ffn):
        up_out[pl.ds(part * ffn, ffn), :] = up_buf[:, pl.ds(part * ffn, ffn)].T
    up_store = whole(up_out, dw_up, store_sem, 4)
    up_store.start()
    att_in.wait()
    for part in range(3):
        qkv_out[pl.ds(part, tokens, stride=3), 0, :] = att_buf[pl.ds(part * dim, dim), :].T
    qkv_store = whole(qkv_out, dw_qkv, store_sem, 5)
    qkv_store.start()
    out_store = whole(att_buf.at[pl.ds(3 * dim, dim)], dw_out, store_sem, 6)
    out_store.start()
    down_in.wait()
    down_store = whole(down_buf, dw_down, store_sem, 7)
    down_store.start()
    for copy in x_store + dx2_store + x1_store + [dx_store, up_store, qkv_store, out_store, down_store]:
        copy.wait()


def finish_call(y_one, o_pos, wo_full, x_two, dx_one, dy_two, du_pos, d_up, d_down, d_att):
    tokens, hidden = y_one.shape
    ffn = d_up.shape[0]
    dim = d_att.shape[0] // 4
    any_spec = pl.BlockSpec(memory_space=pl.ANY)
    dma, vmem = pltpu.SemaphoreType.DMA, pltpu.VMEM
    state = (tokens, hidden)
    out_shape = [jax.ShapeDtypeStruct(shape, F32) for shape in (state, state, state, state, (hidden, ffn), (ffn, hidden), (3 * hidden, 1, dim), (dim, hidden))]
    scratch = [
        vmem(state, F32), vmem(state, BF16), vmem((hidden, hidden), BF16), vmem(state, F32), vmem(state, F32), vmem(state, F32), vmem(state, F32),
        vmem((ffn, hidden), F32), vmem((ffn, hidden), F32), vmem(d_att.shape, F32), vmem((hidden, ffn), F32), vmem((3 * hidden, 1, dim), F32),
        dma((10, 6)), dma((8, 6)),
    ]
    return pl.pallas_call(
        finish_kernel,
        out_shape=out_shape,
        in_specs=[any_spec] * 10,
        out_specs=[any_spec] * 8,
        scratch_shapes=scratch,
        compiler_params=pltpu.CompilerParams(vmem_limit_bytes=VMEM_LIMIT),
        cost_estimate=pl.CostEstimate(flops=2 * 10**9, bytes_accessed=52 * 2**20, transcendentals=0),
        name="finish",
    )(y_one, o_pos, wo_full, x_two, dx_one, dy_two, du_pos, d_up, d_down, d_att)


def last_kernel(x_two, dy_two, du_far, du_far_other, dx_two_in, dx_two_out, x_buf, dy_buf, du_buf, load_sem, store_sem):
    ring = Ring()
    slab = x_buf.shape[1]
    half = slab // 2
    loads, stores, sizes = [], [], (slab, slab, half, half)
    for index, (slot, du, skip) in enumerate(((SAME_O, du_far, 0), (OTHER_O, du_far_other, 0), (SAME_F, du_far, half), (OTHER_T, du_far_other, half))):
        size = sizes[index]
        rows = pl.ds(pl.multiple_of(ring.at(slot) * slab + skip, half), size)
        sources = ((x_two.at[rows], x_buf), (dy_two.at[rows], dy_buf), (du.at[pl.ds(2 * skip, size)], du_buf))
        loads.append([pltpu.make_async_copy(src, dst.at[index, pl.ds(0, size)], load_sem.at[index, which]) for which, (src, dst) in enumerate(sources)])
        stores.append(pltpu.make_async_copy(dy_buf.at[index, pl.ds(0, size)], dx_two_out.at[rows], store_sem.at[index]))
    for copies in loads:
        for copy in copies:
            copy.start()
    for index, copies in enumerate(loads):
        for copy in copies:
            copy.wait()
        rows = pl.ds(0, sizes[index])
        dy_buf[index, rows, :] += rms_back(x_buf[index, rows, :], du_buf[index, rows, :])
        stores[index].start()
    for copy in stores:
        copy.wait()


def last_call(x_two, dy_two, du_far, du_far_other, dx_two):
    tokens, hidden = x_two.shape
    any_spec = pl.BlockSpec(memory_space=pl.ANY)
    buf = pltpu.VMEM((4, tokens // 8, hidden), F32)
    return pl.pallas_call(
        last_kernel,
        out_shape=jax.ShapeDtypeStruct(dx_two.shape, F32),
        in_specs=[any_spec] * 5,
        out_specs=any_spec,
        input_output_aliases={4: 0},
        scratch_shapes=[buf, buf, buf, pltpu.SemaphoreType.DMA((4, 3)), pltpu.SemaphoreType.DMA((4,))],
        cost_estimate=pl.CostEstimate(flops=10**6, bytes_accessed=4 * 2**20, transcendentals=0),
        name="last",
    )(x_two, dy_two, du_far, du_far_other, dx_two)


def local_backward(y_one, y_two, dy_one, dy_two, w_qkv, w_out, w_up, w_down):
    hidden = y_one.shape[2]
    _, _, _, parts, dim = w_qkv.shape
    flat = [tensor.reshape(-1, hidden) for tensor in (y_one, y_two, dy_one, dy_two)]
    qkv_parts = jnp.swapaxes(w_qkv[0, :, 0], 0, 1)
    x_two, dx_one, uc_seq, att_full, part_own, part_near, up_near = mlp_call(*flat, w_up[0], w_down[0], qkv_parts, w_out[0, 0])
    d_up, d_down, d_att, o_pos, du_pos, wo_full, _, du_to_f, du_to_other_t = attention_call(uc_seq, att_full, part_own, part_near, up_near)
    devices = range(lax.axis_size("tp"))
    to_f = [(device, (3 - device // 2) * 2 + device % 2) for device in devices]
    to_other_t = [(device, 4 * (device // 4) + 3 - device % 4) for device in devices]
    du_far, du_far_other = lax.ppermute(du_to_f, "tp", to_f), lax.ppermute(du_to_other_t, "tp", to_other_t)
    tokens = flat[0].shape
    *states, dw_up, dw_down, dw_qkv, dw_out = finish_call(
        flat[0], o_pos.reshape(tokens), wo_full.reshape(-1, hidden), x_two, dx_one, flat[3], du_pos.reshape(tokens), d_up, d_down, d_att
    )
    states[3] = last_call(x_two, flat[3], du_far, du_far_other, states[3])
    states = [tensor.reshape(y_one.shape) for tensor in states]
    return (*states, dw_qkv.reshape(1, hidden, 1, parts, dim), dw_out[None, None], dw_up[None], dw_down[None])


def solution(mesh):
    state_spec = P("dp", "tp", None)
    in_specs = (state_spec, state_spec, state_spec, state_spec, P(None, None, "tp", None, None), P(None, "tp", None, None), P(None, None, "tp"), P(None, "tp", None))
    out_specs = (state_spec, state_spec, state_spec, state_spec, P("dp", None, "tp", None, None), P("dp", "tp", None, None), P("dp", None, "tp"), P("dp", "tp", None))
    return jax.shard_map(local_backward, mesh=mesh, in_specs=in_specs, out_specs=out_specs, check_vma=False)
```

```python
import functools

import jax
import jax.numpy as jnp
from jax import lax
from jax.experimental import pallas as pl
from jax.experimental.pallas import tpu as pltpu
from jax.sharding import PartitionSpec as P

RMS_EPS = 1e-6
LOG2_E = 1.4426950408889634
MESH = pl.DeviceIdType.MESH
BF16, F32 = jnp.bfloat16, jnp.float32
VMEM_LIMIT = 64 * 1024 * 1024 - 65536


def inv_rms(tensor):
    return lax.rsqrt(jnp.mean(tensor * tensor, axis=-1, keepdims=True) + RMS_EPS)


def rms_norm(tensor):
    return tensor * inv_rms(tensor)


def rms_back(tensor, grad_in):
    scale = inv_rms(tensor)
    return scale * grad_in - tensor * (scale * scale * scale) * jnp.mean(grad_in * tensor, axis=-1, keepdims=True)


def gelu_and_slope(tensor):
    root = (2.0 / jnp.pi) ** 0.5
    squared = tensor * tensor
    tanh = jnp.tanh(root * (tensor + 0.044715 * (tensor * squared)))
    cdf = 0.5 * (1.0 + tanh)
    slope = cdf + (0.5 * root) * tensor * ((1.0 - tanh * tanh) * (1.0 + (3 * 0.044715) * squared))
    return tensor * cdf, slope


def dot_nn(left, right):
    return lax.dot_general(left, right, (((1,), (0,)), ((), ())), preferred_element_type=F32)


def dot_nt(left, right):
    return lax.dot_general(left, right, (((1,), (1,)), ((), ())), preferred_element_type=F32)


def dot_tn(left, right):
    return lax.dot_general(left, right, (((0,), (0,)), ((), ())), preferred_element_type=F32)


class Ring:
    def __init__(self):
        me = lax.axis_index("tp")
        chip, core = me // 2, me % 2
        self.me, self.chip, self.core = me, chip, core
        self.chips = (chip, chip + 1 - 2 * (chip % 2), 3 - chip, (chip + 2) % 4)

    def at(self, slot):
        core = self.core if slot % 2 == 0 else 1 - self.core
        return self.chips[slot // 2] * 2 + core

    def at_traced(self, slot):
        relation, other = slot // 2, slot % 2
        own, near_t, near_f, opposite = self.chips
        chip = jnp.where(relation == 0, own, jnp.where(relation == 1, near_t, jnp.where(relation == 2, near_f, opposite)))
        return chip * 2 + (self.core + other) % 2

    def barrier(self):
        barrier = pltpu.get_barrier_semaphore()
        for slot in (1, 2, 3, 4, 5):
            pl.semaphore_signal(barrier, inc=1, device_id={"tp": self.at(slot)}, device_id_type=MESH)
        pl.semaphore_wait(barrier, 5)

    def copy(self, src, dst, send_sem, recv_sem, slot):
        return pltpu.make_async_remote_copy(src_ref=src, dst_ref=dst, send_sem=send_sem, recv_sem=recv_sem, device_id={"tp": self.at(slot)}, device_id_type=MESH)


PARTNER, SAME_T, OTHER_T, SAME_F, OTHER_F, SAME_O, OTHER_O = 1, 2, 3, 4, 5, 6, 7


def mlp_kernel(
    y_one, y_two, dy_one, dy_two, w_up, w_down, w_qkv, w_out,
    x_two, dx_one, uc_seq, uc_two, att_full, part_own, part_near, near_recv,
    u_all, c_all, up_all, down_all, acc, uc_own, relay, y_buf, x_buf, up_raw, qkv_raw, att_own,
    load_sem, y_sem, x_sem, w_send, w_recv, uc_send, uc_recv, att_send, att_recv, a2a_send, a2a_recv, relay_recv, near_sem, two_sem,
):
    ring = Ring()
    half = 512
    slab = 128

    def weight(which, src_slot, dst_slot, to, index):
        buf = (up_all, down_all)[which]
        return ring.copy(buf.at[src_slot], buf.at[dst_slot], w_send.at[index], w_recv.at[dst_slot, which], to)

    def weight_pair(src_slot, dst_slot, to, index):
        return [weight(which, src_slot, dst_slot, to, index + which) for which in (0, 1)]

    w_own = weight_pair(0, 1, PARTNER, 0) + weight_pair(0, 2, SAME_T, 2) + weight_pair(0, 4, SAME_F, 4)
    w_near_t = weight_pair(2, 6, SAME_F, 6) + weight_pair(2, 3, PARTNER, 8)
    w_near_f = weight_pair(4, 5, PARTNER, 10)
    w_far = weight_pair(6, 7, PARTNER, 12)

    def uc_pair(src_slot, dst_slot, to, index):
        return [ring.copy(buf.at[src_slot], buf.at[dst_slot], uc_send.at[index + which], uc_recv.at[dst_slot, which], to) for which, buf in enumerate((u_all, c_all))]

    uc_out = uc_pair(0, 2, SAME_T, 0) + uc_pair(0, 1, PARTNER, 2)
    uc_pass = uc_pair(2, 3, PARTNER, 4)

    def att(src, dst_slot, to, index):
        return ring.copy(src, att_full.at[dst_slot], att_send.at[index], att_recv.at[dst_slot], to)

    att_out = [att(att_own, 4, SAME_F, 0), att(att_own, 1, PARTNER, 1)]
    att_keep = pltpu.make_async_copy(att_own, att_full.at[0], load_sem.at[6])
    att_near_f = [att(att_full.at[4], 5, PARTNER, 2)]

    a2a_out = {slot: ring.copy(uc_own.at[slot], uc_seq.at[slot], a2a_send.at[slot], a2a_recv.at[slot], slot) for slot in (1, 2, 3, 4, 5)}
    a2a_out[SAME_O] = ring.copy(uc_own.at[SAME_O], relay.at[0], a2a_send.at[SAME_O], relay_recv.at[0], SAME_F)
    a2a_out[OTHER_O] = ring.copy(uc_own.at[OTHER_O], relay.at[1], a2a_send.at[OTHER_O], relay_recv.at[1], OTHER_F)
    a2a_pass = [ring.copy(relay.at[index], uc_seq.at[SAME_O + index], a2a_send.at[8 + index], a2a_recv.at[SAME_O + index], SAME_T) for index in (0, 1)]
    two_out = ring.copy(uc_own.at[OTHER_T], uc_two.at[1], a2a_send.at[10], relay_recv.at[2], PARTNER)
    two_keep = pltpu.make_async_copy(uc_own.at[SAME_T], uc_two.at[0], two_sem.at[0])
    two_relay = pltpu.make_async_copy(relay, uc_two.at[pl.ds(2, 2)], two_sem.at[1])
    uc_keep = pltpu.make_async_copy(uc_own.at[0], uc_seq.at[0], load_sem.at[4])

    def start(copies):
        for copy in copies:
            copy.start()

    dim = w_out.shape[0]
    near_rows = near_recv.shape[0]
    near = ring.copy(acc.at[0, pl.ds(0, near_rows)], near_recv, near_sem.at[0], near_sem.at[1], SAME_F)

    loads = [
        pltpu.make_async_copy(w_down, down_all.at[0], load_sem.at[0]),
        pltpu.make_async_copy(w_up, up_raw, load_sem.at[1]),
        pltpu.make_async_copy(y_one, acc.at[0], load_sem.at[2]),
        pltpu.make_async_copy(dy_two, acc.at[1], load_sem.at[3]),
        pltpu.make_async_copy(w_qkv, qkv_raw, load_sem.at[5]),
        pltpu.make_async_copy(w_out, att_own.at[pl.ds(3 * dim, dim)], load_sem.at[7]),
    ]
    start(loads)
    ring.barrier()
    loads[0].wait()
    start(w_own[1::2])
    loads[1].wait()
    for part in range(up_raw.shape[1] // dim):
        up_all[0, pl.ds(part * dim, dim), :] = up_raw[:, pl.ds(part * dim, dim)].T
    start(w_own[0::2])
    loads[2].wait()
    loads[3].wait()

    def normalize(step, carry):
        rows = pl.ds(pl.multiple_of(step * slab, slab), slab)
        u_all[0, rows, :] = rms_norm(acc[0, rows, :]).astype(BF16)
        c_all[0, rows, :] = acc[1, rows, :].astype(BF16)
        acc[0, rows, :] = jnp.zeros((slab, acc.shape[2]), F32)
        acc[1, rows, :] = jnp.zeros((slab, acc.shape[2]), F32)
        return carry

    lax.fori_loop(0, acc.shape[1] // slab, normalize, 0)
    start(uc_out)
    loads[4].wait()
    for part in range(3):
        att_own[pl.ds(part * dim, dim), :] = qkv_raw[part].T
    loads[5].wait()
    att_keep.start()

    def y_loads(step, buf):
        seq = ring.at_traced(7 - step)
        rows = pl.ds(pl.multiple_of(seq * slab, slab), slab)
        return [pltpu.make_async_copy(src.at[rows], y_buf.at[buf, which], y_sem.at[buf, which]) for which, src in enumerate((y_one, y_two, dy_one))]

    def x_stores(step, buf):
        seq = ring.at_traced(7 - step)
        rows = pl.ds(pl.multiple_of(seq * slab, slab), slab)
        return [pltpu.make_async_copy(x_buf.at[buf, which], dst.at[rows], x_sem.at[buf, which]) for which, dst in enumerate((x_two, dx_one))]

    def feed_forward(step, carry):
        slot = jnp.where(step == 3, 4, jnp.where(step == 4, 3, step))

        @pl.when(step >= 1)
        def _():
            for which, buf in enumerate((up_all, down_all)):
                ring.copy(buf.at[slot], buf.at[slot], w_send.at[0], w_recv.at[slot, which], PARTNER).wait_recv()

        @pl.when(step == 2)
        def _():
            start(w_near_t)
            start(att_out)

        @pl.when(step == 3)
        def _():
            start(w_near_f)

        @pl.when(step == 6)
        def _():
            start(w_far)

        @pl.when(step == 7)
        def _():
            start(y_loads(0, 0))

        def rows_step(part, carry):
            rows = pl.ds(pl.multiple_of(part * half, half), half)
            hidden, slope = gelu_and_slope(dot_nt(u_all[0, rows, :], up_all[slot]))
            d_pre = (slope * dot_nt(c_all[0, rows, :], down_all[slot])).astype(BF16)
            acc[0, rows, :] += dot_nn(hidden.astype(BF16), down_all[slot])
            acc[1, rows, :] += dot_nn(d_pre, up_all[slot])
            return carry

        lax.fori_loop(0, acc.shape[1] // half, rows_step, 0)
        return carry

    lax.fori_loop(0, 8, feed_forward, 0)

    def finish(step, carry):
        slot = 7 - step
        buf = step % 2
        seq = ring.at_traced(slot)
        rows = pl.ds(pl.multiple_of(seq * slab, slab), slab)
        for copy in y_loads(step, buf):
            copy.wait()

        @pl.when(step < 7)
        def _():
            start(y_loads(step + 1, 1 - buf))

        @pl.when(step >= 2)
        def _():
            for copy in x_stores(step - 2, buf):
                copy.wait()

        y_first = y_buf[buf, 0]
        x_second = y_buf[buf, 1] - acc[0, rows, :]
        dy_first = y_buf[buf, 2] + rms_back(y_first, acc[1, rows, :])
        x_buf[buf, 0] = x_second
        x_buf[buf, 1] = dy_first
        uc_own[slot, 0] = rms_norm(x_second).astype(BF16)
        uc_own[slot, 1] = dy_first.astype(BF16)
        acc[0, rows, :] = jnp.zeros((slab, acc.shape[2]), F32)
        acc[1, rows, :] = jnp.zeros((slab, acc.shape[2]), F32)
        start(x_stores(step, buf))
        return carry

    lax.fori_loop(0, 8, finish, 0)
    for slot in (7, 6, 5, 4, 3, 2, 1):
        a2a_out[slot].start()
    uc_keep.start()
    two_out.start()
    two_keep.start()
    for step in (6, 7):
        for copy in x_stores(step, step % 2):
            copy.wait()

    def gradients(step, carry):
        first = step // 8
        tokens = (step % 8) // 2
        slot = 4 - 4 * first

        @pl.when((step == 2) | (step == 4) | (step == 6))
        def _():
            for which, buf in enumerate((u_all, c_all)):
                ring.copy(buf.at[tokens], buf.at[tokens], uc_send.at[0], uc_recv.at[tokens, which], PARTNER).wait_recv()

        @pl.when(step == 4)
        def _():
            start(uc_pass)
            for index in (0, 1):
                ring.copy(relay.at[index], relay.at[index], a2a_send.at[0], relay_recv.at[index], PARTNER).wait_recv()
            start(a2a_pass)
            two_relay.start()

        @pl.when(step == 8)
        def _():
            near.start()
            ring.copy(att_own, att_full.at[4], att_send.at[0], att_recv.at[4], PARTNER).wait_recv()
            start(att_near_f)

        rows = pl.ds(pl.multiple_of((step % 2) * half, half), half)
        u_part, c_part = u_all[tokens, rows, :], c_all[tokens, rows, :]
        hidden, slope = gelu_and_slope(dot_nt(up_all[slot], u_part))
        d_pre = (slope * dot_nt(down_all[slot], c_part)).astype(BF16)
        acc[first, pl.ds(0, half), :] += dot_nn(d_pre, u_part)
        acc[first, pl.ds(half, half), :] += dot_nn(hidden.astype(BF16), c_part)
        return carry

    lax.fori_loop(0, 16, gradients, 0)
    out_near = pltpu.make_async_copy(acc.at[0, pl.ds(near_rows, acc.shape[1] - near_rows)], part_near, load_sem.at[0])
    out_own = pltpu.make_async_copy(acc.at[1], part_own, load_sem.at[1])
    out_near.start()
    out_own.start()

    two_out.wait_recv()
    for slot in (1, 5):
        ring.copy(att_own, att_full.at[slot], att_send.at[0], att_recv.at[slot], PARTNER).wait_recv()
    for slot in range(1, 8):
        ring.copy(uc_own.at[slot], uc_seq.at[slot], a2a_send.at[0], a2a_recv.at[slot], PARTNER).wait_recv()
    for copy in w_own + w_near_t + w_near_f + w_far + uc_out + uc_pass + att_out + att_near_f + list(a2a_out.values()) + a2a_pass + [two_out]:
        copy.wait_send()
    near.wait()
    uc_keep.wait()
    two_keep.wait()
    two_relay.wait()
    att_keep.wait()
    out_near.wait()
    out_own.wait()


def mlp_call(y_one, y_two, dy_one, dy_two, w_up, w_down, w_qkv, w_out):
    tokens, hidden = y_one.shape
    ffn = w_down.shape[0]
    dim = w_out.shape[0]
    near_rows = ffn // 2
    any_spec = pl.BlockSpec(memory_space=pl.ANY)
    dma, vmem = pltpu.SemaphoreType.DMA, pltpu.VMEM
    out_shape = (
        jax.ShapeDtypeStruct((tokens, hidden), F32),
        jax.ShapeDtypeStruct((tokens, hidden), F32),
        jax.ShapeDtypeStruct((8, 2, tokens // 8, hidden), BF16),
        jax.ShapeDtypeStruct((4, 2, tokens // 8, hidden), BF16),
        jax.ShapeDtypeStruct((6, 4 * dim, hidden), BF16),
        jax.ShapeDtypeStruct((2 * ffn, hidden), F32),
        jax.ShapeDtypeStruct((2 * ffn - near_rows, hidden), F32),
        jax.ShapeDtypeStruct((near_rows, hidden), F32),
    )
    scratch = [
        vmem((4, tokens, hidden), BF16), vmem((4, tokens, hidden), BF16),
        vmem((8, ffn, hidden), BF16), vmem((8, ffn, hidden), BF16),
        vmem((2, tokens, hidden), F32),
        vmem((8, 2, tokens // 8, hidden), BF16), vmem((2, 2, tokens // 8, hidden), BF16),
        vmem((2, 3, tokens // 8, hidden), F32), vmem((2, 2, tokens // 8, hidden), F32),
        vmem((hidden, ffn), BF16), vmem((3, hidden, dim), BF16), vmem((4 * dim, hidden), BF16),
        dma((8,)), dma((2, 3)), dma((2, 2)), dma((14,)), dma((8, 2)), dma((6,)), dma((4, 2)), dma((3,)), dma((6,)), dma((11,)), dma((8,)), dma((3,)), dma((2,)), dma((2,)),
    ]
    return pl.pallas_call(
        mlp_kernel,
        out_shape=out_shape,
        in_specs=[any_spec] * 8,
        out_specs=(any_spec,) * 8,
        scratch_shapes=scratch,
        compiler_params=pltpu.CompilerParams(collective_id=0, has_side_effects=True, vmem_limit_bytes=VMEM_LIMIT),
        cost_estimate=pl.CostEstimate(flops=70 * 10**9, bytes_accessed=64 * 2**20, transcendentals=0),
        name="feed_forward",
    )(y_one, y_two, dy_one, dy_two, w_up, w_down, w_qkv, w_out)


def attention_kernel(
    scale, uc_seq, uc_two, att_full, part_own, part_near, near_first,
    d_up, d_down, d_att, o_pos, du_pos, wo_full, att_far, uc_far, to_f, to_other_t,
    uc_all, qkv_buf, wo_buf, qkv, d_ctx, d_qkv, o_all, du_all, part_send, part_keep, part_core, own_f, o_relay, near_out, near_buf,
    load_sem, two_sem, w_sem, wo_sem, near_sem, core_send, core_recv, f_sem, far_sem, uc_sem, o_send, o_recv, du_send, du_recv, o_relay_recv, du_relay_recv,
):
    ring = Ring()
    slab, hidden = uc_seq.shape[2], uc_seq.shape[3]
    seq_len = 8 * slab
    dim = att_full.shape[1] // 4
    tile = 512

    def relation_of(step):
        base = step % 4
        return jnp.where(base == 0, 2, jnp.where(base == 3, 3, base - 1))

    def w_loads(heads, buf):
        copies = []
        for index, head in enumerate(heads):
            copies.append(pltpu.make_async_copy(head.at[pl.ds(0, 3 * dim)], qkv_buf.at[buf, pl.ds(index * 3 * dim, 3 * dim)], w_sem.at[buf, index, 0]))
            copies.append(pltpu.make_async_copy(head.at[pl.ds(3 * dim, dim)], wo_buf.at[buf, pl.ds(index * dim, dim)], w_sem.at[buf, index, 1]))
        return copies

    att_t = ring.copy(att_full.at[0], att_far.at[0], far_sem.at[0], far_sem.at[1], SAME_T)
    att_t_core = ring.copy(att_far.at[0], att_far.at[1], far_sem.at[2], far_sem.at[3], PARTNER)
    att_o = ring.copy(att_full.at[SAME_F], att_far.at[2], far_sem.at[4], far_sem.at[5], SAME_T)
    att_o_core = ring.copy(att_far.at[2], att_far.at[3], far_sem.at[6], far_sem.at[7], PARTNER)
    uc_to_t = [ring.copy(uc_seq.at[pl.ds(2 * slot, 2)], uc_far.at[pl.ds(slot, 2)], uc_sem.at[slot], uc_sem.at[slot + 1], SAME_T) for slot in (0, 2)]
    near_load = pltpu.make_async_copy(part_near, near_out, near_sem.at[2])
    near = ring.copy(near_out, near_buf, near_sem.at[0], near_sem.at[1], SAME_F)
    core_copies = [ring.copy(part_send.at[index], part_core.at[index], core_send.at[index], core_recv.at[index], PARTNER) for index in (0, 1)]
    f_copy = ring.copy(part_keep.at[0], own_f, f_sem.at[0], f_sem.at[1], SAME_F)

    rows = part_keep.shape[1]
    first = near_first.shape[0]
    ff_loads = [
        pltpu.make_async_copy(part_own.at[pl.ds(0, rows)], part_send.at[0], load_sem.at[1, 0]),
        pltpu.make_async_copy(part_own.at[pl.ds(rows, rows)], part_send.at[1], load_sem.at[1, 1]),
        pltpu.make_async_copy(near_first, part_core.at[0, pl.ds(0, first)], load_sem.at[2, 0]),
    ]
    ff_stores = [pltpu.make_async_copy(part_send.at[index], dst, load_sem.at[3, index]) for index, dst in enumerate((d_up, d_down))]

    def rows_of(slot):
        return pl.ds(slot * slab, slab)

    def seq_loads(seq, row, src, src_slot, slot, sem):
        return [pltpu.make_async_copy(src.at[src_slot, which], uc_all.at[2 * seq + which, rows_of(slot)], sem.at[row, which]) for which in (0, 1)]

    o_src = o_all.at[0]
    o_out = [
        ring.copy(o_src.at[rows_of(SAME_O)], o_relay.at[0], o_send.at[6], o_relay_recv.at[0], SAME_T),
        ring.copy(o_src.at[rows_of(OTHER_O)], o_relay.at[1], o_send.at[7], o_relay_recv.at[1], SAME_F),
    ] + [ring.copy(o_src.at[rows_of(slot)], o_pos.at[ring.me], o_send.at[slot], o_recv.at[slot], slot) for slot in (5, 4, 3, 2, 1)]
    o_pass = [
        ring.copy(o_relay.at[0], o_pos.at[ring.at(SAME_T)], o_send.at[8], o_recv.at[SAME_O], SAME_F),
        ring.copy(o_relay.at[1], o_pos.at[ring.at(SAME_F)], o_send.at[9], o_recv.at[OTHER_O], OTHER_T),
    ]
    o_keep = pltpu.make_async_copy(o_src.at[rows_of(0)], o_pos.at[ring.me], o_send.at[0])

    late = slab - to_f.shape[0] % slab
    du_rows = {slot: rows_of(slot) for slot in range(1, 8)}
    du_rows[SAME_F], du_rows[OTHER_T] = pl.ds(SAME_F * slab, late), pl.ds(OTHER_T * slab, late)
    du_out = [
        ring.copy(du_all.at[rows_of(SAME_O)], to_f.at[pl.ds(0, slab)], du_send.at[6], du_relay_recv.at[0], SAME_T),
        ring.copy(du_all.at[rows_of(OTHER_O)], to_other_t.at[pl.ds(0, slab)], du_send.at[7], du_relay_recv.at[1], SAME_F),
    ] + [ring.copy(du_all.at[du_rows[slot]], du_pos.at[ring.me, pl.ds(0, du_rows[slot].size)], du_send.at[slot], du_recv.at[slot], slot) for slot in (5, 4, 3, 2, 1)]
    du_keep = pltpu.make_async_copy(du_all.at[rows_of(0)], du_pos.at[ring.me], du_send.at[0])
    du_late = [
        pltpu.make_async_copy(du_all.at[pl.ds(slot * slab + late, slab - late)], dst.at[pl.ds(slab, slab - late)], du_send.at[sem])
        for slot, dst, sem in ((SAME_F, to_f, 8), (OTHER_T, to_other_t, 9))
    ]

    def start(copies):
        for copy in copies:
            copy.start()

    loads = [copy for slot in range(8) for copy in seq_loads(0, slot, uc_seq, slot, slot, load_sem)]
    two_loads = [copy for slot in range(4) for copy in seq_loads(1, slot, uc_two, slot, slot, two_sem)]
    far_loads = [copy for slot in range(4) for copy in seq_loads(1, 4 + slot, uc_far, slot, 4 + slot, two_sem)]
    near_load.start()
    start(loads)
    start(w_loads([att_full.at[5], att_full.at[4]], 0))
    ring.barrier()
    att_t.start()
    att_o.start()
    start(uc_to_t)
    near_load.wait()
    near.start()
    start(two_loads)
    du_all[...] = jnp.zeros_like(du_all)
    part_send[...] = jnp.zeros_like(part_send)
    part_keep[...] = jnp.zeros_like(part_keep)
    for copy in loads:
        copy.wait()

    def chip_step(step, carry):
        buf = step % 2
        seq = step // 4
        relation = relation_of(step)

        @pl.when(step == 4)
        def _():
            for copy in uc_to_t:
                copy.wait_recv()
            start(far_loads)
            for copy in two_loads + far_loads:
                copy.wait()

        for copy in w_loads([att_full.at[0], att_full.at[0]], buf):
            copy.wait()

        @pl.when((step == 0) | (step == 4))
        def _():
            start(w_loads([att_full.at[1], att_full.at[0]], 1))

        @pl.when(step == 3)
        def _():
            start(w_loads([att_full.at[5], att_full.at[4]], 0))

        heads = [ring.at_traced(relation * 2 + other) for other in (1, 0)]
        wo_copies = [pltpu.make_async_copy(wo_buf.at[buf, pl.ds(index * dim, dim)], wo_full.at[head], wo_sem.at[index]) for index, head in enumerate(heads)]
        start(wo_copies)
        qkv[...] = dot_nt(uc_all[2 * seq], qkv_buf[buf]).astype(BF16)
        d_ctx[...] = dot_nt(uc_all[2 * seq + 1], wo_buf[buf]).astype(BF16)
        for index, head in enumerate(heads):
            columns = pl.ds(pl.multiple_of(head * dim, dim), dim)
            own = pl.ds(index * 3 * dim, 3 * dim)
            query, key, value = (qkv[:, pl.ds((index * 3 + part) * dim, dim)] for part in range(3))
            d_out = d_ctx[:, pl.ds(index * dim, dim)]
            scores = dot_nt(query, key) * (scale * LOG2_E)
            grown = jnp.exp2(scores - jnp.max(scores, axis=-1, keepdims=True))
            prob = grown * (1.0 / jnp.sum(grown, axis=-1, keepdims=True))
            prob_b = prob.astype(BF16)
            o_all[seq, :, columns] = dot_nn(prob_b, value).astype(BF16)
            d_prob = dot_nt(d_out, value)
            d_score = (prob * (d_prob - jnp.sum(d_prob * prob, axis=-1, keepdims=True)) * scale).astype(BF16)
            d_qkv[:, pl.ds(index * 3 * dim, dim)] = dot_nn(d_score, key).astype(BF16)
            d_qkv[:, pl.ds((index * 3 + 1) * dim, dim)] = dot_nn(query.T, d_score).T.astype(BF16)
            d_qkv[:, pl.ds((index * 3 + 2) * dim, dim)] = dot_nn(d_out.T, prob_b).T.astype(BF16)

            @pl.when((step < 2) | (step >= 4))
            def _():
                dst = (part_send, part_keep)[index].at[buf]
                dst[pl.ds(0, 3 * dim), :] += dot_tn(d_qkv[:, own], uc_all[2 * seq])
                dst[pl.ds(3 * dim, dim), :] += dot_tn(o_all[seq, :, columns], uc_all[2 * seq + 1])

            if index == 0:
                @pl.when(step == 1)
                def _():
                    att_t.wait_recv()
                    att_t_core.start()

                @pl.when(step == 4)
                def _():
                    core_copies[0].start()

                @pl.when(step == 5)
                def _():
                    core_copies[1].start()

        @pl.when(step < 4)
        def _():
            def du_tile(part, carry):
                rows = pl.ds(pl.multiple_of(part * tile, tile), tile)
                du_all[rows, :] += dot_nn(d_qkv[rows, :], qkv_buf[buf])
                return carry

            lax.fori_loop(0, seq_len // tile, du_tile, 0)

        @pl.when(step == 1)
        def _():
            att_t_core.wait_recv()
            start(w_loads([att_far.at[1], att_far.at[0]], 0))

        @pl.when(step == 2)
        def _():
            att_o.wait_recv()
            att_o_core.start()
            att_o_core.wait_recv()
            start(w_loads([att_far.at[3], att_far.at[2]], 1))

        @pl.when(step == 3)
        def _():
            start(o_out)
            start(du_out)
            start(du_late)
            o_keep.start()
            du_keep.start()

        @pl.when(step == 4)
        def _():
            core_copies[0].wait_recv()
            part_keep[0] += part_core[0]
            f_copy.start()

        for copy in wo_copies:
            copy.wait()
        return carry

    lax.fori_loop(0, 6, chip_step, 0)
    for copy in o_out[:2]:
        copy.wait_recv()
    start(o_pass)
    core_copies[1].wait_recv()
    part_keep[1] += part_core[1]
    for copy in core_copies:
        copy.wait_send()
    start(ff_loads)
    for copy in ff_loads:
        copy.wait()
    near.wait_recv()
    part_send[0, pl.ds(0, first), :] += part_core[0, pl.ds(0, first), :]
    part_send[0, pl.ds(first, rows - first), :] += near_buf[pl.ds(0, rows - first), :]
    part_send[1] += near_buf[pl.ds(rows - first, rows), :]
    start(ff_stores)
    for copy in du_out[2:]:
        copy.wait_recv()
    for slot in range(1, 8):
        ring.copy(o_pos.at[0], o_pos.at[ring.at(slot)], near_sem.at[0], o_recv.at[slot], PARTNER).wait_recv()
    for copy in du_out[:2]:
        copy.wait_recv()
    f_copy.wait_recv()
    part_keep[1] += own_f[...]
    d_att_copy = pltpu.make_async_copy(part_keep.at[1], d_att, load_sem.at[0, 0])
    d_att_copy.start()

    for copy in o_out + du_out + o_pass + uc_to_t + [f_copy, att_t, att_t_core, att_o, att_o_core, near]:
        copy.wait_send()
    for copy in du_late + ff_stores:
        copy.wait()
    o_keep.wait()
    du_keep.wait()
    d_att_copy.wait()


def attention_call(uc_seq, uc_two, att_full, part_own, part_near, near_first):
    slab, hidden = uc_seq.shape[2:]
    rows = att_full.shape[1]
    dim = rows // 4
    seq_len = 8 * slab
    any_spec = pl.BlockSpec(memory_space=pl.ANY)
    dma, vmem = pltpu.SemaphoreType.DMA, pltpu.VMEM
    ffn = part_own.shape[0] // 2
    out_shape = (
        jax.ShapeDtypeStruct((ffn, hidden), F32),
        jax.ShapeDtypeStruct((ffn, hidden), F32),
        jax.ShapeDtypeStruct((rows, hidden), F32),
        jax.ShapeDtypeStruct((8, slab, hidden), BF16),
        jax.ShapeDtypeStruct((8, slab, hidden), F32),
        jax.ShapeDtypeStruct((8, dim, hidden), BF16),
        jax.ShapeDtypeStruct((4, rows, hidden), BF16),
        jax.ShapeDtypeStruct((4, 2, slab, hidden), BF16),
        jax.ShapeDtypeStruct((slab + slab // 2, hidden), F32),
        jax.ShapeDtypeStruct((slab + slab // 2, hidden), F32),
    )
    scratch = [
        vmem((4, seq_len, hidden), BF16), vmem((2, 6 * dim, hidden), BF16), vmem((2, 2 * dim, hidden), BF16),
        vmem((seq_len, 6 * dim), BF16), vmem((seq_len, 2 * dim), BF16), vmem((seq_len, 6 * dim), BF16),
        vmem((2, seq_len, hidden), BF16), vmem((seq_len, hidden), F32),
        vmem((2, rows, hidden), F32), vmem((2, rows, hidden), F32), vmem((2, rows, hidden), F32), vmem((rows, hidden), F32),
        vmem((2, slab, hidden), BF16), vmem(part_near.shape, F32), vmem(part_near.shape, F32),
        dma((8, 2)), dma((8, 2)), dma((2, 2, 2)), dma((2,)), dma((3,)), dma((2,)), dma((2,)), dma((2,)), dma((8,)), dma((4,)),
        dma((10,)), dma((8,)), dma((10,)), dma((8,)), dma((2,)), dma((2,)),
    ]
    return pl.pallas_call(
        functools.partial(attention_kernel, dim ** -0.5),
        out_shape=out_shape,
        in_specs=[any_spec] * 6,
        out_specs=(any_spec,) * 10,
        scratch_shapes=scratch,
        compiler_params=pltpu.CompilerParams(collective_id=1, has_side_effects=True, vmem_limit_bytes=VMEM_LIMIT),
        cost_estimate=pl.CostEstimate(flops=50 * 10**9, bytes_accessed=64 * 2**20, transcendentals=0),
        name="attention",
    )(uc_seq, uc_two, att_full, part_own, part_near, near_first)


def finish_kernel(
    y_one, o_pos, wo_full, x_two, dx_one, dy_two, du_pos, d_up, d_down, d_att,
    x_one_out, x_two_out, dx_one_out, dx_two_out, dw_up, dw_down, dw_qkv, dw_out,
    y_buf, o_buf, wo_buf, x_buf, dx_buf, dy_buf, du_buf, up_buf, down_buf, att_buf, up_out, qkv_out, load_sem, store_sem,
):
    tokens = y_buf.shape[0]
    dim = wo_buf.shape[0] // 8
    chunk = 256
    chunks = [pl.ds(index * chunk, chunk) for index in range(tokens // chunk)]

    def pieces(src, dst, sem, row):
        return [pltpu.make_async_copy(src.at[rows], dst.at[rows], sem.at[row, index]) for index, rows in enumerate(chunks)]

    def whole(src, dst, sem, row):
        return pltpu.make_async_copy(src, dst, sem.at[row, 0])

    ring = Ring()
    slab = tokens // 8
    sizes = (slab, slab, slab, slab // 2, slab // 2, slab)
    slots = [pl.ds(pl.multiple_of(ring.at(slot) * slab, slab), size) for slot, size in enumerate(sizes)]

    def slabs(src, dst, sem, row):
        return [pltpu.make_async_copy(src.at[rows], dst.at[rows], sem.at[row, index]) for index, rows in enumerate(slots)]

    x_in, dy_in, du_in = pieces(x_two, x_buf, load_sem, 0), slabs(dy_two, dy_buf, load_sem, 1), slabs(du_pos, du_buf, load_sem, 2)
    y_in, o_in = pieces(y_one, y_buf, load_sem, 3), pieces(o_pos, o_buf, load_sem, 4)
    wo_in, dx_in = whole(wo_full, wo_buf, load_sem, 5), whole(dx_one, dx_buf, load_sem, 6)
    up_in, down_in, att_in = whole(d_up, up_buf, load_sem, 7), whole(d_down, down_buf, load_sem, 8), whole(d_att, att_buf, load_sem, 9)
    for group in (x_in, *zip(dy_in, du_in)):
        for copy in group:
            copy.start()
    for copy in (dx_in, wo_in):
        copy.start()
    for group in zip(y_in, o_in):
        for copy in group:
            copy.start()
    for copy in (up_in, att_in, down_in):
        copy.start()

    x_store, dx2_store, x1_store = pieces(x_buf, x_two_out, store_sem, 0), slabs(dy_buf, dx_two_out, store_sem, 1), pieces(y_buf, x_one_out, store_sem, 2)
    for index in range(len(chunks)):
        x_in[index].wait()
        x_store[index].start()
    for index, rows in enumerate(slots):
        dy_in[index].wait()
        du_in[index].wait()
        dy_buf[rows, :] += rms_back(x_buf[rows, :], du_buf[rows, :])
        dx2_store[index].start()
    dx_in.wait()
    dx_store = whole(dx_buf, dx_one_out, store_sem, 3)
    dx_store.start()
    wo_in.wait()
    for index, rows in enumerate(chunks):
        y_in[index].wait()
        o_in[index].wait()
        y_buf[rows, :] -= dot_nn(o_buf[rows, :], wo_buf[...])
        x1_store[index].start()
    up_in.wait()
    ffn = up_buf.shape[0]
    for part in range(up_out.shape[0] // ffn):
        up_out[pl.ds(part * ffn, ffn), :] = up_buf[:, pl.ds(part * ffn, ffn)].T
    up_store = whole(up_out, dw_up, store_sem, 4)
    up_store.start()
    att_in.wait()
    for part in range(3):
        qkv_out[pl.ds(part, tokens, stride=3), 0, :] = att_buf[pl.ds(part * dim, dim), :].T
    qkv_store = whole(qkv_out, dw_qkv, store_sem, 5)
    qkv_store.start()
    out_store = whole(att_buf.at[pl.ds(3 * dim, dim)], dw_out, store_sem, 6)
    out_store.start()
    down_in.wait()
    down_store = whole(down_buf, dw_down, store_sem, 7)
    down_store.start()
    for copy in x_store + dx2_store + x1_store + [dx_store, up_store, qkv_store, out_store, down_store]:
        copy.wait()


def finish_call(y_one, o_pos, wo_full, x_two, dx_one, dy_two, du_pos, d_up, d_down, d_att):
    tokens, hidden = y_one.shape
    ffn = d_up.shape[0]
    dim = d_att.shape[0] // 4
    any_spec = pl.BlockSpec(memory_space=pl.ANY)
    dma, vmem = pltpu.SemaphoreType.DMA, pltpu.VMEM
    state = (tokens, hidden)
    out_shape = [jax.ShapeDtypeStruct(shape, F32) for shape in (state, state, state, state, (hidden, ffn), (ffn, hidden), (3 * hidden, 1, dim), (dim, hidden))]
    scratch = [
        vmem(state, F32), vmem(state, BF16), vmem((hidden, hidden), BF16), vmem(state, F32), vmem(state, F32), vmem(state, F32), vmem(state, F32),
        vmem((ffn, hidden), F32), vmem((ffn, hidden), F32), vmem(d_att.shape, F32), vmem((hidden, ffn), F32), vmem((3 * hidden, 1, dim), F32),
        dma((10, 6)), dma((8, 6)),
    ]
    return pl.pallas_call(
        finish_kernel,
        out_shape=out_shape,
        in_specs=[any_spec] * 10,
        out_specs=[any_spec] * 8,
        scratch_shapes=scratch,
        compiler_params=pltpu.CompilerParams(vmem_limit_bytes=VMEM_LIMIT),
        cost_estimate=pl.CostEstimate(flops=2 * 10**9, bytes_accessed=52 * 2**20, transcendentals=0),
        name="finish",
    )(y_one, o_pos, wo_full, x_two, dx_one, dy_two, du_pos, d_up, d_down, d_att)


def last_kernel(x_two, dy_two, du_far, du_far_other, dx_two_in, dx_two_out, x_buf, dy_buf, du_buf, load_sem, store_sem):
    ring = Ring()
    slab = x_buf.shape[1]
    half = slab // 2
    loads, stores, sizes = [], [], (slab, slab, half, half)
    for index, (slot, du, skip) in enumerate(((SAME_O, du_far, 0), (OTHER_O, du_far_other, 0), (SAME_F, du_far, half), (OTHER_T, du_far_other, half))):
        size = sizes[index]
        rows = pl.ds(pl.multiple_of(ring.at(slot) * slab + skip, half), size)
        sources = ((x_two.at[rows], x_buf), (dy_two.at[rows], dy_buf), (du.at[pl.ds(2 * skip, size)], du_buf))
        loads.append([pltpu.make_async_copy(src, dst.at[index, pl.ds(0, size)], load_sem.at[index, which]) for which, (src, dst) in enumerate(sources)])
        stores.append(pltpu.make_async_copy(dy_buf.at[index, pl.ds(0, size)], dx_two_out.at[rows], store_sem.at[index]))
    for copies in loads:
        for copy in copies:
            copy.start()
    for index, copies in enumerate(loads):
        for copy in copies:
            copy.wait()
        rows = pl.ds(0, sizes[index])
        dy_buf[index, rows, :] += rms_back(x_buf[index, rows, :], du_buf[index, rows, :])
        stores[index].start()
    for copy in stores:
        copy.wait()


def last_call(x_two, dy_two, du_far, du_far_other, dx_two):
    tokens, hidden = x_two.shape
    any_spec = pl.BlockSpec(memory_space=pl.ANY)
    buf = pltpu.VMEM((4, tokens // 8, hidden), F32)
    return pl.pallas_call(
        last_kernel,
        out_shape=jax.ShapeDtypeStruct(dx_two.shape, F32),
        in_specs=[any_spec] * 5,
        out_specs=any_spec,
        input_output_aliases={4: 0},
        scratch_shapes=[buf, buf, buf, pltpu.SemaphoreType.DMA((4, 3)), pltpu.SemaphoreType.DMA((4,))],
        cost_estimate=pl.CostEstimate(flops=10**6, bytes_accessed=4 * 2**20, transcendentals=0),
        name="last",
    )(x_two, dy_two, du_far, du_far_other, dx_two)


def local_backward(y_one, y_two, dy_one, dy_two, w_qkv, w_out, w_up, w_down):
    hidden = y_one.shape[2]
    _, _, _, parts, dim = w_qkv.shape
    flat = [tensor.reshape(-1, hidden) for tensor in (y_one, y_two, dy_one, dy_two)]
    qkv_parts = jnp.swapaxes(w_qkv[0, :, 0], 0, 1)
    x_two, dx_one, *shared = mlp_call(*flat, w_up[0], w_down[0], qkv_parts, w_out[0, 0])
    d_up, d_down, d_att, o_pos, du_pos, wo_full, _, _, du_to_f, du_to_other_t = attention_call(*shared)
    devices = range(lax.axis_size("tp"))
    to_f = [(device, (3 - device // 2) * 2 + device % 2) for device in devices]
    to_other_t = [(device, 4 * (device // 4) + 3 - device % 4) for device in devices]
    du_far, du_far_other = lax.ppermute(du_to_f, "tp", to_f), lax.ppermute(du_to_other_t, "tp", to_other_t)
    tokens = flat[0].shape
    *states, dw_up, dw_down, dw_qkv, dw_out = finish_call(
        flat[0], o_pos.reshape(tokens), wo_full.reshape(-1, hidden), x_two, dx_one, flat[3], du_pos.reshape(tokens), d_up, d_down, d_att
    )
    states[3] = last_call(x_two, flat[3], du_far, du_far_other, states[3])
    states = [tensor.reshape(y_one.shape) for tensor in states]
    return (*states, dw_qkv.reshape(1, hidden, 1, parts, dim), dw_out[None, None], dw_up[None], dw_down[None])


def solution(mesh):
    state_spec = P("dp", "tp", None)
    in_specs = (state_spec, state_spec, state_spec, state_spec, P(None, None, "tp", None, None), P(None, "tp", None, None), P(None, None, "tp"), P(None, "tp", None))
    out_specs = (state_spec, state_spec, state_spec, state_spec, P("dp", None, "tp", None, None), P("dp", "tp", None, None), P("dp", None, "tp"), P("dp", "tp", None))
    return jax.shard_map(local_backward, mesh=mesh, in_specs=in_specs, out_specs=out_specs, check_vma=False)
```

```python
import functools

import jax
import jax.numpy as jnp
from jax import lax
from jax.experimental import pallas as pl
from jax.experimental.pallas import tpu as pltpu
from jax.sharding import PartitionSpec as P

RMS_EPS = 1e-6
LOG2_E = 1.4426950408889634
MESH = pl.DeviceIdType.MESH
BF16, F32 = jnp.bfloat16, jnp.float32
VMEM_LIMIT = 64 * 1024 * 1024 - 65536


def inv_rms(tensor):
    return lax.rsqrt(jnp.mean(tensor * tensor, axis=-1, keepdims=True) + RMS_EPS)


def rms_norm(tensor):
    return tensor * inv_rms(tensor)


def rms_back(tensor, grad_in):
    scale = inv_rms(tensor)
    return scale * grad_in - tensor * (scale * scale * scale) * jnp.mean(grad_in * tensor, axis=-1, keepdims=True)


def gelu_and_slope(tensor):
    root = (2.0 / jnp.pi) ** 0.5
    squared = tensor * tensor
    tanh = jnp.tanh(root * (tensor + 0.044715 * (tensor * squared)))
    cdf = 0.5 * (1.0 + tanh)
    slope = cdf + (0.5 * root) * tensor * ((1.0 - tanh * tanh) * (1.0 + (3 * 0.044715) * squared))
    return tensor * cdf, slope


def dot_nn(left, right):
    return lax.dot_general(left, right, (((1,), (0,)), ((), ())), preferred_element_type=F32)


def dot_nt(left, right):
    return lax.dot_general(left, right, (((1,), (1,)), ((), ())), preferred_element_type=F32)


def dot_tn(left, right):
    return lax.dot_general(left, right, (((0,), (0,)), ((), ())), preferred_element_type=F32)


class Ring:
    def __init__(self):
        me = lax.axis_index("tp")
        chip, core = me // 2, me % 2
        self.me, self.chip, self.core = me, chip, core
        self.chips = (chip, chip + 1 - 2 * (chip % 2), 3 - chip, (chip + 2) % 4)

    def at(self, slot):
        core = self.core if slot % 2 == 0 else 1 - self.core
        return self.chips[slot // 2] * 2 + core

    def at_traced(self, slot):
        relation, other = slot // 2, slot % 2
        own, near_t, near_f, opposite = self.chips
        chip = jnp.where(relation == 0, own, jnp.where(relation == 1, near_t, jnp.where(relation == 2, near_f, opposite)))
        return chip * 2 + (self.core + other) % 2

    def barrier(self):
        barrier = pltpu.get_barrier_semaphore()
        for slot in (1, 2, 3, 4, 5):
            pl.semaphore_signal(barrier, inc=1, device_id={"tp": self.at(slot)}, device_id_type=MESH)
        pl.semaphore_wait(barrier, 5)

    def copy(self, src, dst, send_sem, recv_sem, slot):
        return pltpu.make_async_remote_copy(src_ref=src, dst_ref=dst, send_sem=send_sem, recv_sem=recv_sem, device_id={"tp": self.at(slot)}, device_id_type=MESH)


PARTNER, SAME_T, OTHER_T, SAME_F, OTHER_F, SAME_O, OTHER_O = 1, 2, 3, 4, 5, 6, 7


def block_kernel(
    scale,
    y_one, y_two, dy_one, dy_two, w_up, w_down, w_qkv, w_out,
    x_two, dx_one, part_own, near_recv, d_att, o_pos, du_pos, wo_full, to_f, to_other_t,
    uc_seq, uc_two, uc_far, att_full, part_core, own_f, o_relay,
    u_all, c_all, up_all, down_all, acc, spare, part_keep, uc_own, att_own,
    load_sem, y_sem, x_sem, w_send, w_recv, uc_send, uc_recv, att_send, att_recv, a2a_send, a2a_recv, relay_recv, near_sem, two_sem,
    seq_sem, head_sem, wo_sem, core_send, core_recv, f_sem, far_sem, o_send, o_recv, du_send, du_recv, o_relay_recv, du_relay_recv, free_slot,
):
    ring = Ring()
    slabs, slab, hidden = acc.shape[1:]
    seq_len = slabs * slab
    half = seq_len // 2
    dim = w_out.shape[0]
    fours = slabs // 2

    def start(copies):
        for copy in copies:
            copy.start()

    rooms = (0, 1, 2, 3, 4, 5, 1, 3)

    def room(slot):
        return pl.ds(rooms[slot] * half, half)

    def weight_pair(src_slot, dst_slot, to, index):
        return [
            ring.copy(buf.at[room(src_slot)], buf.at[room(dst_slot)], w_send.at[index + which], w_recv.at[dst_slot, which], to)
            for which, buf in enumerate((up_all, down_all))
        ]

    w_own = weight_pair(0, 1, PARTNER, 0) + weight_pair(0, 2, SAME_T, 2) + weight_pair(0, 4, SAME_F, 4)
    w_near_t = weight_pair(2, 6, SAME_F, 6)
    w_near_t_core = weight_pair(2, 3, PARTNER, 8)
    w_near_f = weight_pair(4, 5, PARTNER, 10)
    w_far = weight_pair(6, 7, PARTNER, 12)

    def uc_pair(src_slot, dst_slot, to, index):
        return [ring.copy(buf.at[src_slot], buf.at[dst_slot], uc_send.at[index + which], uc_recv.at[dst_slot, which], to) for which, buf in enumerate((u_all, c_all))]

    uc_out = uc_pair(0, 2, SAME_T, 0) + uc_pair(0, 1, PARTNER, 2)
    uc_pass = uc_pair(2, 3, PARTNER, 4)

    def att(src, dst_slot, to, index):
        return ring.copy(src, att_full.at[dst_slot], att_send.at[index], att_recv.at[dst_slot], to)

    att_keep = pltpu.make_async_copy(att_own, att_full.at[0], load_sem.at[6])
    att_out = [att(att_own, 4, SAME_F, 0), att(att_own, 1, PARTNER, 1)]
    att_t, att_o = att(att_own, 2, SAME_T, 2), att(att_full.at[4], 6, SAME_T, 3)
    att_f_core, att_t_core, att_o_core = att(att_full.at[4], 5, PARTNER, 4), att(att_full.at[2], 3, PARTNER, 5), att(att_full.at[6], 7, PARTNER, 6)

    a2a_out = {slot: ring.copy(uc_own.at[slot], uc_seq.at[slot], a2a_send.at[slot], a2a_recv.at[slot], slot) for slot in (1, 2, 3, 4, 5)}
    a2a_out[SAME_O] = ring.copy(uc_own.at[SAME_O], uc_two.at[2], a2a_send.at[SAME_O], relay_recv.at[0], SAME_F)
    a2a_out[OTHER_O] = ring.copy(uc_own.at[OTHER_O], uc_two.at[3], a2a_send.at[OTHER_O], relay_recv.at[1], OTHER_F)
    a2a_pass = [ring.copy(uc_two.at[2 + index], uc_seq.at[SAME_O + index], a2a_send.at[8 + index], a2a_recv.at[SAME_O + index], SAME_T) for index in (0, 1)]
    uc_keep = pltpu.make_async_copy(uc_own.at[0], uc_seq.at[0], load_sem.at[4])
    two_out = ring.copy(uc_own.at[OTHER_T], uc_two.at[1], a2a_send.at[10], relay_recv.at[2], PARTNER)
    two_keep = pltpu.make_async_copy(uc_own.at[SAME_T], uc_two.at[0], two_sem.at[0])
    near = ring.copy(acc.at[0], near_recv, near_sem.at[0], near_sem.at[1], SAME_F)

    loads = [
        pltpu.make_async_copy(w_down, down_all.at[room(0)], load_sem.at[0]),
        pltpu.make_async_copy(w_up, uc_own.at[:, 0, :, pl.ds(0, half)], load_sem.at[1]),
        pltpu.make_async_copy(y_one, acc.at[0], load_sem.at[2]),
        pltpu.make_async_copy(dy_two, acc.at[1], load_sem.at[3]),
        pltpu.make_async_copy(w_out, att_own.at[pl.ds(3 * dim, dim)], load_sem.at[7]),
    ]
    qkv_loads = [pltpu.make_async_copy(w_qkv.at[part], uc_own.at[:, 1, :, pl.ds(part * dim, dim)], y_sem.at[0, part]) for part in range(3)]
    start(loads)
    start(qkv_loads)
    ring.barrier()
    loads[0].wait()
    start(w_own[1::2])
    loads[1].wait()
    for part in range(half // dim):
        up_all[pl.ds(part * dim, dim), :] = uc_own[:, 0, :, pl.ds(part * dim, dim)].reshape(hidden, dim).T
    start(w_own[0::2])
    loads[2].wait()
    loads[3].wait()

    def normalize(step, carry):
        rows = pl.ds(pl.multiple_of(step * slab, slab), slab)
        u_all[0, rows, :] = rms_norm(acc[0, step]).astype(BF16)
        c_all[0, rows, :] = acc[1, step].astype(BF16)
        acc[0, step] = jnp.zeros((slab, hidden), F32)
        acc[1, step] = jnp.zeros((slab, hidden), F32)
        return carry

    lax.fori_loop(0, slabs, normalize, 0)
    start(uc_out)
    for part in range(3):
        qkv_loads[part].wait()
        att_own[pl.ds(part * dim, dim), :] = uc_own[:, 1, :, pl.ds(part * dim, dim)].reshape(hidden, dim).T
    loads[4].wait()
    att_keep.start()

    def y_loads(step, buf):
        seq = ring.at_traced(7 - step)
        return [pltpu.make_async_copy(src.at[seq], spare.at[buf, which], y_sem.at[buf, which]) for which, src in enumerate((y_one, y_two, dy_one))]

    def x_stores(step, buf):
        seq = ring.at_traced(7 - step)
        return [pltpu.make_async_copy(spare.at[buf, 3 + which], dst.at[seq], x_sem.at[buf, which]) for which, dst in enumerate((x_two, dx_one))]

    def feed_forward(step, carry):
        slot = jnp.where(step == 3, 4, jnp.where(step == 4, 3, step))
        place = pl.ds(pl.multiple_of(jnp.where(step == 6, 1, jnp.where(step == 7, 3, slot)) * half, half), half)

        @pl.when(step >= 1)
        def _():
            for which, buf in enumerate((up_all, down_all)):
                ring.copy(buf.at[place], buf.at[place], w_send.at[0], w_recv.at[slot, which], PARTNER).wait_recv()

        @pl.when(step == 2)
        def _():
            pl.semaphore_wait(free_slot.at[0], 1)
            start(w_near_t)
            start(w_near_t_core)
            start(att_out)

        @pl.when(step == 3)
        def _():
            start(w_near_f)

        @pl.when(step == 6)
        def _():
            pl.semaphore_wait(free_slot.at[1], 1)
            start(w_far)

        @pl.when(step == 7)
        def _():
            start(y_loads(0, 0))

        def rows_step(part, carry):
            rows = pl.ds(pl.multiple_of(part * half, half), half)
            quarter = pl.ds(part * fours, fours)
            hidden_act, slope = gelu_and_slope(dot_nt(u_all[0, rows, :], up_all[place, :]))
            d_pre = (slope * dot_nt(c_all[0, rows, :], down_all[place, :])).astype(BF16)
            acc[0, quarter] += dot_nn(hidden_act.astype(BF16), down_all[place, :]).reshape(fours, slab, hidden)
            acc[1, quarter] += dot_nn(d_pre, up_all[place, :]).reshape(fours, slab, hidden)
            return carry

        lax.fori_loop(0, 2, rows_step, 0)

        @pl.when(step == 1)
        def _():
            pl.semaphore_signal(free_slot.at[0], inc=1, device_id={"tp": ring.at(SAME_F)}, device_id_type=MESH)

        @pl.when(step == 4)
        def _():
            pl.semaphore_signal(free_slot.at[1], inc=1, device_id={"tp": ring.at(PARTNER)}, device_id_type=MESH)

        return carry

    lax.fori_loop(0, 8, feed_forward, 0)

    def finish(step, carry):
        slot = 7 - step
        buf = step % 2
        seq = ring.at_traced(slot)
        for copy in y_loads(step, buf):
            copy.wait()

        @pl.when(step < 7)
        def _():
            start(y_loads(step + 1, 1 - buf))

        @pl.when(step >= 2)
        def _():
            for copy in x_stores(step - 2, buf):
                copy.wait()

        y_first = spare[buf, 0]
        x_second = spare[buf, 1] - acc[0, seq]
        dy_first = spare[buf, 2] + rms_back(y_first, acc[1, seq])
        spare[buf, 3] = x_second
        spare[buf, 4] = dy_first
        uc_own[slot, 0] = rms_norm(x_second).astype(BF16)
        uc_own[slot, 1] = dy_first.astype(BF16)
        acc[0, seq] = jnp.zeros((slab, hidden), F32)
        acc[1, seq] = jnp.zeros((slab, hidden), F32)
        start(x_stores(step, buf))
        return carry

    lax.fori_loop(0, 8, finish, 0)
    for slot in (7, 6, 5, 4, 3, 2, 1):
        a2a_out[slot].start()
    uc_keep.start()
    two_out.start()
    two_keep.start()
    for step in (6, 7):
        for copy in x_stores(step, step % 2):
            copy.wait()

    def gradients(step, carry):
        first = step // 8
        tokens = (step % 8) // 2
        place = pl.ds(pl.multiple_of((4 - 4 * first) * half, half), half)

        @pl.when((step == 2) | (step == 4) | (step == 6))
        def _():
            for which, buf in enumerate((u_all, c_all)):
                ring.copy(buf.at[tokens], buf.at[tokens], uc_send.at[0], uc_recv.at[tokens, which], PARTNER).wait_recv()

        @pl.when(step == 4)
        def _():
            start(uc_pass)
            for index in (0, 1):
                a2a_out[SAME_O + index].wait_recv()
            start(a2a_pass)

        @pl.when(step == 8)
        def _():
            near.start()
            att_out[0].wait_recv()
            att_f_core.start()
            att_t.start()
            att_o.start()

        rows = pl.ds(pl.multiple_of((step % 2) * half, half), half)
        u_part, c_part = u_all[tokens, rows, :], c_all[tokens, rows, :]
        hidden_act, slope = gelu_and_slope(dot_nt(up_all[place, :], u_part))
        d_pre = (slope * dot_nt(down_all[place, :], c_part)).astype(BF16)
        acc[first, pl.ds(0, fours)] += dot_nn(d_pre, u_part).reshape(fours, slab, hidden)
        acc[first, pl.ds(fours, fours)] += dot_nn(hidden_act.astype(BF16), c_part).reshape(fours, slab, hidden)
        return carry

    lax.fori_loop(0, 16, gradients, 0)
    out_own = pltpu.make_async_copy(acc.at[1], part_own, load_sem.at[1])
    out_own.start()
    for copy in w_own + w_near_t + w_near_t_core + w_near_f + w_far + uc_out + uc_pass:
        copy.wait_send()

    def relation_of(step):
        base = step % 4
        return jnp.where(base == 0, 2, jnp.where(base == 3, 3, base - 1))

    def qkv_rows(buf):
        return pl.ds(pl.multiple_of(buf * 6 * dim, 2 * dim), 6 * dim)

    def wo_rows(buf):
        return pl.ds(pl.multiple_of(12 * dim + buf * 2 * dim, 2 * dim), 2 * dim)

    def head_loads(relation, buf):
        copies = []
        for index in (0, 1):
            head = att_full.at[relation * 2 + 1 - index]
            first, second = (pl.ds(pl.multiple_of(base + index * size, dim), size) for base, size in ((buf * 6 * dim, 3 * dim), (12 * dim + buf * 2 * dim, dim)))
            copies.append(pltpu.make_async_copy(head.at[pl.ds(0, 3 * dim)], up_all.at[first], head_sem.at[buf, index, 0]))
            copies.append(pltpu.make_async_copy(head.at[pl.ds(3 * dim, dim)], up_all.at[second], head_sem.at[buf, index, 1]))
        return copies

    def rows_of(slot):
        return pl.ds(slot * slab, slab)

    def seq_loads(seq, src, src_slot, slot):
        return [pltpu.make_async_copy(src.at[src_slot, which], u_all.at[2 * seq + which, rows_of(slot)], seq_sem.at[2 * seq + which, slot]) for which in (0, 1)]

    seq_own = [copy for slot in range(8) for copy in seq_loads(0, uc_seq, slot, slot)]
    seq_two = [copy for slot in range(4) for copy in seq_loads(1, uc_two, slot, slot)]
    seq_far = [copy for slot in range(4) for copy in seq_loads(1, uc_far, slot, 4 + slot)]
    uc_to_t = [ring.copy(uc_seq.at[pl.ds(2 * slot, 2)], uc_far.at[pl.ds(slot, 2)], far_sem.at[slot], far_sem.at[slot + 1], SAME_T) for slot in (0, 2)]
    core_copies = [ring.copy(spare.at[index, pl.ds(0, 4)], part_core.at[index], core_send.at[index], core_recv.at[index], PARTNER) for index in (0, 1)]
    f_copy = ring.copy(part_keep.at[0], own_f, f_sem.at[0], f_sem.at[1], SAME_F)
    core_loads = [pltpu.make_async_copy(part_core.at[index], acc.at[0, pl.ds(0, 4)], load_sem.at[2]) for index in (0, 1)]
    own_f_load = pltpu.make_async_copy(own_f, acc.at[0, pl.ds(4, 4)], load_sem.at[3])

    o_src = c_all.at[0]
    o_out = [
        ring.copy(o_src.at[rows_of(SAME_O)], o_relay.at[0], o_send.at[6], o_relay_recv.at[0], SAME_T),
        ring.copy(o_src.at[rows_of(OTHER_O)], o_relay.at[1], o_send.at[7], o_relay_recv.at[1], SAME_F),
    ] + [ring.copy(o_src.at[rows_of(slot)], o_pos.at[ring.me], o_send.at[slot], o_recv.at[slot], slot) for slot in (5, 4, 3, 2, 1)]
    o_pass = [
        ring.copy(o_relay.at[0], o_pos.at[ring.at(SAME_T)], o_send.at[8], o_recv.at[SAME_O], SAME_F),
        ring.copy(o_relay.at[1], o_pos.at[ring.at(SAME_F)], o_send.at[9], o_recv.at[OTHER_O], OTHER_T),
    ]
    o_keep = pltpu.make_async_copy(o_src.at[rows_of(0)], o_pos.at[ring.me], o_send.at[0])

    late = slab - to_f.shape[0] % slab
    early = {slot: late if slot in (SAME_F, OTHER_T) else slab for slot in range(1, 6)}
    du_out = [
        ring.copy(acc.at[1, SAME_O], to_f.at[pl.ds(0, slab)], du_send.at[6], du_relay_recv.at[0], SAME_T),
        ring.copy(acc.at[1, OTHER_O], to_other_t.at[pl.ds(0, slab)], du_send.at[7], du_relay_recv.at[1], SAME_F),
    ] + [ring.copy(acc.at[1, slot, pl.ds(0, early[slot])], du_pos.at[ring.me, pl.ds(0, early[slot])], du_send.at[slot], du_recv.at[slot], slot) for slot in (5, 4, 3, 2, 1)]
    du_keep = pltpu.make_async_copy(acc.at[1, 0], du_pos.at[ring.me], du_send.at[0])
    du_late = [
        pltpu.make_async_copy(acc.at[1, slot, pl.ds(late, slab - late)], dst.at[pl.ds(slab, slab - late)], du_send.at[sem])
        for slot, dst, sem in ((SAME_F, to_f, 8), (OTHER_T, to_other_t, 9))
    ]

    att_f_core.wait_recv()
    att_keep.wait()
    att_out[1].wait_recv()
    start(head_loads(2, 0))
    spare[...] = jnp.zeros_like(spare)
    part_keep[...] = jnp.zeros_like(part_keep)
    uc_keep.wait()
    for slot in range(1, 8):
        ring.copy(uc_own.at[slot], uc_seq.at[slot], a2a_send.at[0], a2a_recv.at[slot], PARTNER).wait_recv()
    start(seq_own)
    start(uc_to_t)
    two_out.wait_recv()
    two_keep.wait()
    start(seq_two)
    out_own.wait()
    acc[1] = jnp.zeros(acc.shape[1:], F32)
    for copy in seq_own:
        copy.wait()

    def chip_step(step, carry):
        buf = step % 2
        seq = step // 4
        relation = relation_of(step)

        @pl.when(step == 4)
        def _():
            for copy in uc_to_t:
                copy.wait_recv()
            start(seq_far)
            for copy in seq_two + seq_far:
                copy.wait()

        for copy in head_loads(0, buf):
            copy.wait()

        @pl.when((step == 0) | (step == 3) | (step == 4))
        def _():
            start(head_loads(relation_of(step + 1), 1 - buf))

        heads = [ring.at_traced(relation * 2 + other) for other in (1, 0)]
        wo_copies = [
            pltpu.make_async_copy(up_all.at[pl.ds(pl.multiple_of(12 * dim + (2 * buf + index) * dim, dim), dim)], wo_full.at[head], wo_sem.at[index])
            for index, head in enumerate(heads)
        ]
        start(wo_copies)
        c_all[2, :, pl.ds(0, 6 * dim)] = dot_nt(u_all[2 * seq], up_all[qkv_rows(buf), :]).astype(BF16)
        c_all[2, :, pl.ds(6 * dim, 2 * dim)] = dot_nt(u_all[2 * seq + 1], up_all[wo_rows(buf), :]).astype(BF16)
        for index, head in enumerate(heads):
            columns = pl.ds(pl.multiple_of(head * dim, dim), dim)
            own = pl.ds(index * 3 * dim, 3 * dim)
            query, key, value = (c_all[2, :, pl.ds((index * 3 + part) * dim, dim)] for part in range(3))
            d_out = c_all[2, :, pl.ds((6 + index) * dim, dim)]
            scores = dot_nt(query, key) * (scale * LOG2_E)
            grown = jnp.exp2(scores - jnp.max(scores, axis=-1, keepdims=True))
            prob = grown * (1.0 / jnp.sum(grown, axis=-1, keepdims=True))
            prob_b = prob.astype(BF16)
            c_all[seq, :, columns] = dot_nn(prob_b, value).astype(BF16)
            d_prob = dot_nt(d_out, value)
            d_score = (prob * (d_prob - jnp.sum(d_prob * prob, axis=-1, keepdims=True)) * scale).astype(BF16)
            c_all[3, :, pl.ds(index * 3 * dim, dim)] = dot_nn(d_score, key).astype(BF16)
            c_all[3, :, pl.ds((index * 3 + 1) * dim, dim)] = dot_nn(query.T, d_score).T.astype(BF16)
            c_all[3, :, pl.ds((index * 3 + 2) * dim, dim)] = dot_nn(d_out.T, prob_b).T.astype(BF16)
            @pl.when((step < 2) | (step >= 4))
            def _():
                dst = (spare, part_keep)[index].at[buf]
                dst[pl.ds(0, 3)] += dot_tn(c_all[3, :, own], u_all[2 * seq]).reshape(3, dim, hidden)
                dst[3] += dot_tn(c_all[seq, :, columns], u_all[2 * seq + 1])

            if index == 0:
                @pl.when(step == 1)
                def _():
                    att_t.wait_recv()
                    att_t_core.start()

                @pl.when(step == 4)
                def _():
                    core_copies[0].start()

                @pl.when(step == 5)
                def _():
                    core_copies[1].start()

        @pl.when(step < 4)
        def _():
            def du_tile(part, carry):
                rows = pl.ds(pl.multiple_of(part * half, half), half)
                acc[1, pl.ds(part * fours, fours)] += dot_nn(c_all[3, rows, pl.ds(0, 6 * dim)], up_all[qkv_rows(buf), :]).reshape(fours, slab, hidden)
                return carry

            lax.fori_loop(0, 2, du_tile, 0)

        @pl.when(step == 1)
        def _():
            att_t_core.wait_recv()
            start(head_loads(1, 0))

        @pl.when(step == 2)
        def _():
            att_o.wait_recv()
            att_o_core.start()
            att_o_core.wait_recv()
            start(head_loads(3, 1))

        @pl.when(step == 3)
        def _():
            start(o_out)
            start(du_out)
            start(du_late)
            o_keep.start()
            du_keep.start()

        @pl.when(step == 4)
        def _():
            near.wait_send()
            core_copies[0].wait_recv()
            core_loads[0].start()
            core_loads[0].wait()
            part_keep[0] += acc[0, pl.ds(0, 4)]
            f_copy.start()

        for copy in wo_copies:
            copy.wait()
        return carry

    lax.fori_loop(0, 6, chip_step, 0)
    for copy in o_out[:2]:
        copy.wait_recv()
    start(o_pass)
    core_copies[1].wait_recv()
    core_loads[1].start()
    core_loads[1].wait()
    part_keep[1] += acc[0, pl.ds(0, 4)]
    for copy in du_out[2:]:
        copy.wait_recv()
    for slot in range(1, 8):
        ring.copy(o_pos.at[0], o_pos.at[ring.at(slot)], near_sem.at[0], o_recv.at[slot], PARTNER).wait_recv()
    for copy in du_out[:2]:
        copy.wait_recv()
    near.wait_recv()
    f_copy.wait_recv()
    own_f_load.start()
    own_f_load.wait()
    part_keep[1] += acc[0, pl.ds(4, 4)]
    d_att_copy = pltpu.make_async_copy(part_keep.at[1], d_att, load_sem.at[0])
    d_att_copy.start()

    sends = att_out + [att_t, att_o, att_f_core, att_t_core, att_o_core] + list(a2a_out.values()) + a2a_pass + [two_out]
    for copy in sends + o_out + du_out + o_pass + uc_to_t + core_copies + [f_copy]:
        copy.wait_send()
    for copy in du_late:
        copy.wait()
    o_keep.wait()
    du_keep.wait()
    d_att_copy.wait()


def block_call(y_one, y_two, dy_one, dy_two, w_up, w_down, w_qkv, w_out):
    slabs, slab, hidden = y_one.shape
    tokens = slabs * slab
    ffn = w_down.shape[0]
    dim = w_out.shape[0]
    any_spec = pl.BlockSpec(memory_space=pl.ANY)
    dma, vmem, wide, narrow = pltpu.SemaphoreType.DMA, pltpu.VMEM, F32, BF16
    results = [
        ((slabs, slab, hidden), wide), ((slabs, slab, hidden), wide), ((slabs, slab, hidden), wide), ((slabs, slab, hidden), wide),
        ((4, dim, hidden), wide), ((slabs, slab, hidden), narrow), ((slabs, slab, hidden), wide), ((8, dim, hidden), narrow),
        ((slab + slab // 2, hidden), wide), ((slab + slab // 2, hidden), wide),
    ]
    landing = [
        ((8, 2, slab, hidden), narrow), ((4, 2, slab, hidden), narrow), ((4, 2, slab, hidden), narrow), ((8, 4 * dim, hidden), narrow),
        ((2, 4, dim, hidden), wide), ((4, dim, hidden), wide), ((2, slab, hidden), narrow),
    ]
    scratch = [
        vmem((4, tokens, hidden), BF16), vmem((4, tokens, hidden), BF16), vmem((6 * ffn, hidden), BF16), vmem((6 * ffn, hidden), BF16),
        vmem((2, slabs, slab, hidden), F32), vmem((2, 5, slab, hidden), F32), vmem((2, 4, dim, hidden), F32),
        vmem((8, 2, slab, hidden), BF16), vmem((4 * dim, hidden), BF16),
        dma((8,)), dma((2, 3)), dma((2, 2)), dma((14,)), dma((8, 2)), dma((6,)), dma((4, 2)), dma((7,)), dma((8,)), dma((11,)), dma((8,)), dma((3,)), dma((2,)), dma((2,)),
        dma((4, 8)), dma((2, 2, 2)), dma((2,)), dma((2,)), dma((2,)), dma((2,)), dma((4,)), dma((10,)), dma((8,)), dma((10,)), dma((8,)), dma((2,)), dma((2,)),
        pltpu.SemaphoreType.REGULAR((2,)),
    ]
    return pl.pallas_call(
        functools.partial(block_kernel, dim ** -0.5),
        out_shape=[jax.ShapeDtypeStruct(shape, dtype) for shape, dtype in results + landing],
        in_specs=[any_spec] * 8,
        out_specs=[any_spec] * (len(results) + len(landing)),
        scratch_shapes=scratch,
        compiler_params=pltpu.CompilerParams(collective_id=0, has_side_effects=True, vmem_limit_bytes=VMEM_LIMIT),
        cost_estimate=pl.CostEstimate(flops=120 * 10**9, bytes_accessed=128 * 2**20, transcendentals=0),
        name="block",
    )(y_one, y_two, dy_one, dy_two, w_up.reshape(8, hidden // 8, ffn), w_down, w_qkv.reshape(3, 8, hidden // 8, dim), w_out)[: len(results)]


def finish_kernel(
    y_one, o_pos, wo_full, x_two, dx_one, dy_two, du_pos, part_own, near_recv, d_att,
    x_one_out, x_two_out, dx_one_out, dx_two_out, dw_up, dw_down, dw_qkv, dw_out,
    y_buf, o_buf, wo_buf, x_buf, dx_buf, dy_buf, du_buf, own_buf, near_buf, att_buf, up_out, qkv_out, load_sem, store_sem,
):
    tokens = y_buf.shape[0]
    dim = wo_buf.shape[0] // 8
    chunk = 256
    chunks = [pl.ds(index * chunk, chunk) for index in range(tokens // chunk)]

    def pieces(src, dst, sem, row):
        return [pltpu.make_async_copy(src.at[rows], dst.at[rows], sem.at[row, index]) for index, rows in enumerate(chunks)]

    def whole(src, dst, sem, row):
        return pltpu.make_async_copy(src, dst, sem.at[row, 0])

    ring = Ring()
    slab = tokens // 8
    sizes = (slab, slab, slab, slab // 2, slab // 2, slab)
    slots = [pl.ds(pl.multiple_of(ring.at(slot) * slab, slab), size) for slot, size in enumerate(sizes)]

    def slabs(src, dst, sem, row):
        return [pltpu.make_async_copy(src.at[rows], dst.at[rows], sem.at[row, index]) for index, rows in enumerate(slots)]

    x_in, dy_in, du_in = pieces(x_two, x_buf, load_sem, 0), slabs(dy_two, dy_buf, load_sem, 1), slabs(du_pos, du_buf, load_sem, 2)
    y_in, o_in = pieces(y_one, y_buf, load_sem, 3), pieces(o_pos, o_buf, load_sem, 4)
    wo_in, dx_in = whole(wo_full, wo_buf, load_sem, 5), whole(dx_one, dx_buf, load_sem, 6)
    own_in, near_in, att_in = whole(part_own, own_buf, load_sem, 7), whole(near_recv, near_buf, load_sem, 8), whole(d_att, att_buf, load_sem, 9)
    for group in (x_in, *zip(dy_in, du_in)):
        for copy in group:
            copy.start()
    for copy in (dx_in, wo_in):
        copy.start()
    for group in zip(y_in, o_in):
        for copy in group:
            copy.start()
    for copy in (own_in, near_in, att_in):
        copy.start()

    x_store, dx2_store, x1_store = pieces(x_buf, x_two_out, store_sem, 0), slabs(dy_buf, dx_two_out, store_sem, 1), pieces(y_buf, x_one_out, store_sem, 2)
    for index in range(len(chunks)):
        x_in[index].wait()
        x_store[index].start()
    for index, rows in enumerate(slots):
        dy_in[index].wait()
        du_in[index].wait()
        dy_buf[rows, :] += rms_back(x_buf[rows, :], du_buf[rows, :])
        dx2_store[index].start()
    dx_in.wait()
    dx_store = whole(dx_buf, dx_one_out, store_sem, 3)
    dx_store.start()
    wo_in.wait()
    for index, rows in enumerate(chunks):
        y_in[index].wait()
        o_in[index].wait()
        y_buf[rows, :] -= dot_nn(o_buf[rows, :], wo_buf[...])
        x1_store[index].start()
    own_in.wait()
    near_in.wait()
    ffn = up_out.shape[1]
    own_buf[pl.ds(ffn, ffn), :] += near_buf[pl.ds(ffn, ffn), :]
    down_store = whole(own_buf.at[pl.ds(ffn, ffn)], dw_down, store_sem, 7)
    down_store.start()
    for part in range(up_out.shape[0] // ffn):
        columns = pl.ds(part * ffn, ffn)
        up_out[columns, :] = (own_buf[pl.ds(0, ffn), columns] + near_buf[pl.ds(0, ffn), columns]).T
    up_store = whole(up_out, dw_up, store_sem, 4)
    up_store.start()
    att_in.wait()
    for part in range(3):
        qkv_out[pl.ds(part, tokens, stride=3), 0, :] = att_buf[pl.ds(part * dim, dim), :].T
    qkv_store = whole(qkv_out, dw_qkv, store_sem, 5)
    qkv_store.start()
    out_store = whole(att_buf.at[pl.ds(3 * dim, dim)], dw_out, store_sem, 6)
    out_store.start()
    for copy in x_store + dx2_store + x1_store + [dx_store, up_store, qkv_store, out_store, down_store]:
        copy.wait()


def finish_call(y_one, o_pos, wo_full, x_two, dx_one, dy_two, du_pos, part_own, near_recv, d_att):
    tokens, hidden = y_one.shape
    ffn = part_own.shape[0] // 2
    dim = d_att.shape[0] // 4
    any_spec = pl.BlockSpec(memory_space=pl.ANY)
    dma, vmem = pltpu.SemaphoreType.DMA, pltpu.VMEM
    state = (tokens, hidden)
    out_shape = [jax.ShapeDtypeStruct(shape, F32) for shape in (state, state, state, state, (hidden, ffn), (ffn, hidden), (3 * hidden, 1, dim), (dim, hidden))]
    scratch = [
        vmem(state, F32), vmem(state, BF16), vmem((hidden, hidden), BF16), vmem(state, F32), vmem(state, F32), vmem(state, F32), vmem(state, F32),
        vmem(part_own.shape, F32), vmem(part_own.shape, F32), vmem(d_att.shape, F32), vmem((hidden, ffn), F32), vmem((3 * hidden, 1, dim), F32),
        dma((10, 6)), dma((8, 6)),
    ]
    return pl.pallas_call(
        finish_kernel,
        out_shape=out_shape,
        in_specs=[any_spec] * 10,
        out_specs=[any_spec] * 8,
        scratch_shapes=scratch,
        compiler_params=pltpu.CompilerParams(vmem_limit_bytes=VMEM_LIMIT),
        cost_estimate=pl.CostEstimate(flops=2 * 10**9, bytes_accessed=52 * 2**20, transcendentals=0),
        name="finish",
    )(y_one, o_pos, wo_full, x_two, dx_one, dy_two, du_pos, part_own, near_recv, d_att)


def last_kernel(x_two, dy_two, du_far, du_far_other, dx_two_in, dx_two_out, x_buf, dy_buf, du_buf, load_sem, store_sem):
    ring = Ring()
    slab = x_buf.shape[1]
    half = slab // 2
    loads, stores, sizes = [], [], (slab, slab, half, half)
    for index, (slot, du, skip) in enumerate(((SAME_O, du_far, 0), (OTHER_O, du_far_other, 0), (SAME_F, du_far, half), (OTHER_T, du_far_other, half))):
        size = sizes[index]
        rows = pl.ds(pl.multiple_of(ring.at(slot) * slab + skip, half), size)
        sources = ((x_two.at[rows], x_buf), (dy_two.at[rows], dy_buf), (du.at[pl.ds(2 * skip, size)], du_buf))
        loads.append([pltpu.make_async_copy(src, dst.at[index, pl.ds(0, size)], load_sem.at[index, which]) for which, (src, dst) in enumerate(sources)])
        stores.append(pltpu.make_async_copy(dy_buf.at[index, pl.ds(0, size)], dx_two_out.at[rows], store_sem.at[index]))
    for copies in loads:
        for copy in copies:
            copy.start()
    for index, copies in enumerate(loads):
        for copy in copies:
            copy.wait()
        rows = pl.ds(0, sizes[index])
        dy_buf[index, rows, :] += rms_back(x_buf[index, rows, :], du_buf[index, rows, :])
        stores[index].start()
    for copy in stores:
        copy.wait()


def last_call(x_two, dy_two, du_far, du_far_other, dx_two):
    tokens, hidden = x_two.shape
    any_spec = pl.BlockSpec(memory_space=pl.ANY)
    buf = pltpu.VMEM((4, tokens // 8, hidden), F32)
    return pl.pallas_call(
        last_kernel,
        out_shape=jax.ShapeDtypeStruct(dx_two.shape, F32),
        in_specs=[any_spec] * 5,
        out_specs=any_spec,
        input_output_aliases={4: 0},
        scratch_shapes=[buf, buf, buf, pltpu.SemaphoreType.DMA((4, 3)), pltpu.SemaphoreType.DMA((4,))],
        cost_estimate=pl.CostEstimate(flops=10**6, bytes_accessed=4 * 2**20, transcendentals=0),
        name="last",
    )(x_two, dy_two, du_far, du_far_other, dx_two)


def local_backward(y_one, y_two, dy_one, dy_two, w_qkv, w_out, w_up, w_down):
    hidden = y_one.shape[2]
    _, _, _, parts, dim = w_qkv.shape
    qkv_parts = jnp.swapaxes(w_qkv[0, :, 0], 0, 1)
    results = block_call(y_one, y_two, dy_one, dy_two, w_up[0], w_down[0], qkv_parts, w_out[0, 0])
    x_two, dx_one, part_own, near_recv, d_att, o_pos, du_pos, wo_full = (tensor.reshape(-1, hidden) for tensor in results[:8])
    devices = range(lax.axis_size("tp"))
    to_f = [(device, (3 - device // 2) * 2 + device % 2) for device in devices]
    to_other_t = [(device, 4 * (device // 4) + 3 - device % 4) for device in devices]
    du_far, du_far_other = lax.ppermute(results[8], "tp", to_f), lax.ppermute(results[9], "tp", to_other_t)
    y_flat, dy_flat = y_one.reshape(-1, hidden), dy_two.reshape(-1, hidden)
    *states, dw_up, dw_down, dw_qkv, dw_out = finish_call(y_flat, o_pos, wo_full, x_two, dx_one, dy_flat, du_pos, part_own, near_recv, d_att)
    states[3] = last_call(x_two, dy_flat, du_far, du_far_other, states[3])
    states = [tensor.reshape(y_one.shape) for tensor in states]
    return (*states, dw_qkv.reshape(1, hidden, 1, parts, dim), dw_out[None, None], dw_up[None], dw_down[None])


def solution(mesh):
    state_spec = P("dp", "tp", None)
    in_specs = (state_spec, state_spec, state_spec, state_spec, P(None, None, "tp", None, None), P(None, "tp", None, None), P(None, None, "tp"), P(None, "tp", None))
    out_specs = (state_spec, state_spec, state_spec, state_spec, P("dp", None, "tp", None, None), P("dp", "tp", None, None), P("dp", None, "tp"), P("dp", "tp", None))
    return jax.shard_map(local_backward, mesh=mesh, in_specs=in_specs, out_specs=out_specs, check_vma=False)
```

```python
import functools

import jax
import jax.numpy as jnp
from jax import lax
from jax.experimental import pallas as pl
from jax.experimental.pallas import tpu as pltpu
from jax.sharding import PartitionSpec as P

RMS_EPS = 1e-6
LOG2_E = 1.4426950408889634
LATE_ROWS = 80
MESH = pl.DeviceIdType.MESH
BF16, F32 = jnp.bfloat16, jnp.float32
VMEM_LIMIT = 64 * 1024 * 1024 - 65536


def inv_rms(tensor):
    return lax.rsqrt(jnp.mean(tensor * tensor, axis=-1, keepdims=True) + RMS_EPS)


def rms_norm(tensor):
    return tensor * inv_rms(tensor)


def rms_back(tensor, grad_in):
    scale = inv_rms(tensor)
    return scale * grad_in - tensor * (scale * scale * scale) * jnp.mean(grad_in * tensor, axis=-1, keepdims=True)


def gelu_and_slope(tensor):
    root = (2.0 / jnp.pi) ** 0.5
    squared = tensor * tensor
    tanh = jnp.tanh(root * (tensor + 0.044715 * (tensor * squared)))
    cdf = 0.5 * (1.0 + tanh)
    slope = cdf + (0.5 * root) * tensor * ((1.0 - tanh * tanh) * (1.0 + (3 * 0.044715) * squared))
    return tensor * cdf, slope


def dot_nn(left, right):
    return lax.dot_general(left, right, (((1,), (0,)), ((), ())), preferred_element_type=F32)


def dot_nt(left, right):
    return lax.dot_general(left, right, (((1,), (1,)), ((), ())), preferred_element_type=F32)


def dot_tn(left, right):
    return lax.dot_general(left, right, (((0,), (0,)), ((), ())), preferred_element_type=F32)


class Ring:
    def __init__(self):
        me = lax.axis_index("tp")
        chip, core = me // 2, me % 2
        self.me, self.chip, self.core = me, chip, core
        self.chips = (chip, chip + 1 - 2 * (chip % 2), 3 - chip, (chip + 2) % 4)

    def at(self, slot):
        core = self.core if slot % 2 == 0 else 1 - self.core
        return self.chips[slot // 2] * 2 + core

    def at_traced(self, slot):
        relation, other = slot // 2, slot % 2
        own, near_t, near_f, opposite = self.chips
        chip = jnp.where(relation == 0, own, jnp.where(relation == 1, near_t, jnp.where(relation == 2, near_f, opposite)))
        return chip * 2 + (self.core + other) % 2

    def barrier(self):
        barrier = pltpu.get_barrier_semaphore()
        for slot in (1, 2, 3, 4, 5):
            pl.semaphore_signal(barrier, inc=1, device_id={"tp": self.at(slot)}, device_id_type=MESH)
        pl.semaphore_wait(barrier, 5)

    def copy(self, src, dst, send_sem, recv_sem, slot):
        return pltpu.make_async_remote_copy(src_ref=src, dst_ref=dst, send_sem=send_sem, recv_sem=recv_sem, device_id={"tp": self.at(slot)}, device_id_type=MESH)


PARTNER, SAME_T, OTHER_T, SAME_F, OTHER_F, SAME_O, OTHER_O = 1, 2, 3, 4, 5, 6, 7


def block_kernel(
    scale,
    y_one, y_two, dy_one, dy_two, w_up, w_down, w_qkv, w_out,
    x_two, dx_one, part_own, near_recv, d_att, o_pos, du_pos, wo_full, to_f, to_other_t,
    uc_seq, uc_two, att_full, o_relay,
    u_all, c_all, up_all, down_all, acc, spare, part_keep, uc_own, att_own,
    load_sem, y_sem, x_sem, w_send, w_recv, uc_send, uc_recv, att_send, att_recv, a2a_send, a2a_recv, relay_recv, near_sem, two_sem,
    seq_sem, head_sem, wo_sem, core_send, core_recv, f_sem, far_sem, o_send, o_recv, du_send, du_recv, o_relay_recv, du_relay_recv, free_slot,
):
    ring = Ring()
    slabs, slab, hidden = acc.shape[1:]
    seq_len = slabs * slab
    half = seq_len // 2
    dim = w_out.shape[0]
    fours = slabs // 2

    def start(copies):
        for copy in copies:
            copy.start()

    def say_free(index, to):
        pl.semaphore_signal(free_slot.at[index], inc=1, device_id={"tp": ring.at(to)}, device_id_type=MESH)

    rooms = (0, 1, 2, 3, 4, 5, 1, 3)

    def room(slot):
        return pl.ds(rooms[slot] * half, half)

    def weight_pair(src_slot, dst_slot, to, index):
        return [
            ring.copy(buf.at[room(src_slot)], buf.at[room(dst_slot)], w_send.at[index + which], w_recv.at[dst_slot, which], to)
            for which, buf in enumerate((up_all, down_all))
        ]

    w_own = weight_pair(0, 1, PARTNER, 0) + weight_pair(0, 2, SAME_T, 2) + weight_pair(0, 4, SAME_F, 4)
    w_near_t = weight_pair(2, 6, SAME_F, 6)
    w_near_t_core = weight_pair(2, 3, PARTNER, 8)
    w_near_f = weight_pair(4, 5, PARTNER, 10)
    w_far = weight_pair(6, 7, PARTNER, 12)

    def uc_pair(src_slot, dst_slot, to, index):
        return [ring.copy(buf.at[src_slot], buf.at[dst_slot], uc_send.at[index + which], uc_recv.at[dst_slot, which], to) for which, buf in enumerate((u_all, c_all))]

    uc_out = uc_pair(0, 2, SAME_T, 0) + uc_pair(0, 1, PARTNER, 2)
    uc_pass = uc_pair(2, 3, PARTNER, 4)

    def att(src, dst_slot, to, index):
        return ring.copy(src, att_full.at[dst_slot], att_send.at[index], att_recv.at[dst_slot], to)

    att_keep = pltpu.make_async_copy(att_own, att_full.at[0], load_sem.at[6])
    att_out = [att(att_own, 4, SAME_F, 0), att(att_own, 1, PARTNER, 1)]
    att_t, att_o = att(att_own, 2, SAME_T, 2), att(att_full.at[4], 6, SAME_T, 3)
    att_f_core, att_t_core, att_o_core = att(att_full.at[4], 5, PARTNER, 4), att(att_full.at[2], 3, PARTNER, 5), att(att_full.at[6], 7, PARTNER, 6)

    a2a_out = {slot: ring.copy(uc_own.at[slot], uc_seq.at[slot], a2a_send.at[slot], a2a_recv.at[slot], slot) for slot in (1, 2, 3, 4, 5)}
    a2a_out[SAME_O] = ring.copy(uc_own.at[SAME_O], uc_two.at[2], a2a_send.at[SAME_O], relay_recv.at[0], SAME_F)
    a2a_out[OTHER_O] = ring.copy(uc_own.at[OTHER_O], uc_two.at[3], a2a_send.at[OTHER_O], relay_recv.at[1], OTHER_F)
    a2a_pass = [ring.copy(uc_two.at[2 + index], uc_seq.at[SAME_O + index], a2a_send.at[8 + index], a2a_recv.at[SAME_O + index], SAME_T) for index in (0, 1)]
    uc_keep = pltpu.make_async_copy(uc_own.at[0], uc_seq.at[0], load_sem.at[4])
    two_out = ring.copy(uc_own.at[OTHER_T], uc_two.at[1], a2a_send.at[10], relay_recv.at[2], PARTNER)
    two_keep = pltpu.make_async_copy(uc_own.at[SAME_T], uc_two.at[0], two_sem.at[0])
    near = ring.copy(acc.at[0], near_recv, near_sem.at[0], near_sem.at[1], SAME_F)

    loads = [
        pltpu.make_async_copy(w_down, down_all.at[room(0)], load_sem.at[0]),
        pltpu.make_async_copy(w_up, uc_own.at[:, 0, :, pl.ds(0, half)], load_sem.at[1]),
        pltpu.make_async_copy(y_one, acc.at[0], load_sem.at[2]),
        pltpu.make_async_copy(dy_two, acc.at[1], load_sem.at[3]),
        pltpu.make_async_copy(w_out, att_own.at[pl.ds(3 * dim, dim)], load_sem.at[7]),
    ]
    qkv_loads = [pltpu.make_async_copy(w_qkv.at[part], uc_own.at[:, 1, :, pl.ds(part * dim, dim)], y_sem.at[0, part]) for part in range(3)]
    start(loads)
    start(qkv_loads)
    ring.barrier()
    loads[0].wait()
    start(w_own[1::2])
    loads[1].wait()
    for part in range(half // dim):
        up_all[pl.ds(part * dim, dim), :] = uc_own[:, 0, :, pl.ds(part * dim, dim)].reshape(hidden, dim).T
    start(w_own[0::2])
    loads[2].wait()
    loads[3].wait()

    def normalize(step, carry):
        rows = pl.ds(pl.multiple_of(step * slab, slab), slab)
        u_all[0, rows, :] = rms_norm(acc[0, step]).astype(BF16)
        c_all[0, rows, :] = acc[1, step].astype(BF16)
        acc[0, step] = jnp.zeros((slab, hidden), F32)
        acc[1, step] = jnp.zeros((slab, hidden), F32)
        return carry

    lax.fori_loop(0, slabs, normalize, 0)
    start(uc_out)
    for part in range(3):
        qkv_loads[part].wait()
        att_own[pl.ds(part * dim, dim), :] = uc_own[:, 1, :, pl.ds(part * dim, dim)].reshape(hidden, dim).T
    loads[4].wait()
    att_keep.start()

    def y_loads(step, buf):
        seq = ring.at_traced(7 - step)
        return [pltpu.make_async_copy(src.at[seq], spare.at[buf, which], y_sem.at[buf, which]) for which, src in enumerate((y_one, y_two, dy_one))]

    def x_stores(step, buf):
        seq = ring.at_traced(7 - step)
        return [pltpu.make_async_copy(spare.at[buf, 3 + which], dst.at[seq], x_sem.at[buf, which]) for which, dst in enumerate((x_two, dx_one))]

    def feed_forward(step, carry):
        slot = jnp.where(step == 3, 4, jnp.where(step == 4, 3, step))
        place = pl.ds(pl.multiple_of(jnp.where(step == 6, 1, jnp.where(step == 7, 3, slot)) * half, half), half)

        @pl.when(step >= 1)
        def _():
            for which, buf in enumerate((up_all, down_all)):
                ring.copy(buf.at[place], buf.at[place], w_send.at[0], w_recv.at[slot, which], PARTNER).wait_recv()

        @pl.when(step == 2)
        def _():
            pl.semaphore_wait(free_slot.at[0], 1)
            start(w_near_t)
            start(w_near_t_core)
            start(att_out)

        @pl.when(step == 3)
        def _():
            start(w_near_f)

        @pl.when(step == 6)
        def _():
            pl.semaphore_wait(free_slot.at[1], 1)
            start(w_far)

        @pl.when(step == 7)
        def _():
            start(y_loads(0, 0))

        def rows_step(part, carry):
            rows = pl.ds(pl.multiple_of(part * half, half), half)
            quarter = pl.ds(part * fours, fours)
            hidden_act, slope = gelu_and_slope(dot_nt(u_all[0, rows, :], up_all[place, :]))
            d_pre = (slope * dot_nt(c_all[0, rows, :], down_all[place, :])).astype(BF16)
            acc[0, quarter] += dot_nn(hidden_act.astype(BF16), down_all[place, :]).reshape(fours, slab, hidden)
            acc[1, quarter] += dot_nn(d_pre, up_all[place, :]).reshape(fours, slab, hidden)
            return carry

        lax.fori_loop(0, 2, rows_step, 0)

        @pl.when(step == 1)
        def _():
            say_free(0, SAME_F)

        @pl.when(step == 4)
        def _():
            say_free(1, PARTNER)

        return carry

    lax.fori_loop(0, 8, feed_forward, 0)

    def finish(step, carry):
        slot = 7 - step
        buf = step % 2
        seq = ring.at_traced(slot)
        for copy in y_loads(step, buf):
            copy.wait()

        @pl.when(step < 7)
        def _():
            start(y_loads(step + 1, 1 - buf))

        @pl.when(step >= 2)
        def _():
            for copy in x_stores(step - 2, buf):
                copy.wait()

        y_first = spare[buf, 0]
        x_second = spare[buf, 1] - acc[0, seq]
        dy_first = spare[buf, 2] + rms_back(y_first, acc[1, seq])
        spare[buf, 3] = x_second
        spare[buf, 4] = dy_first
        uc_own[slot, 0] = rms_norm(x_second).astype(BF16)
        uc_own[slot, 1] = dy_first.astype(BF16)
        acc[0, seq] = jnp.zeros((slab, hidden), F32)
        acc[1, seq] = jnp.zeros((slab, hidden), F32)
        start(x_stores(step, buf))
        return carry

    lax.fori_loop(0, 8, finish, 0)
    for slot in (7, 6, 5, 4, 3, 2, 1):
        a2a_out[slot].start()
    uc_keep.start()
    two_out.start()
    two_keep.start()
    for step in (6, 7):
        for copy in x_stores(step, step % 2):
            copy.wait()

    def gradients(step, carry):
        first = step // 8
        tokens = (step % 8) // 2
        place = pl.ds(pl.multiple_of((4 - 4 * first) * half, half), half)

        @pl.when((step == 2) | (step == 4) | (step == 6))
        def _():
            for which, buf in enumerate((u_all, c_all)):
                ring.copy(buf.at[tokens], buf.at[tokens], uc_send.at[0], uc_recv.at[tokens, which], PARTNER).wait_recv()

        @pl.when(step == 4)
        def _():
            start(uc_pass)
            for index in (0, 1):
                a2a_out[SAME_O + index].wait_recv()
            start(a2a_pass)

        @pl.when(step == 8)
        def _():
            near.start()
            att_out[0].wait_recv()
            att_f_core.start()
            att_t.start()
            att_o.start()

        rows = pl.ds(pl.multiple_of((step % 2) * half, half), half)
        u_part, c_part = u_all[tokens, rows, :], c_all[tokens, rows, :]
        hidden_act, slope = gelu_and_slope(dot_nt(up_all[place, :], u_part))
        d_pre = (slope * dot_nt(down_all[place, :], c_part)).astype(BF16)
        acc[first, pl.ds(0, fours)] += dot_nn(d_pre, u_part).reshape(fours, slab, hidden)
        acc[first, pl.ds(fours, fours)] += dot_nn(hidden_act.astype(BF16), c_part).reshape(fours, slab, hidden)
        return carry

    lax.fori_loop(0, 16, gradients, 0)
    out_own = pltpu.make_async_copy(acc.at[1], part_own, load_sem.at[1])
    out_own.start()
    for copy in w_own + w_near_t + w_near_t_core + w_near_f + w_far + uc_out + uc_pass:
        copy.wait_send()
    say_free(2, SAME_T)

    def relation_of(step):
        base = step % 4
        return jnp.where(base == 0, 2, jnp.where(base == 3, 3, base - 1))

    def qkv_rows(buf):
        return pl.ds(pl.multiple_of(buf * 6 * dim, 2 * dim), 6 * dim)

    def wo_rows(buf):
        return pl.ds(pl.multiple_of(12 * dim + buf * 2 * dim, 2 * dim), 2 * dim)

    def head_loads(relation, buf):
        copies = []
        for index in (0, 1):
            head = att_full.at[relation * 2 + 1 - index]
            first, second = (pl.ds(pl.multiple_of(base + index * size, dim), size) for base, size in ((buf * 6 * dim, 3 * dim), (12 * dim + buf * 2 * dim, dim)))
            copies.append(pltpu.make_async_copy(head.at[pl.ds(0, 3 * dim)], up_all.at[first], head_sem.at[buf, index, 0]))
            copies.append(pltpu.make_async_copy(head.at[pl.ds(3 * dim, dim)], up_all.at[second], head_sem.at[buf, index, 1]))
        return copies

    def rows_of(slot):
        return pl.ds(slot * slab, slab)

    def seq_loads(seq, src, src_slot, slot):
        return [pltpu.make_async_copy(src.at[src_slot, which], u_all.at[2 * seq + which, rows_of(slot)], seq_sem.at[2 * seq + which, slot]) for which in (0, 1)]

    seq_own = [copy for slot in range(8) for copy in seq_loads(0, uc_seq, slot, slot)]
    seq_two = [copy for slot in range(4) for copy in seq_loads(1, uc_two, slot, slot)]
    uc_to_t = [
        ring.copy(uc_seq.at[slot, which], u_all.at[2 + which, rows_of(4 + index)], far_sem.at[0, 2 * index + which], far_sem.at[1, 2 * index + which], SAME_T)
        for index, slot in enumerate((0, 1, 4, 5))
        for which in (0, 1)
    ]
    core_copies = [ring.copy(spare.at[index, pl.ds(0, 4)], acc.at[0, pl.ds(0, 4)], core_send.at[index], core_recv.at[index], PARTNER) for index in (0, 1)]
    f_copy = ring.copy(part_keep.at[0], acc.at[0, pl.ds(4, 4)], f_sem.at[0], f_sem.at[1], SAME_F)

    o_src = c_all.at[0]
    o_out = [
        ring.copy(o_src.at[rows_of(SAME_O)], o_relay.at[0], o_send.at[6], o_relay_recv.at[0], SAME_T),
        ring.copy(o_src.at[rows_of(OTHER_O)], o_relay.at[1], o_send.at[7], o_relay_recv.at[1], SAME_F),
    ] + [ring.copy(o_src.at[rows_of(slot)], o_pos.at[ring.me], o_send.at[slot], o_recv.at[slot], slot) for slot in (5, 4, 3, 2, 1)]
    o_pass = [
        ring.copy(o_relay.at[0], o_pos.at[ring.at(SAME_T)], o_send.at[8], o_recv.at[SAME_O], SAME_F),
        ring.copy(o_relay.at[1], o_pos.at[ring.at(SAME_F)], o_send.at[9], o_recv.at[OTHER_O], OTHER_T),
    ]
    o_keep = pltpu.make_async_copy(o_src.at[rows_of(0)], o_pos.at[ring.me], o_send.at[0])

    late = slab - LATE_ROWS
    early = {slot: late if slot in (SAME_F, OTHER_T) else slab for slot in range(1, 6)}
    du_out = [
        ring.copy(acc.at[1, SAME_O], to_f.at[pl.ds(0, slab)], du_send.at[6], du_relay_recv.at[0], SAME_T),
        ring.copy(acc.at[1, OTHER_O], to_other_t.at[pl.ds(0, slab)], du_send.at[7], du_relay_recv.at[1], SAME_F),
    ] + [ring.copy(acc.at[1, slot, pl.ds(0, early[slot])], du_pos.at[ring.me, pl.ds(0, early[slot])], du_send.at[slot], du_recv.at[slot], slot) for slot in (5, 4, 3, 2, 1)]
    du_keep = pltpu.make_async_copy(acc.at[1, 0], du_pos.at[ring.me], du_send.at[0])
    du_late = [
        pltpu.make_async_copy(acc.at[1, slot, pl.ds(late, slab - late)], dst.at[pl.ds(slab, slab - late)], du_send.at[sem])
        for slot, dst, sem in ((SAME_F, to_f, 8), (OTHER_T, to_other_t, 9))
    ]

    att_f_core.wait_recv()
    att_keep.wait()
    att_out[1].wait_recv()
    start(head_loads(2, 0))
    spare[...] = jnp.zeros_like(spare)
    part_keep[...] = jnp.zeros_like(part_keep)
    uc_keep.wait()
    for slot in range(1, 8):
        ring.copy(uc_own.at[slot], uc_seq.at[slot], a2a_send.at[0], a2a_recv.at[slot], PARTNER).wait_recv()
    start(seq_own)
    pl.semaphore_wait(free_slot.at[2], 1)
    start(uc_to_t)
    two_out.wait_recv()
    two_keep.wait()
    start(seq_two)
    out_own.wait()
    acc[1] = jnp.zeros(acc.shape[1:], F32)
    for copy in seq_own:
        copy.wait()

    def chip_step(step, carry):
        buf = step % 2
        seq = step // 4
        relation = relation_of(step)

        @pl.when(step == 4)
        def _():
            near.wait_send()
            say_free(3, SAME_F)
            say_free(4, PARTNER)
            for copy in seq_two:
                copy.wait()
            for copy in uc_to_t:
                copy.wait_recv()

        for copy in head_loads(0, buf):
            copy.wait()

        @pl.when((step == 0) | (step == 3) | (step == 4))
        def _():
            start(head_loads(relation_of(step + 1), 1 - buf))

        heads = [ring.at_traced(relation * 2 + other) for other in (1, 0)]
        wo_copies = [
            pltpu.make_async_copy(up_all.at[pl.ds(pl.multiple_of(12 * dim + (2 * buf + index) * dim, dim), dim)], wo_full.at[head], wo_sem.at[index])
            for index, head in enumerate(heads)
        ]
        start(wo_copies)
        c_all[2, :, pl.ds(0, 6 * dim)] = dot_nt(u_all[2 * seq], up_all[qkv_rows(buf), :]).astype(BF16)
        c_all[2, :, pl.ds(6 * dim, 2 * dim)] = dot_nt(u_all[2 * seq + 1], up_all[wo_rows(buf), :]).astype(BF16)
        for index, head in enumerate(heads):
            columns = pl.ds(pl.multiple_of(head * dim, dim), dim)
            own = pl.ds(index * 3 * dim, 3 * dim)
            query, key, value = (c_all[2, :, pl.ds((index * 3 + part) * dim, dim)] for part in range(3))
            d_out = c_all[2, :, pl.ds((6 + index) * dim, dim)]
            scores = dot_nt(query, key) * (scale * LOG2_E)
            grown = jnp.exp2(scores - jnp.max(scores, axis=-1, keepdims=True))
            prob = grown * (1.0 / jnp.sum(grown, axis=-1, keepdims=True))
            prob_b = prob.astype(BF16)
            c_all[seq, :, columns] = dot_nn(prob_b, value).astype(BF16)
            d_prob = dot_nt(d_out, value)
            d_score = (prob * (d_prob - jnp.sum(d_prob * prob, axis=-1, keepdims=True)) * scale).astype(BF16)
            c_all[3, :, pl.ds(index * 3 * dim, dim)] = dot_nn(d_score, key).astype(BF16)
            c_all[3, :, pl.ds((index * 3 + 1) * dim, dim)] = dot_nn(query.T, d_score).T.astype(BF16)
            c_all[3, :, pl.ds((index * 3 + 2) * dim, dim)] = dot_nn(d_out.T, prob_b).T.astype(BF16)
            @pl.when((step < 2) | (step >= 4))
            def _():
                dst = (spare, part_keep)[index].at[buf]
                dst[pl.ds(0, 3)] += dot_tn(c_all[3, :, own], u_all[2 * seq]).reshape(3, dim, hidden)
                dst[3] += dot_tn(c_all[seq, :, columns], u_all[2 * seq + 1])

            if index == 0:
                @pl.when(step == 1)
                def _():
                    att_t.wait_recv()
                    att_t_core.start()

                @pl.when(step == 4)
                def _():
                    pl.semaphore_wait(free_slot.at[4], 1)
                    core_copies[0].start()

                @pl.when(step == 5)
                def _():
                    pl.semaphore_wait(free_slot.at[4], 1)
                    core_copies[1].start()

        @pl.when(step < 4)
        def _():
            def du_tile(part, carry):
                rows = pl.ds(pl.multiple_of(part * half, half), half)
                acc[1, pl.ds(part * fours, fours)] += dot_nn(c_all[3, rows, pl.ds(0, 6 * dim)], up_all[qkv_rows(buf), :]).reshape(fours, slab, hidden)
                return carry

            lax.fori_loop(0, 2, du_tile, 0)

        @pl.when(step == 1)
        def _():
            att_t_core.wait_recv()
            start(head_loads(1, 0))

        @pl.when(step == 2)
        def _():
            att_o.wait_recv()
            att_o_core.start()
            att_o_core.wait_recv()
            start(head_loads(3, 1))

        @pl.when(step == 3)
        def _():
            start(o_out)
            start(du_out)
            start(du_late)
            o_keep.start()
            du_keep.start()

        @pl.when(step == 4)
        def _():
            core_copies[0].wait_recv()
            part_keep[0] += acc[0, pl.ds(0, 4)]
            say_free(4, PARTNER)
            pl.semaphore_wait(free_slot.at[3], 1)
            f_copy.start()

        for copy in wo_copies:
            copy.wait()
        return carry

    lax.fori_loop(0, 6, chip_step, 0)
    for copy in o_out[:2]:
        copy.wait_recv()
    start(o_pass)
    core_copies[1].wait_recv()
    part_keep[1] += acc[0, pl.ds(0, 4)]
    for copy in du_out[2:]:
        copy.wait_recv()
    for slot in range(1, 8):
        ring.copy(o_pos.at[0], o_pos.at[ring.at(slot)], near_sem.at[0], o_recv.at[slot], PARTNER).wait_recv()
    for copy in du_out[:2]:
        copy.wait_recv()
    near.wait_recv()
    f_copy.wait_recv()
    part_keep[1] += acc[0, pl.ds(4, 4)]
    d_att_copy = pltpu.make_async_copy(part_keep.at[1], d_att, load_sem.at[0])
    d_att_copy.start()

    sends = att_out + [att_t, att_o, att_f_core, att_t_core, att_o_core] + list(a2a_out.values()) + a2a_pass + [two_out]
    for copy in sends + o_out + du_out + o_pass + uc_to_t + core_copies + [f_copy]:
        copy.wait_send()
    for copy in du_late:
        copy.wait()
    o_keep.wait()
    du_keep.wait()
    d_att_copy.wait()


def block_call(y_one, y_two, dy_one, dy_two, w_up, w_down, w_qkv, w_out):
    slabs, slab, hidden = y_one.shape
    tokens = slabs * slab
    ffn = w_down.shape[0]
    dim = w_out.shape[0]
    any_spec = pl.BlockSpec(memory_space=pl.ANY)
    dma, vmem, wide, narrow = pltpu.SemaphoreType.DMA, pltpu.VMEM, F32, BF16
    results = [
        ((slabs, slab, hidden), wide), ((slabs, slab, hidden), wide), ((slabs, slab, hidden), wide), ((slabs, slab, hidden), wide),
        ((4, dim, hidden), wide), ((slabs, slab, hidden), narrow), ((slabs, slab, hidden), wide), ((8, dim, hidden), narrow),
        ((slab + LATE_ROWS, hidden), wide), ((slab + LATE_ROWS, hidden), wide),
    ]
    landing = [
        ((8, 2, slab, hidden), narrow), ((4, 2, slab, hidden), narrow), ((8, 4 * dim, hidden), narrow), ((2, slab, hidden), narrow),
    ]
    scratch = [
        vmem((4, tokens, hidden), BF16), vmem((4, tokens, hidden), BF16), vmem((6 * ffn, hidden), BF16), vmem((6 * ffn, hidden), BF16),
        vmem((2, slabs, slab, hidden), F32), vmem((2, 5, slab, hidden), F32), vmem((2, 4, dim, hidden), F32),
        vmem((8, 2, slab, hidden), BF16), vmem((4 * dim, hidden), BF16),
        dma((8,)), dma((2, 3)), dma((2, 2)), dma((14,)), dma((8, 2)), dma((6,)), dma((4, 2)), dma((7,)), dma((8,)), dma((11,)), dma((8,)), dma((3,)), dma((2,)), dma((2,)),
        dma((4, 8)), dma((2, 2, 2)), dma((2,)), dma((2,)), dma((2,)), dma((2,)), dma((2, 8)), dma((10,)), dma((8,)), dma((10,)), dma((8,)), dma((2,)), dma((2,)),
        pltpu.SemaphoreType.REGULAR((5,)),
    ]
    return pl.pallas_call(
        functools.partial(block_kernel, dim ** -0.5),
        out_shape=[jax.ShapeDtypeStruct(shape, dtype) for shape, dtype in results + landing],
        in_specs=[any_spec] * 8,
        out_specs=[any_spec] * (len(results) + len(landing)),
        scratch_shapes=scratch,
        compiler_params=pltpu.CompilerParams(collective_id=0, has_side_effects=True, vmem_limit_bytes=VMEM_LIMIT),
        cost_estimate=pl.CostEstimate(flops=120 * 10**9, bytes_accessed=128 * 2**20, transcendentals=0),
        name="block",
    )(y_one, y_two, dy_one, dy_two, w_up.reshape(8, hidden // 8, ffn), w_down, w_qkv.reshape(3, 8, hidden // 8, dim), w_out)[: len(results)]


def finish_kernel(
    y_one, o_pos, wo_full, x_two, dx_one, dy_two, du_pos, part_own, near_recv, d_att,
    x_one_out, x_two_out, dx_one_out, dx_two_out, dw_up, dw_down, dw_qkv, dw_out,
    y_buf, o_buf, wo_buf, x_buf, dx_buf, dy_buf, du_buf, own_buf, near_buf, att_buf, up_out, qkv_out, load_sem, store_sem,
):
    tokens = y_buf.shape[0]
    dim = wo_buf.shape[0] // 8
    chunk = 256
    chunks = [pl.ds(index * chunk, chunk) for index in range(tokens // chunk)]

    def pieces(src, dst, sem, row):
        return [pltpu.make_async_copy(src.at[rows], dst.at[rows], sem.at[row, index]) for index, rows in enumerate(chunks)]

    def whole(src, dst, sem, row):
        return pltpu.make_async_copy(src, dst, sem.at[row, 0])

    ring = Ring()
    slab = tokens // 8
    sizes = (slab, slab, slab, slab - LATE_ROWS, slab - LATE_ROWS, slab)
    slots = [pl.ds(pl.multiple_of(ring.at(slot) * slab, slab), size) for slot, size in enumerate(sizes)]

    def slabs(src, dst, sem, row):
        return [pltpu.make_async_copy(src.at[rows], dst.at[rows], sem.at[row, index]) for index, rows in enumerate(slots)]

    x_in, dy_in, du_in = pieces(x_two, x_buf, load_sem, 0), slabs(dy_two, dy_buf, load_sem, 1), slabs(du_pos, du_buf, load_sem, 2)
    y_in, o_in = pieces(y_one, y_buf, load_sem, 3), pieces(o_pos, o_buf, load_sem, 4)
    wo_in, dx_in = whole(wo_full, wo_buf, load_sem, 5), whole(dx_one, dx_buf, load_sem, 6)
    own_in, near_in, att_in = whole(part_own, own_buf, load_sem, 7), whole(near_recv, near_buf, load_sem, 8), whole(d_att, att_buf, load_sem, 9)
    for group in (x_in, *zip(dy_in, du_in)):
        for copy in group:
            copy.start()
    for copy in (dx_in, wo_in):
        copy.start()
    for group in zip(y_in, o_in):
        for copy in group:
            copy.start()
    for copy in (own_in, near_in, att_in):
        copy.start()

    x_store, dx2_store, x1_store = pieces(x_buf, x_two_out, store_sem, 0), slabs(dy_buf, dx_two_out, store_sem, 1), pieces(y_buf, x_one_out, store_sem, 2)
    for index in range(len(chunks)):
        x_in[index].wait()
        x_store[index].start()
    for index, rows in enumerate(slots):
        dy_in[index].wait()
        du_in[index].wait()
        dy_buf[rows, :] += rms_back(x_buf[rows, :], du_buf[rows, :])
        dx2_store[index].start()
    dx_in.wait()
    dx_store = whole(dx_buf, dx_one_out, store_sem, 3)
    dx_store.start()
    wo_in.wait()
    for index, rows in enumerate(chunks):
        y_in[index].wait()
        o_in[index].wait()
        y_buf[rows, :] -= dot_nn(o_buf[rows, :], wo_buf[...])
        x1_store[index].start()
    own_in.wait()
    near_in.wait()
    ffn = up_out.shape[1]
    own_buf[pl.ds(ffn, ffn), :] += near_buf[pl.ds(ffn, ffn), :]
    down_store = whole(own_buf.at[pl.ds(ffn, ffn)], dw_down, store_sem, 7)
    down_store.start()
    for part in range(up_out.shape[0] // ffn):
        columns = pl.ds(part * ffn, ffn)
        up_out[columns, :] = (own_buf[pl.ds(0, ffn), columns] + near_buf[pl.ds(0, ffn), columns]).T
    up_store = whole(up_out, dw_up, store_sem, 4)
    up_store.start()
    att_in.wait()
    for part in range(3):
        qkv_out[pl.ds(part, tokens, stride=3), 0, :] = att_buf[pl.ds(part * dim, dim), :].T
    qkv_store = whole(qkv_out, dw_qkv, store_sem, 5)
    qkv_store.start()
    out_store = whole(att_buf.at[pl.ds(3 * dim, dim)], dw_out, store_sem, 6)
    out_store.start()
    for copy in x_store + dx2_store + x1_store + [dx_store, up_store, qkv_store, out_store, down_store]:
        copy.wait()


def finish_call(y_one, o_pos, wo_full, x_two, dx_one, dy_two, du_pos, part_own, near_recv, d_att):
    tokens, hidden = y_one.shape
    ffn = part_own.shape[0] // 2
    dim = d_att.shape[0] // 4
    any_spec = pl.BlockSpec(memory_space=pl.ANY)
    dma, vmem = pltpu.SemaphoreType.DMA, pltpu.VMEM
    state = (tokens, hidden)
    out_shape = [jax.ShapeDtypeStruct(shape, F32) for shape in (state, state, state, state, (hidden, ffn), (ffn, hidden), (3 * hidden, 1, dim), (dim, hidden))]
    scratch = [
        vmem(state, F32), vmem(state, BF16), vmem((hidden, hidden), BF16), vmem(state, F32), vmem(state, F32), vmem(state, F32), vmem(state, F32),
        vmem(part_own.shape, F32), vmem(part_own.shape, F32), vmem(d_att.shape, F32), vmem((hidden, ffn), F32), vmem((3 * hidden, 1, dim), F32),
        dma((10, 6)), dma((8, 6)),
    ]
    return pl.pallas_call(
        finish_kernel,
        out_shape=out_shape,
        in_specs=[any_spec] * 10,
        out_specs=[any_spec] * 8,
        scratch_shapes=scratch,
        compiler_params=pltpu.CompilerParams(vmem_limit_bytes=VMEM_LIMIT),
        cost_estimate=pl.CostEstimate(flops=2 * 10**9, bytes_accessed=52 * 2**20, transcendentals=0),
        name="finish",
    )(y_one, o_pos, wo_full, x_two, dx_one, dy_two, du_pos, part_own, near_recv, d_att)


def last_kernel(x_two, dy_two, du_far, du_far_other, dx_two_in, dx_two_out, x_buf, dy_buf, du_buf, load_sem, store_sem):
    ring = Ring()
    slab = x_buf.shape[1]
    early = slab - LATE_ROWS
    loads, stores, sizes = [], [], (slab, slab, LATE_ROWS, LATE_ROWS)
    for index, (slot, du, skip) in enumerate(((SAME_O, du_far, 0), (OTHER_O, du_far_other, 0), (SAME_F, du_far, early), (OTHER_T, du_far_other, early))):
        size = sizes[index]
        rows = pl.ds(pl.multiple_of(ring.at(slot) * slab + skip, 16), size)
        sources = ((x_two.at[rows], x_buf), (dy_two.at[rows], dy_buf), (du.at[pl.ds(slab if skip else 0, size)], du_buf))
        loads.append([pltpu.make_async_copy(src, dst.at[index, pl.ds(0, size)], load_sem.at[index, which]) for which, (src, dst) in enumerate(sources)])
        stores.append(pltpu.make_async_copy(dy_buf.at[index, pl.ds(0, size)], dx_two_out.at[rows], store_sem.at[index]))
    for copies in loads:
        for copy in copies:
            copy.start()
    for index, copies in enumerate(loads):
        for copy in copies:
            copy.wait()
        rows = pl.ds(0, sizes[index])
        dy_buf[index, rows, :] += rms_back(x_buf[index, rows, :], du_buf[index, rows, :])
        stores[index].start()
    for copy in stores:
        copy.wait()


def last_call(x_two, dy_two, du_far, du_far_other, dx_two):
    tokens, hidden = x_two.shape
    any_spec = pl.BlockSpec(memory_space=pl.ANY)
    buf = pltpu.VMEM((4, tokens // 8, hidden), F32)
    return pl.pallas_call(
        last_kernel,
        out_shape=jax.ShapeDtypeStruct(dx_two.shape, F32),
        in_specs=[any_spec] * 5,
        out_specs=any_spec,
        input_output_aliases={4: 0},
        scratch_shapes=[buf, buf, buf, pltpu.SemaphoreType.DMA((4, 3)), pltpu.SemaphoreType.DMA((4,))],
        cost_estimate=pl.CostEstimate(flops=10**6, bytes_accessed=4 * 2**20, transcendentals=0),
        name="last",
    )(x_two, dy_two, du_far, du_far_other, dx_two)


def local_backward(y_one, y_two, dy_one, dy_two, w_qkv, w_out, w_up, w_down):
    hidden = y_one.shape[2]
    _, _, _, parts, dim = w_qkv.shape
    qkv_parts = jnp.swapaxes(w_qkv[0, :, 0], 0, 1)
    results = block_call(y_one, y_two, dy_one, dy_two, w_up[0], w_down[0], qkv_parts, w_out[0, 0])
    x_two, dx_one, part_own, near_recv, d_att, o_pos, du_pos, wo_full = (tensor.reshape(-1, hidden) for tensor in results[:8])
    devices = range(lax.axis_size("tp"))
    to_f = [(device, (3 - device // 2) * 2 + device % 2) for device in devices]
    to_other_t = [(device, 4 * (device // 4) + 3 - device % 4) for device in devices]
    du_far, du_far_other = lax.ppermute(results[8], "tp", to_f), lax.ppermute(results[9], "tp", to_other_t)
    y_flat, dy_flat = y_one.reshape(-1, hidden), dy_two.reshape(-1, hidden)
    *states, dw_up, dw_down, dw_qkv, dw_out = finish_call(y_flat, o_pos, wo_full, x_two, dx_one, dy_flat, du_pos, part_own, near_recv, d_att)
    states[3] = last_call(x_two, dy_flat, du_far, du_far_other, states[3])
    states = [tensor.reshape(y_one.shape) for tensor in states]
    return (*states, dw_qkv.reshape(1, hidden, 1, parts, dim), dw_out[None, None], dw_up[None], dw_down[None])


def solution(mesh):
    state_spec = P("dp", "tp", None)
    in_specs = (state_spec, state_spec, state_spec, state_spec, P(None, None, "tp", None, None), P(None, "tp", None, None), P(None, None, "tp"), P(None, "tp", None))
    out_specs = (state_spec, state_spec, state_spec, state_spec, P("dp", None, "tp", None, None), P("dp", "tp", None, None), P("dp", None, "tp"), P("dp", "tp", None))
    return jax.shard_map(local_backward, mesh=mesh, in_specs=in_specs, out_specs=out_specs, check_vma=False)
```

```python
import functools

import jax
import jax.numpy as jnp
from jax import lax
from jax.experimental import pallas as pl
from jax.experimental.pallas import tpu as pltpu
from jax.sharding import PartitionSpec as P

RMS_EPS = 1e-6
LOG2_E = 1.4426950408889634
LATE_ROWS = 80
MESH = pl.DeviceIdType.MESH
BF16, F32 = jnp.bfloat16, jnp.float32
VMEM_LIMIT = 64 * 1024 * 1024 - 65536


def inv_rms(tensor):
    return lax.rsqrt(jnp.mean(tensor * tensor, axis=-1, keepdims=True) + RMS_EPS)


def rms_norm(tensor):
    return tensor * inv_rms(tensor)


def rms_back(tensor, grad_in):
    scale = inv_rms(tensor)
    return scale * grad_in - tensor * (scale * scale * scale) * jnp.mean(grad_in * tensor, axis=-1, keepdims=True)


def gelu_and_slope(tensor):
    root = (2.0 / jnp.pi) ** 0.5
    squared = tensor * tensor
    tanh = jnp.tanh(root * (tensor + 0.044715 * (tensor * squared)))
    cdf = 0.5 * (1.0 + tanh)
    slope = cdf + (0.5 * root) * tensor * ((1.0 - tanh * tanh) * (1.0 + (3 * 0.044715) * squared))
    return tensor * cdf, slope


def dot_nn(left, right):
    return lax.dot_general(left, right, (((1,), (0,)), ((), ())), preferred_element_type=F32)


def dot_nt(left, right):
    return lax.dot_general(left, right, (((1,), (1,)), ((), ())), preferred_element_type=F32)


def dot_tn(left, right):
    return lax.dot_general(left, right, (((0,), (0,)), ((), ())), preferred_element_type=F32)


class Ring:
    def __init__(self):
        me = lax.axis_index("tp")
        chip, core = me // 2, me % 2
        self.me, self.chip, self.core = me, chip, core
        self.chips = (chip, chip + 1 - 2 * (chip % 2), 3 - chip, (chip + 2) % 4)

    def at(self, slot):
        core = self.core if slot % 2 == 0 else 1 - self.core
        return self.chips[slot // 2] * 2 + core

    def at_traced(self, slot):
        relation, other = slot // 2, slot % 2
        own, near_t, near_f, opposite = self.chips
        chip = jnp.where(relation == 0, own, jnp.where(relation == 1, near_t, jnp.where(relation == 2, near_f, opposite)))
        return chip * 2 + (self.core + other) % 2

    def barrier(self):
        barrier = pltpu.get_barrier_semaphore()
        for slot in (1, 2, 3, 4, 5):
            pl.semaphore_signal(barrier, inc=1, device_id={"tp": self.at(slot)}, device_id_type=MESH)
        pl.semaphore_wait(barrier, 5)

    def copy(self, src, dst, send_sem, recv_sem, slot):
        return pltpu.make_async_remote_copy(src_ref=src, dst_ref=dst, send_sem=send_sem, recv_sem=recv_sem, device_id={"tp": self.at(slot)}, device_id_type=MESH)


PARTNER, SAME_T, OTHER_T, SAME_F, OTHER_F, SAME_O, OTHER_O = 1, 2, 3, 4, 5, 6, 7


def block_kernel(
    scale,
    y_one, y_two, dy_one, dy_two, w_up, w_down, w_qkv, w_out,
    x_two, dx_one, part_own, near_recv, d_att, o_pos, du_pos, wo_full, to_f,
    uc_seq, uc_two, att_full, o_relay, du_relay,
    u_all, c_all, up_all, down_all, acc, spare, part_keep, uc_own, att_own,
    load_sem, y_sem, x_sem, w_send, w_recv, uc_send, uc_recv, att_send, att_recv, a2a_send, a2a_recv, relay_recv, near_sem, two_sem,
    seq_sem, head_sem, wo_sem, core_send, core_recv, f_sem, far_sem, o_send, o_recv, du_send, du_recv, o_relay_recv, du_relay_recv, free_slot,
):
    ring = Ring()
    slabs, slab, hidden = acc.shape[1:]
    seq_len = slabs * slab
    half = seq_len // 2
    dim = w_out.shape[0]
    fours = slabs // 2

    def start(copies):
        for copy in copies:
            copy.start()

    def say_free(index, to):
        pl.semaphore_signal(free_slot.at[index], inc=1, device_id={"tp": ring.at(to)}, device_id_type=MESH)

    rooms = (0, 1, 2, 3, 4, 5, 1, 3)

    def room(slot):
        return pl.ds(rooms[slot] * half, half)

    def weight_pair(src_slot, dst_slot, to, index):
        return [
            ring.copy(buf.at[room(src_slot)], buf.at[room(dst_slot)], w_send.at[index + which], w_recv.at[dst_slot, which], to)
            for which, buf in enumerate((up_all, down_all))
        ]

    w_own = weight_pair(0, 1, PARTNER, 0) + weight_pair(0, 2, SAME_T, 2) + weight_pair(0, 4, SAME_F, 4)
    w_near_t = weight_pair(2, 6, SAME_F, 6)
    w_near_t_core = weight_pair(2, 3, PARTNER, 8)
    w_near_f = weight_pair(4, 5, PARTNER, 10)
    w_far = weight_pair(6, 7, PARTNER, 12)

    def uc_pair(src_slot, dst_slot, to, index):
        return [ring.copy(buf.at[src_slot], buf.at[dst_slot], uc_send.at[index + which], uc_recv.at[dst_slot, which], to) for which, buf in enumerate((u_all, c_all))]

    uc_out = uc_pair(0, 2, SAME_T, 0) + uc_pair(0, 1, PARTNER, 2)
    uc_pass = uc_pair(2, 3, PARTNER, 4)

    def att(src, dst_slot, to, index):
        return ring.copy(src, att_full.at[dst_slot], att_send.at[index], att_recv.at[dst_slot], to)

    att_keep = pltpu.make_async_copy(att_own, att_full.at[0], load_sem.at[6])
    att_out = [att(att_own, 4, SAME_F, 0), att(att_own, 1, PARTNER, 1)]
    att_t, att_o = att(att_own, 2, SAME_T, 2), att(att_full.at[4], 6, SAME_T, 3)
    att_f_core, att_t_core, att_o_core = att(att_full.at[4], 5, PARTNER, 4), att(att_full.at[2], 3, PARTNER, 5), att(att_full.at[6], 7, PARTNER, 6)

    a2a_out = {slot: ring.copy(uc_own.at[slot], uc_seq.at[slot], a2a_send.at[slot], a2a_recv.at[slot], slot) for slot in (1, 2, 3, 4, 5)}
    a2a_out[SAME_O] = ring.copy(uc_own.at[SAME_O], uc_two.at[2], a2a_send.at[SAME_O], relay_recv.at[0], SAME_F)
    a2a_out[OTHER_O] = ring.copy(uc_own.at[OTHER_O], uc_two.at[3], a2a_send.at[OTHER_O], relay_recv.at[1], OTHER_F)
    a2a_pass = [ring.copy(uc_two.at[2 + index], uc_seq.at[SAME_O + index], a2a_send.at[8 + index], a2a_recv.at[SAME_O + index], SAME_T) for index in (0, 1)]
    uc_keep = pltpu.make_async_copy(uc_own.at[0], uc_seq.at[0], load_sem.at[4])
    two_out = ring.copy(uc_own.at[OTHER_T], uc_two.at[1], a2a_send.at[10], relay_recv.at[2], PARTNER)
    two_keep = pltpu.make_async_copy(uc_own.at[SAME_T], uc_two.at[0], two_sem.at[0])
    near = ring.copy(acc.at[0], near_recv, near_sem.at[0], near_sem.at[1], SAME_F)

    loads = [
        pltpu.make_async_copy(w_down, down_all.at[room(0)], load_sem.at[0]),
        pltpu.make_async_copy(w_up, uc_own.at[:, 0, :, pl.ds(0, half)], load_sem.at[1]),
        pltpu.make_async_copy(y_one, acc.at[0], load_sem.at[2]),
        pltpu.make_async_copy(dy_two, acc.at[1], load_sem.at[3]),
        pltpu.make_async_copy(w_out, att_own.at[pl.ds(3 * dim, dim)], load_sem.at[7]),
    ]
    qkv_loads = [pltpu.make_async_copy(w_qkv.at[part], uc_own.at[:, 1, :, pl.ds(part * dim, dim)], y_sem.at[0, part]) for part in range(3)]
    start(loads)
    start(qkv_loads)
    ring.barrier()
    loads[0].wait()
    start(w_own[1::2])
    loads[1].wait()
    for part in range(half // dim):
        up_all[pl.ds(part * dim, dim), :] = uc_own[:, 0, :, pl.ds(part * dim, dim)].reshape(hidden, dim).T
    start(w_own[0::2])
    loads[2].wait()
    loads[3].wait()

    def normalize(step, carry):
        rows = pl.ds(pl.multiple_of(step * slab, slab), slab)
        u_all[0, rows, :] = rms_norm(acc[0, step]).astype(BF16)
        c_all[0, rows, :] = acc[1, step].astype(BF16)
        acc[0, step] = jnp.zeros((slab, hidden), F32)
        acc[1, step] = jnp.zeros((slab, hidden), F32)
        return carry

    lax.fori_loop(0, slabs, normalize, 0)
    start(uc_out)
    for part in range(3):
        qkv_loads[part].wait()
        att_own[pl.ds(part * dim, dim), :] = uc_own[:, 1, :, pl.ds(part * dim, dim)].reshape(hidden, dim).T
    loads[4].wait()
    att_keep.start()

    def y_loads(step, buf):
        seq = ring.at_traced(7 - step)
        return [pltpu.make_async_copy(src.at[seq], spare.at[buf, which], y_sem.at[buf, which]) for which, src in enumerate((y_one, y_two, dy_one))]

    def x_stores(step, buf):
        seq = ring.at_traced(7 - step)
        return [pltpu.make_async_copy(spare.at[buf, 3 + which], dst.at[seq], x_sem.at[buf, which]) for which, dst in enumerate((x_two, dx_one))]

    def feed_forward(step, carry):
        slot = jnp.where(step == 3, 4, jnp.where(step == 4, 3, step))
        place = pl.ds(pl.multiple_of(jnp.where(step == 6, 1, jnp.where(step == 7, 3, slot)) * half, half), half)

        @pl.when(step >= 1)
        def _():
            for which, buf in enumerate((up_all, down_all)):
                ring.copy(buf.at[place], buf.at[place], w_send.at[0], w_recv.at[slot, which], PARTNER).wait_recv()

        @pl.when(step == 2)
        def _():
            pl.semaphore_wait(free_slot.at[0], 1)
            start(w_near_t)
            start(w_near_t_core)
            start(att_out)

        @pl.when(step == 3)
        def _():
            start(w_near_f)

        @pl.when(step == 6)
        def _():
            pl.semaphore_wait(free_slot.at[1], 1)
            start(w_far)

        @pl.when(step == 7)
        def _():
            start(y_loads(0, 0))

        def rows_step(part, carry):
            rows = pl.ds(pl.multiple_of(part * half, half), half)
            quarter = pl.ds(part * fours, fours)
            hidden_act, slope = gelu_and_slope(dot_nt(u_all[0, rows, :], up_all[place, :]))
            d_pre = (slope * dot_nt(c_all[0, rows, :], down_all[place, :])).astype(BF16)
            acc[0, quarter] += dot_nn(hidden_act.astype(BF16), down_all[place, :]).reshape(fours, slab, hidden)
            acc[1, quarter] += dot_nn(d_pre, up_all[place, :]).reshape(fours, slab, hidden)
            return carry

        lax.fori_loop(0, 2, rows_step, 0)

        @pl.when(step == 1)
        def _():
            say_free(0, SAME_F)

        @pl.when(step == 4)
        def _():
            say_free(1, PARTNER)

        return carry

    lax.fori_loop(0, 8, feed_forward, 0)

    def finish(step, carry):
        slot = 7 - step
        buf = step % 2
        seq = ring.at_traced(slot)
        for copy in y_loads(step, buf):
            copy.wait()

        @pl.when(step < 7)
        def _():
            start(y_loads(step + 1, 1 - buf))

        @pl.when(step >= 2)
        def _():
            for copy in x_stores(step - 2, buf):
                copy.wait()

        y_first = spare[buf, 0]
        x_second = spare[buf, 1] - acc[0, seq]
        dy_first = spare[buf, 2] + rms_back(y_first, acc[1, seq])
        spare[buf, 3] = x_second
        spare[buf, 4] = dy_first
        uc_own[slot, 0] = rms_norm(x_second).astype(BF16)
        uc_own[slot, 1] = dy_first.astype(BF16)
        acc[0, seq] = jnp.zeros((slab, hidden), F32)
        acc[1, seq] = jnp.zeros((slab, hidden), F32)
        start(x_stores(step, buf))
        return carry

    lax.fori_loop(0, 8, finish, 0)
    for slot in (7, 6, 5, 4, 3, 2, 1):
        a2a_out[slot].start()
    uc_keep.start()
    two_out.start()
    two_keep.start()
    for step in (6, 7):
        for copy in x_stores(step, step % 2):
            copy.wait()

    def gradients(step, carry):
        first = step // 8
        tokens = (step % 8) // 2
        place = pl.ds(pl.multiple_of((4 - 4 * first) * half, half), half)

        @pl.when((step == 2) | (step == 4) | (step == 6))
        def _():
            for which, buf in enumerate((u_all, c_all)):
                ring.copy(buf.at[tokens], buf.at[tokens], uc_send.at[0], uc_recv.at[tokens, which], PARTNER).wait_recv()

        @pl.when(step == 4)
        def _():
            start(uc_pass)
            for index in (0, 1):
                a2a_out[SAME_O + index].wait_recv()
            start(a2a_pass)

        @pl.when(step == 8)
        def _():
            near.start()
            att_out[0].wait_recv()
            att_f_core.start()
            att_t.start()
            att_o.start()

        rows = pl.ds(pl.multiple_of((step % 2) * half, half), half)
        u_part, c_part = u_all[tokens, rows, :], c_all[tokens, rows, :]
        hidden_act, slope = gelu_and_slope(dot_nt(up_all[place, :], u_part))
        d_pre = (slope * dot_nt(down_all[place, :], c_part)).astype(BF16)
        acc[first, pl.ds(0, fours)] += dot_nn(d_pre, u_part).reshape(fours, slab, hidden)
        acc[first, pl.ds(fours, fours)] += dot_nn(hidden_act.astype(BF16), c_part).reshape(fours, slab, hidden)
        return carry

    lax.fori_loop(0, 16, gradients, 0)
    out_own = pltpu.make_async_copy(acc.at[1], part_own, load_sem.at[1])
    out_own.start()
    for copy in w_own + w_near_t + w_near_t_core + w_near_f + w_far + uc_out + uc_pass:
        copy.wait_send()
    say_free(2, SAME_T)

    def relation_of(step):
        base = step % 4
        return jnp.where(base == 0, 2, jnp.where(base == 3, 3, base - 1))

    def qkv_rows(buf):
        return pl.ds(pl.multiple_of(buf * 6 * dim, 2 * dim), 6 * dim)

    def wo_rows(buf):
        return pl.ds(pl.multiple_of(12 * dim + buf * 2 * dim, 2 * dim), 2 * dim)

    def head_loads(relation, buf):
        copies = []
        for index in (0, 1):
            head = att_full.at[relation * 2 + 1 - index]
            first, second = (pl.ds(pl.multiple_of(base + index * size, dim), size) for base, size in ((buf * 6 * dim, 3 * dim), (12 * dim + buf * 2 * dim, dim)))
            copies.append(pltpu.make_async_copy(head.at[pl.ds(0, 3 * dim)], up_all.at[first], head_sem.at[buf, index, 0]))
            copies.append(pltpu.make_async_copy(head.at[pl.ds(3 * dim, dim)], up_all.at[second], head_sem.at[buf, index, 1]))
        return copies

    def rows_of(slot):
        return pl.ds(slot * slab, slab)

    def seq_loads(seq, src, src_slot, slot):
        return [pltpu.make_async_copy(src.at[src_slot, which], u_all.at[2 * seq + which, rows_of(slot)], seq_sem.at[2 * seq + which, slot]) for which in (0, 1)]

    seq_own = [copy for slot in range(8) for copy in seq_loads(0, uc_seq, slot, slot)]
    seq_two = [copy for slot in range(4) for copy in seq_loads(1, uc_two, slot, slot)]
    uc_to_t = [
        ring.copy(uc_seq.at[slot, which], u_all.at[2 + which, rows_of(4 + index)], far_sem.at[0, 2 * index + which], far_sem.at[1, 2 * index + which], SAME_T)
        for index, slot in enumerate((0, 1, 4, 5))
        for which in (0, 1)
    ]
    core_copies = [ring.copy(spare.at[index, pl.ds(0, 4)], acc.at[0, pl.ds(0, 4)], core_send.at[index], core_recv.at[index], PARTNER) for index in (0, 1)]
    f_copy = ring.copy(part_keep.at[0], acc.at[0, pl.ds(4, 4)], f_sem.at[0], f_sem.at[1], SAME_F)

    o_src = c_all.at[0]
    o_out = [
        ring.copy(o_src.at[rows_of(SAME_O)], o_relay.at[0], o_send.at[6], o_relay_recv.at[0], SAME_T),
        ring.copy(o_src.at[rows_of(OTHER_O)], o_relay.at[1], o_send.at[7], o_relay_recv.at[1], SAME_F),
    ] + [ring.copy(o_src.at[rows_of(slot)], o_pos.at[ring.me], o_send.at[slot], o_recv.at[slot], slot) for slot in (5, 4, 3, 2, 1)]
    o_pass = [
        ring.copy(o_relay.at[0], o_pos.at[ring.at(SAME_T)], o_send.at[8], o_recv.at[SAME_O], SAME_F),
        ring.copy(o_relay.at[1], o_pos.at[ring.at(SAME_F)], o_send.at[9], o_recv.at[OTHER_O], OTHER_T),
    ]
    o_keep = pltpu.make_async_copy(o_src.at[rows_of(0)], o_pos.at[ring.me], o_send.at[0])

    late = slab - LATE_ROWS
    early = {slot: late if slot == SAME_F else slab for slot in range(1, 6)}
    du_out = [
        ring.copy(acc.at[1, SAME_O], to_f.at[pl.ds(0, slab)], du_send.at[6], du_relay_recv.at[0], SAME_T),
        ring.copy(acc.at[1, OTHER_O], du_relay, du_send.at[7], du_relay_recv.at[1], SAME_F),
    ] + [ring.copy(acc.at[1, slot, pl.ds(0, early[slot])], du_pos.at[ring.me, pl.ds(0, early[slot])], du_send.at[slot], du_recv.at[slot], slot) for slot in (5, 4, 3, 2, 1)]
    du_keep = pltpu.make_async_copy(acc.at[1, 0], du_pos.at[ring.me], du_send.at[0])
    du_late = pltpu.make_async_copy(acc.at[1, SAME_F, pl.ds(late, slab - late)], to_f.at[pl.ds(slab, slab - late)], du_send.at[8])
    du_pass = ring.copy(du_relay, du_pos.at[ring.at(SAME_F)], du_send.at[9], du_recv.at[OTHER_O], OTHER_T)

    att_f_core.wait_recv()
    att_keep.wait()
    att_out[1].wait_recv()
    start(head_loads(2, 0))
    uc_keep.wait()
    for slot in range(1, 8):
        ring.copy(uc_own.at[slot], uc_seq.at[slot], a2a_send.at[0], a2a_recv.at[slot], PARTNER).wait_recv()
    start(seq_own)
    pl.semaphore_wait(free_slot.at[2], 1)
    start(uc_to_t)
    two_out.wait_recv()
    two_keep.wait()
    start(seq_two)
    out_own.wait()
    acc[1] = jnp.zeros(acc.shape[1:], F32)
    for copy in seq_own:
        copy.wait()

    def chip_step(step, carry):
        buf = step % 2
        seq = step // 4
        relation = relation_of(step)

        @pl.when(step == 4)
        def _():
            near.wait_send()
            say_free(3, SAME_F)
            say_free(4, PARTNER)
            for copy in seq_two:
                copy.wait()
            for copy in uc_to_t:
                copy.wait_recv()

        for copy in head_loads(0, buf):
            copy.wait()

        @pl.when((step == 0) | (step == 3) | (step == 4))
        def _():
            start(head_loads(relation_of(step + 1), 1 - buf))

        kept = pl.ds(pl.multiple_of(jnp.where(step < 2, step, 2) * seq_len, seq_len), seq_len)
        heads = [ring.at_traced(relation * 2 + other) for other in (1, 0)]
        wo_copies = [
            pltpu.make_async_copy(up_all.at[pl.ds(pl.multiple_of(12 * dim + (2 * buf + index) * dim, dim), dim)], wo_full.at[head], wo_sem.at[index])
            for index, head in enumerate(heads)
        ]
        start(wo_copies)
        c_all[2, :, pl.ds(0, 6 * dim)] = dot_nt(u_all[2 * seq], up_all[qkv_rows(buf), :]).astype(BF16)
        c_all[2, :, pl.ds(6 * dim, 2 * dim)] = dot_nt(u_all[2 * seq + 1], up_all[wo_rows(buf), :]).astype(BF16)
        for index, head in enumerate(heads):
            columns = pl.ds(pl.multiple_of(head * dim, dim), dim)
            own = pl.ds(index * 3 * dim, 3 * dim)
            query, key, value = (c_all[2, :, pl.ds((index * 3 + part) * dim, dim)] for part in range(3))
            d_out = c_all[2, :, pl.ds((6 + index) * dim, dim)]
            scores = dot_nt(query, key) * (scale * LOG2_E)
            grown = jnp.exp2(scores - jnp.max(scores, axis=-1, keepdims=True))
            prob = grown * (1.0 / jnp.sum(grown, axis=-1, keepdims=True))
            prob_b = prob.astype(BF16)
            c_all[seq, :, columns] = dot_nn(prob_b, value).astype(BF16)
            d_prob = dot_nt(d_out, value)
            d_score = (prob * (d_prob - jnp.sum(d_prob * prob, axis=-1, keepdims=True)) * scale).astype(BF16)
            down_all[kept, pl.ds(index * 3 * dim, dim)] = dot_nn(d_score, key).astype(BF16)
            down_all[kept, pl.ds((index * 3 + 1) * dim, dim)] = dot_nn(query.T, d_score).T.astype(BF16)
            down_all[kept, pl.ds((index * 3 + 2) * dim, dim)] = dot_nn(d_out.T, prob_b).T.astype(BF16)
            @pl.when(step >= 4)
            def _():
                dst = (spare, part_keep)[index].at[buf]
                dst[pl.ds(0, 3)] += dot_tn(down_all[kept, own], u_all[2]).reshape(3, dim, hidden)
                dst[3] += dot_tn(c_all[1, :, columns], u_all[3])

            if index == 0:
                @pl.when(step == 1)
                def _():
                    att_t.wait_recv()
                    att_t_core.start()

                @pl.when(step == 4)
                def _():
                    pl.semaphore_wait(free_slot.at[4], 1)
                    core_copies[0].start()

                @pl.when(step == 5)
                def _():
                    pl.semaphore_wait(free_slot.at[4], 1)
                    core_copies[1].start()

        @pl.when(step == 1)
        def _():
            att_t_core.wait_recv()
            start(head_loads(1, 0))

        @pl.when(step == 2)
        def _():
            att_o.wait_recv()
            att_o_core.start()

        @pl.when(step < 4)
        def _():
            def du_tile(part, carry):
                rows = pl.ds(pl.multiple_of(jnp.where(step < 2, step, 2) * seq_len + part * half, half), half)
                acc[1, pl.ds(part * fours, fours)] += dot_nn(down_all[rows, pl.ds(0, 6 * dim)], up_all[qkv_rows(buf), :]).reshape(fours, slab, hidden)
                return carry

            lax.fori_loop(0, 2, du_tile, 0)

        @pl.when(step == 2)
        def _():
            att_o_core.wait_recv()
            start(head_loads(3, 1))

        @pl.when(step == 3)
        def _():
            start(o_out)
            start(du_out)
            du_late.start()
            o_keep.start()
            du_keep.start()

            def own_gradients(pair, carry):
                own_rows = pl.ds(pl.multiple_of(pair * seq_len, seq_len), seq_len)
                for index, other in enumerate((1, 0)):
                    columns = pl.ds(pl.multiple_of(ring.at_traced(relation_of(pair) * 2 + other) * dim, dim), dim)
                    dst = (spare, part_keep)[index].at[pair]
                    dst[pl.ds(0, 3)] = dot_tn(down_all[own_rows, pl.ds(index * 3 * dim, 3 * dim)], u_all[0]).reshape(3, dim, hidden)
                    dst[3] = dot_tn(c_all[0, :, columns], u_all[1])
                return carry

            lax.fori_loop(0, 2, own_gradients, 0)

        @pl.when(step == 4)
        def _():
            core_copies[0].wait_recv()
            part_keep[0] += acc[0, pl.ds(0, 4)]
            say_free(4, PARTNER)
            pl.semaphore_wait(free_slot.at[3], 1)
            f_copy.start()

        for copy in wo_copies:
            copy.wait()
        return carry

    lax.fori_loop(0, 6, chip_step, 0)
    for copy in o_out[:2]:
        copy.wait_recv()
    start(o_pass)
    du_out[1].wait_recv()
    du_pass.start()
    core_copies[1].wait_recv()
    part_keep[1] += acc[0, pl.ds(0, 4)]
    for copy in du_out[2:]:
        copy.wait_recv()
    for slot in range(1, 8):
        ring.copy(o_pos.at[0], o_pos.at[ring.at(slot)], near_sem.at[0], o_recv.at[slot], PARTNER).wait_recv()
    du_out[0].wait_recv()
    du_pass.wait_recv()
    near.wait_recv()
    f_copy.wait_recv()
    part_keep[1] += acc[0, pl.ds(4, 4)]
    d_att_copy = pltpu.make_async_copy(part_keep.at[1], d_att, load_sem.at[0])
    d_att_copy.start()

    sends = att_out + [att_t, att_o, att_f_core, att_t_core, att_o_core] + list(a2a_out.values()) + a2a_pass + [two_out]
    for copy in sends + o_out + du_out + o_pass + uc_to_t + core_copies + [du_pass, f_copy]:
        copy.wait_send()
    du_late.wait()
    o_keep.wait()
    du_keep.wait()
    d_att_copy.wait()


def block_call(y_one, y_two, dy_one, dy_two, w_up, w_down, w_qkv, w_out):
    slabs, slab, hidden = y_one.shape
    tokens = slabs * slab
    ffn = w_down.shape[0]
    dim = w_out.shape[0]
    any_spec = pl.BlockSpec(memory_space=pl.ANY)
    dma, vmem, wide, narrow = pltpu.SemaphoreType.DMA, pltpu.VMEM, F32, BF16
    results = [
        ((slabs, slab, hidden), wide), ((slabs, slab, hidden), wide), ((slabs, slab, hidden), wide), ((slabs, slab, hidden), wide),
        ((4, dim, hidden), wide), ((slabs, slab, hidden), narrow), ((slabs, slab, hidden), wide), ((8, dim, hidden), narrow),
        ((slab + LATE_ROWS, hidden), wide),
    ]
    landing = [
        ((8, 2, slab, hidden), narrow), ((4, 2, slab, hidden), narrow), ((8, 4 * dim, hidden), narrow), ((2, slab, hidden), narrow), ((slab, hidden), wide),
    ]
    scratch = [
        vmem((4, tokens, hidden), BF16), vmem((4, tokens, hidden), BF16), vmem((6 * ffn, hidden), BF16), vmem((6 * ffn, hidden), BF16),
        vmem((2, slabs, slab, hidden), F32), vmem((2, 5, slab, hidden), F32), vmem((2, 4, dim, hidden), F32),
        vmem((8, 2, slab, hidden), BF16), vmem((4 * dim, hidden), BF16),
        dma((8,)), dma((2, 3)), dma((2, 2)), dma((14,)), dma((8, 2)), dma((6,)), dma((4, 2)), dma((7,)), dma((8,)), dma((11,)), dma((8,)), dma((3,)), dma((2,)), dma((2,)),
        dma((4, 8)), dma((2, 2, 2)), dma((2,)), dma((2,)), dma((2,)), dma((2,)), dma((2, 8)), dma((10,)), dma((8,)), dma((10,)), dma((8,)), dma((2,)), dma((2,)),
        pltpu.SemaphoreType.REGULAR((5,)),
    ]
    return pl.pallas_call(
        functools.partial(block_kernel, dim ** -0.5),
        out_shape=[jax.ShapeDtypeStruct(shape, dtype) for shape, dtype in results + landing],
        in_specs=[any_spec] * 8,
        out_specs=[any_spec] * (len(results) + len(landing)),
        scratch_shapes=scratch,
        compiler_params=pltpu.CompilerParams(collective_id=0, has_side_effects=True, vmem_limit_bytes=VMEM_LIMIT),
        cost_estimate=pl.CostEstimate(flops=120 * 10**9, bytes_accessed=128 * 2**20, transcendentals=0),
        name="block",
    )(y_one, y_two, dy_one, dy_two, w_up.reshape(8, hidden // 8, ffn), w_down, w_qkv.reshape(3, 8, hidden // 8, dim), w_out)[: len(results)]


def finish_kernel(
    y_one, o_pos, wo_full, x_two, dx_one, dy_two, du_pos, part_own, near_recv, d_att,
    x_one_out, x_two_out, dx_one_out, dx_two_out, dw_up, dw_down, dw_qkv, dw_out,
    y_buf, o_buf, wo_buf, x_buf, dx_buf, dy_buf, du_buf, own_buf, near_buf, att_buf, up_out, qkv_out, load_sem, store_sem,
):
    tokens = y_buf.shape[0]
    dim = wo_buf.shape[0] // 8
    chunk = 256
    chunks = [pl.ds(index * chunk, chunk) for index in range(tokens // chunk)]

    def pieces(src, dst, sem, row):
        return [pltpu.make_async_copy(src.at[rows], dst.at[rows], sem.at[row, index]) for index, rows in enumerate(chunks)]

    def whole(src, dst, sem, row):
        return pltpu.make_async_copy(src, dst, sem.at[row, 0])

    ring = Ring()
    slab = tokens // 8
    sizes = {0: slab, PARTNER: slab, SAME_T: slab, OTHER_T: slab, SAME_F: slab - LATE_ROWS, OTHER_F: slab, OTHER_O: slab}
    slots = [pl.ds(pl.multiple_of(ring.at(slot) * slab, slab), size) for slot, size in sizes.items()]

    def slabs(src, dst, sem, row):
        return [pltpu.make_async_copy(src.at[rows], dst.at[rows], sem.at[row, index]) for index, rows in enumerate(slots)]

    x_in, dy_in, du_in = pieces(x_two, x_buf, load_sem, 0), slabs(dy_two, dy_buf, load_sem, 1), slabs(du_pos, du_buf, load_sem, 2)
    y_in, o_in = pieces(y_one, y_buf, load_sem, 3), pieces(o_pos, o_buf, load_sem, 4)
    wo_in, dx_in = whole(wo_full, wo_buf, load_sem, 5), whole(dx_one, dx_buf, load_sem, 6)
    own_in, near_in, att_in = whole(part_own, own_buf, load_sem, 7), whole(near_recv, near_buf, load_sem, 8), whole(d_att, att_buf, load_sem, 9)
    for group in (x_in, *zip(dy_in, du_in)):
        for copy in group:
            copy.start()
    for copy in (dx_in, wo_in):
        copy.start()
    for group in zip(y_in, o_in):
        for copy in group:
            copy.start()
    for copy in (own_in, near_in, att_in):
        copy.start()

    x_store, dx2_store, x1_store = pieces(x_buf, x_two_out, store_sem, 0), slabs(dy_buf, dx_two_out, store_sem, 1), pieces(y_buf, x_one_out, store_sem, 2)
    for index in range(len(chunks)):
        x_in[index].wait()
        x_store[index].start()
    for index, rows in enumerate(slots):
        dy_in[index].wait()
        du_in[index].wait()
        dy_buf[rows, :] += rms_back(x_buf[rows, :], du_buf[rows, :])
        dx2_store[index].start()
    dx_in.wait()
    dx_store = whole(dx_buf, dx_one_out, store_sem, 3)
    dx_store.start()
    wo_in.wait()
    for index, rows in enumerate(chunks):
        y_in[index].wait()
        o_in[index].wait()
        y_buf[rows, :] -= dot_nn(o_buf[rows, :], wo_buf[...])
        x1_store[index].start()
    own_in.wait()
    near_in.wait()
    ffn = up_out.shape[1]
    own_buf[pl.ds(ffn, ffn), :] += near_buf[pl.ds(ffn, ffn), :]
    down_store = whole(own_buf.at[pl.ds(ffn, ffn)], dw_down, store_sem, 7)
    down_store.start()
    for part in range(up_out.shape[0] // ffn):
        columns = pl.ds(part * ffn, ffn)
        up_out[columns, :] = (own_buf[pl.ds(0, ffn), columns] + near_buf[pl.ds(0, ffn), columns]).T
    up_store = whole(up_out, dw_up, store_sem, 4)
    up_store.start()
    att_in.wait()
    for part in range(3):
        qkv_out[pl.ds(part, tokens, stride=3), 0, :] = att_buf[pl.ds(part * dim, dim), :].T
    qkv_store = whole(qkv_out, dw_qkv, store_sem, 5)
    qkv_store.start()
    out_store = whole(att_buf.at[pl.ds(3 * dim, dim)], dw_out, store_sem, 6)
    out_store.start()
    for copy in x_store + dx2_store + x1_store + [dx_store, up_store, qkv_store, out_store, down_store]:
        copy.wait()


def finish_call(y_one, o_pos, wo_full, x_two, dx_one, dy_two, du_pos, part_own, near_recv, d_att):
    tokens, hidden = y_one.shape
    ffn = part_own.shape[0] // 2
    dim = d_att.shape[0] // 4
    any_spec = pl.BlockSpec(memory_space=pl.ANY)
    dma, vmem = pltpu.SemaphoreType.DMA, pltpu.VMEM
    state = (tokens, hidden)
    out_shape = [jax.ShapeDtypeStruct(shape, F32) for shape in (state, state, state, state, (hidden, ffn), (ffn, hidden), (3 * hidden, 1, dim), (dim, hidden))]
    scratch = [
        vmem(state, F32), vmem(state, BF16), vmem((hidden, hidden), BF16), vmem(state, F32), vmem(state, F32), vmem(state, F32), vmem(state, F32),
        vmem(part_own.shape, F32), vmem(part_own.shape, F32), vmem(d_att.shape, F32), vmem((hidden, ffn), F32), vmem((3 * hidden, 1, dim), F32),
        dma((10, 7)), dma((8, 7)),
    ]
    return pl.pallas_call(
        finish_kernel,
        out_shape=out_shape,
        in_specs=[any_spec] * 10,
        out_specs=[any_spec] * 8,
        scratch_shapes=scratch,
        compiler_params=pltpu.CompilerParams(vmem_limit_bytes=VMEM_LIMIT),
        cost_estimate=pl.CostEstimate(flops=2 * 10**9, bytes_accessed=52 * 2**20, transcendentals=0),
        name="finish",
    )(y_one, o_pos, wo_full, x_two, dx_one, dy_two, du_pos, part_own, near_recv, d_att)


def last_kernel(x_two, dy_two, du_far, dx_two_in, dx_two_out, x_buf, dy_buf, du_buf, load_sem, store_sem):
    ring = Ring()
    slab = x_buf.shape[1]
    loads, stores, sizes = [], [], (slab, LATE_ROWS)
    for index, (slot, skip) in enumerate(((SAME_O, 0), (SAME_F, slab - LATE_ROWS))):
        size = sizes[index]
        rows = pl.ds(pl.multiple_of(ring.at(slot) * slab + skip, 16), size)
        sources = ((x_two.at[rows], x_buf), (dy_two.at[rows], dy_buf), (du_far.at[pl.ds(index * slab, size)], du_buf))
        loads.append([pltpu.make_async_copy(src, dst.at[index, pl.ds(0, size)], load_sem.at[index, which]) for which, (src, dst) in enumerate(sources)])
        stores.append(pltpu.make_async_copy(dy_buf.at[index, pl.ds(0, size)], dx_two_out.at[rows], store_sem.at[index]))
    for copies in loads:
        for copy in copies:
            copy.start()
    for index, copies in enumerate(loads):
        for copy in copies:
            copy.wait()
        rows = pl.ds(0, sizes[index])
        dy_buf[index, rows, :] += rms_back(x_buf[index, rows, :], du_buf[index, rows, :])
        stores[index].start()
    for copy in stores:
        copy.wait()


def last_call(x_two, dy_two, du_far, dx_two):
    tokens, hidden = x_two.shape
    any_spec = pl.BlockSpec(memory_space=pl.ANY)
    buf = pltpu.VMEM((2, tokens // 8, hidden), F32)
    return pl.pallas_call(
        last_kernel,
        out_shape=jax.ShapeDtypeStruct(dx_two.shape, F32),
        in_specs=[any_spec] * 4,
        out_specs=any_spec,
        input_output_aliases={3: 0},
        scratch_shapes=[buf, buf, buf, pltpu.SemaphoreType.DMA((2, 3)), pltpu.SemaphoreType.DMA((2,))],
        cost_estimate=pl.CostEstimate(flops=10**6, bytes_accessed=4 * 2**20, transcendentals=0),
        name="last",
    )(x_two, dy_two, du_far, dx_two)


def local_backward(y_one, y_two, dy_one, dy_two, w_qkv, w_out, w_up, w_down):
    hidden = y_one.shape[2]
    _, _, _, parts, dim = w_qkv.shape
    qkv_parts = jnp.swapaxes(w_qkv[0, :, 0], 0, 1)
    results = block_call(y_one, y_two, dy_one, dy_two, w_up[0], w_down[0], qkv_parts, w_out[0, 0])
    x_two, dx_one, part_own, near_recv, d_att, o_pos, du_pos, wo_full = (tensor.reshape(-1, hidden) for tensor in results[:8])
    devices = range(lax.axis_size("tp"))
    to_f = [(device, (3 - device // 2) * 2 + device % 2) for device in devices]
    du_far = lax.ppermute(results[8], "tp", to_f)
    y_flat, dy_flat = y_one.reshape(-1, hidden), dy_two.reshape(-1, hidden)
    *states, dw_up, dw_down, dw_qkv, dw_out = finish_call(y_flat, o_pos, wo_full, x_two, dx_one, dy_flat, du_pos, part_own, near_recv, d_att)
    states[3] = last_call(x_two, dy_flat, du_far, states[3])
    states = [tensor.reshape(y_one.shape) for tensor in states]
    return (*states, dw_qkv.reshape(1, hidden, 1, parts, dim), dw_out[None, None], dw_up[None], dw_down[None])


def solution(mesh):
    state_spec = P("dp", "tp", None)
    in_specs = (state_spec, state_spec, state_spec, state_spec, P(None, None, "tp", None, None), P(None, "tp", None, None), P(None, None, "tp"), P(None, "tp", None))
    out_specs = (state_spec, state_spec, state_spec, state_spec, P("dp", None, "tp", None, None), P("dp", "tp", None, None), P("dp", None, "tp"), P("dp", "tp", None))
    return jax.shard_map(local_backward, mesh=mesh, in_specs=in_specs, out_specs=out_specs, check_vma=False)
```

```python
import functools

import jax
import jax.numpy as jnp
from jax import lax
from jax.experimental import pallas as pl
from jax.experimental.pallas import tpu as pltpu
from jax.sharding import PartitionSpec as P

RMS_EPS = 1e-6
LOG2_E = 1.4426950408889634
LATE_ROWS = 96
FAR_ROWS = 16
MESH = pl.DeviceIdType.MESH
BF16, F32 = jnp.bfloat16, jnp.float32
VMEM_LIMIT = 64 * 1024 * 1024 - 65536


def inv_rms(tensor):
    return lax.rsqrt(jnp.mean(tensor * tensor, axis=-1, keepdims=True) + RMS_EPS)


def rms_norm(tensor):
    return tensor * inv_rms(tensor)


def rms_back(tensor, grad_in):
    scale = inv_rms(tensor)
    return scale * grad_in - tensor * (scale * scale * scale) * jnp.mean(grad_in * tensor, axis=-1, keepdims=True)


def gelu_and_slope(tensor):
    root = (2.0 / jnp.pi) ** 0.5
    squared = tensor * tensor
    tanh = jnp.tanh(root * (tensor + 0.044715 * (tensor * squared)))
    cdf = 0.5 * (1.0 + tanh)
    slope = cdf + (0.5 * root) * tensor * ((1.0 - tanh * tanh) * (1.0 + (3 * 0.044715) * squared))
    return tensor * cdf, slope


def dot_nn(left, right):
    return lax.dot_general(left, right, (((1,), (0,)), ((), ())), preferred_element_type=F32)


def dot_nt(left, right):
    return lax.dot_general(left, right, (((1,), (1,)), ((), ())), preferred_element_type=F32)


def dot_tn(left, right):
    return lax.dot_general(left, right, (((0,), (0,)), ((), ())), preferred_element_type=F32)


class Ring:
    def __init__(self):
        me = lax.axis_index("tp")
        chip, core = me // 2, me % 2
        self.me, self.chip, self.core = me, chip, core
        self.chips = (chip, chip + 1 - 2 * (chip % 2), 3 - chip, (chip + 2) % 4)

    def at(self, slot):
        core = self.core if slot % 2 == 0 else 1 - self.core
        return self.chips[slot // 2] * 2 + core

    def at_traced(self, slot):
        relation, other = slot // 2, slot % 2
        own, near_t, near_f, opposite = self.chips
        chip = jnp.where(relation == 0, own, jnp.where(relation == 1, near_t, jnp.where(relation == 2, near_f, opposite)))
        return chip * 2 + (self.core + other) % 2

    def barrier(self):
        barrier = pltpu.get_barrier_semaphore()
        for slot in (1, 2, 3, 4, 5):
            pl.semaphore_signal(barrier, inc=1, device_id={"tp": self.at(slot)}, device_id_type=MESH)
        pl.semaphore_wait(barrier, 5)

    def copy(self, src, dst, send_sem, recv_sem, slot):
        return pltpu.make_async_remote_copy(src_ref=src, dst_ref=dst, send_sem=send_sem, recv_sem=recv_sem, device_id={"tp": self.at(slot)}, device_id_type=MESH)


PARTNER, SAME_T, OTHER_T, SAME_F, OTHER_F, SAME_O, OTHER_O = 1, 2, 3, 4, 5, 6, 7


def block_kernel(
    scale,
    y_one, y_two, dy_one, dy_two, w_up, w_down, w_qkv, w_out,
    x_two, dx_one, part_own, near_recv, d_att, o_pos, du_pos, wo_full, to_f,
    uc_seq, uc_two, att_full, o_relay, du_relay,
    u_all, c_all, up_all, down_all, acc, spare, part_keep, uc_own, att_own,
    load_sem, y_sem, x_sem, w_send, w_recv, uc_send, uc_recv, att_send, att_recv, a2a_send, a2a_recv, relay_recv, near_sem, two_sem,
    seq_sem, head_sem, wo_sem, core_send, core_recv, f_sem, far_sem, o_send, o_recv, du_send, du_recv, o_relay_recv, du_relay_recv, far_recv, free_slot,
):
    ring = Ring()
    slabs, slab, hidden = acc.shape[1:]
    seq_len = slabs * slab
    half = seq_len // 2
    dim = w_out.shape[0]
    fours = slabs // 2

    def start(copies):
        for copy in copies:
            copy.start()

    def say_free(index, to):
        pl.semaphore_signal(free_slot.at[index], inc=1, device_id={"tp": ring.at(to)}, device_id_type=MESH)

    rooms = (0, 1, 2, 3, 4, 5, 1, 3)

    def room(slot):
        return pl.ds(rooms[slot] * half, half)

    def weight_pair(src_slot, dst_slot, to, index):
        return [
            ring.copy(buf.at[room(src_slot)], buf.at[room(dst_slot)], w_send.at[index + which], w_recv.at[dst_slot, which], to)
            for which, buf in enumerate((up_all, down_all))
        ]

    w_own = weight_pair(0, 1, PARTNER, 0) + weight_pair(0, 2, SAME_T, 2) + weight_pair(0, 4, SAME_F, 4)
    def far_part(src_slot, first, count, to, index, recv_sem):
        src, dst = (pl.ds(rooms[slot] * half + first, count) for slot in (src_slot, 6))
        return [ring.copy(buf.at[src], buf.at[dst], w_send.at[index + which], recv_sem.at[which], to) for which, buf in enumerate((up_all, down_all))]

    w_near_t = far_part(2, FAR_ROWS, half - FAR_ROWS, SAME_F, 6, w_recv.at[6])
    w_over_t = far_part(4, 0, FAR_ROWS, SAME_T, 14, far_recv)
    w_near_t_core = weight_pair(2, 3, PARTNER, 8)
    w_near_f = weight_pair(4, 5, PARTNER, 10)
    w_far = weight_pair(6, 7, PARTNER, 12)

    def uc_pair(src_slot, dst_slot, to, index):
        return [ring.copy(buf.at[src_slot], buf.at[dst_slot], uc_send.at[index + which], uc_recv.at[dst_slot, which], to) for which, buf in enumerate((u_all, c_all))]

    u_to_t, c_to_t = uc_pair(0, 2, SAME_T, 0)
    uc_core = uc_pair(0, 1, PARTNER, 2)
    uc_pass = uc_pair(2, 3, PARTNER, 4)

    def att(src, dst_slot, to, index):
        return ring.copy(src, att_full.at[dst_slot], att_send.at[index], att_recv.at[dst_slot], to)

    att_keep = pltpu.make_async_copy(att_own, att_full.at[0], load_sem.at[6])
    att_out = [att(att_own, 4, SAME_F, 0), att(att_own, 1, PARTNER, 1)]
    att_t, att_o = att(att_own, 2, SAME_T, 2), att(att_full.at[4], 6, SAME_T, 3)
    att_f_core, att_t_core, att_o_core = att(att_full.at[4], 5, PARTNER, 4), att(att_full.at[2], 3, PARTNER, 5), att(att_full.at[6], 7, PARTNER, 6)

    a2a_out = {slot: ring.copy(uc_own.at[slot], uc_seq.at[slot], a2a_send.at[slot], a2a_recv.at[slot], slot) for slot in (1, 2, 3, 4, 5)}
    a2a_out[SAME_O] = ring.copy(uc_own.at[SAME_O], uc_two.at[2], a2a_send.at[SAME_O], relay_recv.at[0], SAME_F)
    a2a_out[OTHER_O] = ring.copy(uc_own.at[OTHER_O], uc_two.at[3], a2a_send.at[OTHER_O], relay_recv.at[1], OTHER_F)
    a2a_pass = [ring.copy(uc_two.at[2 + index], uc_seq.at[SAME_O + index], a2a_send.at[8 + index], a2a_recv.at[SAME_O + index], SAME_T) for index in (0, 1)]
    uc_keep = pltpu.make_async_copy(uc_own.at[0], uc_seq.at[0], load_sem.at[4])
    two_out = ring.copy(uc_own.at[OTHER_T], uc_two.at[1], a2a_send.at[10], relay_recv.at[2], PARTNER)
    two_keep = pltpu.make_async_copy(uc_own.at[SAME_T], uc_two.at[0], two_sem.at[0])
    near = ring.copy(acc.at[0], near_recv, near_sem.at[0], near_sem.at[1], SAME_F)

    loads = [
        pltpu.make_async_copy(w_down, down_all.at[room(0)], load_sem.at[0]),
        pltpu.make_async_copy(w_up, uc_own.at[:, 0, :, pl.ds(0, half)], load_sem.at[1]),
        pltpu.make_async_copy(y_one, acc.at[0], load_sem.at[2]),
        pltpu.make_async_copy(dy_two, acc.at[1], load_sem.at[3]),
        pltpu.make_async_copy(w_out, att_own.at[pl.ds(3 * dim, dim)], load_sem.at[7]),
    ]
    qkv_loads = [pltpu.make_async_copy(w_qkv.at[part], uc_own.at[:, 1, :, pl.ds(part * dim, dim)], y_sem.at[0, part]) for part in range(3)]
    start(loads)
    start(qkv_loads)
    ring.barrier()
    loads[0].wait()
    start(w_own[1::2])
    loads[1].wait()
    for part in range(half // dim):
        up_all[pl.ds(part * dim, dim), :] = uc_own[:, 0, :, pl.ds(part * dim, dim)].reshape(hidden, dim).T
    start(w_own[0::2])
    loads[2].wait()
    loads[3].wait()

    def normalize(step, carry):
        rows = pl.ds(pl.multiple_of(step * slab, slab), slab)
        u_all[0, rows, :] = rms_norm(acc[0, step]).astype(BF16)
        c_all[0, rows, :] = acc[1, step].astype(BF16)
        acc[0, step] = jnp.zeros((slab, hidden), F32)
        acc[1, step] = jnp.zeros((slab, hidden), F32)
        return carry

    lax.fori_loop(0, slabs, normalize, 0)
    u_to_t.start()
    start(uc_core)
    for part in range(3):
        qkv_loads[part].wait()
        att_own[pl.ds(part * dim, dim), :] = uc_own[:, 1, :, pl.ds(part * dim, dim)].reshape(hidden, dim).T
    loads[4].wait()
    att_keep.start()

    def y_loads(step, buf):
        seq = ring.at_traced(7 - step)
        return [pltpu.make_async_copy(src.at[seq], spare.at[buf, which], y_sem.at[buf, which]) for which, src in enumerate((y_one, y_two, dy_one))]

    def x_stores(step, buf):
        seq = ring.at_traced(7 - step)
        return [pltpu.make_async_copy(spare.at[buf, 3 + which], dst.at[seq], x_sem.at[buf, which]) for which, dst in enumerate((x_two, dx_one))]

    def feed_forward(step, carry):
        slot = jnp.where(step == 3, 4, jnp.where(step == 4, 3, step))
        place = pl.ds(pl.multiple_of(jnp.where(step == 6, 1, jnp.where(step == 7, 3, slot)) * half, half), half)

        @pl.when((step >= 1) & (step != 6))
        def _():
            for which, buf in enumerate((up_all, down_all)):
                ring.copy(buf.at[place], buf.at[place], w_send.at[0], w_recv.at[slot, which], PARTNER).wait_recv()

        @pl.when(step == 6)
        def _():
            for copy in w_near_t + w_over_t:
                copy.wait_recv()

        @pl.when(step == 2)
        def _():
            pl.semaphore_wait(free_slot.at[0], 1)
            start(w_near_t)
            start(w_near_t_core)
            start(att_out)

        @pl.when(step == 3)
        def _():
            pl.semaphore_wait(free_slot.at[5], 1)
            start(w_over_t)
            c_to_t.start()
            start(w_near_f)

        @pl.when(step == 6)
        def _():
            pl.semaphore_wait(free_slot.at[1], 1)
            start(w_far)

        @pl.when(step == 7)
        def _():
            start(y_loads(0, 0))

        def rows_step(part, carry):
            rows = pl.ds(pl.multiple_of(part * half, half), half)
            quarter = pl.ds(part * fours, fours)
            hidden_act, slope = gelu_and_slope(dot_nt(u_all[0, rows, :], up_all[place, :]))
            d_pre = (slope * dot_nt(c_all[0, rows, :], down_all[place, :])).astype(BF16)
            acc[0, quarter] += dot_nn(hidden_act.astype(BF16), down_all[place, :]).reshape(fours, slab, hidden)
            acc[1, quarter] += dot_nn(d_pre, up_all[place, :]).reshape(fours, slab, hidden)
            return carry

        lax.fori_loop(0, 2, rows_step, 0)

        @pl.when(step == 1)
        def _():
            say_free(0, SAME_F)
            say_free(5, SAME_T)

        @pl.when(step == 4)
        def _():
            say_free(1, PARTNER)

        return carry

    lax.fori_loop(0, 8, feed_forward, 0)

    def finish(step, carry):
        slot = 7 - step
        buf = step % 2
        seq = ring.at_traced(slot)
        for copy in y_loads(step, buf):
            copy.wait()

        @pl.when(step < 7)
        def _():
            start(y_loads(step + 1, 1 - buf))

        @pl.when(step >= 2)
        def _():
            for copy in x_stores(step - 2, buf):
                copy.wait()

        y_first = spare[buf, 0]
        x_second = spare[buf, 1] - acc[0, seq]
        dy_first = spare[buf, 2] + rms_back(y_first, acc[1, seq])
        spare[buf, 3] = x_second
        spare[buf, 4] = dy_first
        uc_own[slot, 0] = rms_norm(x_second).astype(BF16)
        uc_own[slot, 1] = dy_first.astype(BF16)
        acc[0, seq] = jnp.zeros((slab, hidden), F32)
        acc[1, seq] = jnp.zeros((slab, hidden), F32)
        start(x_stores(step, buf))
        return carry

    lax.fori_loop(0, 8, finish, 0)
    for slot in (7, 6, 5, 4, 3, 2, 1):
        a2a_out[slot].start()
    uc_keep.start()
    two_out.start()
    two_keep.start()
    for step in (6, 7):
        for copy in x_stores(step, step % 2):
            copy.wait()

    def gradients(step, carry):
        first = step // 8
        tokens = (step % 8) // 2
        place = pl.ds(pl.multiple_of((4 - 4 * first) * half, half), half)

        @pl.when((step == 2) | (step == 4) | (step == 6))
        def _():
            for which, buf in enumerate((u_all, c_all)):
                ring.copy(buf.at[tokens], buf.at[tokens], uc_send.at[0], uc_recv.at[tokens, which], PARTNER).wait_recv()

        @pl.when(step == 4)
        def _():
            start(uc_pass)
            for index in (0, 1):
                a2a_out[SAME_O + index].wait_recv()
            start(a2a_pass)

        @pl.when(step == 8)
        def _():
            near.start()
            att_out[0].wait_recv()
            att_f_core.start()
            att_t.start()
            att_o.start()

        rows = pl.ds(pl.multiple_of((step % 2) * half, half), half)
        u_part, c_part = u_all[tokens, rows, :], c_all[tokens, rows, :]
        hidden_act, slope = gelu_and_slope(dot_nt(up_all[place, :], u_part))
        d_pre = (slope * dot_nt(down_all[place, :], c_part)).astype(BF16)
        acc[first, pl.ds(0, fours)] += dot_nn(d_pre, u_part).reshape(fours, slab, hidden)
        acc[first, pl.ds(fours, fours)] += dot_nn(hidden_act.astype(BF16), c_part).reshape(fours, slab, hidden)
        return carry

    lax.fori_loop(0, 16, gradients, 0)
    out_own = pltpu.make_async_copy(acc.at[1], part_own, load_sem.at[1])
    out_own.start()
    for copy in w_own + w_near_t + w_over_t + w_near_t_core + w_near_f + w_far + [u_to_t, c_to_t] + uc_core + uc_pass:
        copy.wait_send()
    say_free(2, SAME_T)

    def relation_of(step):
        base = step % 4
        return jnp.where(base == 0, 2, jnp.where(base == 3, 3, base - 1))

    def qkv_rows(buf):
        return pl.ds(pl.multiple_of(buf * 6 * dim, 2 * dim), 6 * dim)

    def wo_rows(buf):
        return pl.ds(pl.multiple_of(12 * dim + buf * 2 * dim, 2 * dim), 2 * dim)

    def head_loads(relation, buf):
        copies = []
        for index in (0, 1):
            head = att_full.at[relation * 2 + 1 - index]
            first, second = (pl.ds(pl.multiple_of(base + index * size, dim), size) for base, size in ((buf * 6 * dim, 3 * dim), (12 * dim + buf * 2 * dim, dim)))
            copies.append(pltpu.make_async_copy(head.at[pl.ds(0, 3 * dim)], up_all.at[first], head_sem.at[buf, index, 0]))
            copies.append(pltpu.make_async_copy(head.at[pl.ds(3 * dim, dim)], up_all.at[second], head_sem.at[buf, index, 1]))
        return copies

    def rows_of(slot):
        return pl.ds(slot * slab, slab)

    def seq_loads(seq, src, src_slot, slot):
        return [pltpu.make_async_copy(src.at[src_slot, which], u_all.at[2 * seq + which, rows_of(slot)], seq_sem.at[2 * seq + which, slot]) for which in (0, 1)]

    seq_own = [copy for slot in range(8) for copy in seq_loads(0, uc_seq, slot, slot)]
    seq_two = [copy for slot in range(4) for copy in seq_loads(1, uc_two, slot, slot)]
    uc_to_t = [
        ring.copy(uc_seq.at[slot, which], u_all.at[2 + which, rows_of(4 + index)], far_sem.at[0, 2 * index + which], far_sem.at[1, 2 * index + which], SAME_T)
        for which in (0, 1)
        for index, slot in enumerate((0, 1, 4, 5))
    ]
    core_copies = [ring.copy(spare.at[index, pl.ds(0, 4)], acc.at[0, pl.ds(0, 4)], core_send.at[index], core_recv.at[index], PARTNER) for index in (0, 1)]
    f_copy = ring.copy(part_keep.at[0], acc.at[0, pl.ds(4, 4)], f_sem.at[0], f_sem.at[1], SAME_F)

    o_src = c_all.at[0]
    o_out = [
        ring.copy(o_src.at[rows_of(SAME_O)], o_relay.at[0], o_send.at[6], o_relay_recv.at[0], SAME_T),
        ring.copy(o_src.at[rows_of(OTHER_O)], o_relay.at[1], o_send.at[7], o_relay_recv.at[1], SAME_F),
    ] + [ring.copy(o_src.at[rows_of(slot)], o_pos.at[ring.me], o_send.at[slot], o_recv.at[slot], slot) for slot in (5, 4, 3, 2, 1)]
    o_pass = [
        ring.copy(o_relay.at[0], o_pos.at[ring.at(SAME_T)], o_send.at[8], o_recv.at[SAME_O], SAME_F),
        ring.copy(o_relay.at[1], o_pos.at[ring.at(SAME_F)], o_send.at[9], o_recv.at[OTHER_O], OTHER_T),
    ]
    o_keep = pltpu.make_async_copy(o_src.at[rows_of(0)], o_pos.at[ring.me], o_send.at[0])

    late = slab - LATE_ROWS
    early = {slot: late if slot == SAME_F else slab for slot in range(1, 6)}
    du_out = [
        ring.copy(acc.at[1, SAME_O], to_f.at[pl.ds(0, slab)], du_send.at[6], du_relay_recv.at[0], SAME_T),
        ring.copy(acc.at[1, OTHER_O], du_relay, du_send.at[7], du_relay_recv.at[1], SAME_F),
    ] + [ring.copy(acc.at[1, slot, pl.ds(0, early[slot])], du_pos.at[ring.me, pl.ds(0, early[slot])], du_send.at[slot], du_recv.at[slot], slot) for slot in (5, 4, 3, 2, 1)]
    du_keep = pltpu.make_async_copy(acc.at[1, 0], du_pos.at[ring.me], du_send.at[0])
    du_late = pltpu.make_async_copy(acc.at[1, SAME_F, pl.ds(late, slab - late)], to_f.at[pl.ds(slab, slab - late)], du_send.at[8])
    du_pass = ring.copy(du_relay, du_pos.at[ring.at(SAME_F)], du_send.at[9], du_recv.at[OTHER_O], OTHER_T)

    att_f_core.wait_recv()
    att_keep.wait()
    att_out[1].wait_recv()
    start(head_loads(2, 0))
    uc_keep.wait()
    for slot in range(1, 8):
        ring.copy(uc_own.at[slot], uc_seq.at[slot], a2a_send.at[0], a2a_recv.at[slot], PARTNER).wait_recv()
    start(seq_own)
    pl.semaphore_wait(free_slot.at[2], 1)
    start(uc_to_t)
    two_out.wait_recv()
    two_keep.wait()
    start(seq_two)
    out_own.wait()
    acc[1] = jnp.zeros(acc.shape[1:], F32)
    for copy in seq_own:
        copy.wait()

    def chip_step(step, carry):
        buf = step % 2
        seq = step // 4
        relation = relation_of(step)

        @pl.when(step == 4)
        def _():
            near.wait_send()
            say_free(3, SAME_F)
            say_free(4, PARTNER)
            for copy in seq_two:
                copy.wait()
            for copy in uc_to_t[:4]:
                copy.wait_recv()

        for copy in head_loads(0, buf):
            copy.wait()

        @pl.when((step == 0) | (step == 3) | (step == 4))
        def _():
            start(head_loads(relation_of(step + 1), 1 - buf))

        kept = pl.ds(pl.multiple_of(jnp.where(step < 2, step, 2) * seq_len, seq_len), seq_len)
        heads = [ring.at_traced(relation * 2 + other) for other in (1, 0)]
        wo_copies = [
            pltpu.make_async_copy(up_all.at[pl.ds(pl.multiple_of(12 * dim + (2 * buf + index) * dim, dim), dim)], wo_full.at[head], wo_sem.at[index])
            for index, head in enumerate(heads)
        ]
        start(wo_copies)
        c_all[2, :, pl.ds(0, 6 * dim)] = dot_nt(u_all[2 * seq], up_all[qkv_rows(buf), :]).astype(BF16)
        for index, head in enumerate(heads):
            columns = pl.ds(pl.multiple_of(head * dim, dim), dim)
            own = pl.ds(index * 3 * dim, 3 * dim)
            query, key, value = (c_all[2, :, pl.ds((index * 3 + part) * dim, dim)] for part in range(3))
            scores = dot_nt(query, key) * (scale * LOG2_E)
            grown = jnp.exp2(scores - jnp.max(scores, axis=-1, keepdims=True))
            prob = grown * (1.0 / jnp.sum(grown, axis=-1, keepdims=True))
            prob_b = prob.astype(BF16)
            c_all[seq, :, columns] = dot_nn(prob_b, value).astype(BF16)
            if index == 0:
                @pl.when(step == 4)
                def _():
                    for copy in uc_to_t[4:]:
                        copy.wait_recv()

                c_all[2, :, pl.ds(6 * dim, 2 * dim)] = dot_nt(u_all[2 * seq + 1], up_all[wo_rows(buf), :]).astype(BF16)
            d_out = c_all[2, :, pl.ds((6 + index) * dim, dim)]
            d_prob = dot_nt(d_out, value)
            d_score = (prob * (d_prob - jnp.sum(d_prob * prob, axis=-1, keepdims=True)) * scale).astype(BF16)
            down_all[kept, pl.ds(index * 3 * dim, dim)] = dot_nn(d_score, key).astype(BF16)
            down_all[kept, pl.ds((index * 3 + 1) * dim, dim)] = dot_nn(query.T, d_score).T.astype(BF16)
            down_all[kept, pl.ds((index * 3 + 2) * dim, dim)] = dot_nn(d_out.T, prob_b).T.astype(BF16)
            @pl.when(step >= 4)
            def _():
                dst = (spare, part_keep)[index].at[buf]
                dst[pl.ds(0, 3)] += dot_tn(down_all[kept, own], u_all[2]).reshape(3, dim, hidden)
                dst[3] += dot_tn(c_all[1, :, columns], u_all[3])

            if index == 0:
                @pl.when(step == 1)
                def _():
                    att_t.wait_recv()
                    att_t_core.start()

                @pl.when(step == 4)
                def _():
                    pl.semaphore_wait(free_slot.at[4], 1)
                    core_copies[0].start()

                @pl.when(step == 5)
                def _():
                    pl.semaphore_wait(free_slot.at[4], 1)
                    core_copies[1].start()

        @pl.when(step == 1)
        def _():
            att_t_core.wait_recv()
            start(head_loads(1, 0))

        @pl.when(step == 2)
        def _():
            att_o.wait_recv()
            att_o_core.start()

        @pl.when(step < 4)
        def _():
            def du_tile(part, carry):
                rows = pl.ds(pl.multiple_of(jnp.where(step < 2, step, 2) * seq_len + part * half, half), half)
                acc[1, pl.ds(part * fours, fours)] += dot_nn(down_all[rows, pl.ds(0, 6 * dim)], up_all[qkv_rows(buf), :]).reshape(fours, slab, hidden)
                return carry

            lax.fori_loop(0, 2, du_tile, 0)

        @pl.when(step == 2)
        def _():
            att_o_core.wait_recv()
            start(head_loads(3, 1))

        @pl.when(step == 3)
        def _():
            start(o_out)
            start(du_out)
            du_late.start()
            o_keep.start()
            du_keep.start()

            def own_gradients(pair, carry):
                own_rows = pl.ds(pl.multiple_of(pair * seq_len, seq_len), seq_len)
                for index, other in enumerate((1, 0)):
                    columns = pl.ds(pl.multiple_of(ring.at_traced(relation_of(pair) * 2 + other) * dim, dim), dim)
                    dst = (spare, part_keep)[index].at[pair]
                    dst[pl.ds(0, 3)] = dot_tn(down_all[own_rows, pl.ds(index * 3 * dim, 3 * dim)], u_all[0]).reshape(3, dim, hidden)
                    dst[3] = dot_tn(c_all[0, :, columns], u_all[1])
                return carry

            lax.fori_loop(0, 2, own_gradients, 0)

        @pl.when(step == 4)
        def _():
            core_copies[0].wait_recv()
            part_keep[0] += acc[0, pl.ds(0, 4)]
            say_free(4, PARTNER)
            pl.semaphore_wait(free_slot.at[3], 1)
            f_copy.start()

        for copy in wo_copies:
            copy.wait()
        return carry

    lax.fori_loop(0, 6, chip_step, 0)
    for copy in o_out[:2]:
        copy.wait_recv()
    start(o_pass)
    du_out[1].wait_recv()
    du_pass.start()
    core_copies[1].wait_recv()
    part_keep[1] += acc[0, pl.ds(0, 4)]
    for copy in du_out[2:]:
        copy.wait_recv()
    for slot in range(1, 8):
        ring.copy(o_pos.at[0], o_pos.at[ring.at(slot)], near_sem.at[0], o_recv.at[slot], PARTNER).wait_recv()
    du_out[0].wait_recv()
    du_pass.wait_recv()
    near.wait_recv()
    f_copy.wait_recv()
    part_keep[1] += acc[0, pl.ds(4, 4)]
    d_att_copy = pltpu.make_async_copy(part_keep.at[1], d_att, load_sem.at[0])
    d_att_copy.start()

    sends = att_out + [att_t, att_o, att_f_core, att_t_core, att_o_core] + list(a2a_out.values()) + a2a_pass + [two_out]
    for copy in sends + o_out + du_out + o_pass + uc_to_t + core_copies + [du_pass, f_copy]:
        copy.wait_send()
    du_late.wait()
    o_keep.wait()
    du_keep.wait()
    d_att_copy.wait()


def block_call(y_one, y_two, dy_one, dy_two, w_up, w_down, w_qkv, w_out):
    slabs, slab, hidden = y_one.shape
    tokens = slabs * slab
    ffn = w_down.shape[0]
    dim = w_out.shape[0]
    any_spec = pl.BlockSpec(memory_space=pl.ANY)
    dma, vmem, wide, narrow = pltpu.SemaphoreType.DMA, pltpu.VMEM, F32, BF16
    results = [
        ((slabs, slab, hidden), wide), ((slabs, slab, hidden), wide), ((slabs, slab, hidden), wide), ((slabs, slab, hidden), wide),
        ((4, dim, hidden), wide), ((slabs, slab, hidden), narrow), ((slabs, slab, hidden), wide), ((8, dim, hidden), narrow),
        ((slab + LATE_ROWS, hidden), wide),
    ]
    landing = [
        ((8, 2, slab, hidden), narrow), ((4, 2, slab, hidden), narrow), ((8, 4 * dim, hidden), narrow), ((2, slab, hidden), narrow), ((slab, hidden), wide),
    ]
    scratch = [
        vmem((4, tokens, hidden), BF16), vmem((4, tokens, hidden), BF16), vmem((6 * ffn, hidden), BF16), vmem((6 * ffn, hidden), BF16),
        vmem((2, slabs, slab, hidden), F32), vmem((2, 5, slab, hidden), F32), vmem((2, 4, dim, hidden), F32),
        vmem((8, 2, slab, hidden), BF16), vmem((4 * dim, hidden), BF16),
        dma((8,)), dma((2, 3)), dma((2, 2)), dma((16,)), dma((8, 2)), dma((6,)), dma((4, 2)), dma((7,)), dma((8,)), dma((11,)), dma((8,)), dma((3,)), dma((2,)), dma((2,)),
        dma((4, 8)), dma((2, 2, 2)), dma((2,)), dma((2,)), dma((2,)), dma((2,)), dma((2, 8)), dma((10,)), dma((8,)), dma((10,)), dma((8,)), dma((2,)), dma((2,)), dma((2,)),
        pltpu.SemaphoreType.REGULAR((6,)),
    ]
    return pl.pallas_call(
        functools.partial(block_kernel, dim ** -0.5),
        out_shape=[jax.ShapeDtypeStruct(shape, dtype) for shape, dtype in results + landing],
        in_specs=[any_spec] * 8,
        out_specs=[any_spec] * (len(results) + len(landing)),
        scratch_shapes=scratch,
        compiler_params=pltpu.CompilerParams(collective_id=0, has_side_effects=True, vmem_limit_bytes=VMEM_LIMIT),
        cost_estimate=pl.CostEstimate(flops=120 * 10**9, bytes_accessed=128 * 2**20, transcendentals=0),
        name="block",
    )(y_one, y_two, dy_one, dy_two, w_up.reshape(8, hidden // 8, ffn), w_down, w_qkv.reshape(3, 8, hidden // 8, dim), w_out)[: len(results)]


def finish_kernel(
    y_one, o_pos, wo_full, x_two, dx_one, dy_two, du_pos, part_own, near_recv, d_att,
    x_one_out, x_two_out, dx_one_out, dx_two_out, dw_up, dw_down, dw_qkv, dw_out,
    y_buf, o_buf, wo_buf, x_buf, dx_buf, dy_buf, du_buf, own_buf, near_buf, att_buf, up_out, qkv_out, load_sem, store_sem,
):
    tokens = y_buf.shape[0]
    dim = wo_buf.shape[0] // 8
    chunk = 256
    chunks = [pl.ds(index * chunk, chunk) for index in range(tokens // chunk)]

    def pieces(src, dst, sem, row):
        return [pltpu.make_async_copy(src.at[rows], dst.at[rows], sem.at[row, index]) for index, rows in enumerate(chunks)]

    def whole(src, dst, sem, row):
        return pltpu.make_async_copy(src, dst, sem.at[row, 0])

    ring = Ring()
    slab = tokens // 8
    sizes = {0: slab, PARTNER: slab, SAME_T: slab, OTHER_T: slab, SAME_F: slab - LATE_ROWS, OTHER_F: slab, OTHER_O: slab}
    slots = [pl.ds(pl.multiple_of(ring.at(slot) * slab, slab), size) for slot, size in sizes.items()]

    def slabs(src, dst, sem, row):
        return [pltpu.make_async_copy(src.at[rows], dst.at[rows], sem.at[row, index]) for index, rows in enumerate(slots)]

    x_in, dy_in, du_in = pieces(x_two, x_buf, load_sem, 0), slabs(dy_two, dy_buf, load_sem, 1), slabs(du_pos, du_buf, load_sem, 2)
    y_in, o_in = pieces(y_one, y_buf, load_sem, 3), pieces(o_pos, o_buf, load_sem, 4)
    wo_in, dx_in = whole(wo_full, wo_buf, load_sem, 5), pieces(dx_one, dx_buf, load_sem, 6)
    own_in, near_in, att_in = whole(part_own, own_buf, load_sem, 7), whole(near_recv, near_buf, load_sem, 8), whole(d_att, att_buf, load_sem, 9)
    order = [own_in, near_in, att_in, wo_in, *(copy for group in zip(y_in, o_in) for copy in group), *x_in, *(copy for group in zip(dy_in, du_in) for copy in group), *dx_in]
    for copy in order:
        copy.start()

    x_store, dx2_store, x1_store = pieces(x_buf, x_two_out, store_sem, 0), slabs(dy_buf, dx_two_out, store_sem, 1), pieces(y_buf, x_one_out, store_sem, 2)
    dx_store = pieces(dx_buf, dx_one_out, store_sem, 3)
    own_in.wait()
    near_in.wait()
    ffn = up_out.shape[1]
    own_buf[pl.ds(ffn, ffn), :] += near_buf[pl.ds(ffn, ffn), :]
    down_store = whole(own_buf.at[pl.ds(ffn, ffn)], dw_down, store_sem, 7)
    down_store.start()
    for part in range(up_out.shape[0] // ffn):
        columns = pl.ds(part * ffn, ffn)
        up_out[columns, :] = (own_buf[pl.ds(0, ffn), columns] + near_buf[pl.ds(0, ffn), columns]).T
    up_store = whole(up_out, dw_up, store_sem, 4)
    up_store.start()
    att_in.wait()
    for part in range(3):
        qkv_out[pl.ds(part, tokens, stride=3), 0, :] = att_buf[pl.ds(part * dim, dim), :].T
    qkv_store = whole(qkv_out, dw_qkv, store_sem, 5)
    qkv_store.start()
    out_store = whole(att_buf.at[pl.ds(3 * dim, dim)], dw_out, store_sem, 6)
    out_store.start()
    wo_in.wait()
    for index, rows in enumerate(chunks):
        y_in[index].wait()
        o_in[index].wait()
        y_buf[rows, :] -= dot_nn(o_buf[rows, :], wo_buf[...])
        x1_store[index].start()
    for index in range(len(chunks)):
        x_in[index].wait()
        x_store[index].start()
    for index, rows in enumerate(slots):
        dy_in[index].wait()
        du_in[index].wait()
        dy_buf[rows, :] += rms_back(x_buf[rows, :], du_buf[rows, :])
        dx2_store[index].start()
    for index in range(len(chunks)):
        dx_in[index].wait()
        dx_store[index].start()
    for copy in x_store + dx2_store + x1_store + dx_store + [up_store, qkv_store, out_store, down_store]:
        copy.wait()


def finish_call(y_one, o_pos, wo_full, x_two, dx_one, dy_two, du_pos, part_own, near_recv, d_att):
    tokens, hidden = y_one.shape
    ffn = part_own.shape[0] // 2
    dim = d_att.shape[0] // 4
    any_spec = pl.BlockSpec(memory_space=pl.ANY)
    dma, vmem = pltpu.SemaphoreType.DMA, pltpu.VMEM
    state = (tokens, hidden)
    out_shape = [jax.ShapeDtypeStruct(shape, F32) for shape in (state, state, state, state, (hidden, ffn), (ffn, hidden), (3 * hidden, 1, dim), (dim, hidden))]
    scratch = [
        vmem(state, F32), vmem(state, BF16), vmem((hidden, hidden), BF16), vmem(state, F32), vmem(state, F32), vmem(state, F32), vmem(state, F32),
        vmem(part_own.shape, F32), vmem(part_own.shape, F32), vmem(d_att.shape, F32), vmem((hidden, ffn), F32), vmem((3 * hidden, 1, dim), F32),
        dma((10, 7)), dma((8, 7)),
    ]
    return pl.pallas_call(
        finish_kernel,
        out_shape=out_shape,
        in_specs=[any_spec] * 10,
        out_specs=[any_spec] * 8,
        scratch_shapes=scratch,
        compiler_params=pltpu.CompilerParams(vmem_limit_bytes=VMEM_LIMIT),
        cost_estimate=pl.CostEstimate(flops=2 * 10**9, bytes_accessed=52 * 2**20, transcendentals=0),
        name="finish",
    )(y_one, o_pos, wo_full, x_two, dx_one, dy_two, du_pos, part_own, near_recv, d_att)


def last_kernel(x_two, dy_two, du_far, dx_two_in, dx_two_out, x_buf, dy_buf, du_buf, load_sem, store_sem):
    ring = Ring()
    slab = x_buf.shape[1]
    loads, stores, sizes = [], [], (slab, LATE_ROWS)
    for index, (slot, skip) in enumerate(((SAME_O, 0), (SAME_F, slab - LATE_ROWS))):
        size = sizes[index]
        rows = pl.ds(pl.multiple_of(ring.at(slot) * slab + skip, 16), size)
        sources = ((x_two.at[rows], x_buf), (dy_two.at[rows], dy_buf), (du_far.at[pl.ds(index * slab, size)], du_buf))
        loads.append([pltpu.make_async_copy(src, dst.at[index, pl.ds(0, size)], load_sem.at[index, which]) for which, (src, dst) in enumerate(sources)])
        stores.append(pltpu.make_async_copy(dy_buf.at[index, pl.ds(0, size)], dx_two_out.at[rows], store_sem.at[index]))
    for copies in loads:
        for copy in copies:
            copy.start()
    for index, copies in enumerate(loads):
        for copy in copies:
            copy.wait()
        rows = pl.ds(0, sizes[index])
        dy_buf[index, rows, :] += rms_back(x_buf[index, rows, :], du_buf[index, rows, :])
        stores[index].start()
    for copy in stores:
        copy.wait()


def last_call(x_two, dy_two, du_far, dx_two):
    tokens, hidden = x_two.shape
    any_spec = pl.BlockSpec(memory_space=pl.ANY)
    buf = pltpu.VMEM((2, tokens // 8, hidden), F32)
    return pl.pallas_call(
        last_kernel,
        out_shape=jax.ShapeDtypeStruct(dx_two.shape, F32),
        in_specs=[any_spec] * 4,
        out_specs=any_spec,
        input_output_aliases={3: 0},
        scratch_shapes=[buf, buf, buf, pltpu.SemaphoreType.DMA((2, 3)), pltpu.SemaphoreType.DMA((2,))],
        cost_estimate=pl.CostEstimate(flops=10**6, bytes_accessed=4 * 2**20, transcendentals=0),
        name="last",
    )(x_two, dy_two, du_far, dx_two)


def local_backward(y_one, y_two, dy_one, dy_two, w_qkv, w_out, w_up, w_down):
    hidden = y_one.shape[2]
    _, _, _, parts, dim = w_qkv.shape
    qkv_parts = jnp.swapaxes(w_qkv[0, :, 0], 0, 1)
    results = block_call(y_one, y_two, dy_one, dy_two, w_up[0], w_down[0], qkv_parts, w_out[0, 0])
    x_two, dx_one, part_own, near_recv, d_att, o_pos, du_pos, wo_full = (tensor.reshape(-1, hidden) for tensor in results[:8])
    devices = range(lax.axis_size("tp"))
    to_f = [(device, (3 - device // 2) * 2 + device % 2) for device in devices]
    du_far = lax.ppermute(results[8], "tp", to_f)
    y_flat, dy_flat = y_one.reshape(-1, hidden), dy_two.reshape(-1, hidden)
    *states, dw_up, dw_down, dw_qkv, dw_out = finish_call(y_flat, o_pos, wo_full, x_two, dx_one, dy_flat, du_pos, part_own, near_recv, d_att)
    states[3] = last_call(x_two, dy_flat, du_far, states[3])
    states = [tensor.reshape(y_one.shape) for tensor in states]
    return (*states, dw_qkv.reshape(1, hidden, 1, parts, dim), dw_out[None, None], dw_up[None], dw_down[None])


def solution(mesh):
    state_spec = P("dp", "tp", None)
    in_specs = (state_spec, state_spec, state_spec, state_spec, P(None, None, "tp", None, None), P(None, "tp", None, None), P(None, None, "tp"), P(None, "tp", None))
    out_specs = (state_spec, state_spec, state_spec, state_spec, P("dp", None, "tp", None, None), P("dp", "tp", None, None), P("dp", None, "tp"), P("dp", "tp", None))
    return jax.shard_map(local_backward, mesh=mesh, in_specs=in_specs, out_specs=out_specs, check_vma=False)
```

```python
import functools

import jax
import jax.numpy as jnp
from jax import lax
from jax.experimental import pallas as pl
from jax.experimental.pallas import tpu as pltpu
from jax.sharding import PartitionSpec as P

RMS_EPS = 1e-6
LOG2_E = 1.4426950408889634
LATE_ROWS = 96
FAR_ROWS = 32
MESH = pl.DeviceIdType.MESH
BF16, F32 = jnp.bfloat16, jnp.float32
VMEM_LIMIT = 64 * 1024 * 1024 - 65536


def inv_rms(tensor):
    return lax.rsqrt(jnp.mean(tensor * tensor, axis=-1, keepdims=True) + RMS_EPS)


def rms_norm(tensor):
    return tensor * inv_rms(tensor)


def rms_back(tensor, grad_in):
    scale = inv_rms(tensor)
    return scale * grad_in - tensor * (scale * scale * scale) * jnp.mean(grad_in * tensor, axis=-1, keepdims=True)


def gelu_and_slope(tensor):
    root = (2.0 / jnp.pi) ** 0.5
    squared = tensor * tensor
    tanh = jnp.tanh(root * (tensor + 0.044715 * (tensor * squared)))
    cdf = 0.5 * (1.0 + tanh)
    slope = cdf + (0.5 * root) * tensor * ((1.0 - tanh * tanh) * (1.0 + (3 * 0.044715) * squared))
    return tensor * cdf, slope


def dot_nn(left, right):
    return lax.dot_general(left, right, (((1,), (0,)), ((), ())), preferred_element_type=F32)


def dot_nt(left, right):
    return lax.dot_general(left, right, (((1,), (1,)), ((), ())), preferred_element_type=F32)


def dot_tn(left, right):
    return lax.dot_general(left, right, (((0,), (0,)), ((), ())), preferred_element_type=F32)


class Ring:
    def __init__(self):
        me = lax.axis_index("tp")
        chip, core = me // 2, me % 2
        self.me, self.chip, self.core = me, chip, core
        self.chips = (chip, chip + 1 - 2 * (chip % 2), 3 - chip, (chip + 2) % 4)

    def at(self, slot):
        core = self.core if slot % 2 == 0 else 1 - self.core
        return self.chips[slot // 2] * 2 + core

    def at_traced(self, slot):
        relation, other = slot // 2, slot % 2
        own, near_t, near_f, opposite = self.chips
        chip = jnp.where(relation == 0, own, jnp.where(relation == 1, near_t, jnp.where(relation == 2, near_f, opposite)))
        return chip * 2 + (self.core + other) % 2

    def barrier(self):
        barrier = pltpu.get_barrier_semaphore()
        for slot in (1, 2, 3, 4, 5):
            pl.semaphore_signal(barrier, inc=1, device_id={"tp": self.at(slot)}, device_id_type=MESH)
        pl.semaphore_wait(barrier, 5)

    def copy(self, src, dst, send_sem, recv_sem, slot):
        return pltpu.make_async_remote_copy(src_ref=src, dst_ref=dst, send_sem=send_sem, recv_sem=recv_sem, device_id={"tp": self.at(slot)}, device_id_type=MESH)


PARTNER, SAME_T, OTHER_T, SAME_F, OTHER_F, SAME_O, OTHER_O = 1, 2, 3, 4, 5, 6, 7


def block_kernel(
    scale,
    y_one, y_two, dy_one, dy_two, w_up, w_down, w_qkv, w_out,
    x_two, dx_one, part_own, near_recv, d_att, o_pos, du_pos, wo_full, to_f,
    uc_seq, uc_two, att_full, o_relay, du_relay,
    u_all, c_all, up_all, down_all, acc, spare, part_keep, uc_own,
    load_sem, y_sem, x_sem, w_send, w_recv, uc_send, uc_recv, att_send, att_recv, a2a_send, a2a_recv, relay_recv, near_sem, two_sem,
    seq_sem, head_sem, wo_sem, core_send, core_recv, f_sem, far_sem, o_send, o_recv, du_send, du_recv, o_relay_recv, du_relay_recv, far_recv, free_slot,
):
    ring = Ring()
    slabs, slab, hidden = acc.shape[1:]
    seq_len = slabs * slab
    half = seq_len // 2
    dim = w_out.shape[0]
    fours = slabs // 2

    def start(copies):
        for copy in copies:
            copy.start()

    def say_free(index, to):
        pl.semaphore_signal(free_slot.at[index], inc=1, device_id={"tp": ring.at(to)}, device_id_type=MESH)

    rooms = (0, 1, 2, 3, 4, 5, 1, 3)

    def room(slot):
        return pl.ds(rooms[slot] * half, half)

    def weight_pair(src_slot, dst_slot, to, index):
        return [
            ring.copy(buf.at[room(src_slot)], buf.at[room(dst_slot)], w_send.at[index + which], w_recv.at[dst_slot, which], to)
            for which, buf in enumerate((up_all, down_all))
        ]

    w_own = weight_pair(0, 1, PARTNER, 0) + weight_pair(0, 2, SAME_T, 2) + weight_pair(0, 4, SAME_F, 4)
    def far_part(src_slot, first, count, to, index, recv_sem):
        src, dst = (pl.ds(rooms[slot] * half + first, count) for slot in (src_slot, 6))
        return [ring.copy(buf.at[src], buf.at[dst], w_send.at[index + which], recv_sem.at[which], to) for which, buf in enumerate((up_all, down_all))]

    w_near_t = far_part(2, FAR_ROWS, half - FAR_ROWS, SAME_F, 6, w_recv.at[6])
    w_over_t = far_part(4, 0, FAR_ROWS, SAME_T, 14, far_recv)
    w_near_t_core = weight_pair(2, 3, PARTNER, 8)
    w_near_f = weight_pair(4, 5, PARTNER, 10)
    w_far = weight_pair(6, 7, PARTNER, 12)

    def uc_pair(src_slot, dst_slot, to, index):
        return [ring.copy(buf.at[src_slot], buf.at[dst_slot], uc_send.at[index + which], uc_recv.at[dst_slot, which], to) for which, buf in enumerate((u_all, c_all))]

    u_to_t, c_to_t = uc_pair(0, 2, SAME_T, 0)
    uc_core = uc_pair(0, 1, PARTNER, 2)
    uc_pass = uc_pair(2, 3, PARTNER, 4)

    def att(src, dst_slot, to, index):
        return ring.copy(src, att_full.at[dst_slot], att_send.at[index], att_recv.at[dst_slot], to)

    att_keep = [pltpu.make_async_copy(uc_own.at[part, 0], att_full.at[0, pl.ds(part * dim, dim)], x_sem.at[part // 2, part % 2]) for part in range(4)]
    att_out = [att(att_full.at[0], 4, SAME_F, 0), att(att_full.at[0], 1, PARTNER, 1)]
    att_t, att_o = att(att_full.at[0], 2, SAME_T, 2), att(att_full.at[4], 6, SAME_T, 3)
    att_f_core, att_t_core, att_o_core = att(att_full.at[4], 5, PARTNER, 4), att(att_full.at[2], 3, PARTNER, 5), att(att_full.at[6], 7, PARTNER, 6)

    a2a_out = {slot: ring.copy(uc_own.at[slot], uc_seq.at[slot], a2a_send.at[slot], a2a_recv.at[slot], slot) for slot in (1, 2, 3, 4, 5)}
    a2a_out[SAME_O] = ring.copy(uc_own.at[SAME_O], uc_two.at[2], a2a_send.at[SAME_O], relay_recv.at[0], SAME_F)
    a2a_out[OTHER_O] = ring.copy(uc_own.at[OTHER_O], uc_two.at[3], a2a_send.at[OTHER_O], relay_recv.at[1], OTHER_F)
    a2a_pass = [ring.copy(uc_two.at[2 + index], uc_seq.at[SAME_O + index], a2a_send.at[8 + index], a2a_recv.at[SAME_O + index], SAME_T) for index in (0, 1)]
    uc_keep = pltpu.make_async_copy(uc_own.at[0], uc_seq.at[0], load_sem.at[4])
    two_out = ring.copy(uc_own.at[OTHER_T], uc_two.at[1], a2a_send.at[10], relay_recv.at[2], PARTNER)
    two_keep = pltpu.make_async_copy(uc_own.at[SAME_T], uc_two.at[0], two_sem.at[0])
    near = ring.copy(acc.at[0], near_recv, near_sem.at[0], near_sem.at[1], SAME_F)

    loads = [
        pltpu.make_async_copy(w_down, down_all.at[room(0)], load_sem.at[0]),
        pltpu.make_async_copy(w_up, uc_own.at[:, 0, :, pl.ds(0, half)], load_sem.at[1]),
        pltpu.make_async_copy(y_one, acc.at[0], load_sem.at[2]),
        pltpu.make_async_copy(dy_two, acc.at[1], load_sem.at[3]),
    ]
    qkv_loads = [pltpu.make_async_copy(w_qkv.at[part], uc_own.at[:, 1, :, pl.ds(part * dim, dim)], y_sem.at[0, part]) for part in range(3)]
    start(loads)
    start(qkv_loads)
    ring.barrier()
    loads[0].wait()
    start(w_own[1::2])
    loads[1].wait()
    for part in range(half // dim):
        up_all[pl.ds(part * dim, dim), :] = uc_own[:, 0, :, pl.ds(part * dim, dim)].reshape(hidden, dim).T
    start(w_own[0::2])
    out_load = pltpu.make_async_copy(w_out, uc_own.at[3, 0], load_sem.at[7])
    out_load.start()
    loads[2].wait()
    loads[3].wait()

    def normalize(step, carry):
        rows = pl.ds(pl.multiple_of(step * slab, slab), slab)
        u_all[0, rows, :] = rms_norm(acc[0, step]).astype(BF16)
        c_all[0, rows, :] = acc[1, step].astype(BF16)
        acc[0, step] = jnp.zeros((slab, hidden), F32)
        acc[1, step] = jnp.zeros((slab, hidden), F32)
        return carry

    lax.fori_loop(0, slabs, normalize, 0)
    u_to_t.start()
    start(uc_core)
    for part in range(3):
        qkv_loads[part].wait()
        uc_own[part, 0] = uc_own[:, 1, :, pl.ds(part * dim, dim)].reshape(hidden, dim).T
    out_load.wait()
    start(att_keep)

    def y_loads(step, buf):
        seq = ring.at_traced(7 - step)
        return [pltpu.make_async_copy(src.at[seq], spare.at[buf, which], y_sem.at[buf, which]) for which, src in enumerate((y_one, y_two, dy_one))]

    def x_stores(step, buf):
        seq = ring.at_traced(7 - step)
        return [pltpu.make_async_copy(spare.at[buf, 3 + which], dst.at[seq], x_sem.at[buf, which]) for which, dst in enumerate((x_two, dx_one))]

    def feed_forward(step, carry):
        slot = jnp.where(step == 3, 4, jnp.where(step == 4, 3, step))
        place = pl.ds(pl.multiple_of(jnp.where(step == 6, 1, jnp.where(step == 7, 3, slot)) * half, half), half)

        @pl.when((step == 1) | ((step >= 3) & (step != 6)))
        def _():
            for which, buf in enumerate((up_all, down_all)):
                ring.copy(buf.at[place], buf.at[place], w_send.at[0], w_recv.at[slot, which], PARTNER).wait_recv()

        @pl.when(step == 6)
        def _():
            for copy in w_near_t + w_over_t:
                copy.wait_recv()

        @pl.when(step == 2)
        def _():
            pl.semaphore_wait(free_slot.at[0], 1)
            for which, buf in ((1, down_all), (0, up_all)):
                ring.copy(buf.at[room(2)], buf.at[room(2)], w_send.at[0], w_recv.at[2, which], PARTNER).wait_recv()
                w_near_t[which].start()
                w_near_t_core[which].start()
            for copy in att_keep:
                copy.wait()
            start(att_out)

        @pl.when(step == 3)
        def _():
            pl.semaphore_wait(free_slot.at[5], 1)
            start(w_over_t)
            c_to_t.start()
            start(w_near_f)

        @pl.when(step == 6)
        def _():
            pl.semaphore_wait(free_slot.at[1], 1)
            start(w_far)

        @pl.when(step == 7)
        def _():
            start(y_loads(0, 0))

        def rows_step(part, carry):
            rows = pl.ds(pl.multiple_of(part * half, half), half)
            quarter = pl.ds(part * fours, fours)
            hidden_act, slope = gelu_and_slope(dot_nt(u_all[0, rows, :], up_all[place, :]))
            d_pre = (slope * dot_nt(c_all[0, rows, :], down_all[place, :])).astype(BF16)
            acc[0, quarter] += dot_nn(hidden_act.astype(BF16), down_all[place, :]).reshape(fours, slab, hidden)
            acc[1, quarter] += dot_nn(d_pre, up_all[place, :]).reshape(fours, slab, hidden)
            return carry

        lax.fori_loop(0, 2, rows_step, 0)

        @pl.when(step == 1)
        def _():
            say_free(0, SAME_F)
            say_free(5, SAME_T)

        @pl.when(step == 4)
        def _():
            say_free(1, PARTNER)

        return carry

    lax.fori_loop(0, 8, feed_forward, 0)

    def finish(step, carry):
        slot = 7 - step
        buf = step % 2
        seq = ring.at_traced(slot)
        for copy in y_loads(step, buf):
            copy.wait()

        @pl.when(step < 7)
        def _():
            start(y_loads(step + 1, 1 - buf))

        @pl.when(step >= 2)
        def _():
            for copy in x_stores(step - 2, buf):
                copy.wait()

        y_first = spare[buf, 0]
        x_second = spare[buf, 1] - acc[0, seq]
        dy_first = spare[buf, 2] + rms_back(y_first, acc[1, seq])
        spare[buf, 3] = x_second
        spare[buf, 4] = dy_first
        uc_own[slot, 0] = rms_norm(x_second).astype(BF16)
        uc_own[slot, 1] = dy_first.astype(BF16)
        acc[0, seq] = jnp.zeros((slab, hidden), F32)
        acc[1, seq] = jnp.zeros((slab, hidden), F32)
        start(x_stores(step, buf))
        return carry

    lax.fori_loop(0, 8, finish, 0)
    for slot in (7, 6, 5, 4, 3, 2, 1):
        a2a_out[slot].start()
    uc_keep.start()
    two_out.start()
    two_keep.start()
    for step in (6, 7):
        for copy in x_stores(step, step % 2):
            copy.wait()

    def gradients(step, carry):
        first = step // 8
        tokens = (step % 8) // 2
        place = pl.ds(pl.multiple_of((4 - 4 * first) * half, half), half)

        @pl.when((step == 2) | (step == 4) | (step == 6))
        def _():
            for which, buf in enumerate((u_all, c_all)):
                ring.copy(buf.at[tokens], buf.at[tokens], uc_send.at[0], uc_recv.at[tokens, which], PARTNER).wait_recv()

        @pl.when(step == 4)
        def _():
            start(uc_pass)
            for index in (0, 1):
                a2a_out[SAME_O + index].wait_recv()
            start(a2a_pass)

        @pl.when(step == 8)
        def _():
            near.start()
            att_out[0].wait_recv()
            att_f_core.start()
            att_t.start()
            att_o.start()

        rows = pl.ds(pl.multiple_of((step % 2) * half, half), half)
        u_part, c_part = u_all[tokens, rows, :], c_all[tokens, rows, :]
        hidden_act, slope = gelu_and_slope(dot_nt(up_all[place, :], u_part))
        d_pre = (slope * dot_nt(down_all[place, :], c_part)).astype(BF16)
        acc[first, pl.ds(0, fours)] += dot_nn(d_pre, u_part).reshape(fours, slab, hidden)
        acc[first, pl.ds(fours, fours)] += dot_nn(hidden_act.astype(BF16), c_part).reshape(fours, slab, hidden)
        return carry

    lax.fori_loop(0, 16, gradients, 0)
    out_own = pltpu.make_async_copy(acc.at[1], part_own, load_sem.at[1])
    out_own.start()
    for copy in w_own + w_near_t + w_over_t + w_near_t_core + w_near_f + w_far + [u_to_t, c_to_t] + uc_core + uc_pass:
        copy.wait_send()
    say_free(2, SAME_T)

    def relation_of(step):
        base = step % 4
        return jnp.where(base == 0, 2, jnp.where(base == 3, 3, base - 1))

    def qkv_rows(buf):
        return pl.ds(pl.multiple_of(buf * 6 * dim, 2 * dim), 6 * dim)

    def wo_rows(buf):
        return pl.ds(pl.multiple_of(12 * dim + buf * 2 * dim, 2 * dim), 2 * dim)

    def head_loads(relation, buf):
        copies = []
        for index in (0, 1):
            head = att_full.at[relation * 2 + 1 - index]
            first, second = (pl.ds(pl.multiple_of(base + index * size, dim), size) for base, size in ((buf * 6 * dim, 3 * dim), (12 * dim + buf * 2 * dim, dim)))
            copies.append(pltpu.make_async_copy(head.at[pl.ds(0, 3 * dim)], up_all.at[first], head_sem.at[buf, index, 0]))
            copies.append(pltpu.make_async_copy(head.at[pl.ds(3 * dim, dim)], up_all.at[second], head_sem.at[buf, index, 1]))
        return copies

    def rows_of(slot):
        return pl.ds(slot * slab, slab)

    def seq_loads(seq, src, src_slot, slot):
        return [pltpu.make_async_copy(src.at[src_slot, which], u_all.at[2 * seq + which, rows_of(slot)], seq_sem.at[2 * seq + which, slot]) for which in (0, 1)]

    seq_own = [copy for slot in range(8) for copy in seq_loads(0, uc_seq, slot, slot)]
    seq_two = [copy for slot in range(4) for copy in seq_loads(1, uc_two, slot, slot)]
    uc_to_t = [
        ring.copy(uc_seq.at[slot, which], u_all.at[2 + which, rows_of(4 + index)], far_sem.at[0, 2 * index + which], far_sem.at[1, 2 * index + which], SAME_T)
        for which in (0, 1)
        for index, slot in enumerate((0, 1, 4, 5))
    ]
    core_copies = [ring.copy(spare.at[index, pl.ds(0, 4)], acc.at[0, pl.ds(0, 4)], core_send.at[index], core_recv.at[index], PARTNER) for index in (0, 1)]
    f_copy = ring.copy(part_keep.at[0], acc.at[0, pl.ds(4, 4)], f_sem.at[0], f_sem.at[1], SAME_F)

    o_src = c_all.at[0]
    o_out = [
        ring.copy(o_src.at[rows_of(SAME_O)], o_relay.at[0], o_send.at[6], o_relay_recv.at[0], SAME_T),
        ring.copy(o_src.at[rows_of(OTHER_O)], o_relay.at[1], o_send.at[7], o_relay_recv.at[1], SAME_F),
    ] + [ring.copy(o_src.at[rows_of(slot)], o_pos.at[ring.me], o_send.at[slot], o_recv.at[slot], slot) for slot in (5, 4, 3, 2, 1)]
    o_pass = [
        ring.copy(o_relay.at[0], o_pos.at[ring.at(SAME_T)], o_send.at[8], o_recv.at[SAME_O], SAME_F),
        ring.copy(o_relay.at[1], o_pos.at[ring.at(SAME_F)], o_send.at[9], o_recv.at[OTHER_O], OTHER_T),
    ]
    o_keep = pltpu.make_async_copy(o_src.at[rows_of(0)], o_pos.at[ring.me], o_send.at[0])

    late = slab - LATE_ROWS
    early = {slot: late if slot == SAME_F else slab for slot in range(1, 6)}
    du_out = [
        ring.copy(acc.at[1, SAME_O], to_f.at[pl.ds(0, slab)], du_send.at[6], du_relay_recv.at[0], SAME_T),
        ring.copy(acc.at[1, OTHER_O], du_relay, du_send.at[7], du_relay_recv.at[1], SAME_F),
    ] + [ring.copy(acc.at[1, slot, pl.ds(0, early[slot])], du_pos.at[ring.me, pl.ds(0, early[slot])], du_send.at[slot], du_recv.at[slot], slot) for slot in (5, 4, 3, 2, 1)]
    du_keep = pltpu.make_async_copy(acc.at[1, 0], du_pos.at[ring.me], du_send.at[0])
    du_late = pltpu.make_async_copy(acc.at[1, SAME_F, pl.ds(late, slab - late)], to_f.at[pl.ds(slab, slab - late)], du_send.at[8])
    du_pass = ring.copy(du_relay, du_pos.at[ring.at(SAME_F)], du_send.at[9], du_recv.at[OTHER_O], OTHER_T)

    att_f_core.wait_recv()
    att_out[1].wait_recv()
    start(head_loads(2, 0))
    start(head_loads(0, 1))

    def arrive(slots):
        for slot in slots:
            if slot:
                ring.copy(uc_own.at[slot], uc_seq.at[slot], a2a_send.at[0], a2a_recv.at[slot], PARTNER).wait_recv()
            start(seq_own[2 * slot : 2 * slot + 2])

    def project(first, count):
        rows = pl.ds(first, count)
        for buf in (0, 1):
            c_all[2 + buf, rows, pl.ds(0, 6 * dim)] = dot_nt(u_all[0, rows, :], up_all[qkv_rows(buf), :]).astype(BF16)
            c_all[2 + buf, rows, pl.ds(6 * dim, 2 * dim)] = dot_nt(u_all[1, rows, :], up_all[wo_rows(buf), :]).astype(BF16)

    uc_keep.wait()
    arrive((0, 1, 4, 5, 2, 3))
    pl.semaphore_wait(free_slot.at[2], 1)
    start(uc_to_t)
    two_out.wait_recv()
    two_keep.wait()
    start(seq_two)
    out_own.wait()
    acc[1] = jnp.zeros(acc.shape[1:], F32)
    for copy in seq_own[:12] + head_loads(2, 0) + head_loads(0, 1):
        copy.wait()
    project(0, 6 * slab)
    arrive((6, 7))
    for copy in seq_own[12:]:
        copy.wait()
    project(6 * slab, 2 * slab)

    def chip_step(step, carry):
        buf = step % 2
        seq = step // 4
        relation = relation_of(step)

        @pl.when(step == 4)
        def _():
            near.wait_send()
            say_free(3, SAME_F)
            say_free(4, PARTNER)
            for copy in seq_two:
                copy.wait()
            for copy in uc_to_t[:4]:
                copy.wait_recv()

        @pl.when(step >= 2)
        def _():
            for copy in head_loads(0, buf):
                copy.wait()

        @pl.when((step == 3) | (step == 4))
        def _():
            start(head_loads(relation_of(step + 1), 1 - buf))

        kept = pl.ds(pl.multiple_of(jnp.where(step < 2, step, 2) * seq_len, seq_len), seq_len)
        heads = [ring.at_traced(relation * 2 + other) for other in (1, 0)]
        wo_copies = [
            pltpu.make_async_copy(up_all.at[pl.ds(pl.multiple_of(12 * dim + (2 * buf + index) * dim, dim), dim)], wo_full.at[head], wo_sem.at[index])
            for index, head in enumerate(heads)
        ]
        start(wo_copies)

        @pl.when(step >= 2)
        def _():
            c_all[2 + buf, :, pl.ds(0, 6 * dim)] = dot_nt(u_all[2 * seq], up_all[qkv_rows(buf), :]).astype(BF16)

        for index, head in enumerate(heads):
            columns = pl.ds(pl.multiple_of(head * dim, dim), dim)
            own = pl.ds(index * 3 * dim, 3 * dim)
            query, key, value = (c_all[2 + buf, :, pl.ds((index * 3 + part) * dim, dim)] for part in range(3))
            scores = dot_nt(query, key) * (scale * LOG2_E)
            grown = jnp.exp2(scores - jnp.max(scores, axis=-1, keepdims=True))
            prob = grown * (1.0 / jnp.sum(grown, axis=-1, keepdims=True))
            prob_b = prob.astype(BF16)
            c_all[seq, :, columns] = dot_nn(prob_b, value).astype(BF16)
            if index == 0:
                @pl.when(step == 4)
                def _():
                    for copy in uc_to_t[4:]:
                        copy.wait_recv()

                @pl.when(step >= 2)
                def _():
                    c_all[2 + buf, :, pl.ds(6 * dim, 2 * dim)] = dot_nt(u_all[2 * seq + 1], up_all[wo_rows(buf), :]).astype(BF16)

            d_out = c_all[2 + buf, :, pl.ds((6 + index) * dim, dim)]
            d_prob = dot_nt(d_out, value)
            d_score = (prob * (d_prob - jnp.sum(d_prob * prob, axis=-1, keepdims=True)) * scale).astype(BF16)
            down_all[kept, pl.ds(index * 3 * dim, dim)] = dot_nn(d_score, key).astype(BF16)
            down_all[kept, pl.ds((index * 3 + 1) * dim, dim)] = dot_nn(query.T, d_score).T.astype(BF16)
            down_all[kept, pl.ds((index * 3 + 2) * dim, dim)] = dot_nn(d_out.T, prob_b).T.astype(BF16)
            @pl.when(step >= 4)
            def _():
                dst = (spare, part_keep)[index].at[buf]
                dst[pl.ds(0, 3)] += dot_tn(down_all[kept, own], u_all[2]).reshape(3, dim, hidden)
                dst[3] += dot_tn(c_all[1, :, columns], u_all[3])

            if index == 0:
                @pl.when(step == 1)
                def _():
                    att_t.wait_recv()
                    att_t_core.start()

                @pl.when(step == 4)
                def _():
                    pl.semaphore_wait(free_slot.at[4], 1)
                    core_copies[0].start()

                @pl.when(step == 5)
                def _():
                    pl.semaphore_wait(free_slot.at[4], 1)
                    core_copies[1].start()

        @pl.when(step == 1)
        def _():
            att_t_core.wait_recv()
            start(head_loads(1, 0))

        @pl.when(step == 2)
        def _():
            att_o.wait_recv()
            att_o_core.start()

        @pl.when(step < 4)
        def _():
            def du_tile(part, carry):
                rows = pl.ds(pl.multiple_of(jnp.where(step < 2, step, 2) * seq_len + part * half, half), half)
                acc[1, pl.ds(part * fours, fours)] += dot_nn(down_all[rows, pl.ds(0, 6 * dim)], up_all[qkv_rows(buf), :]).reshape(fours, slab, hidden)
                return carry

            lax.fori_loop(0, 2, du_tile, 0)

        @pl.when(step == 2)
        def _():
            att_o_core.wait_recv()
            start(head_loads(3, 1))

        @pl.when(step == 3)
        def _():
            start(o_out)
            start(du_out)
            du_late.start()
            o_keep.start()
            du_keep.start()

            def own_gradients(pair, carry):
                own_rows = pl.ds(pl.multiple_of(pair * seq_len, seq_len), seq_len)
                for index, other in enumerate((1, 0)):
                    columns = pl.ds(pl.multiple_of(ring.at_traced(relation_of(pair) * 2 + other) * dim, dim), dim)
                    dst = (spare, part_keep)[index].at[pair]
                    dst[pl.ds(0, 3)] = dot_tn(down_all[own_rows, pl.ds(index * 3 * dim, 3 * dim)], u_all[0]).reshape(3, dim, hidden)
                    dst[3] = dot_tn(c_all[0, :, columns], u_all[1])
                return carry

            lax.fori_loop(0, 2, own_gradients, 0)

        @pl.when(step == 4)
        def _():
            core_copies[0].wait_recv()
            part_keep[0] += acc[0, pl.ds(0, 4)]
            say_free(4, PARTNER)
            pl.semaphore_wait(free_slot.at[3], 1)
            f_copy.start()

        for copy in wo_copies:
            copy.wait()
        return carry

    lax.fori_loop(0, 6, chip_step, 0)
    for copy in o_out[:2]:
        copy.wait_recv()
    start(o_pass)
    du_out[1].wait_recv()
    du_pass.start()
    core_copies[1].wait_recv()
    part_keep[1] += acc[0, pl.ds(0, 4)]
    for copy in du_out[2:]:
        copy.wait_recv()
    for slot in range(1, 8):
        ring.copy(o_pos.at[0], o_pos.at[ring.at(slot)], near_sem.at[0], o_recv.at[slot], PARTNER).wait_recv()
    du_out[0].wait_recv()
    du_pass.wait_recv()
    near.wait_recv()
    f_copy.wait_recv()
    part_keep[1] += acc[0, pl.ds(4, 4)]
    d_att_copy = pltpu.make_async_copy(part_keep.at[1], d_att, load_sem.at[0])
    d_att_copy.start()

    sends = att_out + [att_t, att_o, att_f_core, att_t_core, att_o_core] + list(a2a_out.values()) + a2a_pass + [two_out]
    for copy in sends + o_out + du_out + o_pass + uc_to_t + core_copies + [du_pass, f_copy]:
        copy.wait_send()
    du_late.wait()
    o_keep.wait()
    du_keep.wait()
    d_att_copy.wait()


def block_call(y_one, y_two, dy_one, dy_two, w_up, w_down, w_qkv, w_out):
    slabs, slab, hidden = y_one.shape
    tokens = slabs * slab
    ffn = w_down.shape[0]
    dim = w_out.shape[0]
    any_spec = pl.BlockSpec(memory_space=pl.ANY)
    dma, vmem, wide, narrow = pltpu.SemaphoreType.DMA, pltpu.VMEM, F32, BF16
    results = [
        ((slabs, slab, hidden), wide), ((slabs, slab, hidden), wide), ((slabs, slab, hidden), wide), ((slabs, slab, hidden), wide),
        ((4, dim, hidden), wide), ((slabs, slab, hidden), narrow), ((slabs, slab, hidden), wide), ((8, dim, hidden), narrow),
        ((slab + LATE_ROWS, hidden), wide),
    ]
    landing = [
        ((8, 2, slab, hidden), narrow), ((4, 2, slab, hidden), narrow), ((8, 4 * dim, hidden), narrow), ((2, slab, hidden), narrow), ((slab, hidden), wide),
    ]
    scratch = [
        vmem((4, tokens, hidden), BF16), vmem((4, tokens, hidden), BF16), vmem((6 * ffn, hidden), BF16), vmem((6 * ffn, hidden), BF16),
        vmem((2, slabs, slab, hidden), F32), vmem((2, 5, slab, hidden), F32), vmem((2, 4, dim, hidden), F32),
        vmem((8, 2, slab, hidden), BF16),
        dma((8,)), dma((2, 3)), dma((2, 2)), dma((16,)), dma((8, 2)), dma((6,)), dma((4, 2)), dma((7,)), dma((8,)), dma((11,)), dma((8,)), dma((3,)), dma((2,)), dma((2,)),
        dma((4, 8)), dma((2, 2, 2)), dma((2,)), dma((2,)), dma((2,)), dma((2,)), dma((2, 8)), dma((10,)), dma((8,)), dma((10,)), dma((8,)), dma((2,)), dma((2,)), dma((2,)),
        pltpu.SemaphoreType.REGULAR((6,)),
    ]
    return pl.pallas_call(
        functools.partial(block_kernel, dim ** -0.5),
        out_shape=[jax.ShapeDtypeStruct(shape, dtype) for shape, dtype in results + landing],
        in_specs=[any_spec] * 8,
        out_specs=[any_spec] * (len(results) + len(landing)),
        scratch_shapes=scratch,
        compiler_params=pltpu.CompilerParams(collective_id=0, has_side_effects=True, vmem_limit_bytes=VMEM_LIMIT),
        cost_estimate=pl.CostEstimate(flops=120 * 10**9, bytes_accessed=128 * 2**20, transcendentals=0),
        name="block",
    )(y_one, y_two, dy_one, dy_two, w_up.reshape(8, hidden // 8, ffn), w_down, w_qkv.reshape(3, 8, hidden // 8, dim), w_out)[: len(results)]


def finish_kernel(
    y_one, o_pos, wo_full, x_two, dx_one, dy_two, du_pos, part_own, near_recv, d_att,
    x_one_out, x_two_out, dx_one_out, dx_two_out, dw_up, dw_down, dw_qkv, dw_out,
    y_buf, o_buf, wo_buf, x_buf, dx_buf, dy_buf, du_buf, own_buf, near_buf, att_buf, up_out, qkv_out, load_sem, store_sem,
):
    tokens = y_buf.shape[0]
    dim = wo_buf.shape[0] // 8
    chunk = 256
    chunks = [pl.ds(index * chunk, chunk) for index in range(tokens // chunk)]

    def pieces(src, dst, sem, row):
        return [pltpu.make_async_copy(src.at[rows], dst.at[rows], sem.at[row, index]) for index, rows in enumerate(chunks)]

    def whole(src, dst, sem, row):
        return pltpu.make_async_copy(src, dst, sem.at[row, 0])

    ring = Ring()
    slab = tokens // 8
    sizes = {0: slab, PARTNER: slab, SAME_T: slab, OTHER_T: slab, SAME_F: slab - LATE_ROWS, OTHER_F: slab, OTHER_O: slab}
    slots = [pl.ds(pl.multiple_of(ring.at(slot) * slab, slab), size) for slot, size in sizes.items()]

    def slabs(src, dst, sem, row):
        return [pltpu.make_async_copy(src.at[rows], dst.at[rows], sem.at[row, index]) for index, rows in enumerate(slots)]

    x_in, dy_in, du_in = pieces(x_two, x_buf, load_sem, 0), slabs(dy_two, dy_buf, load_sem, 1), slabs(du_pos, du_buf, load_sem, 2)
    y_in, o_in = pieces(y_one, y_buf, load_sem, 3), pieces(o_pos, o_buf, load_sem, 4)
    wo_in, dx_in = whole(wo_full, wo_buf, load_sem, 5), pieces(dx_one, dx_buf, load_sem, 6)
    own_in, near_in, att_in = whole(part_own, own_buf, load_sem, 7), whole(near_recv, near_buf, load_sem, 8), whole(d_att, att_buf, load_sem, 9)
    order = [own_in, near_in, att_in, wo_in, *(copy for group in zip(y_in, o_in) for copy in group), *x_in, *(copy for group in zip(dy_in, du_in) for copy in group), *dx_in]
    for copy in order:
        copy.start()

    x_store, dx2_store, x1_store = pieces(x_buf, x_two_out, store_sem, 0), slabs(dy_buf, dx_two_out, store_sem, 1), pieces(y_buf, x_one_out, store_sem, 2)
    dx_store = pieces(dx_buf, dx_one_out, store_sem, 3)
    own_in.wait()
    near_in.wait()
    ffn = up_out.shape[1]
    own_buf[pl.ds(ffn, ffn), :] += near_buf[pl.ds(ffn, ffn), :]
    down_store = whole(own_buf.at[pl.ds(ffn, ffn)], dw_down, store_sem, 7)
    down_store.start()
    for part in range(up_out.shape[0] // ffn):
        columns = pl.ds(part * ffn, ffn)
        up_out[columns, :] = (own_buf[pl.ds(0, ffn), columns] + near_buf[pl.ds(0, ffn), columns]).T
    up_store = whole(up_out, dw_up, store_sem, 4)
    up_store.start()
    att_in.wait()
    for part in range(3):
        qkv_out[pl.ds(part, tokens, stride=3), 0, :] = att_buf[pl.ds(part * dim, dim), :].T
    qkv_store = whole(qkv_out, dw_qkv, store_sem, 5)
    qkv_store.start()
    out_store = whole(att_buf.at[pl.ds(3 * dim, dim)], dw_out, store_sem, 6)
    out_store.start()
    wo_in.wait()
    for index, rows in enumerate(chunks):
        y_in[index].wait()
        o_in[index].wait()
        y_buf[rows, :] -= dot_nn(o_buf[rows, :], wo_buf[...])
        x1_store[index].start()
    for index in range(len(chunks)):
        x_in[index].wait()
        x_store[index].start()
    for index, rows in enumerate(slots):
        dy_in[index].wait()
        du_in[index].wait()
        dy_buf[rows, :] += rms_back(x_buf[rows, :], du_buf[rows, :])
        dx2_store[index].start()
    for index in range(len(chunks)):
        dx_in[index].wait()
        dx_store[index].start()
    for copy in x_store + dx2_store + x1_store + dx_store + [up_store, qkv_store, out_store, down_store]:
        copy.wait()


def finish_call(y_one, o_pos, wo_full, x_two, dx_one, dy_two, du_pos, part_own, near_recv, d_att):
    tokens, hidden = y_one.shape
    ffn = part_own.shape[0] // 2
    dim = d_att.shape[0] // 4
    any_spec = pl.BlockSpec(memory_space=pl.ANY)
    dma, vmem = pltpu.SemaphoreType.DMA, pltpu.VMEM
    state = (tokens, hidden)
    out_shape = [jax.ShapeDtypeStruct(shape, F32) for shape in (state, state, state, state, (hidden, ffn), (ffn, hidden), (3 * hidden, 1, dim), (dim, hidden))]
    scratch = [
        vmem(state, F32), vmem(state, BF16), vmem((hidden, hidden), BF16), vmem(state, F32), vmem(state, F32), vmem(state, F32), vmem(state, F32),
        vmem(part_own.shape, F32), vmem(part_own.shape, F32), vmem(d_att.shape, F32), vmem((hidden, ffn), F32), vmem((3 * hidden, 1, dim), F32),
        dma((10, 7)), dma((8, 7)),
    ]
    return pl.pallas_call(
        finish_kernel,
        out_shape=out_shape,
        in_specs=[any_spec] * 10,
        out_specs=[any_spec] * 8,
        scratch_shapes=scratch,
        compiler_params=pltpu.CompilerParams(vmem_limit_bytes=VMEM_LIMIT),
        cost_estimate=pl.CostEstimate(flops=2 * 10**9, bytes_accessed=52 * 2**20, transcendentals=0),
        name="finish",
    )(y_one, o_pos, wo_full, x_two, dx_one, dy_two, du_pos, part_own, near_recv, d_att)


def last_kernel(x_two, dy_two, du_far, dx_two_in, dx_two_out, x_buf, dy_buf, du_buf, load_sem, store_sem):
    ring = Ring()
    slab = x_buf.shape[1]
    loads, stores, sizes = [], [], (slab, LATE_ROWS)
    for index, (slot, skip) in enumerate(((SAME_O, 0), (SAME_F, slab - LATE_ROWS))):
        size = sizes[index]
        rows = pl.ds(pl.multiple_of(ring.at(slot) * slab + skip, 16), size)
        sources = ((x_two.at[rows], x_buf), (dy_two.at[rows], dy_buf), (du_far.at[pl.ds(index * slab, size)], du_buf))
        loads.append([pltpu.make_async_copy(src, dst.at[index, pl.ds(0, size)], load_sem.at[index, which]) for which, (src, dst) in enumerate(sources)])
        stores.append(pltpu.make_async_copy(dy_buf.at[index, pl.ds(0, size)], dx_two_out.at[rows], store_sem.at[index]))
    for copies in loads:
        for copy in copies:
            copy.start()
    for index, copies in enumerate(loads):
        for copy in copies:
            copy.wait()
        rows = pl.ds(0, sizes[index])
        dy_buf[index, rows, :] += rms_back(x_buf[index, rows, :], du_buf[index, rows, :])
        stores[index].start()
    for copy in stores:
        copy.wait()


def last_call(x_two, dy_two, du_far, dx_two):
    tokens, hidden = x_two.shape
    any_spec = pl.BlockSpec(memory_space=pl.ANY)
    buf = pltpu.VMEM((2, tokens // 8, hidden), F32)
    return pl.pallas_call(
        last_kernel,
        out_shape=jax.ShapeDtypeStruct(dx_two.shape, F32),
        in_specs=[any_spec] * 4,
        out_specs=any_spec,
        input_output_aliases={3: 0},
        scratch_shapes=[buf, buf, buf, pltpu.SemaphoreType.DMA((2, 3)), pltpu.SemaphoreType.DMA((2,))],
        cost_estimate=pl.CostEstimate(flops=10**6, bytes_accessed=4 * 2**20, transcendentals=0),
        name="last",
    )(x_two, dy_two, du_far, dx_two)


def local_backward(y_one, y_two, dy_one, dy_two, w_qkv, w_out, w_up, w_down):
    hidden = y_one.shape[2]
    _, _, _, parts, dim = w_qkv.shape
    qkv_parts = jnp.swapaxes(w_qkv[0, :, 0], 0, 1)
    results = block_call(y_one, y_two, dy_one, dy_two, w_up[0], w_down[0], qkv_parts, w_out[0, 0])
    x_two, dx_one, part_own, near_recv, d_att, o_pos, du_pos, wo_full = (tensor.reshape(-1, hidden) for tensor in results[:8])
    devices = range(lax.axis_size("tp"))
    to_f = [(device, (3 - device // 2) * 2 + device % 2) for device in devices]
    du_far = lax.ppermute(results[8], "tp", to_f)
    y_flat, dy_flat = y_one.reshape(-1, hidden), dy_two.reshape(-1, hidden)
    *states, dw_up, dw_down, dw_qkv, dw_out = finish_call(y_flat, o_pos, wo_full, x_two, dx_one, dy_flat, du_pos, part_own, near_recv, d_att)
    states[3] = last_call(x_two, dy_flat, du_far, states[3])
    states = [tensor.reshape(y_one.shape) for tensor in states]
    return (*states, dw_qkv.reshape(1, hidden, 1, parts, dim), dw_out[None, None], dw_up[None], dw_down[None])


def solution(mesh):
    state_spec = P("dp", "tp", None)
    in_specs = (state_spec, state_spec, state_spec, state_spec, P(None, None, "tp", None, None), P(None, "tp", None, None), P(None, None, "tp"), P(None, "tp", None))
    out_specs = (state_spec, state_spec, state_spec, state_spec, P("dp", None, "tp", None, None), P("dp", "tp", None, None), P("dp", None, "tp"), P("dp", "tp", None))
    return jax.shard_map(local_backward, mesh=mesh, in_specs=in_specs, out_specs=out_specs, check_vma=False)
```

```python
import functools

import jax
import jax.numpy as jnp
from jax import lax
from jax.experimental import pallas as pl
from jax.experimental.pallas import tpu as pltpu
from jax.sharding import PartitionSpec as P

RMS_EPS = 1e-6
LOG2_E = 1.4426950408889634
LATE_ROWS = 96
FAR_ROWS = 16
MESH = pl.DeviceIdType.MESH
BF16, F32 = jnp.bfloat16, jnp.float32
VMEM_LIMIT = 64 * 1024 * 1024 - 65536


def inv_rms(tensor):
    return lax.rsqrt(jnp.mean(tensor * tensor, axis=-1, keepdims=True) + RMS_EPS)


def rms_norm(tensor):
    return tensor * inv_rms(tensor)


def rms_back(tensor, grad_in):
    scale = inv_rms(tensor)
    return scale * grad_in - tensor * (scale * scale * scale) * jnp.mean(grad_in * tensor, axis=-1, keepdims=True)


def gelu_and_slope(tensor):
    root = (2.0 / jnp.pi) ** 0.5
    squared = tensor * tensor
    tanh = jnp.tanh(root * (tensor + 0.044715 * (tensor * squared)))
    cdf = 0.5 * (1.0 + tanh)
    slope = cdf + (0.5 * root) * tensor * ((1.0 - tanh * tanh) * (1.0 + (3 * 0.044715) * squared))
    return tensor * cdf, slope


def dot_nn(left, right):
    return lax.dot_general(left, right, (((1,), (0,)), ((), ())), preferred_element_type=F32)


def dot_nt(left, right):
    return lax.dot_general(left, right, (((1,), (1,)), ((), ())), preferred_element_type=F32)


def dot_tn(left, right):
    return lax.dot_general(left, right, (((0,), (0,)), ((), ())), preferred_element_type=F32)


class Ring:
    def __init__(self):
        me = lax.axis_index("tp")
        chip, core = me // 2, me % 2
        self.me, self.chip, self.core = me, chip, core
        self.chips = (chip, chip + 1 - 2 * (chip % 2), 3 - chip, (chip + 2) % 4)

    def at(self, slot):
        core = self.core if slot % 2 == 0 else 1 - self.core
        return self.chips[slot // 2] * 2 + core

    def at_traced(self, slot):
        relation, other = slot // 2, slot % 2
        own, near_t, near_f, opposite = self.chips
        chip = jnp.where(relation == 0, own, jnp.where(relation == 1, near_t, jnp.where(relation == 2, near_f, opposite)))
        return chip * 2 + (self.core + other) % 2

    def arrive(self):
        for slot in (1, 2, 3, 4, 5):
            pl.semaphore_signal(pltpu.get_barrier_semaphore(), inc=1, device_id={"tp": self.at(slot)}, device_id_type=MESH)

    def meet(self):
        pl.semaphore_wait(pltpu.get_barrier_semaphore(), 5)

    def copy(self, src, dst, send_sem, recv_sem, slot):
        return pltpu.make_async_remote_copy(src_ref=src, dst_ref=dst, send_sem=send_sem, recv_sem=recv_sem, device_id={"tp": self.at(slot)}, device_id_type=MESH)


PARTNER, SAME_T, OTHER_T, SAME_F, OTHER_F, SAME_O, OTHER_O = 1, 2, 3, 4, 5, 6, 7


def block_kernel(
    scale,
    y_one, y_two, dy_one, dy_two, w_up, w_down, w_qkv, w_out,
    x_two, dx_one, part_own, near_recv, d_att, o_pos, du_pos, wo_full, to_f,
    uc_seq, uc_two, att_full, o_relay, du_relay,
    u_all, c_all, up_all, down_all, acc, spare, part_keep, uc_own,
    load_sem, y_sem, x_sem, w_send, w_recv, uc_send, uc_recv, att_send, att_recv, a2a_send, a2a_recv, relay_recv, near_sem, two_sem,
    seq_sem, head_sem, wo_sem, core_send, core_recv, f_sem, far_sem, o_send, o_recv, du_send, du_recv, o_relay_recv, du_relay_recv, far_recv, free_slot,
):
    ring = Ring()
    slabs, slab, hidden = acc.shape[1:]
    seq_len = slabs * slab
    half = seq_len // 2
    dim = w_out.shape[0]
    fours = slabs // 2

    def start(copies):
        for copy in copies:
            copy.start()

    def say_free(index, to):
        pl.semaphore_signal(free_slot.at[index], inc=1, device_id={"tp": ring.at(to)}, device_id_type=MESH)

    rooms = (0, 1, 2, 3, 4, 5, 1, 3)

    def room(slot):
        return pl.ds(rooms[slot] * half, half)

    def weight_pair(src_slot, dst_slot, to, index):
        return [
            ring.copy(buf.at[room(src_slot)], buf.at[room(dst_slot)], w_send.at[index + which], w_recv.at[dst_slot, which], to)
            for which, buf in enumerate((up_all, down_all))
        ]

    w_own = weight_pair(0, 1, PARTNER, 0) + weight_pair(0, 2, SAME_T, 2) + weight_pair(0, 4, SAME_F, 4)
    def far_part(src_slot, first, count, to, index, recv_sem):
        src, dst = (pl.ds(rooms[slot] * half + first, count) for slot in (src_slot, 6))
        return [ring.copy(buf.at[src], buf.at[dst], w_send.at[index + which], recv_sem.at[which], to) for which, buf in enumerate((up_all, down_all))]

    w_near_t = far_part(2, FAR_ROWS, half - FAR_ROWS, SAME_F, 6, w_recv.at[6])
    w_over_t = far_part(4, 0, FAR_ROWS, SAME_T, 14, far_recv)
    w_near_t_core = weight_pair(2, 3, PARTNER, 8)
    w_near_f = weight_pair(4, 5, PARTNER, 10)
    w_far = weight_pair(6, 7, PARTNER, 12)

    def uc_pair(src_slot, dst_slot, to, index):
        return [ring.copy(buf.at[src_slot], buf.at[dst_slot], uc_send.at[index + which], uc_recv.at[dst_slot, which], to) for which, buf in enumerate((u_all, c_all))]

    u_to_t, c_to_t = uc_pair(0, 2, SAME_T, 0)
    uc_core = uc_pair(0, 1, PARTNER, 2)
    uc_pass = uc_pair(2, 3, PARTNER, 4)

    def att(src, dst_slot, to, index):
        return ring.copy(src, att_full.at[dst_slot], att_send.at[index], att_recv.at[dst_slot], to)

    att_keep = [pltpu.make_async_copy(uc_own.at[part, 0], att_full.at[0, pl.ds(part * dim, dim)], x_sem.at[part // 2, part % 2]) for part in range(4)]
    att_out = [att(att_full.at[0], 4, SAME_F, 0), att(att_full.at[0], 1, PARTNER, 1)]
    att_t, att_o = att(att_full.at[0], 2, SAME_T, 2), att(att_full.at[4], 6, SAME_T, 3)
    att_f_core, att_t_core, att_o_core = att(att_full.at[4], 5, PARTNER, 4), att(att_full.at[2], 3, PARTNER, 5), att(att_full.at[6], 7, PARTNER, 6)

    a2a_out = {slot: ring.copy(uc_own.at[slot], uc_seq.at[slot], a2a_send.at[slot], a2a_recv.at[slot], slot) for slot in (1, 2, 3, 4, 5)}
    a2a_out[SAME_O] = ring.copy(uc_own.at[SAME_O], uc_two.at[2], a2a_send.at[SAME_O], relay_recv.at[0], SAME_F)
    a2a_out[OTHER_O] = ring.copy(uc_own.at[OTHER_O], uc_two.at[3], a2a_send.at[OTHER_O], relay_recv.at[1], OTHER_F)
    a2a_pass = [ring.copy(uc_two.at[2 + index], uc_seq.at[SAME_O + index], a2a_send.at[8 + index], a2a_recv.at[SAME_O + index], SAME_T) for index in (0, 1)]
    uc_keep = pltpu.make_async_copy(uc_own.at[0], uc_seq.at[0], load_sem.at[4])
    two_out = ring.copy(uc_own.at[OTHER_T], uc_two.at[1], a2a_send.at[10], relay_recv.at[2], PARTNER)
    two_keep = pltpu.make_async_copy(uc_own.at[SAME_T], uc_two.at[0], two_sem.at[0])
    near = ring.copy(acc.at[0], near_recv, near_sem.at[0], near_sem.at[1], SAME_F)

    loads = [
        pltpu.make_async_copy(w_down, down_all.at[room(0)], load_sem.at[0]),
        pltpu.make_async_copy(w_up, uc_own.at[:, 0, :, pl.ds(0, half)], load_sem.at[1]),
        pltpu.make_async_copy(y_one, acc.at[0], load_sem.at[2]),
        pltpu.make_async_copy(dy_two, acc.at[1], load_sem.at[3]),
    ]
    qkv_loads = [pltpu.make_async_copy(w_qkv.at[part], uc_own.at[:, 1, :, pl.ds(part * dim, dim)], y_sem.at[0, part]) for part in range(3)]
    ring.arrive()
    start(loads)
    start(qkv_loads)
    ring.meet()
    loads[0].wait()
    start(w_own[1::2])
    loads[1].wait()
    for part in range(half // dim):
        up_all[pl.ds(part * dim, dim), :] = uc_own[:, 0, :, pl.ds(part * dim, dim)].reshape(hidden, dim).T
    start(w_own[0::2])
    out_load = pltpu.make_async_copy(w_out, uc_own.at[3, 0], load_sem.at[7])
    out_load.start()
    loads[2].wait()
    loads[3].wait()

    def normalize(step, carry):
        rows = pl.ds(pl.multiple_of(step * slab, slab), slab)
        u_all[0, rows, :] = rms_norm(acc[0, step]).astype(BF16)
        c_all[0, rows, :] = acc[1, step].astype(BF16)
        acc[0, step] = jnp.zeros((slab, hidden), F32)
        acc[1, step] = jnp.zeros((slab, hidden), F32)
        return carry

    lax.fori_loop(0, slabs, normalize, 0)
    u_to_t.start()
    start(uc_core)
    for part in range(3):
        qkv_loads[part].wait()
        uc_own[part, 0] = uc_own[:, 1, :, pl.ds(part * dim, dim)].reshape(hidden, dim).T
    out_load.wait()
    start(att_keep)

    def y_loads(step, buf):
        seq = ring.at_traced(7 - step)
        return [pltpu.make_async_copy(src.at[seq], spare.at[buf, which], y_sem.at[buf, which]) for which, src in enumerate((y_one, y_two, dy_one))]

    def x_stores(step, buf):
        seq = ring.at_traced(7 - step)
        return [pltpu.make_async_copy(spare.at[buf, 3 + which], dst.at[seq], x_sem.at[buf, which]) for which, dst in enumerate((x_two, dx_one))]

    def feed_forward(step, carry):
        slot = jnp.where(step == 3, 4, jnp.where(step == 4, 3, step))
        place = pl.ds(pl.multiple_of(jnp.where(step == 6, 1, jnp.where(step == 7, 3, slot)) * half, half), half)

        @pl.when((step == 1) | ((step >= 3) & (step != 6)))
        def _():
            for which, buf in enumerate((up_all, down_all)):
                ring.copy(buf.at[place], buf.at[place], w_send.at[0], w_recv.at[slot, which], PARTNER).wait_recv()

        @pl.when(step == 6)
        def _():
            for copy in w_near_t + w_over_t:
                copy.wait_recv()

        @pl.when(step == 2)
        def _():
            pl.semaphore_wait(free_slot.at[0], 1)
            for which, buf in ((1, down_all), (0, up_all)):
                ring.copy(buf.at[room(2)], buf.at[room(2)], w_send.at[0], w_recv.at[2, which], PARTNER).wait_recv()
                w_near_t[which].start()
                w_near_t_core[which].start()
            for copy in att_keep:
                copy.wait()
            start(att_out)

        @pl.when(step == 3)
        def _():
            pl.semaphore_wait(free_slot.at[5], 1)
            start(w_over_t)
            c_to_t.start()
            start(w_near_f)

        @pl.when(step == 6)
        def _():
            pl.semaphore_wait(free_slot.at[1], 1)
            start(w_far)

        @pl.when(step == 7)
        def _():
            start(y_loads(0, 0))

        def rows_step(part, carry):
            rows = pl.ds(pl.multiple_of(part * half, half), half)
            quarter = pl.ds(part * fours, fours)
            hidden_act, slope = gelu_and_slope(dot_nt(u_all[0, rows, :], up_all[place, :]))
            d_pre = (slope * dot_nt(c_all[0, rows, :], down_all[place, :])).astype(BF16)
            acc[0, quarter] += dot_nn(hidden_act.astype(BF16), down_all[place, :]).reshape(fours, slab, hidden)
            acc[1, quarter] += dot_nn(d_pre, up_all[place, :]).reshape(fours, slab, hidden)
            return carry

        lax.fori_loop(0, 2, rows_step, 0)

        @pl.when(step == 1)
        def _():
            say_free(0, SAME_F)
            say_free(5, SAME_T)

        @pl.when(step == 4)
        def _():
            say_free(1, PARTNER)

        return carry

    lax.fori_loop(0, 8, feed_forward, 0)

    def finish(step, carry):
        slot = 7 - step
        buf = step % 2
        seq = ring.at_traced(slot)
        for copy in y_loads(step, buf):
            copy.wait()

        @pl.when(step < 7)
        def _():
            start(y_loads(step + 1, 1 - buf))

        @pl.when(step >= 2)
        def _():
            for copy in x_stores(step - 2, buf):
                copy.wait()

        y_first = spare[buf, 0]
        x_second = spare[buf, 1] - acc[0, seq]
        dy_first = spare[buf, 2] + rms_back(y_first, acc[1, seq])
        spare[buf, 3] = x_second
        spare[buf, 4] = dy_first
        uc_own[slot, 0] = rms_norm(x_second).astype(BF16)
        uc_own[slot, 1] = dy_first.astype(BF16)
        acc[0, seq] = jnp.zeros((slab, hidden), F32)
        acc[1, seq] = jnp.zeros((slab, hidden), F32)
        start(x_stores(step, buf))
        return carry

    lax.fori_loop(0, 8, finish, 0)
    for slot in (7, 6, 5, 4, 3, 2, 1):
        a2a_out[slot].start()
    uc_keep.start()
    two_out.start()
    two_keep.start()
    for step in (6, 7):
        for copy in x_stores(step, step % 2):
            copy.wait()

    def gradients(step, carry):
        first = step // 8
        tokens = (step % 8) // 2
        place = pl.ds(pl.multiple_of((4 - 4 * first) * half, half), half)

        @pl.when((step == 2) | (step == 4) | (step == 6))
        def _():
            for which, buf in enumerate((u_all, c_all)):
                ring.copy(buf.at[tokens], buf.at[tokens], uc_send.at[0], uc_recv.at[tokens, which], PARTNER).wait_recv()

        @pl.when(step == 4)
        def _():
            start(uc_pass)
            for index in (0, 1):
                a2a_out[SAME_O + index].wait_recv()
            start(a2a_pass)

        @pl.when(step == 8)
        def _():
            near.start()
            att_out[0].wait_recv()
            att_f_core.start()
            att_t.start()
            att_o.start()

        rows = pl.ds(pl.multiple_of((step % 2) * half, half), half)
        u_part, c_part = u_all[tokens, rows, :], c_all[tokens, rows, :]
        hidden_act, slope = gelu_and_slope(dot_nt(up_all[place, :], u_part))
        d_pre = (slope * dot_nt(down_all[place, :], c_part)).astype(BF16)
        acc[first, pl.ds(0, fours)] += dot_nn(d_pre, u_part).reshape(fours, slab, hidden)
        acc[first, pl.ds(fours, fours)] += dot_nn(hidden_act.astype(BF16), c_part).reshape(fours, slab, hidden)
        return carry

    lax.fori_loop(0, 16, gradients, 0)
    out_own = pltpu.make_async_copy(acc.at[1], part_own, load_sem.at[1])
    out_own.start()
    for copy in w_own + w_near_t + w_over_t + w_near_t_core + w_near_f + w_far + [u_to_t, c_to_t] + uc_core + uc_pass:
        copy.wait_send()
    say_free(2, SAME_T)

    def relation_of(step):
        base = step % 4
        return jnp.where(base == 0, 2, jnp.where(base == 3, 3, base - 1))

    def qkv_rows(buf):
        return pl.ds(pl.multiple_of(buf * 6 * dim, 2 * dim), 6 * dim)

    def wo_rows(buf):
        return pl.ds(pl.multiple_of(12 * dim + buf * 2 * dim, 2 * dim), 2 * dim)

    def head_loads(relation, buf):
        copies = []
        for index in (0, 1):
            head = att_full.at[relation * 2 + 1 - index]
            first, second = (pl.ds(pl.multiple_of(base + index * size, dim), size) for base, size in ((buf * 6 * dim, 3 * dim), (12 * dim + buf * 2 * dim, dim)))
            copies.append(pltpu.make_async_copy(head.at[pl.ds(0, 3 * dim)], up_all.at[first], head_sem.at[buf, index, 0]))
            copies.append(pltpu.make_async_copy(head.at[pl.ds(3 * dim, dim)], up_all.at[second], head_sem.at[buf, index, 1]))
        return copies

    def rows_of(slot):
        return pl.ds(slot * slab, slab)

    def seq_loads(seq, src, src_slot, slot):
        return [pltpu.make_async_copy(src.at[src_slot, which], u_all.at[2 * seq + which, rows_of(slot)], seq_sem.at[2 * seq + which, slot]) for which in (0, 1)]

    seq_own = [copy for slot in range(8) for copy in seq_loads(0, uc_seq, slot, slot)]
    seq_two = [copy for slot in range(4) for copy in seq_loads(1, uc_two, slot, slot)]
    uc_to_t = [
        ring.copy(uc_seq.at[slot, which], u_all.at[2 + which, rows_of(4 + index)], far_sem.at[0, 2 * index + which], far_sem.at[1, 2 * index + which], SAME_T)
        for which in (0, 1)
        for index, slot in enumerate((0, 1, 4, 5))
    ]
    core_copies = [ring.copy(spare.at[index, pl.ds(0, 4)], acc.at[0, pl.ds(0, 4)], core_send.at[index], core_recv.at[index], PARTNER) for index in (0, 1)]
    f_copy = ring.copy(part_keep.at[0], acc.at[0, pl.ds(4, 4)], f_sem.at[0], f_sem.at[1], SAME_F)

    o_src = c_all.at[0]
    o_out = [
        ring.copy(o_src.at[rows_of(SAME_O)], o_relay.at[0], o_send.at[6], o_relay_recv.at[0], SAME_T),
        ring.copy(o_src.at[rows_of(OTHER_O)], o_relay.at[1], o_send.at[7], o_relay_recv.at[1], SAME_F),
    ] + [ring.copy(o_src.at[rows_of(slot)], o_pos.at[ring.me], o_send.at[slot], o_recv.at[slot], slot) for slot in (5, 4, 3, 2, 1)]
    o_pass = [
        ring.copy(o_relay.at[0], o_pos.at[ring.at(SAME_T)], o_send.at[8], o_recv.at[SAME_O], SAME_F),
        ring.copy(o_relay.at[1], o_pos.at[ring.at(SAME_F)], o_send.at[9], o_recv.at[OTHER_O], OTHER_T),
    ]
    o_keep = pltpu.make_async_copy(o_src.at[rows_of(0)], o_pos.at[ring.me], o_send.at[0])

    late = slab - LATE_ROWS
    early = {slot: late if slot == SAME_F else slab for slot in range(1, 6)}
    du_out = [
        ring.copy(acc.at[1, SAME_O], to_f.at[pl.ds(0, slab)], du_send.at[6], du_relay_recv.at[0], SAME_T),
        ring.copy(acc.at[1, OTHER_O], du_relay, du_send.at[7], du_relay_recv.at[1], SAME_F),
    ] + [ring.copy(acc.at[1, slot, pl.ds(0, early[slot])], du_pos.at[ring.me, pl.ds(0, early[slot])], du_send.at[slot], du_recv.at[slot], slot) for slot in (5, 4, 3, 2, 1)]
    du_keep = pltpu.make_async_copy(acc.at[1, 0], du_pos.at[ring.me], du_send.at[0])
    du_late = pltpu.make_async_copy(acc.at[1, SAME_F, pl.ds(late, slab - late)], to_f.at[pl.ds(slab, slab - late)], du_send.at[8])
    du_pass = ring.copy(du_relay, du_pos.at[ring.at(SAME_F)], du_send.at[9], du_recv.at[OTHER_O], OTHER_T)

    att_f_core.wait_recv()
    att_out[1].wait_recv()
    start(head_loads(2, 0))
    start(head_loads(0, 1))

    def arrive(slots):
        for slot in slots:
            if slot:
                ring.copy(uc_own.at[slot], uc_seq.at[slot], a2a_send.at[0], a2a_recv.at[slot], PARTNER).wait_recv()
            start(seq_own[2 * slot : 2 * slot + 2])

    def project(first, count):
        rows = pl.ds(first, count)
        for buf in (0, 1):
            c_all[2 + buf, rows, pl.ds(0, 6 * dim)] = dot_nt(u_all[0, rows, :], up_all[qkv_rows(buf), :]).astype(BF16)
            c_all[2 + buf, rows, pl.ds(6 * dim, 2 * dim)] = dot_nt(u_all[1, rows, :], up_all[wo_rows(buf), :]).astype(BF16)

    uc_keep.wait()
    arrive((0, 1, 4, 5, 2, 3))
    pl.semaphore_wait(free_slot.at[2], 1)
    start(uc_to_t)
    two_out.wait_recv()
    two_keep.wait()
    start(seq_two)
    out_own.wait()
    acc[1] = jnp.zeros(acc.shape[1:], F32)
    for copy in seq_own[:12] + head_loads(2, 0) + head_loads(0, 1):
        copy.wait()
    project(0, 6 * slab)
    arrive((6, 7))
    for copy in seq_own[12:]:
        copy.wait()
    project(6 * slab, 2 * slab)

    def chip_step(step, carry):
        buf = step % 2
        seq = step // 4
        relation = relation_of(step)

        @pl.when(step == 4)
        def _():
            near.wait_send()
            say_free(3, SAME_F)
            say_free(4, PARTNER)
            for copy in seq_two:
                copy.wait()
            for copy in uc_to_t[:4]:
                copy.wait_recv()

        @pl.when(step >= 2)
        def _():
            for copy in head_loads(0, buf):
                copy.wait()

        @pl.when((step == 3) | (step == 4))
        def _():
            start(head_loads(relation_of(step + 1), 1 - buf))

        kept = pl.ds(pl.multiple_of(jnp.where(step < 2, step, 2) * seq_len, seq_len), seq_len)
        heads = [ring.at_traced(relation * 2 + other) for other in (1, 0)]
        wo_copies = [
            pltpu.make_async_copy(up_all.at[pl.ds(pl.multiple_of(12 * dim + (2 * buf + index) * dim, dim), dim)], wo_full.at[head], wo_sem.at[index])
            for index, head in enumerate(heads)
        ]
        start(wo_copies)

        @pl.when(step >= 2)
        def _():
            c_all[2 + buf, :, pl.ds(0, 6 * dim)] = dot_nt(u_all[2 * seq], up_all[qkv_rows(buf), :]).astype(BF16)

        for index, head in enumerate(heads):
            columns = pl.ds(pl.multiple_of(head * dim, dim), dim)
            own = pl.ds(index * 3 * dim, 3 * dim)
            query, key, value = (c_all[2 + buf, :, pl.ds((index * 3 + part) * dim, dim)] for part in range(3))
            scores = dot_nt(query, key) * (scale * LOG2_E)
            grown = jnp.exp2(scores - jnp.max(scores, axis=-1, keepdims=True))
            prob = grown * (1.0 / jnp.sum(grown, axis=-1, keepdims=True))
            prob_b = prob.astype(BF16)
            c_all[seq, :, columns] = dot_nn(prob_b, value).astype(BF16)
            if index == 0:
                @pl.when(step == 4)
                def _():
                    for copy in uc_to_t[4:]:
                        copy.wait_recv()

                @pl.when(step >= 2)
                def _():
                    c_all[2 + buf, :, pl.ds(6 * dim, 2 * dim)] = dot_nt(u_all[2 * seq + 1], up_all[wo_rows(buf), :]).astype(BF16)

            d_out = c_all[2 + buf, :, pl.ds((6 + index) * dim, dim)]
            d_prob = dot_nt(d_out, value)
            d_score = (prob * (d_prob - jnp.sum(d_prob * prob, axis=-1, keepdims=True)) * scale).astype(BF16)
            down_all[kept, pl.ds(index * 3 * dim, dim)] = dot_nn(d_score, key).astype(BF16)
            down_all[kept, pl.ds((index * 3 + 1) * dim, dim)] = dot_nn(query.T, d_score).T.astype(BF16)
            down_all[kept, pl.ds((index * 3 + 2) * dim, dim)] = dot_nn(d_out.T, prob_b).T.astype(BF16)
            @pl.when(step >= 4)
            def _():
                dst = (spare, part_keep)[index].at[buf]
                dst[pl.ds(0, 3)] += dot_tn(down_all[kept, own], u_all[2]).reshape(3, dim, hidden)
                dst[3] += dot_tn(c_all[1, :, columns], u_all[3])

            if index == 0:
                @pl.when(step == 1)
                def _():
                    att_t.wait_recv()
                    att_t_core.start()

                @pl.when(step == 4)
                def _():
                    pl.semaphore_wait(free_slot.at[4], 1)
                    core_copies[0].start()

                @pl.when(step == 5)
                def _():
                    pl.semaphore_wait(free_slot.at[4], 1)
                    core_copies[1].start()

        @pl.when(step == 1)
        def _():
            att_t_core.wait_recv()
            start(head_loads(1, 0))

        @pl.when(step == 2)
        def _():
            att_o.wait_recv()
            att_o_core.start()

        @pl.when(step < 4)
        def _():
            def du_tile(part, carry):
                rows = pl.ds(pl.multiple_of(jnp.where(step < 2, step, 2) * seq_len + part * half, half), half)
                acc[1, pl.ds(part * fours, fours)] += dot_nn(down_all[rows, pl.ds(0, 6 * dim)], up_all[qkv_rows(buf), :]).reshape(fours, slab, hidden)
                return carry

            lax.fori_loop(0, 2, du_tile, 0)

        @pl.when(step == 2)
        def _():
            att_o_core.wait_recv()
            start(head_loads(3, 1))

        @pl.when(step == 3)
        def _():
            start(o_out)
            start(du_out)
            du_late.start()
            o_keep.start()
            du_keep.start()

            def own_gradients(pair, carry):
                own_rows = pl.ds(pl.multiple_of(pair * seq_len, seq_len), seq_len)
                for index, other in enumerate((1, 0)):
                    columns = pl.ds(pl.multiple_of(ring.at_traced(relation_of(pair) * 2 + other) * dim, dim), dim)
                    dst = (spare, part_keep)[index].at[pair]
                    dst[pl.ds(0, 3)] = dot_tn(down_all[own_rows, pl.ds(index * 3 * dim, 3 * dim)], u_all[0]).reshape(3, dim, hidden)
                    dst[3] = dot_tn(c_all[0, :, columns], u_all[1])
                return carry

            lax.fori_loop(0, 2, own_gradients, 0)

        @pl.when(step == 4)
        def _():
            core_copies[0].wait_recv()
            part_keep[0] += acc[0, pl.ds(0, 4)]
            say_free(4, PARTNER)
            pl.semaphore_wait(free_slot.at[3], 1)
            f_copy.start()

        for copy in wo_copies:
            copy.wait()
        return carry

    lax.fori_loop(0, 6, chip_step, 0)
    for copy in o_out[:2]:
        copy.wait_recv()
    start(o_pass)
    du_out[1].wait_recv()
    du_pass.start()
    core_copies[1].wait_recv()
    part_keep[1] += acc[0, pl.ds(0, 4)]
    for copy in du_out[2:]:
        copy.wait_recv()
    for slot in range(1, 8):
        ring.copy(o_pos.at[0], o_pos.at[ring.at(slot)], near_sem.at[0], o_recv.at[slot], PARTNER).wait_recv()
    du_out[0].wait_recv()
    du_pass.wait_recv()
    near.wait_recv()
    f_copy.wait_recv()
    part_keep[1] += acc[0, pl.ds(4, 4)]
    d_att_copy = pltpu.make_async_copy(part_keep.at[1], d_att, load_sem.at[0])
    d_att_copy.start()

    sends = att_out + [att_t, att_o, att_f_core, att_t_core, att_o_core] + list(a2a_out.values()) + a2a_pass + [two_out]
    for copy in sends + o_out + du_out + o_pass + uc_to_t + core_copies + [du_pass, f_copy]:
        copy.wait_send()
    du_late.wait()
    o_keep.wait()
    du_keep.wait()
    d_att_copy.wait()


def block_call(y_one, y_two, dy_one, dy_two, w_up, w_down, w_qkv, w_out):
    slabs, slab, hidden = y_one.shape
    tokens = slabs * slab
    ffn = w_down.shape[0]
    dim = w_out.shape[0]
    any_spec = pl.BlockSpec(memory_space=pl.ANY)
    dma, vmem, wide, narrow = pltpu.SemaphoreType.DMA, pltpu.VMEM, F32, BF16
    results = [
        ((slabs, slab, hidden), wide), ((slabs, slab, hidden), wide), ((slabs, slab, hidden), wide), ((slabs, slab, hidden), wide),
        ((4, dim, hidden), wide), ((slabs, slab, hidden), narrow), ((slabs, slab, hidden), wide), ((8, dim, hidden), narrow),
        ((slab + LATE_ROWS, hidden), wide),
    ]
    landing = [
        ((8, 2, slab, hidden), narrow), ((4, 2, slab, hidden), narrow), ((8, 4 * dim, hidden), narrow), ((2, slab, hidden), narrow), ((slab, hidden), wide),
    ]
    scratch = [
        vmem((4, tokens, hidden), BF16), vmem((4, tokens, hidden), BF16), vmem((6 * ffn, hidden), BF16), vmem((6 * ffn, hidden), BF16),
        vmem((2, slabs, slab, hidden), F32), vmem((2, 5, slab, hidden), F32), vmem((2, 4, dim, hidden), F32),
        vmem((8, 2, slab, hidden), BF16),
        dma((8,)), dma((2, 3)), dma((2, 2)), dma((16,)), dma((8, 2)), dma((6,)), dma((4, 2)), dma((7,)), dma((8,)), dma((11,)), dma((8,)), dma((3,)), dma((2,)), dma((2,)),
        dma((4, 8)), dma((2, 2, 2)), dma((2,)), dma((2,)), dma((2,)), dma((2,)), dma((2, 8)), dma((10,)), dma((8,)), dma((10,)), dma((8,)), dma((2,)), dma((2,)), dma((2,)),
        pltpu.SemaphoreType.REGULAR((6,)),
    ]
    return pl.pallas_call(
        functools.partial(block_kernel, dim ** -0.5),
        out_shape=[jax.ShapeDtypeStruct(shape, dtype) for shape, dtype in results + landing],
        in_specs=[any_spec] * 8,
        out_specs=[any_spec] * (len(results) + len(landing)),
        scratch_shapes=scratch,
        compiler_params=pltpu.CompilerParams(collective_id=0, has_side_effects=True, vmem_limit_bytes=VMEM_LIMIT),
        cost_estimate=pl.CostEstimate(flops=120 * 10**9, bytes_accessed=128 * 2**20, transcendentals=0),
        name="block",
    )(y_one, y_two, dy_one, dy_two, w_up.reshape(8, hidden // 8, ffn), w_down, w_qkv.reshape(3, 8, hidden // 8, dim), w_out)[: len(results)]


def finish_kernel(
    y_one, o_pos, wo_full, x_two, dx_one, dy_two, du_pos, part_own, near_recv, d_att,
    x_one_out, x_two_out, dx_one_out, dx_two_out, dw_up, dw_down, dw_qkv, dw_out,
    y_buf, o_buf, wo_buf, x_buf, dx_buf, dy_buf, du_buf, own_buf, near_buf, att_buf, up_out, qkv_out, load_sem, store_sem,
):
    tokens = y_buf.shape[0]
    dim = wo_buf.shape[0] // 8
    chunk = 256
    chunks = [pl.ds(index * chunk, chunk) for index in range(tokens // chunk)]

    def pieces(src, dst, sem, row):
        return [pltpu.make_async_copy(src.at[rows], dst.at[rows], sem.at[row, index]) for index, rows in enumerate(chunks)]

    def whole(src, dst, sem, row):
        return pltpu.make_async_copy(src, dst, sem.at[row, 0])

    ring = Ring()
    slab = tokens // 8
    sizes = {0: slab, PARTNER: slab, SAME_T: slab, OTHER_T: slab, SAME_F: slab - LATE_ROWS, OTHER_F: slab, OTHER_O: slab}
    slots = [pl.ds(pl.multiple_of(ring.at(slot) * slab, slab), size) for slot, size in sizes.items()]

    def slabs(src, dst, sem, row):
        return [pltpu.make_async_copy(src.at[rows], dst.at[rows], sem.at[row, index]) for index, rows in enumerate(slots)]

    x_in, dy_in, du_in = pieces(x_two, x_buf, load_sem, 0), slabs(dy_two, dy_buf, load_sem, 1), slabs(du_pos, du_buf, load_sem, 2)
    y_in, o_in = pieces(y_one, y_buf, load_sem, 3), pieces(o_pos, o_buf, load_sem, 4)
    wo_in, dx_in = whole(wo_full, wo_buf, load_sem, 5), pieces(dx_one, dx_buf, load_sem, 6)
    own_in, near_in, att_in = whole(part_own, own_buf, load_sem, 7), whole(near_recv, near_buf, load_sem, 8), whole(d_att, att_buf, load_sem, 9)
    order = [own_in, near_in, att_in, wo_in, *(copy for group in zip(y_in, o_in) for copy in group), *x_in, *(copy for group in zip(dy_in, du_in) for copy in group), *dx_in]
    for copy in order:
        copy.start()

    x_store, dx2_store, x1_store = pieces(x_buf, x_two_out, store_sem, 0), slabs(dy_buf, dx_two_out, store_sem, 1), pieces(y_buf, x_one_out, store_sem, 2)
    dx_store = pieces(dx_buf, dx_one_out, store_sem, 3)
    own_in.wait()
    near_in.wait()
    ffn = up_out.shape[1]
    own_buf[pl.ds(ffn, ffn), :] += near_buf[pl.ds(ffn, ffn), :]
    down_store = whole(own_buf.at[pl.ds(ffn, ffn)], dw_down, store_sem, 7)
    down_store.start()
    for part in range(up_out.shape[0] // ffn):
        columns = pl.ds(part * ffn, ffn)
        up_out[columns, :] = (own_buf[pl.ds(0, ffn), columns] + near_buf[pl.ds(0, ffn), columns]).T
    up_store = whole(up_out, dw_up, store_sem, 4)
    up_store.start()
    att_in.wait()
    for part in range(3):
        qkv_out[pl.ds(part, tokens, stride=3), 0, :] = att_buf[pl.ds(part * dim, dim), :].T
    qkv_store = whole(qkv_out, dw_qkv, store_sem, 5)
    qkv_store.start()
    out_store = whole(att_buf.at[pl.ds(3 * dim, dim)], dw_out, store_sem, 6)
    out_store.start()
    wo_in.wait()
    for index, rows in enumerate(chunks):
        y_in[index].wait()
        o_in[index].wait()
        y_buf[rows, :] -= dot_nn(o_buf[rows, :], wo_buf[...])
        x1_store[index].start()
    for index in range(len(chunks)):
        x_in[index].wait()
        x_store[index].start()
    for index, rows in enumerate(slots):
        dy_in[index].wait()
        du_in[index].wait()
        dy_buf[rows, :] += rms_back(x_buf[rows, :], du_buf[rows, :])
        dx2_store[index].start()
    for index in range(len(chunks)):
        dx_in[index].wait()
        dx_store[index].start()
    for copy in x_store + dx2_store + x1_store + dx_store + [up_store, qkv_store, out_store, down_store]:
        copy.wait()


def finish_call(y_one, o_pos, wo_full, x_two, dx_one, dy_two, du_pos, part_own, near_recv, d_att):
    tokens, hidden = y_one.shape
    ffn = part_own.shape[0] // 2
    dim = d_att.shape[0] // 4
    any_spec = pl.BlockSpec(memory_space=pl.ANY)
    dma, vmem = pltpu.SemaphoreType.DMA, pltpu.VMEM
    state = (tokens, hidden)
    out_shape = [jax.ShapeDtypeStruct(shape, F32) for shape in (state, state, state, state, (hidden, ffn), (ffn, hidden), (3 * hidden, 1, dim), (dim, hidden))]
    scratch = [
        vmem(state, F32), vmem(state, BF16), vmem((hidden, hidden), BF16), vmem(state, F32), vmem(state, F32), vmem(state, F32), vmem(state, F32),
        vmem(part_own.shape, F32), vmem(part_own.shape, F32), vmem(d_att.shape, F32), vmem((hidden, ffn), F32), vmem((3 * hidden, 1, dim), F32),
        dma((10, 7)), dma((8, 7)),
    ]
    return pl.pallas_call(
        finish_kernel,
        out_shape=out_shape,
        in_specs=[any_spec] * 10,
        out_specs=[any_spec] * 8,
        scratch_shapes=scratch,
        compiler_params=pltpu.CompilerParams(vmem_limit_bytes=VMEM_LIMIT),
        cost_estimate=pl.CostEstimate(flops=2 * 10**9, bytes_accessed=52 * 2**20, transcendentals=0),
        name="finish",
    )(y_one, o_pos, wo_full, x_two, dx_one, dy_two, du_pos, part_own, near_recv, d_att)


def last_kernel(x_two, dy_two, du_far, dx_two_in, dx_two_out, x_buf, dy_buf, du_buf, load_sem, store_sem):
    ring = Ring()
    slab = x_buf.shape[1]
    loads, stores, sizes = [], [], (slab, LATE_ROWS)
    for index, (slot, skip) in enumerate(((SAME_O, 0), (SAME_F, slab - LATE_ROWS))):
        size = sizes[index]
        rows = pl.ds(pl.multiple_of(ring.at(slot) * slab + skip, 16), size)
        sources = ((x_two.at[rows], x_buf), (dy_two.at[rows], dy_buf), (du_far.at[pl.ds(index * slab, size)], du_buf))
        loads.append([pltpu.make_async_copy(src, dst.at[index, pl.ds(0, size)], load_sem.at[index, which]) for which, (src, dst) in enumerate(sources)])
        stores.append(pltpu.make_async_copy(dy_buf.at[index, pl.ds(0, size)], dx_two_out.at[rows], store_sem.at[index]))
    for copies in loads:
        for copy in copies:
            copy.start()
    for index, copies in enumerate(loads):
        for copy in copies:
            copy.wait()
        rows = pl.ds(0, sizes[index])
        dy_buf[index, rows, :] += rms_back(x_buf[index, rows, :], du_buf[index, rows, :])
        stores[index].start()
    for copy in stores:
        copy.wait()


def last_call(x_two, dy_two, du_far, dx_two):
    tokens, hidden = x_two.shape
    any_spec = pl.BlockSpec(memory_space=pl.ANY)
    buf = pltpu.VMEM((2, tokens // 8, hidden), F32)
    return pl.pallas_call(
        last_kernel,
        out_shape=jax.ShapeDtypeStruct(dx_two.shape, F32),
        in_specs=[any_spec] * 4,
        out_specs=any_spec,
        input_output_aliases={3: 0},
        scratch_shapes=[buf, buf, buf, pltpu.SemaphoreType.DMA((2, 3)), pltpu.SemaphoreType.DMA((2,))],
        cost_estimate=pl.CostEstimate(flops=10**6, bytes_accessed=4 * 2**20, transcendentals=0),
        name="last",
    )(x_two, dy_two, du_far, dx_two)


def local_backward(y_one, y_two, dy_one, dy_two, w_qkv, w_out, w_up, w_down):
    hidden = y_one.shape[2]
    _, _, _, parts, dim = w_qkv.shape
    qkv_parts = jnp.swapaxes(w_qkv[0, :, 0], 0, 1)
    results = block_call(y_one, y_two, dy_one, dy_two, w_up[0], w_down[0], qkv_parts, w_out[0, 0])
    x_two, dx_one, part_own, near_recv, d_att, o_pos, du_pos, wo_full = (tensor.reshape(-1, hidden) for tensor in results[:8])
    devices = range(lax.axis_size("tp"))
    to_f = [(device, (3 - device // 2) * 2 + device % 2) for device in devices]
    du_far = lax.ppermute(results[8], "tp", to_f)
    y_flat, dy_flat = y_one.reshape(-1, hidden), dy_two.reshape(-1, hidden)
    *states, dw_up, dw_down, dw_qkv, dw_out = finish_call(y_flat, o_pos, wo_full, x_two, dx_one, dy_flat, du_pos, part_own, near_recv, d_att)
    states[3] = last_call(x_two, dy_flat, du_far, states[3])
    states = [tensor.reshape(y_one.shape) for tensor in states]
    return (*states, dw_qkv.reshape(1, hidden, 1, parts, dim), dw_out[None, None], dw_up[None], dw_down[None])


def solution(mesh):
    state_spec = P("dp", "tp", None)
    in_specs = (state_spec, state_spec, state_spec, state_spec, P(None, None, "tp", None, None), P(None, "tp", None, None), P(None, None, "tp"), P(None, "tp", None))
    out_specs = (state_spec, state_spec, state_spec, state_spec, P("dp", None, "tp", None, None), P("dp", "tp", None, None), P("dp", None, "tp"), P("dp", "tp", None))
    return jax.shard_map(local_backward, mesh=mesh, in_specs=in_specs, out_specs=out_specs, check_vma=False)
```

```python
import functools

import jax
import jax.numpy as jnp
from jax import lax
from jax.experimental import pallas as pl
from jax.experimental.pallas import tpu as pltpu
from jax.sharding import PartitionSpec as P

RMS_EPS = 1e-6
LOG2_E = 1.4426950408889634
LATE_ROWS = 96
FAR_ROWS = 16
MESH = pl.DeviceIdType.MESH
BF16, F32 = jnp.bfloat16, jnp.float32
VMEM_LIMIT = 64 * 1024 * 1024 - 65536


def inv_rms(tensor):
    return lax.rsqrt(jnp.mean(tensor * tensor, axis=-1, keepdims=True) + RMS_EPS)


def rms_norm(tensor):
    return tensor * inv_rms(tensor)


def rms_back(tensor, grad_in):
    scale = inv_rms(tensor)
    return scale * grad_in - tensor * (scale * scale * scale) * jnp.mean(grad_in * tensor, axis=-1, keepdims=True)


def gelu_and_slope(tensor):
    root = (2.0 / jnp.pi) ** 0.5
    squared = tensor * tensor
    tanh = jnp.tanh(root * (tensor + 0.044715 * (tensor * squared)))
    cdf = 0.5 * (1.0 + tanh)
    slope = cdf + (0.5 * root) * tensor * ((1.0 - tanh * tanh) * (1.0 + (3 * 0.044715) * squared))
    return tensor * cdf, slope


def dot_nn(left, right):
    return lax.dot_general(left, right, (((1,), (0,)), ((), ())), preferred_element_type=F32)


def dot_nt(left, right):
    return lax.dot_general(left, right, (((1,), (1,)), ((), ())), preferred_element_type=F32)


def dot_tn(left, right):
    return lax.dot_general(left, right, (((0,), (0,)), ((), ())), preferred_element_type=F32)


class Ring:
    def __init__(self):
        me = lax.axis_index("tp")
        chip, core = me // 2, me % 2
        self.me, self.chip, self.core = me, chip, core
        self.chips = (chip, chip + 1 - 2 * (chip % 2), 3 - chip, (chip + 2) % 4)

    def at(self, slot):
        core = self.core if slot % 2 == 0 else 1 - self.core
        return self.chips[slot // 2] * 2 + core

    def at_traced(self, slot):
        relation, other = slot // 2, slot % 2
        own, near_t, near_f, opposite = self.chips
        chip = jnp.where(relation == 0, own, jnp.where(relation == 1, near_t, jnp.where(relation == 2, near_f, opposite)))
        return chip * 2 + (self.core + other) % 2

    def arrive(self):
        for slot in (1, 2, 3, 4, 5):
            pl.semaphore_signal(pltpu.get_barrier_semaphore(), inc=1, device_id={"tp": self.at(slot)}, device_id_type=MESH)

    def meet(self):
        pl.semaphore_wait(pltpu.get_barrier_semaphore(), 5)

    def copy(self, src, dst, send_sem, recv_sem, slot):
        return pltpu.make_async_remote_copy(src_ref=src, dst_ref=dst, send_sem=send_sem, recv_sem=recv_sem, device_id={"tp": self.at(slot)}, device_id_type=MESH)


PARTNER, SAME_T, OTHER_T, SAME_F, OTHER_F, SAME_O, OTHER_O = 1, 2, 3, 4, 5, 6, 7


def block_kernel(
    scale,
    y_one, y_two, dy_one, dy_two, w_up, w_down, w_qkv, w_out,
    x_two, dx_one, part_own, near_recv, d_att, o_pos, du_pos, wo_full, to_f,
    uc_seq, uc_two, att_full, o_relay, du_relay,
    u_all, c_all, up_all, down_all, acc, spare, part_keep, uc_own,
    load_sem, y_sem, x_sem, w_send, w_recv, uc_send, uc_recv, att_send, att_recv, a2a_send, a2a_recv, relay_recv, near_sem, two_sem,
    seq_sem, head_sem, wo_sem, core_send, core_recv, f_sem, far_sem, o_send, o_recv, du_send, du_recv, o_relay_recv, du_relay_recv, far_recv, free_slot,
):
    ring = Ring()
    slabs, slab, hidden = acc.shape[1:]
    seq_len = slabs * slab
    half = seq_len // 2
    dim = w_out.shape[0]
    fours = slabs // 2

    def start(copies):
        for copy in copies:
            copy.start()

    def say_free(index, to):
        pl.semaphore_signal(free_slot.at[index], inc=1, device_id={"tp": ring.at(to)}, device_id_type=MESH)

    rooms = (0, 1, 2, 3, 4, 5, 1, 3)

    def room(slot):
        return pl.ds(rooms[slot] * half, half)

    def weight_pair(src_slot, dst_slot, to, index):
        return [
            ring.copy(buf.at[room(src_slot)], buf.at[room(dst_slot)], w_send.at[index + which], w_recv.at[dst_slot, which], to)
            for which, buf in enumerate((up_all, down_all))
        ]

    w_own = weight_pair(0, 1, PARTNER, 0) + weight_pair(0, 2, SAME_T, 2) + weight_pair(0, 4, SAME_F, 4)
    def far_part(src_slot, first, count, to, index, recv_sem):
        src, dst = (pl.ds(rooms[slot] * half + first, count) for slot in (src_slot, 6))
        return [ring.copy(buf.at[src], buf.at[dst], w_send.at[index + which], recv_sem.at[which], to) for which, buf in enumerate((up_all, down_all))]

    w_near_t = far_part(2, FAR_ROWS, half - FAR_ROWS, SAME_F, 6, w_recv.at[6])
    w_over_t = far_part(4, 0, FAR_ROWS, SAME_T, 14, far_recv)
    w_near_t_core = weight_pair(2, 3, PARTNER, 8)
    w_near_f = weight_pair(4, 5, PARTNER, 10)
    w_far = weight_pair(6, 7, PARTNER, 12)

    def uc_pair(src_slot, dst_slot, to, index):
        return [ring.copy(buf.at[src_slot], buf.at[dst_slot], uc_send.at[index + which], uc_recv.at[dst_slot, which], to) for which, buf in enumerate((u_all, c_all))]

    u_to_t, c_to_t = uc_pair(0, 2, SAME_T, 0)
    uc_core = uc_pair(0, 1, PARTNER, 2)
    uc_pass = uc_pair(2, 3, PARTNER, 4)

    def att(src, dst_slot, to, index):
        return ring.copy(src, att_full.at[dst_slot], att_send.at[index], att_recv.at[dst_slot], to)

    att_keep = [pltpu.make_async_copy(uc_own.at[part, 0], att_full.at[0, pl.ds(part * dim, dim)], x_sem.at[part // 2, part % 2]) for part in range(4)]
    att_out = [att(att_full.at[0], 4, SAME_F, 0), att(att_full.at[0], 1, PARTNER, 1)]
    att_t, att_o = att(att_full.at[0], 2, SAME_T, 2), att(att_full.at[4], 6, SAME_T, 3)
    att_f_core, att_t_core, att_o_core = att(att_full.at[4], 5, PARTNER, 4), att(att_full.at[2], 3, PARTNER, 5), att(att_full.at[6], 7, PARTNER, 6)

    a2a_out = {slot: ring.copy(uc_own.at[slot], uc_seq.at[slot], a2a_send.at[slot], a2a_recv.at[slot], slot) for slot in (1, 2, 3, 4, 5)}
    a2a_out[SAME_O] = ring.copy(uc_own.at[SAME_O], uc_two.at[2], a2a_send.at[SAME_O], relay_recv.at[0], SAME_F)
    a2a_out[OTHER_O] = ring.copy(uc_own.at[OTHER_O], uc_two.at[3], a2a_send.at[OTHER_O], relay_recv.at[1], OTHER_F)
    a2a_pass = [ring.copy(uc_two.at[2 + index], uc_seq.at[SAME_O + index], a2a_send.at[8 + index], a2a_recv.at[SAME_O + index], SAME_T) for index in (0, 1)]
    uc_keep = pltpu.make_async_copy(uc_own.at[0], uc_seq.at[0], load_sem.at[4])
    two_out = ring.copy(uc_own.at[OTHER_T], uc_two.at[1], a2a_send.at[10], relay_recv.at[2], PARTNER)
    two_keep = pltpu.make_async_copy(uc_own.at[SAME_T], uc_two.at[0], two_sem.at[0])
    near = ring.copy(acc.at[0], near_recv, near_sem.at[0], near_sem.at[1], SAME_F)

    loads = [
        pltpu.make_async_copy(w_down, down_all.at[room(0)], load_sem.at[0]),
        pltpu.make_async_copy(w_up, uc_own.at[:, 0, :, pl.ds(0, half)], load_sem.at[1]),
        pltpu.make_async_copy(y_one, acc.at[0], load_sem.at[2]),
        pltpu.make_async_copy(dy_two, acc.at[1], load_sem.at[3]),
    ]
    qkv_loads = [pltpu.make_async_copy(w_qkv.at[part], uc_own.at[:, 1, :, pl.ds(part * dim, dim)], y_sem.at[0, part]) for part in range(3)]
    ring.arrive()
    start(loads)
    start(qkv_loads)
    ring.meet()
    loads[0].wait()
    start(w_own[1::2])
    loads[1].wait()
    for part in range(half // dim):
        up_all[pl.ds(part * dim, dim), :] = uc_own[:, 0, :, pl.ds(part * dim, dim)].reshape(hidden, dim).T
    start(w_own[0::2])
    out_load = pltpu.make_async_copy(w_out, uc_own.at[3, 0], load_sem.at[7])
    out_load.start()
    loads[2].wait()
    loads[3].wait()

    def normalize(step, carry):
        rows = pl.ds(pl.multiple_of(step * slab, slab), slab)
        u_all[0, rows, :] = rms_norm(acc[0, step]).astype(BF16)
        c_all[0, rows, :] = acc[1, step].astype(BF16)
        acc[0, step] = jnp.zeros((slab, hidden), F32)
        acc[1, step] = jnp.zeros((slab, hidden), F32)
        return carry

    lax.fori_loop(0, slabs, normalize, 0)
    u_to_t.start()
    start(uc_core)
    for part in range(3):
        qkv_loads[part].wait()
        uc_own[part, 0] = uc_own[:, 1, :, pl.ds(part * dim, dim)].reshape(hidden, dim).T
    out_load.wait()
    start(att_keep)

    def y_loads(step, buf):
        seq = ring.at_traced(7 - step)
        return [pltpu.make_async_copy(src.at[seq], spare.at[buf, which], y_sem.at[buf, which]) for which, src in enumerate((y_one, y_two, dy_one))]

    def x_stores(step, buf):
        seq = ring.at_traced(7 - step)
        return [pltpu.make_async_copy(spare.at[buf, 3 + which], dst.at[seq], x_sem.at[buf, which]) for which, dst in enumerate((x_two, dx_one))]

    def feed_forward(step, carry):
        slot = jnp.where(step == 3, 4, jnp.where(step == 4, 3, step))
        place = pl.ds(pl.multiple_of(jnp.where(step == 6, 1, jnp.where(step == 7, 3, slot)) * half, half), half)

        @pl.when((step == 1) | ((step >= 3) & (step != 6)))
        def _():
            for which, buf in enumerate((up_all, down_all)):
                ring.copy(buf.at[place], buf.at[place], w_send.at[0], w_recv.at[slot, which], PARTNER).wait_recv()

        @pl.when(step == 6)
        def _():
            for copy in w_near_t + w_over_t:
                copy.wait_recv()

        @pl.when(step == 2)
        def _():
            pl.semaphore_wait(free_slot.at[0], 1)
            for which, buf in ((1, down_all), (0, up_all)):
                ring.copy(buf.at[room(2)], buf.at[room(2)], w_send.at[0], w_recv.at[2, which], PARTNER).wait_recv()
                w_near_t[which].start()
                w_near_t_core[which].start()
            for copy in att_keep:
                copy.wait()
            start(att_out)

        @pl.when(step == 3)
        def _():
            pl.semaphore_wait(free_slot.at[5], 1)
            start(w_over_t)
            c_to_t.start()
            start(w_near_f)

        @pl.when(step == 6)
        def _():
            pl.semaphore_wait(free_slot.at[1], 1)
            start(w_far)

        @pl.when(step == 7)
        def _():
            start(y_loads(0, 0))

        def rows_step(part, carry):
            rows = pl.ds(pl.multiple_of(part * half, half), half)
            quarter = pl.ds(part * fours, fours)
            hidden_act, slope = gelu_and_slope(dot_nt(u_all[0, rows, :], up_all[place, :]))
            d_pre = (slope * dot_nt(c_all[0, rows, :], down_all[place, :])).astype(BF16)
            acc[0, quarter] += dot_nn(hidden_act.astype(BF16), down_all[place, :]).reshape(fours, slab, hidden)
            acc[1, quarter] += dot_nn(d_pre, up_all[place, :]).reshape(fours, slab, hidden)
            return carry

        lax.fori_loop(0, 2, rows_step, 0)

        @pl.when(step == 1)
        def _():
            say_free(0, SAME_F)
            say_free(5, SAME_T)

        @pl.when(step == 4)
        def _():
            say_free(1, PARTNER)

        return carry

    lax.fori_loop(0, 8, feed_forward, 0)

    def finish(step, carry):
        slot = 7 - step
        buf = step % 2
        seq = ring.at_traced(slot)
        for copy in y_loads(step, buf):
            copy.wait()

        @pl.when(step < 7)
        def _():
            start(y_loads(step + 1, 1 - buf))

        @pl.when(step >= 2)
        def _():
            for copy in x_stores(step - 2, buf):
                copy.wait()

        y_first = spare[buf, 0]
        x_second = spare[buf, 1] - acc[0, seq]
        dy_first = spare[buf, 2] + rms_back(y_first, acc[1, seq])
        spare[buf, 3] = x_second
        spare[buf, 4] = dy_first
        uc_own[slot, 0] = rms_norm(x_second).astype(BF16)
        uc_own[slot, 1] = dy_first.astype(BF16)
        acc[0, seq] = jnp.zeros((slab, hidden), F32)
        acc[1, seq] = jnp.zeros((slab, hidden), F32)
        start(x_stores(step, buf))
        return carry

    lax.fori_loop(0, 8, finish, 0)
    for slot in (7, 6, 5, 4, 3, 2, 1):
        a2a_out[slot].start()
    uc_keep.start()
    two_out.start()
    two_keep.start()
    for step in (6, 7):
        for copy in x_stores(step, step % 2):
            copy.wait()

    def gradients(step, carry):
        first = step // 8
        tokens = (step % 8) // 2
        place = pl.ds(pl.multiple_of((4 - 4 * first) * half, half), half)

        @pl.when((step == 2) | (step == 4) | (step == 6))
        def _():
            for which, buf in enumerate((u_all, c_all)):
                ring.copy(buf.at[tokens], buf.at[tokens], uc_send.at[0], uc_recv.at[tokens, which], PARTNER).wait_recv()

        @pl.when(step == 4)
        def _():
            start(uc_pass)
            for index in (0, 1):
                a2a_out[SAME_O + index].wait_recv()
            start(a2a_pass)

        @pl.when(step == 8)
        def _():
            near.start()
            att_out[0].wait_recv()
            att_f_core.start()
            att_t.start()
            att_o.start()

        rows = pl.ds(pl.multiple_of((step % 2) * half, half), half)
        u_part, c_part = u_all[tokens, rows, :], c_all[tokens, rows, :]
        hidden_act, slope = gelu_and_slope(dot_nt(up_all[place, :], u_part))
        d_pre = (slope * dot_nt(down_all[place, :], c_part)).astype(BF16)
        acc[first, pl.ds(0, fours)] += dot_nn(d_pre, u_part).reshape(fours, slab, hidden)
        acc[first, pl.ds(fours, fours)] += dot_nn(hidden_act.astype(BF16), c_part).reshape(fours, slab, hidden)
        return carry

    lax.fori_loop(0, 16, gradients, 0)
    out_own = pltpu.make_async_copy(acc.at[1], part_own, load_sem.at[1])
    out_own.start()
    for copy in w_own + w_near_t + w_over_t + w_near_t_core + w_near_f + w_far + [u_to_t, c_to_t] + uc_core + uc_pass:
        copy.wait_send()
    say_free(2, SAME_T)

    def relation_of(step):
        base = step % 4
        return jnp.where(base == 0, 2, jnp.where(base == 3, 3, base - 1))

    def qkv_rows(buf):
        return pl.ds(pl.multiple_of(buf * 6 * dim, 2 * dim), 6 * dim)

    def wo_rows(buf):
        return pl.ds(pl.multiple_of(12 * dim + buf * 2 * dim, 2 * dim), 2 * dim)

    def head_loads(relation, buf):
        copies = []
        for index in (0, 1):
            head = att_full.at[relation * 2 + 1 - index]
            first, second = (pl.ds(pl.multiple_of(base + index * size, dim), size) for base, size in ((buf * 6 * dim, 3 * dim), (12 * dim + buf * 2 * dim, dim)))
            copies.append(pltpu.make_async_copy(head.at[pl.ds(0, 3 * dim)], up_all.at[first], head_sem.at[buf, index, 0]))
            copies.append(pltpu.make_async_copy(head.at[pl.ds(3 * dim, dim)], up_all.at[second], head_sem.at[buf, index, 1]))
        return copies

    def rows_of(slot):
        return pl.ds(slot * slab, slab)

    def seq_loads(seq, src, src_slot, slot):
        return [pltpu.make_async_copy(src.at[src_slot, which], u_all.at[2 * seq + which, rows_of(slot)], seq_sem.at[2 * seq + which, slot]) for which in (0, 1)]

    seq_own = [copy for slot in range(8) for copy in seq_loads(0, uc_seq, slot, slot)]
    seq_two = [copy for slot in range(4) for copy in seq_loads(1, uc_two, slot, slot)]
    uc_to_t = [
        ring.copy(u_all.at[which, rows_of(slot)], u_all.at[2 + which, rows_of(4 + index)], far_sem.at[0, 2 * index + which], far_sem.at[1, 2 * index + which], SAME_T)
        for which in (0, 1)
        for index, slot in enumerate((0, 1, 4, 5))
    ]
    core_copies = [ring.copy(spare.at[index, pl.ds(0, 4)], acc.at[0, pl.ds(0, 4)], core_send.at[index], core_recv.at[index], PARTNER) for index in (0, 1)]
    f_copy = ring.copy(part_keep.at[0], acc.at[0, pl.ds(4, 4)], f_sem.at[0], f_sem.at[1], SAME_F)

    o_src = c_all.at[0]
    o_out = [
        ring.copy(o_src.at[rows_of(SAME_O)], o_relay.at[0], o_send.at[6], o_relay_recv.at[0], SAME_T),
        ring.copy(o_src.at[rows_of(OTHER_O)], o_relay.at[1], o_send.at[7], o_relay_recv.at[1], SAME_F),
    ] + [ring.copy(o_src.at[rows_of(slot)], o_pos.at[ring.me], o_send.at[slot], o_recv.at[slot], slot) for slot in (5, 4, 3, 2, 1)]
    o_pass = [
        ring.copy(o_relay.at[0], o_pos.at[ring.at(SAME_T)], o_send.at[8], o_recv.at[SAME_O], SAME_F),
        ring.copy(o_relay.at[1], o_pos.at[ring.at(SAME_F)], o_send.at[9], o_recv.at[OTHER_O], OTHER_T),
    ]
    o_keep = pltpu.make_async_copy(o_src.at[rows_of(0)], o_pos.at[ring.me], o_send.at[0])

    late = slab - LATE_ROWS
    early = {slot: late if slot == SAME_F else slab for slot in range(1, 6)}
    du_out = [
        ring.copy(acc.at[1, SAME_O], to_f.at[pl.ds(0, slab)], du_send.at[6], du_relay_recv.at[0], SAME_T),
        ring.copy(acc.at[1, OTHER_O], du_relay, du_send.at[7], du_relay_recv.at[1], SAME_F),
    ] + [ring.copy(acc.at[1, slot, pl.ds(0, early[slot])], du_pos.at[ring.me, pl.ds(0, early[slot])], du_send.at[slot], du_recv.at[slot], slot) for slot in (5, 4, 3, 2, 1)]
    du_keep = pltpu.make_async_copy(acc.at[1, 0], du_pos.at[ring.me], du_send.at[0])
    du_late = pltpu.make_async_copy(acc.at[1, SAME_F, pl.ds(late, slab - late)], to_f.at[pl.ds(slab, slab - late)], du_send.at[8])
    du_pass = ring.copy(du_relay, du_pos.at[ring.at(SAME_F)], du_send.at[9], du_recv.at[OTHER_O], OTHER_T)

    att_f_core.wait_recv()
    att_out[1].wait_recv()
    start(head_loads(2, 0))
    start(head_loads(0, 1))

    def arrive(slots):
        for slot in slots:
            if slot:
                ring.copy(uc_own.at[slot], uc_seq.at[slot], a2a_send.at[0], a2a_recv.at[slot], PARTNER).wait_recv()
            start(seq_own[2 * slot : 2 * slot + 2])

    def project(first, count):
        rows = pl.ds(first, count)
        for buf in (0, 1):
            c_all[2 + buf, rows, pl.ds(0, 6 * dim)] = dot_nt(u_all[0, rows, :], up_all[qkv_rows(buf), :]).astype(BF16)
            c_all[2 + buf, rows, pl.ds(6 * dim, 2 * dim)] = dot_nt(u_all[1, rows, :], up_all[wo_rows(buf), :]).astype(BF16)

    uc_keep.wait()
    arrive((0, 1, 4, 5, 2, 3))
    two_out.wait_recv()
    two_keep.wait()
    start(seq_two)
    out_own.wait()
    acc[1] = jnp.zeros(acc.shape[1:], F32)
    for copy in seq_own[:12] + head_loads(2, 0) + head_loads(0, 1):
        copy.wait()
    pl.semaphore_wait(free_slot.at[2], 1)
    start(uc_to_t)
    project(0, 6 * slab)
    arrive((6, 7))
    for copy in seq_own[12:]:
        copy.wait()
    project(6 * slab, 2 * slab)

    def chip_step(step, carry):
        buf = step % 2
        seq = step // 4
        relation = relation_of(step)

        @pl.when(step == 4)
        def _():
            near.wait_send()
            say_free(3, SAME_F)
            say_free(4, PARTNER)
            for copy in seq_two:
                copy.wait()
            for copy in uc_to_t[:4]:
                copy.wait_recv()

        @pl.when(step >= 2)
        def _():
            for copy in head_loads(0, buf):
                copy.wait()

        @pl.when((step == 3) | (step == 4))
        def _():
            start(head_loads(relation_of(step + 1), 1 - buf))

        kept = pl.ds(pl.multiple_of(jnp.where(step < 2, step, 2) * seq_len, seq_len), seq_len)
        heads = [ring.at_traced(relation * 2 + other) for other in (1, 0)]
        wo_copies = [
            pltpu.make_async_copy(up_all.at[pl.ds(pl.multiple_of(12 * dim + (2 * buf + index) * dim, dim), dim)], wo_full.at[head], wo_sem.at[index])
            for index, head in enumerate(heads)
        ]
        start(wo_copies)

        @pl.when(step >= 2)
        def _():
            c_all[2 + buf, :, pl.ds(0, 6 * dim)] = dot_nt(u_all[2 * seq], up_all[qkv_rows(buf), :]).astype(BF16)

        for index, head in enumerate(heads):
            columns = pl.ds(pl.multiple_of(head * dim, dim), dim)
            own = pl.ds(index * 3 * dim, 3 * dim)
            query, key, value = (c_all[2 + buf, :, pl.ds((index * 3 + part) * dim, dim)] for part in range(3))
            scores = dot_nt(query, key) * (scale * LOG2_E)
            grown = jnp.exp2(scores - jnp.max(scores, axis=-1, keepdims=True))
            prob = grown * (1.0 / jnp.sum(grown, axis=-1, keepdims=True))
            prob_b = prob.astype(BF16)
            c_all[seq, :, columns] = dot_nn(prob_b, value).astype(BF16)
            if index == 0:
                @pl.when(step == 4)
                def _():
                    for copy in uc_to_t[4:]:
                        copy.wait_recv()

                @pl.when(step >= 2)
                def _():
                    c_all[2 + buf, :, pl.ds(6 * dim, 2 * dim)] = dot_nt(u_all[2 * seq + 1], up_all[wo_rows(buf), :]).astype(BF16)

            d_out = c_all[2 + buf, :, pl.ds((6 + index) * dim, dim)]
            d_prob = dot_nt(d_out, value)
            d_score = (prob * (d_prob - jnp.sum(d_prob * prob, axis=-1, keepdims=True)) * scale).astype(BF16)
            down_all[kept, pl.ds(index * 3 * dim, dim)] = dot_nn(d_score, key).astype(BF16)
            down_all[kept, pl.ds((index * 3 + 1) * dim, dim)] = dot_nn(query.T, d_score).T.astype(BF16)
            down_all[kept, pl.ds((index * 3 + 2) * dim, dim)] = dot_nn(d_out.T, prob_b).T.astype(BF16)
            @pl.when(step >= 4)
            def _():
                dst = (spare, part_keep)[index].at[buf]
                dst[pl.ds(0, 3)] += dot_tn(down_all[kept, own], u_all[2]).reshape(3, dim, hidden)
                dst[3] += dot_tn(c_all[1, :, columns], u_all[3])

            if index == 0:
                @pl.when(step == 1)
                def _():
                    att_t.wait_recv()
                    att_t_core.start()

                @pl.when(step == 4)
                def _():
                    pl.semaphore_wait(free_slot.at[4], 1)
                    core_copies[0].start()

                @pl.when(step == 5)
                def _():
                    pl.semaphore_wait(free_slot.at[4], 1)
                    core_copies[1].start()

        @pl.when(step == 1)
        def _():
            att_t_core.wait_recv()
            start(head_loads(1, 0))

        @pl.when(step == 2)
        def _():
            att_o.wait_recv()
            att_o_core.start()

        @pl.when(step < 4)
        def _():
            def du_tile(part, carry):
                rows = pl.ds(pl.multiple_of(jnp.where(step < 2, step, 2) * seq_len + part * half, half), half)
                acc[1, pl.ds(part * fours, fours)] += dot_nn(down_all[rows, pl.ds(0, 6 * dim)], up_all[qkv_rows(buf), :]).reshape(fours, slab, hidden)
                return carry

            lax.fori_loop(0, 2, du_tile, 0)

        @pl.when(step == 2)
        def _():
            att_o_core.wait_recv()
            start(head_loads(3, 1))

        @pl.when(step == 3)
        def _():
            start(o_out)
            start(du_out)
            du_late.start()
            o_keep.start()
            du_keep.start()

            def own_gradients(pair, carry):
                own_rows = pl.ds(pl.multiple_of(pair * seq_len, seq_len), seq_len)
                for index, other in enumerate((1, 0)):
                    columns = pl.ds(pl.multiple_of(ring.at_traced(relation_of(pair) * 2 + other) * dim, dim), dim)
                    dst = (spare, part_keep)[index].at[pair]
                    dst[pl.ds(0, 3)] = dot_tn(down_all[own_rows, pl.ds(index * 3 * dim, 3 * dim)], u_all[0]).reshape(3, dim, hidden)
                    dst[3] = dot_tn(c_all[0, :, columns], u_all[1])
                return carry

            lax.fori_loop(0, 2, own_gradients, 0)

        @pl.when(step == 4)
        def _():
            core_copies[0].wait_recv()
            part_keep[0] += acc[0, pl.ds(0, 4)]
            say_free(4, PARTNER)
            pl.semaphore_wait(free_slot.at[3], 1)
            f_copy.start()

        for copy in wo_copies:
            copy.wait()
        return carry

    lax.fori_loop(0, 6, chip_step, 0)
    for copy in o_out[:2]:
        copy.wait_recv()
    start(o_pass)
    du_out[1].wait_recv()
    du_pass.start()
    core_copies[1].wait_recv()
    part_keep[1] += acc[0, pl.ds(0, 4)]
    for copy in du_out[2:]:
        copy.wait_recv()
    for slot in range(1, 8):
        ring.copy(o_pos.at[0], o_pos.at[ring.at(slot)], near_sem.at[0], o_recv.at[slot], PARTNER).wait_recv()
    du_out[0].wait_recv()
    du_pass.wait_recv()
    near.wait_recv()
    f_copy.wait_recv()
    part_keep[1] += acc[0, pl.ds(4, 4)]
    d_att_copy = pltpu.make_async_copy(part_keep.at[1], d_att, load_sem.at[0])
    d_att_copy.start()

    sends = att_out + [att_t, att_o, att_f_core, att_t_core, att_o_core] + list(a2a_out.values()) + a2a_pass + [two_out]
    for copy in sends + o_out + du_out + o_pass + uc_to_t + core_copies + [du_pass, f_copy]:
        copy.wait_send()
    du_late.wait()
    o_keep.wait()
    du_keep.wait()
    d_att_copy.wait()


def block_call(y_one, y_two, dy_one, dy_two, w_up, w_down, w_qkv, w_out):
    slabs, slab, hidden = y_one.shape
    tokens = slabs * slab
    ffn = w_down.shape[0]
    dim = w_out.shape[0]
    any_spec = pl.BlockSpec(memory_space=pl.ANY)
    dma, vmem, wide, narrow = pltpu.SemaphoreType.DMA, pltpu.VMEM, F32, BF16
    results = [
        ((slabs, slab, hidden), wide), ((slabs, slab, hidden), wide), ((slabs, slab, hidden), wide), ((slabs, slab, hidden), wide),
        ((4, dim, hidden), wide), ((slabs, slab, hidden), narrow), ((slabs, slab, hidden), wide), ((8, dim, hidden), narrow),
        ((slab + LATE_ROWS, hidden), wide),
    ]
    landing = [
        ((8, 2, slab, hidden), narrow), ((4, 2, slab, hidden), narrow), ((8, 4 * dim, hidden), narrow), ((2, slab, hidden), narrow), ((slab, hidden), wide),
    ]
    scratch = [
        vmem((4, tokens, hidden), BF16), vmem((4, tokens, hidden), BF16), vmem((6 * ffn, hidden), BF16), vmem((6 * ffn, hidden), BF16),
        vmem((2, slabs, slab, hidden), F32), vmem((2, 5, slab, hidden), F32), vmem((2, 4, dim, hidden), F32),
        vmem((8, 2, slab, hidden), BF16),
        dma((8,)), dma((2, 3)), dma((2, 2)), dma((16,)), dma((8, 2)), dma((6,)), dma((4, 2)), dma((7,)), dma((8,)), dma((11,)), dma((8,)), dma((3,)), dma((2,)), dma((2,)),
        dma((4, 8)), dma((2, 2, 2)), dma((2,)), dma((2,)), dma((2,)), dma((2,)), dma((2, 8)), dma((10,)), dma((8,)), dma((10,)), dma((8,)), dma((2,)), dma((2,)), dma((2,)),
        pltpu.SemaphoreType.REGULAR((6,)),
    ]
    return pl.pallas_call(
        functools.partial(block_kernel, dim ** -0.5),
        out_shape=[jax.ShapeDtypeStruct(shape, dtype) for shape, dtype in results + landing],
        in_specs=[any_spec] * 8,
        out_specs=[any_spec] * (len(results) + len(landing)),
        scratch_shapes=scratch,
        compiler_params=pltpu.CompilerParams(collective_id=0, has_side_effects=True, vmem_limit_bytes=VMEM_LIMIT),
        cost_estimate=pl.CostEstimate(flops=120 * 10**9, bytes_accessed=128 * 2**20, transcendentals=0),
        name="block",
    )(y_one, y_two, dy_one, dy_two, w_up.reshape(8, hidden // 8, ffn), w_down, w_qkv.reshape(3, 8, hidden // 8, dim), w_out)[: len(results)]


def finish_kernel(
    y_one, o_pos, wo_full, x_two, dx_one, dy_two, du_pos, part_own, near_recv, d_att,
    x_one_out, x_two_out, dx_one_out, dx_two_out, dw_up, dw_down, dw_qkv, dw_out,
    y_buf, o_buf, wo_buf, x_buf, dx_buf, dy_buf, du_buf, own_buf, near_buf, att_buf, up_out, qkv_out, load_sem, store_sem,
):
    tokens = y_buf.shape[0]
    dim = wo_buf.shape[0] // 8
    chunk = 256
    chunks = [pl.ds(index * chunk, chunk) for index in range(tokens // chunk)]

    def pieces(src, dst, sem, row):
        return [pltpu.make_async_copy(src.at[rows], dst.at[rows], sem.at[row, index]) for index, rows in enumerate(chunks)]

    def whole(src, dst, sem, row):
        return pltpu.make_async_copy(src, dst, sem.at[row, 0])

    ring = Ring()
    slab = tokens // 8
    sizes = {0: slab, PARTNER: slab, SAME_T: slab, OTHER_T: slab, SAME_F: slab - LATE_ROWS, OTHER_F: slab, OTHER_O: slab}
    slots = [pl.ds(pl.multiple_of(ring.at(slot) * slab, slab), size) for slot, size in sizes.items()]

    def slabs(src, dst, sem, row):
        return [pltpu.make_async_copy(src.at[rows], dst.at[rows], sem.at[row, index]) for index, rows in enumerate(slots)]

    x_in, dy_in, du_in = pieces(x_two, x_buf, load_sem, 0), slabs(dy_two, dy_buf, load_sem, 1), slabs(du_pos, du_buf, load_sem, 2)
    y_in, o_in = pieces(y_one, y_buf, load_sem, 3), pieces(o_pos, o_buf, load_sem, 4)
    wo_in, dx_in = whole(wo_full, wo_buf, load_sem, 5), pieces(dx_one, dx_buf, load_sem, 6)
    own_in, near_in, att_in = whole(part_own, own_buf, load_sem, 7), whole(near_recv, near_buf, load_sem, 8), whole(d_att, att_buf, load_sem, 9)
    order = [own_in, near_in, att_in, wo_in, *(copy for group in zip(y_in, o_in) for copy in group), *x_in, *(copy for group in zip(dy_in, du_in) for copy in group), *dx_in]
    for copy in order:
        copy.start()

    x_store, dx2_store, x1_store = pieces(x_buf, x_two_out, store_sem, 0), slabs(dy_buf, dx_two_out, store_sem, 1), pieces(y_buf, x_one_out, store_sem, 2)
    dx_store = pieces(dx_buf, dx_one_out, store_sem, 3)
    own_in.wait()
    near_in.wait()
    ffn = up_out.shape[1]
    own_buf[pl.ds(ffn, ffn), :] += near_buf[pl.ds(ffn, ffn), :]
    down_store = whole(own_buf.at[pl.ds(ffn, ffn)], dw_down, store_sem, 7)
    down_store.start()
    for part in range(up_out.shape[0] // ffn):
        columns = pl.ds(part * ffn, ffn)
        up_out[columns, :] = (own_buf[pl.ds(0, ffn), columns] + near_buf[pl.ds(0, ffn), columns]).T
    up_store = whole(up_out, dw_up, store_sem, 4)
    up_store.start()
    att_in.wait()
    for part in range(3):
        qkv_out[pl.ds(part, tokens, stride=3), 0, :] = att_buf[pl.ds(part * dim, dim), :].T
    qkv_store = whole(qkv_out, dw_qkv, store_sem, 5)
    qkv_store.start()
    out_store = whole(att_buf.at[pl.ds(3 * dim, dim)], dw_out, store_sem, 6)
    out_store.start()
    wo_in.wait()
    for index, rows in enumerate(chunks):
        y_in[index].wait()
        o_in[index].wait()
        y_buf[rows, :] -= dot_nn(o_buf[rows, :], wo_buf[...])
        x1_store[index].start()
    for index in range(len(chunks)):
        x_in[index].wait()
        x_store[index].start()
    for index, rows in enumerate(slots):
        dy_in[index].wait()
        du_in[index].wait()
        dy_buf[rows, :] += rms_back(x_buf[rows, :], du_buf[rows, :])
        dx2_store[index].start()
    for index in range(len(chunks)):
        dx_in[index].wait()
        dx_store[index].start()
    for copy in x_store + dx2_store + x1_store + dx_store + [up_store, qkv_store, out_store, down_store]:
        copy.wait()


def finish_call(y_one, o_pos, wo_full, x_two, dx_one, dy_two, du_pos, part_own, near_recv, d_att):
    tokens, hidden = y_one.shape
    ffn = part_own.shape[0] // 2
    dim = d_att.shape[0] // 4
    any_spec = pl.BlockSpec(memory_space=pl.ANY)
    dma, vmem = pltpu.SemaphoreType.DMA, pltpu.VMEM
    state = (tokens, hidden)
    out_shape = [jax.ShapeDtypeStruct(shape, F32) for shape in (state, state, state, state, (hidden, ffn), (ffn, hidden), (3 * hidden, 1, dim), (dim, hidden))]
    scratch = [
        vmem(state, F32), vmem(state, BF16), vmem((hidden, hidden), BF16), vmem(state, F32), vmem(state, F32), vmem(state, F32), vmem(state, F32),
        vmem(part_own.shape, F32), vmem(part_own.shape, F32), vmem(d_att.shape, F32), vmem((hidden, ffn), F32), vmem((3 * hidden, 1, dim), F32),
        dma((10, 7)), dma((8, 7)),
    ]
    return pl.pallas_call(
        finish_kernel,
        out_shape=out_shape,
        in_specs=[any_spec] * 10,
        out_specs=[any_spec] * 8,
        scratch_shapes=scratch,
        compiler_params=pltpu.CompilerParams(vmem_limit_bytes=VMEM_LIMIT),
        cost_estimate=pl.CostEstimate(flops=2 * 10**9, bytes_accessed=52 * 2**20, transcendentals=0),
        name="finish",
    )(y_one, o_pos, wo_full, x_two, dx_one, dy_two, du_pos, part_own, near_recv, d_att)


def last_kernel(x_two, dy_two, du_far, dx_two_in, dx_two_out, x_buf, dy_buf, du_buf, load_sem, store_sem):
    ring = Ring()
    slab = x_buf.shape[1]
    loads, stores, sizes = [], [], (slab, LATE_ROWS)
    for index, (slot, skip) in enumerate(((SAME_O, 0), (SAME_F, slab - LATE_ROWS))):
        size = sizes[index]
        rows = pl.ds(pl.multiple_of(ring.at(slot) * slab + skip, 16), size)
        sources = ((x_two.at[rows], x_buf), (dy_two.at[rows], dy_buf), (du_far.at[pl.ds(index * slab, size)], du_buf))
        loads.append([pltpu.make_async_copy(src, dst.at[index, pl.ds(0, size)], load_sem.at[index, which]) for which, (src, dst) in enumerate(sources)])
        stores.append(pltpu.make_async_copy(dy_buf.at[index, pl.ds(0, size)], dx_two_out.at[rows], store_sem.at[index]))
    for copies in loads:
        for copy in copies:
            copy.start()
    for index, copies in enumerate(loads):
        for copy in copies:
            copy.wait()
        rows = pl.ds(0, sizes[index])
        dy_buf[index, rows, :] += rms_back(x_buf[index, rows, :], du_buf[index, rows, :])
        stores[index].start()
    for copy in stores:
        copy.wait()


def last_call(x_two, dy_two, du_far, dx_two):
    tokens, hidden = x_two.shape
    any_spec = pl.BlockSpec(memory_space=pl.ANY)
    buf = pltpu.VMEM((2, tokens // 8, hidden), F32)
    return pl.pallas_call(
        last_kernel,
        out_shape=jax.ShapeDtypeStruct(dx_two.shape, F32),
        in_specs=[any_spec] * 4,
        out_specs=any_spec,
        input_output_aliases={3: 0},
        scratch_shapes=[buf, buf, buf, pltpu.SemaphoreType.DMA((2, 3)), pltpu.SemaphoreType.DMA((2,))],
        cost_estimate=pl.CostEstimate(flops=10**6, bytes_accessed=4 * 2**20, transcendentals=0),
        name="last",
    )(x_two, dy_two, du_far, dx_two)


def local_backward(y_one, y_two, dy_one, dy_two, w_qkv, w_out, w_up, w_down):
    hidden = y_one.shape[2]
    _, _, _, parts, dim = w_qkv.shape
    qkv_parts = jnp.swapaxes(w_qkv[0, :, 0], 0, 1)
    results = block_call(y_one, y_two, dy_one, dy_two, w_up[0], w_down[0], qkv_parts, w_out[0, 0])
    x_two, dx_one, part_own, near_recv, d_att, o_pos, du_pos, wo_full = (tensor.reshape(-1, hidden) for tensor in results[:8])
    devices = range(lax.axis_size("tp"))
    to_f = [(device, (3 - device // 2) * 2 + device % 2) for device in devices]
    du_far = lax.ppermute(results[8], "tp", to_f)
    y_flat, dy_flat = y_one.reshape(-1, hidden), dy_two.reshape(-1, hidden)
    *states, dw_up, dw_down, dw_qkv, dw_out = finish_call(y_flat, o_pos, wo_full, x_two, dx_one, dy_flat, du_pos, part_own, near_recv, d_att)
    states[3] = last_call(x_two, dy_flat, du_far, states[3])
    states = [tensor.reshape(y_one.shape) for tensor in states]
    return (*states, dw_qkv.reshape(1, hidden, 1, parts, dim), dw_out[None, None], dw_up[None], dw_down[None])


def solution(mesh):
    state_spec = P("dp", "tp", None)
    in_specs = (state_spec, state_spec, state_spec, state_spec, P(None, None, "tp", None, None), P(None, "tp", None, None), P(None, None, "tp"), P(None, "tp", None))
    out_specs = (state_spec, state_spec, state_spec, state_spec, P("dp", None, "tp", None, None), P("dp", "tp", None, None), P("dp", None, "tp"), P("dp", "tp", None))
    return jax.shard_map(local_backward, mesh=mesh, in_specs=in_specs, out_specs=out_specs, check_vma=False)
```

```python
import functools

import jax
import jax.numpy as jnp
from jax import lax
from jax.experimental import pallas as pl
from jax.experimental.pallas import tpu as pltpu
from jax.sharding import PartitionSpec as P

RMS_EPS = 1e-6
LOG2_E = 1.4426950408889634
LATE_ROWS = 96
FAR_ROWS = 16
MESH = pl.DeviceIdType.MESH
BF16, F32 = jnp.bfloat16, jnp.float32
VMEM_LIMIT = 64 * 1024 * 1024 - 65536


def inv_rms(tensor):
    return lax.rsqrt(jnp.mean(tensor * tensor, axis=-1, keepdims=True) + RMS_EPS)


def rms_norm(tensor):
    return tensor * inv_rms(tensor)


def rms_back(tensor, grad_in):
    scale = inv_rms(tensor)
    return scale * grad_in - tensor * (scale * scale * scale) * jnp.mean(grad_in * tensor, axis=-1, keepdims=True)


def gelu_and_slope(tensor):
    root = (2.0 / jnp.pi) ** 0.5
    squared = tensor * tensor
    tanh = jnp.tanh(root * (tensor + 0.044715 * (tensor * squared)))
    cdf = 0.5 * (1.0 + tanh)
    slope = cdf + (0.5 * root) * tensor * ((1.0 - tanh * tanh) * (1.0 + (3 * 0.044715) * squared))
    return tensor * cdf, slope


def dot_nn(left, right):
    return lax.dot_general(left, right, (((1,), (0,)), ((), ())), preferred_element_type=F32)


def dot_nt(left, right):
    return lax.dot_general(left, right, (((1,), (1,)), ((), ())), preferred_element_type=F32)


def dot_tn(left, right):
    return lax.dot_general(left, right, (((0,), (0,)), ((), ())), preferred_element_type=F32)


class Ring:
    def __init__(self):
        me = lax.axis_index("tp")
        chip, core = me // 2, me % 2
        self.me, self.chip, self.core = me, chip, core
        self.chips = (chip, chip + 1 - 2 * (chip % 2), 3 - chip, (chip + 2) % 4)

    def at(self, slot):
        core = self.core if slot % 2 == 0 else 1 - self.core
        return self.chips[slot // 2] * 2 + core

    def at_traced(self, slot):
        relation, other = slot // 2, slot % 2
        own, near_t, near_f, opposite = self.chips
        chip = jnp.where(relation == 0, own, jnp.where(relation == 1, near_t, jnp.where(relation == 2, near_f, opposite)))
        return chip * 2 + (self.core + other) % 2

    def arrive(self):
        for slot in (1, 2, 3, 4, 5):
            pl.semaphore_signal(pltpu.get_barrier_semaphore(), inc=1, device_id={"tp": self.at(slot)}, device_id_type=MESH)

    def meet(self):
        pl.semaphore_wait(pltpu.get_barrier_semaphore(), 5)

    def copy(self, src, dst, send_sem, recv_sem, slot):
        return pltpu.make_async_remote_copy(src_ref=src, dst_ref=dst, send_sem=send_sem, recv_sem=recv_sem, device_id={"tp": self.at(slot)}, device_id_type=MESH)


PARTNER, SAME_T, OTHER_T, SAME_F, OTHER_F, SAME_O, OTHER_O = 1, 2, 3, 4, 5, 6, 7


def block_kernel(
    scale,
    y_one, y_two, dy_one, dy_two, w_up, w_down, w_qkv, w_out,
    x_two, dx_one, part_own, near_recv, d_att, o_pos, du_pos, wo_full, to_f,
    uc_seq, uc_two, att_full, o_relay, du_relay,
    u_all, c_all, up_all, down_all, acc, spare, part_keep, uc_own,
    load_sem, y_sem, x_sem, w_send, w_recv, uc_send, uc_recv, att_send, att_recv, a2a_send, a2a_recv, relay_recv, near_sem, two_sem,
    seq_sem, head_sem, wo_sem, core_send, core_recv, f_sem, far_sem, o_send, o_recv, du_send, du_recv, o_relay_recv, du_relay_recv, far_recv, free_slot,
):
    ring = Ring()
    slabs, slab, hidden = acc.shape[1:]
    seq_len = slabs * slab
    half = seq_len // 2
    dim = w_out.shape[0]
    fours = slabs // 2

    def start(copies):
        for copy in copies:
            copy.start()

    def say_free(index, to):
        pl.semaphore_signal(free_slot.at[index], inc=1, device_id={"tp": ring.at(to)}, device_id_type=MESH)

    rooms = (0, 1, 2, 3, 4, 5, 1, 3)

    def room(slot):
        return pl.ds(rooms[slot] * half, half)

    def weight_pair(src_slot, dst_slot, to, index):
        return [
            ring.copy(buf.at[room(src_slot)], buf.at[room(dst_slot)], w_send.at[index + which], w_recv.at[dst_slot, which], to)
            for which, buf in enumerate((up_all, down_all))
        ]

    w_own = weight_pair(0, 1, PARTNER, 0) + weight_pair(0, 2, SAME_T, 2) + weight_pair(0, 4, SAME_F, 4)
    def far_part(src_slot, first, count, to, index, recv_sem):
        src, dst = (pl.ds(rooms[slot] * half + first, count) for slot in (src_slot, 6))
        return [ring.copy(buf.at[src], buf.at[dst], w_send.at[index + which], recv_sem.at[which], to) for which, buf in enumerate((up_all, down_all))]

    w_near_t = far_part(2, FAR_ROWS, half - FAR_ROWS, SAME_F, 6, w_recv.at[6])
    w_over_t = far_part(4, 0, FAR_ROWS, SAME_T, 14, far_recv)
    w_near_t_core = weight_pair(2, 3, PARTNER, 8)
    w_near_f = weight_pair(4, 5, PARTNER, 10)
    w_far = weight_pair(6, 7, PARTNER, 12)

    def uc_pair(src_slot, dst_slot, to, index):
        return [ring.copy(buf.at[src_slot], buf.at[dst_slot], uc_send.at[index + which], uc_recv.at[dst_slot, which], to) for which, buf in enumerate((u_all, c_all))]

    u_to_t, c_to_t = uc_pair(0, 2, SAME_T, 0)
    uc_core = uc_pair(0, 1, PARTNER, 2)
    uc_pass = uc_pair(2, 3, PARTNER, 4)

    def att(src, dst_slot, to, index):
        return ring.copy(src, att_full.at[dst_slot], att_send.at[index], att_recv.at[dst_slot], to)

    att_keep = [pltpu.make_async_copy(uc_own.at[part, 0], att_full.at[0, pl.ds(part * dim, dim)], x_sem.at[part // 2, part % 2]) for part in range(4)]
    att_out = [att(att_full.at[0], 4, SAME_F, 0), att(att_full.at[0], 1, PARTNER, 1)]
    att_t, att_o = att(att_full.at[0], 2, SAME_T, 2), att(att_full.at[4], 6, SAME_T, 3)
    att_f_core, att_t_core, att_o_core = att(att_full.at[4], 5, PARTNER, 4), att(att_full.at[2], 3, PARTNER, 5), att(att_full.at[6], 7, PARTNER, 6)

    a2a_out = {slot: ring.copy(uc_own.at[slot], uc_seq.at[slot], a2a_send.at[slot], a2a_recv.at[slot], slot) for slot in (1, 2, 3, 4, 5)}
    a2a_out[SAME_O] = ring.copy(uc_own.at[SAME_O], uc_two.at[2], a2a_send.at[SAME_O], relay_recv.at[0], SAME_F)
    a2a_out[OTHER_O] = ring.copy(uc_own.at[OTHER_O], uc_two.at[3], a2a_send.at[OTHER_O], relay_recv.at[1], OTHER_F)
    a2a_pass = [ring.copy(uc_two.at[2 + index], uc_seq.at[SAME_O + index], a2a_send.at[8 + index], a2a_recv.at[SAME_O + index], SAME_T) for index in (0, 1)]
    uc_keep = pltpu.make_async_copy(uc_own.at[0], uc_seq.at[0], load_sem.at[4])
    two_out = ring.copy(uc_own.at[OTHER_T], uc_two.at[1], a2a_send.at[10], relay_recv.at[2], PARTNER)
    two_keep = pltpu.make_async_copy(uc_own.at[SAME_T], uc_two.at[0], two_sem.at[0])
    near = ring.copy(acc.at[0], near_recv, near_sem.at[0], near_sem.at[1], SAME_F)

    loads = [
        pltpu.make_async_copy(w_down, down_all.at[room(0)], load_sem.at[0]),
        pltpu.make_async_copy(w_up, uc_own.at[:, 0, :, pl.ds(0, half)], load_sem.at[1]),
        pltpu.make_async_copy(y_one, acc.at[0], load_sem.at[2]),
        pltpu.make_async_copy(dy_two, acc.at[1], load_sem.at[3]),
    ]
    qkv_loads = [pltpu.make_async_copy(w_qkv.at[part], uc_own.at[:, 1, :, pl.ds(part * dim, dim)], y_sem.at[0, part]) for part in range(3)]
    ring.arrive()
    start(loads)
    start(qkv_loads)
    ring.meet()
    loads[0].wait()
    start(w_own[1::2])
    loads[1].wait()
    for part in range(half // dim):
        up_all[pl.ds(part * dim, dim), :] = uc_own[:, 0, :, pl.ds(part * dim, dim)].reshape(hidden, dim).T
    start(w_own[0::2])
    out_load = pltpu.make_async_copy(w_out, uc_own.at[3, 0], load_sem.at[7])
    out_load.start()
    loads[2].wait()
    loads[3].wait()

    def normalize(step, carry):
        rows = pl.ds(pl.multiple_of(step * slab, slab), slab)
        u_all[0, rows, :] = rms_norm(acc[0, step]).astype(BF16)
        c_all[0, rows, :] = acc[1, step].astype(BF16)
        acc[0, step] = jnp.zeros((slab, hidden), F32)
        acc[1, step] = jnp.zeros((slab, hidden), F32)
        return carry

    lax.fori_loop(0, slabs, normalize, 0)
    u_to_t.start()
    start(uc_core)
    for part in range(3):
        qkv_loads[part].wait()
        uc_own[part, 0] = uc_own[:, 1, :, pl.ds(part * dim, dim)].reshape(hidden, dim).T
    out_load.wait()
    start(att_keep)

    def y_loads(step, buf):
        seq = ring.at_traced(7 - step)
        return [pltpu.make_async_copy(src.at[seq], spare.at[buf, which], y_sem.at[buf, which]) for which, src in enumerate((y_one, y_two, dy_one))]

    def x_stores(step, buf):
        seq = ring.at_traced(7 - step)
        return [pltpu.make_async_copy(spare.at[buf, 3 + which], dst.at[seq], x_sem.at[buf, which]) for which, dst in enumerate((x_two, dx_one))]

    def feed_forward(step, carry):
        slot = jnp.where(step == 3, 4, jnp.where(step == 4, 3, step))
        place = pl.ds(pl.multiple_of(jnp.where(step == 6, 1, jnp.where(step == 7, 3, slot)) * half, half), half)

        @pl.when((step == 1) | ((step >= 3) & (step != 6)))
        def _():
            for which, buf in enumerate((up_all, down_all)):
                ring.copy(buf.at[place], buf.at[place], w_send.at[0], w_recv.at[slot, which], PARTNER).wait_recv()

        @pl.when(step == 6)
        def _():
            for copy in w_near_t + w_over_t:
                copy.wait_recv()

        @pl.when(step == 2)
        def _():
            pl.semaphore_wait(free_slot.at[0], 1)
            for which, buf in ((1, down_all), (0, up_all)):
                ring.copy(buf.at[room(2)], buf.at[room(2)], w_send.at[0], w_recv.at[2, which], PARTNER).wait_recv()
                w_near_t[which].start()
                w_near_t_core[which].start()
            for copy in att_keep:
                copy.wait()
            start(att_out)

        @pl.when(step == 3)
        def _():
            pl.semaphore_wait(free_slot.at[5], 1)
            start(w_over_t)
            c_to_t.start()
            start(w_near_f)

        @pl.when(step == 6)
        def _():
            pl.semaphore_wait(free_slot.at[1], 1)
            start(w_far)

        @pl.when(step == 7)
        def _():
            start(y_loads(0, 0))

        def rows_step(part, carry):
            rows = pl.ds(pl.multiple_of(part * half, half), half)
            quarter = pl.ds(part * fours, fours)
            hidden_act, slope = gelu_and_slope(dot_nt(u_all[0, rows, :], up_all[place, :]))
            d_pre = (slope * dot_nt(c_all[0, rows, :], down_all[place, :])).astype(BF16)
            acc[0, quarter] += dot_nn(hidden_act.astype(BF16), down_all[place, :]).reshape(fours, slab, hidden)
            acc[1, quarter] += dot_nn(d_pre, up_all[place, :]).reshape(fours, slab, hidden)
            return carry

        lax.fori_loop(0, 2, rows_step, 0)

        @pl.when(step == 1)
        def _():
            say_free(0, SAME_F)
            say_free(5, SAME_T)

        @pl.when(step == 4)
        def _():
            say_free(1, PARTNER)

        return carry

    lax.fori_loop(0, 8, feed_forward, 0)

    def finish(step, carry):
        slot = 7 - step
        buf = step % 2
        seq = ring.at_traced(slot)
        for copy in y_loads(step, buf):
            copy.wait()

        @pl.when(step < 7)
        def _():
            start(y_loads(step + 1, 1 - buf))

        @pl.when(step >= 2)
        def _():
            for copy in x_stores(step - 2, buf):
                copy.wait()

        y_first = spare[buf, 0]
        x_second = spare[buf, 1] - acc[0, seq]
        dy_first = spare[buf, 2] + rms_back(y_first, acc[1, seq])
        spare[buf, 3] = x_second
        spare[buf, 4] = dy_first
        uc_own[slot, 0] = rms_norm(x_second).astype(BF16)
        uc_own[slot, 1] = dy_first.astype(BF16)
        acc[0, seq] = jnp.zeros((slab, hidden), F32)
        acc[1, seq] = jnp.zeros((slab, hidden), F32)
        start(x_stores(step, buf))
        return carry

    lax.fori_loop(0, 8, finish, 0)
    for slot in (7, 6, 5, 4, 3, 2, 1):
        a2a_out[slot].start()
    uc_keep.start()
    two_out.start()
    two_keep.start()
    for step in (6, 7):
        for copy in x_stores(step, step % 2):
            copy.wait()

    def gradients(step, carry):
        first = step // 8
        tokens = (step % 8) // 2
        place = pl.ds(pl.multiple_of((4 - 4 * first) * half, half), half)

        @pl.when(step == 0)
        def _():
            u_to_t.wait_recv()
            uc_pass[0].start()

        @pl.when((step == 2) | (step == 6))
        def _():
            for which, buf in enumerate((u_all, c_all)):
                ring.copy(buf.at[tokens], buf.at[tokens], uc_send.at[0], uc_recv.at[tokens, which], PARTNER).wait_recv()

        @pl.when(step == 4)
        def _():
            c_to_t.wait_recv()
            uc_pass[1].start()
            for index in (0, 1):
                a2a_out[SAME_O + index].wait_recv()
            start(a2a_pass)

        @pl.when(step == 8)
        def _():
            near.start()
            att_out[0].wait_recv()
            att_f_core.start()
            att_t.start()
            att_o.start()

        rows = pl.ds(pl.multiple_of((step % 2) * half, half), half)
        u_part, c_part = u_all[tokens, rows, :], c_all[tokens, rows, :]
        hidden_act, slope = gelu_and_slope(dot_nt(up_all[place, :], u_part))
        d_pre = (slope * dot_nt(down_all[place, :], c_part)).astype(BF16)
        acc[first, pl.ds(0, fours)] += dot_nn(d_pre, u_part).reshape(fours, slab, hidden)
        acc[first, pl.ds(fours, fours)] += dot_nn(hidden_act.astype(BF16), c_part).reshape(fours, slab, hidden)
        return carry

    lax.fori_loop(0, 16, gradients, 0)
    out_own = pltpu.make_async_copy(acc.at[1], part_own, load_sem.at[1])
    out_own.start()
    for copy in w_own + w_near_t + w_over_t + w_near_t_core + w_near_f + w_far + [u_to_t, c_to_t] + uc_core + uc_pass:
        copy.wait_send()
    say_free(2, SAME_T)

    def relation_of(step):
        base = step % 4
        return jnp.where(base == 0, 2, jnp.where(base == 3, 3, base - 1))

    def qkv_rows(buf):
        return pl.ds(pl.multiple_of(buf * 6 * dim, 2 * dim), 6 * dim)

    def wo_rows(buf):
        return pl.ds(pl.multiple_of(12 * dim + buf * 2 * dim, 2 * dim), 2 * dim)

    def head_loads(relation, buf):
        copies = []
        for index in (0, 1):
            head = att_full.at[relation * 2 + 1 - index]
            first, second = (pl.ds(pl.multiple_of(base + index * size, dim), size) for base, size in ((buf * 6 * dim, 3 * dim), (12 * dim + buf * 2 * dim, dim)))
            copies.append(pltpu.make_async_copy(head.at[pl.ds(0, 3 * dim)], up_all.at[first], head_sem.at[buf, index, 0]))
            copies.append(pltpu.make_async_copy(head.at[pl.ds(3 * dim, dim)], up_all.at[second], head_sem.at[buf, index, 1]))
        return copies

    def rows_of(slot):
        return pl.ds(slot * slab, slab)

    def seq_loads(seq, src, src_slot, slot):
        return [pltpu.make_async_copy(src.at[src_slot, which], u_all.at[2 * seq + which, rows_of(slot)], seq_sem.at[2 * seq + which, slot]) for which in (0, 1)]

    seq_own = [copy for slot in range(8) for copy in seq_loads(0, uc_seq, slot, slot)]
    seq_two = [copy for slot in range(4) for copy in seq_loads(1, uc_two, slot, slot)]
    uc_to_t = [
        ring.copy(u_all.at[which, rows_of(slot)], u_all.at[2 + which, rows_of(4 + index)], far_sem.at[0, 2 * index + which], far_sem.at[1, 2 * index + which], SAME_T)
        for which in (0, 1)
        for index, slot in enumerate((0, 1, 4, 5))
    ]
    core_copies = [ring.copy(spare.at[index, pl.ds(0, 4)], acc.at[0, pl.ds(0, 4)], core_send.at[index], core_recv.at[index], PARTNER) for index in (0, 1)]
    f_copy = ring.copy(part_keep.at[0], acc.at[0, pl.ds(4, 4)], f_sem.at[0], f_sem.at[1], SAME_F)

    o_src = c_all.at[0]
    o_out = [
        ring.copy(o_src.at[rows_of(SAME_O)], o_relay.at[0], o_send.at[6], o_relay_recv.at[0], SAME_T),
        ring.copy(o_src.at[rows_of(OTHER_O)], o_relay.at[1], o_send.at[7], o_relay_recv.at[1], SAME_F),
    ] + [ring.copy(o_src.at[rows_of(slot)], o_pos.at[ring.me], o_send.at[slot], o_recv.at[slot], slot) for slot in (5, 4, 3, 2, 1)]
    o_pass = [
        ring.copy(o_relay.at[0], o_pos.at[ring.at(SAME_T)], o_send.at[8], o_recv.at[SAME_O], SAME_F),
        ring.copy(o_relay.at[1], o_pos.at[ring.at(SAME_F)], o_send.at[9], o_recv.at[OTHER_O], OTHER_T),
    ]
    o_keep = pltpu.make_async_copy(o_src.at[rows_of(0)], o_pos.at[ring.me], o_send.at[0])

    late = slab - LATE_ROWS
    early = {slot: late if slot == SAME_F else slab for slot in range(1, 6)}
    du_out = [
        ring.copy(acc.at[1, SAME_O], to_f.at[pl.ds(0, slab)], du_send.at[6], du_relay_recv.at[0], SAME_T),
        ring.copy(acc.at[1, OTHER_O], du_relay, du_send.at[7], du_relay_recv.at[1], SAME_F),
    ] + [ring.copy(acc.at[1, slot, pl.ds(0, early[slot])], du_pos.at[ring.me, pl.ds(0, early[slot])], du_send.at[slot], du_recv.at[slot], slot) for slot in (5, 4, 3, 2, 1)]
    du_keep = pltpu.make_async_copy(acc.at[1, 0], du_pos.at[ring.me], du_send.at[0])
    du_late = pltpu.make_async_copy(acc.at[1, SAME_F, pl.ds(late, slab - late)], to_f.at[pl.ds(slab, slab - late)], du_send.at[8])
    du_pass = ring.copy(du_relay, du_pos.at[ring.at(SAME_F)], du_send.at[9], du_recv.at[OTHER_O], OTHER_T)

    att_f_core.wait_recv()
    att_out[1].wait_recv()
    start(head_loads(2, 0))
    start(head_loads(0, 1))

    def arrive(slots):
        for slot in slots:
            if slot:
                ring.copy(uc_own.at[slot], uc_seq.at[slot], a2a_send.at[0], a2a_recv.at[slot], PARTNER).wait_recv()
            start(seq_own[2 * slot : 2 * slot + 2])

    def project(first, count):
        rows = pl.ds(first, count)
        for buf in (0, 1):
            c_all[2 + buf, rows, pl.ds(0, 6 * dim)] = dot_nt(u_all[0, rows, :], up_all[qkv_rows(buf), :]).astype(BF16)
            c_all[2 + buf, rows, pl.ds(6 * dim, 2 * dim)] = dot_nt(u_all[1, rows, :], up_all[wo_rows(buf), :]).astype(BF16)

    uc_keep.wait()
    arrive((0, 1, 4, 5, 2, 3))
    two_out.wait_recv()
    two_keep.wait()
    start(seq_two)
    out_own.wait()
    acc[1] = jnp.zeros(acc.shape[1:], F32)
    for copy in seq_own[:12] + head_loads(2, 0) + head_loads(0, 1):
        copy.wait()
    pl.semaphore_wait(free_slot.at[2], 1)
    start(uc_to_t)
    project(0, 6 * slab)
    arrive((6, 7))
    for copy in seq_own[12:]:
        copy.wait()
    project(6 * slab, 2 * slab)

    def chip_step(step, carry):
        buf = step % 2
        seq = step // 4
        relation = relation_of(step)

        @pl.when(step == 4)
        def _():
            near.wait_send()
            say_free(3, SAME_F)
            say_free(4, PARTNER)
            for copy in seq_two:
                copy.wait()
            for copy in uc_to_t[:4]:
                copy.wait_recv()

        @pl.when(step >= 2)
        def _():
            for copy in head_loads(0, buf):
                copy.wait()

        @pl.when((step == 3) | (step == 4))
        def _():
            start(head_loads(relation_of(step + 1), 1 - buf))

        kept = pl.ds(pl.multiple_of(jnp.where(step < 2, step, 2) * seq_len, seq_len), seq_len)
        heads = [ring.at_traced(relation * 2 + other) for other in (1, 0)]
        wo_copies = [
            pltpu.make_async_copy(up_all.at[pl.ds(pl.multiple_of(12 * dim + (2 * buf + index) * dim, dim), dim)], wo_full.at[head], wo_sem.at[index])
            for index, head in enumerate(heads)
        ]
        start(wo_copies)

        @pl.when(step >= 2)
        def _():
            c_all[2 + buf, :, pl.ds(0, 6 * dim)] = dot_nt(u_all[2 * seq], up_all[qkv_rows(buf), :]).astype(BF16)

        for index, head in enumerate(heads):
            columns = pl.ds(pl.multiple_of(head * dim, dim), dim)
            own = pl.ds(index * 3 * dim, 3 * dim)
            query, key, value = (c_all[2 + buf, :, pl.ds((index * 3 + part) * dim, dim)] for part in range(3))
            scores = dot_nt(query, key) * (scale * LOG2_E)
            grown = jnp.exp2(scores - jnp.max(scores, axis=-1, keepdims=True))
            prob = grown * (1.0 / jnp.sum(grown, axis=-1, keepdims=True))
            prob_b = prob.astype(BF16)
            c_all[seq, :, columns] = dot_nn(prob_b, value).astype(BF16)
            if index == 0:
                @pl.when(step == 4)
                def _():
                    for copy in uc_to_t[4:]:
                        copy.wait_recv()

                @pl.when(step >= 2)
                def _():
                    c_all[2 + buf, :, pl.ds(6 * dim, 2 * dim)] = dot_nt(u_all[2 * seq + 1], up_all[wo_rows(buf), :]).astype(BF16)

            d_out = c_all[2 + buf, :, pl.ds((6 + index) * dim, dim)]
            d_prob = dot_nt(d_out, value)
            d_score = (prob * (d_prob - jnp.sum(d_prob * prob, axis=-1, keepdims=True)) * scale).astype(BF16)
            down_all[kept, pl.ds(index * 3 * dim, dim)] = dot_nn(d_score, key).astype(BF16)
            down_all[kept, pl.ds((index * 3 + 1) * dim, dim)] = dot_nn(query.T, d_score).T.astype(BF16)
            down_all[kept, pl.ds((index * 3 + 2) * dim, dim)] = dot_nn(d_out.T, prob_b).T.astype(BF16)
            @pl.when(step >= 4)
            def _():
                dst = (spare, part_keep)[index].at[buf]
                dst[pl.ds(0, 3)] += dot_tn(down_all[kept, own], u_all[2]).reshape(3, dim, hidden)
                dst[3] += dot_tn(c_all[1, :, columns], u_all[3])

            if index == 0:
                @pl.when(step == 1)
                def _():
                    att_t.wait_recv()
                    att_t_core.start()

                @pl.when(step == 4)
                def _():
                    pl.semaphore_wait(free_slot.at[4], 1)
                    core_copies[0].start()

                @pl.when(step == 5)
                def _():
                    pl.semaphore_wait(free_slot.at[4], 1)
                    core_copies[1].start()

        @pl.when(step == 1)
        def _():
            att_t_core.wait_recv()
            start(head_loads(1, 0))

        @pl.when(step == 2)
        def _():
            att_o.wait_recv()
            att_o_core.start()

        @pl.when(step < 4)
        def _():
            def du_tile(part, carry):
                rows = pl.ds(pl.multiple_of(jnp.where(step < 2, step, 2) * seq_len + part * half, half), half)
                acc[1, pl.ds(part * fours, fours)] += dot_nn(down_all[rows, pl.ds(0, 6 * dim)], up_all[qkv_rows(buf), :]).reshape(fours, slab, hidden)
                return carry

            lax.fori_loop(0, 2, du_tile, 0)

        @pl.when(step == 2)
        def _():
            att_o_core.wait_recv()
            start(head_loads(3, 1))

        @pl.when(step == 3)
        def _():
            start(o_out)
            start(du_out)
            du_late.start()
            o_keep.start()
            du_keep.start()

            def own_gradients(pair, carry):
                own_rows = pl.ds(pl.multiple_of(pair * seq_len, seq_len), seq_len)
                for index, other in enumerate((1, 0)):
                    columns = pl.ds(pl.multiple_of(ring.at_traced(relation_of(pair) * 2 + other) * dim, dim), dim)
                    dst = (spare, part_keep)[index].at[pair]
                    dst[pl.ds(0, 3)] = dot_tn(down_all[own_rows, pl.ds(index * 3 * dim, 3 * dim)], u_all[0]).reshape(3, dim, hidden)
                    dst[3] = dot_tn(c_all[0, :, columns], u_all[1])
                return carry

            lax.fori_loop(0, 2, own_gradients, 0)

        @pl.when(step == 4)
        def _():
            core_copies[0].wait_recv()
            part_keep[0] += acc[0, pl.ds(0, 4)]
            say_free(4, PARTNER)
            pl.semaphore_wait(free_slot.at[3], 1)
            f_copy.start()

        for copy in wo_copies:
            copy.wait()
        return carry

    lax.fori_loop(0, 6, chip_step, 0)
    for copy in o_out[:2]:
        copy.wait_recv()
    start(o_pass)
    du_out[1].wait_recv()
    du_pass.start()
    core_copies[1].wait_recv()
    part_keep[1] += acc[0, pl.ds(0, 4)]
    for copy in du_out[2:]:
        copy.wait_recv()
    for slot in range(1, 8):
        ring.copy(o_pos.at[0], o_pos.at[ring.at(slot)], near_sem.at[0], o_recv.at[slot], PARTNER).wait_recv()
    du_out[0].wait_recv()
    du_pass.wait_recv()
    near.wait_recv()
    f_copy.wait_recv()
    part_keep[1] += acc[0, pl.ds(4, 4)]
    d_att_copy = pltpu.make_async_copy(part_keep.at[1], d_att, load_sem.at[0])
    d_att_copy.start()

    sends = att_out + [att_t, att_o, att_f_core, att_t_core, att_o_core] + list(a2a_out.values()) + a2a_pass + [two_out]
    for copy in sends + o_out + du_out + o_pass + uc_to_t + core_copies + [du_pass, f_copy]:
        copy.wait_send()
    du_late.wait()
    o_keep.wait()
    du_keep.wait()
    d_att_copy.wait()


def block_call(y_one, y_two, dy_one, dy_two, w_up, w_down, w_qkv, w_out):
    slabs, slab, hidden = y_one.shape
    tokens = slabs * slab
    ffn = w_down.shape[0]
    dim = w_out.shape[0]
    any_spec = pl.BlockSpec(memory_space=pl.ANY)
    dma, vmem, wide, narrow = pltpu.SemaphoreType.DMA, pltpu.VMEM, F32, BF16
    results = [
        ((slabs, slab, hidden), wide), ((slabs, slab, hidden), wide), ((slabs, slab, hidden), wide), ((slabs, slab, hidden), wide),
        ((4, dim, hidden), wide), ((slabs, slab, hidden), narrow), ((slabs, slab, hidden), wide), ((8, dim, hidden), narrow),
        ((slab + LATE_ROWS, hidden), wide),
    ]
    landing = [
        ((8, 2, slab, hidden), narrow), ((4, 2, slab, hidden), narrow), ((8, 4 * dim, hidden), narrow), ((2, slab, hidden), narrow), ((slab, hidden), wide),
    ]
    scratch = [
        vmem((4, tokens, hidden), BF16), vmem((4, tokens, hidden), BF16), vmem((6 * ffn, hidden), BF16), vmem((6 * ffn, hidden), BF16),
        vmem((2, slabs, slab, hidden), F32), vmem((2, 5, slab, hidden), F32), vmem((2, 4, dim, hidden), F32),
        vmem((8, 2, slab, hidden), BF16),
        dma((8,)), dma((2, 3)), dma((2, 2)), dma((16,)), dma((8, 2)), dma((6,)), dma((4, 2)), dma((7,)), dma((8,)), dma((11,)), dma((8,)), dma((3,)), dma((2,)), dma((2,)),
        dma((4, 8)), dma((2, 2, 2)), dma((2,)), dma((2,)), dma((2,)), dma((2,)), dma((2, 8)), dma((10,)), dma((8,)), dma((10,)), dma((8,)), dma((2,)), dma((2,)), dma((2,)),
        pltpu.SemaphoreType.REGULAR((6,)),
    ]
    return pl.pallas_call(
        functools.partial(block_kernel, dim ** -0.5),
        out_shape=[jax.ShapeDtypeStruct(shape, dtype) for shape, dtype in results + landing],
        in_specs=[any_spec] * 8,
        out_specs=[any_spec] * (len(results) + len(landing)),
        scratch_shapes=scratch,
        compiler_params=pltpu.CompilerParams(collective_id=0, has_side_effects=True, vmem_limit_bytes=VMEM_LIMIT),
        cost_estimate=pl.CostEstimate(flops=120 * 10**9, bytes_accessed=128 * 2**20, transcendentals=0),
        name="block",
    )(y_one, y_two, dy_one, dy_two, w_up.reshape(8, hidden // 8, ffn), w_down, w_qkv.reshape(3, 8, hidden // 8, dim), w_out)[: len(results)]


def finish_kernel(
    y_one, o_pos, wo_full, x_two, dx_one, dy_two, du_pos, part_own, near_recv, d_att,
    x_one_out, x_two_out, dx_one_out, dx_two_out, dw_up, dw_down, dw_qkv, dw_out,
    y_buf, o_buf, wo_buf, x_buf, dx_buf, dy_buf, du_buf, own_buf, near_buf, att_buf, up_out, qkv_out, load_sem, store_sem,
):
    tokens = y_buf.shape[0]
    dim = wo_buf.shape[0] // 8
    chunk = 256
    chunks = [pl.ds(index * chunk, chunk) for index in range(tokens // chunk)]

    def pieces(src, dst, sem, row):
        return [pltpu.make_async_copy(src.at[rows], dst.at[rows], sem.at[row, index]) for index, rows in enumerate(chunks)]

    def whole(src, dst, sem, row):
        return pltpu.make_async_copy(src, dst, sem.at[row, 0])

    ring = Ring()
    slab = tokens // 8
    sizes = {0: slab, PARTNER: slab, SAME_T: slab, OTHER_T: slab, SAME_F: slab - LATE_ROWS, OTHER_F: slab, OTHER_O: slab}
    slots = [pl.ds(pl.multiple_of(ring.at(slot) * slab, slab), size) for slot, size in sizes.items()]

    def slabs(src, dst, sem, row):
        return [pltpu.make_async_copy(src.at[rows], dst.at[rows], sem.at[row, index]) for index, rows in enumerate(slots)]

    x_in, dy_in, du_in = pieces(x_two, x_buf, load_sem, 0), slabs(dy_two, dy_buf, load_sem, 1), slabs(du_pos, du_buf, load_sem, 2)
    y_in, o_in = pieces(y_one, y_buf, load_sem, 3), pieces(o_pos, o_buf, load_sem, 4)
    wo_in, dx_in = whole(wo_full, wo_buf, load_sem, 5), pieces(dx_one, dx_buf, load_sem, 6)
    own_in, near_in, att_in = whole(part_own, own_buf, load_sem, 7), whole(near_recv, near_buf, load_sem, 8), whole(d_att, att_buf, load_sem, 9)
    order = [own_in, near_in, att_in, wo_in, *(copy for group in zip(y_in, o_in) for copy in group), *x_in, *(copy for group in zip(dy_in, du_in) for copy in group), *dx_in]
    for copy in order:
        copy.start()

    x_store, dx2_store, x1_store = pieces(x_buf, x_two_out, store_sem, 0), slabs(dy_buf, dx_two_out, store_sem, 1), pieces(y_buf, x_one_out, store_sem, 2)
    dx_store = pieces(dx_buf, dx_one_out, store_sem, 3)
    own_in.wait()
    near_in.wait()
    ffn = up_out.shape[1]
    own_buf[pl.ds(ffn, ffn), :] += near_buf[pl.ds(ffn, ffn), :]
    down_store = whole(own_buf.at[pl.ds(ffn, ffn)], dw_down, store_sem, 7)
    down_store.start()
    for part in range(up_out.shape[0] // ffn):
        columns = pl.ds(part * ffn, ffn)
        up_out[columns, :] = (own_buf[pl.ds(0, ffn), columns] + near_buf[pl.ds(0, ffn), columns]).T
    up_store = whole(up_out, dw_up, store_sem, 4)
    up_store.start()
    att_in.wait()
    for part in range(3):
        qkv_out[pl.ds(part, tokens, stride=3), 0, :] = att_buf[pl.ds(part * dim, dim), :].T
    qkv_store = whole(qkv_out, dw_qkv, store_sem, 5)
    qkv_store.start()
    out_store = whole(att_buf.at[pl.ds(3 * dim, dim)], dw_out, store_sem, 6)
    out_store.start()
    wo_in.wait()
    for index, rows in enumerate(chunks):
        y_in[index].wait()
        o_in[index].wait()
        y_buf[rows, :] -= dot_nn(o_buf[rows, :], wo_buf[...])
        x1_store[index].start()
    for index in range(len(chunks)):
        x_in[index].wait()
        x_store[index].start()
    for index, rows in enumerate(slots):
        dy_in[index].wait()
        du_in[index].wait()
        dy_buf[rows, :] += rms_back(x_buf[rows, :], du_buf[rows, :])
        dx2_store[index].start()
    for index in range(len(chunks)):
        dx_in[index].wait()
        dx_store[index].start()
    for copy in x_store + dx2_store + x1_store + dx_store + [up_store, qkv_store, out_store, down_store]:
        copy.wait()


def finish_call(y_one, o_pos, wo_full, x_two, dx_one, dy_two, du_pos, part_own, near_recv, d_att):
    tokens, hidden = y_one.shape
    ffn = part_own.shape[0] // 2
    dim = d_att.shape[0] // 4
    any_spec = pl.BlockSpec(memory_space=pl.ANY)
    dma, vmem = pltpu.SemaphoreType.DMA, pltpu.VMEM
    state = (tokens, hidden)
    out_shape = [jax.ShapeDtypeStruct(shape, F32) for shape in (state, state, state, state, (hidden, ffn), (ffn, hidden), (3 * hidden, 1, dim), (dim, hidden))]
    scratch = [
        vmem(state, F32), vmem(state, BF16), vmem((hidden, hidden), BF16), vmem(state, F32), vmem(state, F32), vmem(state, F32), vmem(state, F32),
        vmem(part_own.shape, F32), vmem(part_own.shape, F32), vmem(d_att.shape, F32), vmem((hidden, ffn), F32), vmem((3 * hidden, 1, dim), F32),
        dma((10, 7)), dma((8, 7)),
    ]
    return pl.pallas_call(
        finish_kernel,
        out_shape=out_shape,
        in_specs=[any_spec] * 10,
        out_specs=[any_spec] * 8,
        scratch_shapes=scratch,
        compiler_params=pltpu.CompilerParams(vmem_limit_bytes=VMEM_LIMIT),
        cost_estimate=pl.CostEstimate(flops=2 * 10**9, bytes_accessed=52 * 2**20, transcendentals=0),
        name="finish",
    )(y_one, o_pos, wo_full, x_two, dx_one, dy_two, du_pos, part_own, near_recv, d_att)


def last_kernel(x_two, dy_two, du_far, dx_two_in, dx_two_out, x_buf, dy_buf, du_buf, load_sem, store_sem):
    ring = Ring()
    slab = x_buf.shape[1]
    loads, stores, sizes = [], [], (slab, LATE_ROWS)
    for index, (slot, skip) in enumerate(((SAME_O, 0), (SAME_F, slab - LATE_ROWS))):
        size = sizes[index]
        rows = pl.ds(pl.multiple_of(ring.at(slot) * slab + skip, 16), size)
        sources = ((x_two.at[rows], x_buf), (dy_two.at[rows], dy_buf), (du_far.at[pl.ds(index * slab, size)], du_buf))
        loads.append([pltpu.make_async_copy(src, dst.at[index, pl.ds(0, size)], load_sem.at[index, which]) for which, (src, dst) in enumerate(sources)])
        stores.append(pltpu.make_async_copy(dy_buf.at[index, pl.ds(0, size)], dx_two_out.at[rows], store_sem.at[index]))
    for copies in loads:
        for copy in copies:
            copy.start()
    for index, copies in enumerate(loads):
        for copy in copies:
            copy.wait()
        rows = pl.ds(0, sizes[index])
        dy_buf[index, rows, :] += rms_back(x_buf[index, rows, :], du_buf[index, rows, :])
        stores[index].start()
    for copy in stores:
        copy.wait()


def last_call(x_two, dy_two, du_far, dx_two):
    tokens, hidden = x_two.shape
    any_spec = pl.BlockSpec(memory_space=pl.ANY)
    buf = pltpu.VMEM((2, tokens // 8, hidden), F32)
    return pl.pallas_call(
        last_kernel,
        out_shape=jax.ShapeDtypeStruct(dx_two.shape, F32),
        in_specs=[any_spec] * 4,
        out_specs=any_spec,
        input_output_aliases={3: 0},
        scratch_shapes=[buf, buf, buf, pltpu.SemaphoreType.DMA((2, 3)), pltpu.SemaphoreType.DMA((2,))],
        cost_estimate=pl.CostEstimate(flops=10**6, bytes_accessed=4 * 2**20, transcendentals=0),
        name="last",
    )(x_two, dy_two, du_far, dx_two)


def local_backward(y_one, y_two, dy_one, dy_two, w_qkv, w_out, w_up, w_down):
    hidden = y_one.shape[2]
    _, _, _, parts, dim = w_qkv.shape
    qkv_parts = jnp.swapaxes(w_qkv[0, :, 0], 0, 1)
    results = block_call(y_one, y_two, dy_one, dy_two, w_up[0], w_down[0], qkv_parts, w_out[0, 0])
    x_two, dx_one, part_own, near_recv, d_att, o_pos, du_pos, wo_full = (tensor.reshape(-1, hidden) for tensor in results[:8])
    devices = range(lax.axis_size("tp"))
    to_f = [(device, (3 - device // 2) * 2 + device % 2) for device in devices]
    du_far = lax.ppermute(results[8], "tp", to_f)
    y_flat, dy_flat = y_one.reshape(-1, hidden), dy_two.reshape(-1, hidden)
    *states, dw_up, dw_down, dw_qkv, dw_out = finish_call(y_flat, o_pos, wo_full, x_two, dx_one, dy_flat, du_pos, part_own, near_recv, d_att)
    states[3] = last_call(x_two, dy_flat, du_far, states[3])
    states = [tensor.reshape(y_one.shape) for tensor in states]
    return (*states, dw_qkv.reshape(1, hidden, 1, parts, dim), dw_out[None, None], dw_up[None], dw_down[None])


def solution(mesh):
    state_spec = P("dp", "tp", None)
    in_specs = (state_spec, state_spec, state_spec, state_spec, P(None, None, "tp", None, None), P(None, "tp", None, None), P(None, None, "tp"), P(None, "tp", None))
    out_specs = (state_spec, state_spec, state_spec, state_spec, P("dp", None, "tp", None, None), P("dp", "tp", None, None), P("dp", None, "tp"), P("dp", "tp", None))
    return jax.shard_map(local_backward, mesh=mesh, in_specs=in_specs, out_specs=out_specs, check_vma=False)
```

```python
import functools

import jax
import jax.numpy as jnp
from jax import lax
from jax.experimental import pallas as pl
from jax.experimental.pallas import tpu as pltpu
from jax.sharding import PartitionSpec as P

RMS_EPS = 1e-6
LOG2_E = 1.4426950408889634
LATE_ROWS = 80
FAR_ROWS = 16
MESH = pl.DeviceIdType.MESH
BF16, F32 = jnp.bfloat16, jnp.float32
VMEM_LIMIT = 64 * 1024 * 1024 - 65536


def inv_rms(tensor):
    return lax.rsqrt(jnp.mean(tensor * tensor, axis=-1, keepdims=True) + RMS_EPS)


def rms_norm(tensor):
    return tensor * inv_rms(tensor)


def rms_back(tensor, grad_in):
    scale = inv_rms(tensor)
    return scale * grad_in - tensor * (scale * scale * scale) * jnp.mean(grad_in * tensor, axis=-1, keepdims=True)


def gelu_and_slope(tensor):
    root = (2.0 / jnp.pi) ** 0.5
    squared = tensor * tensor
    tanh = jnp.tanh(root * (tensor + 0.044715 * (tensor * squared)))
    cdf = 0.5 * (1.0 + tanh)
    slope = cdf + (0.5 * root) * tensor * ((1.0 - tanh * tanh) * (1.0 + (3 * 0.044715) * squared))
    return tensor * cdf, slope


def dot_nn(left, right):
    return lax.dot_general(left, right, (((1,), (0,)), ((), ())), preferred_element_type=F32)


def dot_nt(left, right):
    return lax.dot_general(left, right, (((1,), (1,)), ((), ())), preferred_element_type=F32)


def dot_tn(left, right):
    return lax.dot_general(left, right, (((0,), (0,)), ((), ())), preferred_element_type=F32)


class Ring:
    def __init__(self):
        me = lax.axis_index("tp")
        chip, core = me // 2, me % 2
        self.me, self.chip, self.core = me, chip, core
        self.chips = (chip, chip + 1 - 2 * (chip % 2), 3 - chip, (chip + 2) % 4)

    def at(self, slot):
        core = self.core if slot % 2 == 0 else 1 - self.core
        return self.chips[slot // 2] * 2 + core

    def at_traced(self, slot):
        relation, other = slot // 2, slot % 2
        own, near_t, near_f, opposite = self.chips
        chip = jnp.where(relation == 0, own, jnp.where(relation == 1, near_t, jnp.where(relation == 2, near_f, opposite)))
        return chip * 2 + (self.core + other) % 2

    def arrive(self):
        for slot in (1, 2, 3, 4, 5):
            pl.semaphore_signal(pltpu.get_barrier_semaphore(), inc=1, device_id={"tp": self.at(slot)}, device_id_type=MESH)

    def meet(self):
        pl.semaphore_wait(pltpu.get_barrier_semaphore(), 5)

    def copy(self, src, dst, send_sem, recv_sem, slot):
        return pltpu.make_async_remote_copy(src_ref=src, dst_ref=dst, send_sem=send_sem, recv_sem=recv_sem, device_id={"tp": self.at(slot)}, device_id_type=MESH)


PARTNER, SAME_T, OTHER_T, SAME_F, OTHER_F, SAME_O, OTHER_O = 1, 2, 3, 4, 5, 6, 7


def block_kernel(
    scale,
    y_one, y_two, dy_one, dy_two, w_up, w_down, w_qkv, w_out,
    x_two, dx_one, part_own, near_recv, d_att, o_pos, du_pos, wo_full, to_f,
    uc_seq, uc_two, att_full, o_relay, du_relay,
    u_all, c_all, up_all, down_all, acc, spare, part_keep, uc_own,
    load_sem, y_sem, x_sem, w_send, w_recv, uc_send, uc_recv, att_send, att_recv, a2a_send, a2a_recv, relay_recv, near_sem, two_sem,
    seq_sem, head_sem, wo_sem, core_send, core_recv, f_sem, far_sem, o_send, o_recv, du_send, du_recv, o_relay_recv, du_relay_recv, far_recv, free_slot,
):
    ring = Ring()
    slabs, slab, hidden = acc.shape[1:]
    seq_len = slabs * slab
    half = seq_len // 2
    dim = w_out.shape[0]
    fours = slabs // 2

    def start(copies):
        for copy in copies:
            copy.start()

    def say_free(index, to):
        pl.semaphore_signal(free_slot.at[index], inc=1, device_id={"tp": ring.at(to)}, device_id_type=MESH)

    rooms = (0, 1, 2, 3, 4, 5, 1, 3)

    def room(slot):
        return pl.ds(rooms[slot] * half, half)

    def weight_pair(src_slot, dst_slot, to, index):
        return [
            ring.copy(buf.at[room(src_slot)], buf.at[room(dst_slot)], w_send.at[index + which], w_recv.at[dst_slot, which], to)
            for which, buf in enumerate((up_all, down_all))
        ]

    w_own = weight_pair(0, 1, PARTNER, 0) + weight_pair(0, 2, SAME_T, 2) + weight_pair(0, 4, SAME_F, 4)
    def far_part(src_slot, first, count, to, index, recv_sem):
        src, dst = (pl.ds(rooms[slot] * half + first, count) for slot in (src_slot, 6))
        return [ring.copy(buf.at[src], buf.at[dst], w_send.at[index + which], recv_sem.at[which], to) for which, buf in enumerate((up_all, down_all))]

    w_near_t = far_part(2, FAR_ROWS, half - FAR_ROWS, SAME_F, 6, w_recv.at[6])
    w_over_t = far_part(4, 0, FAR_ROWS, SAME_T, 14, far_recv)
    w_near_t_core = weight_pair(2, 3, PARTNER, 8)
    w_near_f = weight_pair(4, 5, PARTNER, 10)
    w_far = weight_pair(6, 7, PARTNER, 12)

    def uc_pair(src_slot, dst_slot, to, index):
        return [ring.copy(buf.at[src_slot], buf.at[dst_slot], uc_send.at[index + which], uc_recv.at[dst_slot, which], to) for which, buf in enumerate((u_all, c_all))]

    u_to_t, c_to_t = uc_pair(0, 2, SAME_T, 0)
    uc_core = uc_pair(0, 1, PARTNER, 2)
    uc_pass = uc_pair(2, 3, PARTNER, 4)

    def att(src, dst_slot, to, index):
        return ring.copy(src, att_full.at[dst_slot], att_send.at[index], att_recv.at[dst_slot], to)

    att_keep = [pltpu.make_async_copy(uc_own.at[part, 0], att_full.at[0, pl.ds(part * dim, dim)], x_sem.at[part // 2, part % 2]) for part in range(4)]
    att_out = [att(att_full.at[0], 4, SAME_F, 0), att(att_full.at[0], 1, PARTNER, 1)]
    att_t, att_o = att(att_full.at[0], 2, SAME_T, 2), att(att_full.at[4], 6, SAME_T, 3)
    att_f_core, att_t_core, att_o_core = att(att_full.at[4], 5, PARTNER, 4), att(att_full.at[2], 3, PARTNER, 5), att(att_full.at[6], 7, PARTNER, 6)

    a2a_out = {slot: ring.copy(uc_own.at[slot], uc_seq.at[slot], a2a_send.at[slot], a2a_recv.at[slot], slot) for slot in (1, 2, 3, 4, 5)}
    a2a_out[SAME_O] = ring.copy(uc_own.at[SAME_O], uc_two.at[2], a2a_send.at[SAME_O], relay_recv.at[0], SAME_F)
    a2a_out[OTHER_O] = ring.copy(uc_own.at[OTHER_O], uc_two.at[3], a2a_send.at[OTHER_O], relay_recv.at[1], OTHER_F)
    a2a_pass = [ring.copy(uc_two.at[2 + index], uc_seq.at[SAME_O + index], a2a_send.at[8 + index], a2a_recv.at[SAME_O + index], SAME_T) for index in (0, 1)]
    uc_keep = pltpu.make_async_copy(uc_own.at[0], uc_seq.at[0], load_sem.at[4])
    two_out = ring.copy(uc_own.at[OTHER_T], uc_two.at[1], a2a_send.at[10], relay_recv.at[2], PARTNER)
    two_keep = pltpu.make_async_copy(uc_own.at[SAME_T], uc_two.at[0], two_sem.at[0])
    near = ring.copy(acc.at[0], near_recv, near_sem.at[0], near_sem.at[1], SAME_F)

    loads = [
        pltpu.make_async_copy(w_down, down_all.at[room(0)], load_sem.at[0]),
        pltpu.make_async_copy(w_up, uc_own.at[:, 0, :, pl.ds(0, half)], load_sem.at[1]),
        pltpu.make_async_copy(y_one, acc.at[0], load_sem.at[2]),
        pltpu.make_async_copy(dy_two, acc.at[1], load_sem.at[3]),
    ]
    qkv_loads = [pltpu.make_async_copy(w_qkv.at[part], uc_own.at[:, 1, :, pl.ds(part * dim, dim)], y_sem.at[0, part]) for part in range(3)]
    ring.arrive()
    start(loads)
    start(qkv_loads)
    ring.meet()
    loads[0].wait()
    start(w_own[1::2])
    loads[1].wait()
    for part in range(half // dim):
        up_all[pl.ds(part * dim, dim), :] = uc_own[:, 0, :, pl.ds(part * dim, dim)].reshape(hidden, dim).T
    start(w_own[0::2])
    out_load = pltpu.make_async_copy(w_out, uc_own.at[3, 0], load_sem.at[7])
    out_load.start()
    loads[2].wait()
    loads[3].wait()

    def normalize(step, carry):
        rows = pl.ds(pl.multiple_of(step * slab, slab), slab)
        u_all[0, rows, :] = rms_norm(acc[0, step]).astype(BF16)
        c_all[0, rows, :] = acc[1, step].astype(BF16)
        acc[0, step] = jnp.zeros((slab, hidden), F32)
        acc[1, step] = jnp.zeros((slab, hidden), F32)
        return carry

    lax.fori_loop(0, slabs, normalize, 0)
    u_to_t.start()
    start(uc_core)
    for part in range(3):
        qkv_loads[part].wait()
        uc_own[part, 0] = uc_own[:, 1, :, pl.ds(part * dim, dim)].reshape(hidden, dim).T
    out_load.wait()
    start(att_keep)

    def y_loads(step, buf):
        seq = ring.at_traced(7 - step)
        return [pltpu.make_async_copy(src.at[seq], spare.at[buf, which], y_sem.at[buf, which]) for which, src in enumerate((y_one, y_two, dy_one))]

    def x_stores(step, buf):
        seq = ring.at_traced(7 - step)
        return [pltpu.make_async_copy(spare.at[buf, 3 + which], dst.at[seq], x_sem.at[buf, which]) for which, dst in enumerate((x_two, dx_one))]

    def feed_forward(step, carry):
        slot = jnp.where(step == 3, 4, jnp.where(step == 4, 3, step))
        place = pl.ds(pl.multiple_of(jnp.where(step == 6, 1, jnp.where(step == 7, 3, slot)) * half, half), half)

        @pl.when((step == 1) | ((step >= 3) & (step != 6)))
        def _():
            for which, buf in enumerate((up_all, down_all)):
                ring.copy(buf.at[place], buf.at[place], w_send.at[0], w_recv.at[slot, which], PARTNER).wait_recv()

        @pl.when(step == 6)
        def _():
            for copy in w_near_t + w_over_t:
                copy.wait_recv()

        @pl.when(step == 2)
        def _():
            pl.semaphore_wait(free_slot.at[0], 1)
            for which, buf in ((1, down_all), (0, up_all)):
                ring.copy(buf.at[room(2)], buf.at[room(2)], w_send.at[0], w_recv.at[2, which], PARTNER).wait_recv()
                w_near_t[which].start()
                w_near_t_core[which].start()
            for copy in att_keep:
                copy.wait()
            start(att_out)

        @pl.when(step == 3)
        def _():
            pl.semaphore_wait(free_slot.at[5], 1)
            start(w_over_t)
            c_to_t.start()
            start(w_near_f)

        @pl.when(step == 6)
        def _():
            pl.semaphore_wait(free_slot.at[1], 1)
            start(w_far)

        @pl.when(step == 7)
        def _():
            start(y_loads(0, 0))

        def rows_step(part, carry):
            rows = pl.ds(pl.multiple_of(part * half, half), half)
            quarter = pl.ds(part * fours, fours)
            hidden_act, slope = gelu_and_slope(dot_nt(u_all[0, rows, :], up_all[place, :]))
            d_pre = (slope * dot_nt(c_all[0, rows, :], down_all[place, :])).astype(BF16)
            acc[0, quarter] += dot_nn(hidden_act.astype(BF16), down_all[place, :]).reshape(fours, slab, hidden)
            acc[1, quarter] += dot_nn(d_pre, up_all[place, :]).reshape(fours, slab, hidden)
            return carry

        lax.fori_loop(0, 2, rows_step, 0)

        @pl.when(step == 1)
        def _():
            say_free(0, SAME_F)
            say_free(5, SAME_T)

        @pl.when(step == 4)
        def _():
            say_free(1, PARTNER)

        return carry

    lax.fori_loop(0, 8, feed_forward, 0)

    def finish(step, carry):
        slot = 7 - step
        buf = step % 2
        seq = ring.at_traced(slot)
        for copy in y_loads(step, buf):
            copy.wait()

        @pl.when(step < 7)
        def _():
            start(y_loads(step + 1, 1 - buf))

        @pl.when(step >= 2)
        def _():
            for copy in x_stores(step - 2, buf):
                copy.wait()

        y_first = spare[buf, 0]
        x_second = spare[buf, 1] - acc[0, seq]
        dy_first = spare[buf, 2] + rms_back(y_first, acc[1, seq])
        spare[buf, 3] = x_second
        spare[buf, 4] = dy_first
        uc_own[slot, 0] = rms_norm(x_second).astype(BF16)
        uc_own[slot, 1] = dy_first.astype(BF16)
        acc[0, seq] = jnp.zeros((slab, hidden), F32)
        acc[1, seq] = jnp.zeros((slab, hidden), F32)
        start(x_stores(step, buf))
        return carry

    lax.fori_loop(0, 8, finish, 0)
    for slot in (7, 6, 5, 4, 3, 2, 1):
        a2a_out[slot].start()
    uc_keep.start()
    two_out.start()
    two_keep.start()
    for step in (6, 7):
        for copy in x_stores(step, step % 2):
            copy.wait()

    def gradients(step, carry):
        first = step // 8
        tokens = (step % 8) // 2
        place = pl.ds(pl.multiple_of((4 - 4 * first) * half, half), half)

        @pl.when(step == 0)
        def _():
            u_to_t.wait_recv()
            uc_pass[0].start()

        @pl.when((step == 2) | (step == 6))
        def _():
            for which, buf in enumerate((u_all, c_all)):
                ring.copy(buf.at[tokens], buf.at[tokens], uc_send.at[0], uc_recv.at[tokens, which], PARTNER).wait_recv()

        @pl.when(step == 4)
        def _():
            c_to_t.wait_recv()
            uc_pass[1].start()
            for index in (0, 1):
                a2a_out[SAME_O + index].wait_recv()
            start(a2a_pass)

        @pl.when(step == 8)
        def _():
            near.start()
            att_out[0].wait_recv()
            att_f_core.start()
            att_t.start()
            att_o.start()

        rows = pl.ds(pl.multiple_of((step % 2) * half, half), half)
        u_part, c_part = u_all[tokens, rows, :], c_all[tokens, rows, :]
        hidden_act, slope = gelu_and_slope(dot_nt(up_all[place, :], u_part))
        d_pre = (slope * dot_nt(down_all[place, :], c_part)).astype(BF16)
        acc[first, pl.ds(0, fours)] += dot_nn(d_pre, u_part).reshape(fours, slab, hidden)
        acc[first, pl.ds(fours, fours)] += dot_nn(hidden_act.astype(BF16), c_part).reshape(fours, slab, hidden)
        return carry

    lax.fori_loop(0, 16, gradients, 0)
    out_own = pltpu.make_async_copy(acc.at[1], part_own, load_sem.at[1])
    out_own.start()
    for copy in w_own + w_near_t + w_over_t + w_near_t_core + w_near_f + w_far + [u_to_t, c_to_t] + uc_core + uc_pass:
        copy.wait_send()
    say_free(2, SAME_T)

    def relation_of(step):
        base = step % 4
        return jnp.where(base == 0, 2, jnp.where(base == 3, 3, base - 1))

    def qkv_rows(buf):
        return pl.ds(pl.multiple_of(buf * 6 * dim, 2 * dim), 6 * dim)

    def wo_rows(buf):
        return pl.ds(pl.multiple_of(12 * dim + buf * 2 * dim, 2 * dim), 2 * dim)

    def head_loads(relation, buf):
        copies = []
        for index in (0, 1):
            head = att_full.at[relation * 2 + 1 - index]
            first, second = (pl.ds(pl.multiple_of(base + index * size, dim), size) for base, size in ((buf * 6 * dim, 3 * dim), (12 * dim + buf * 2 * dim, dim)))
            copies.append(pltpu.make_async_copy(head.at[pl.ds(0, 3 * dim)], up_all.at[first], head_sem.at[buf, index, 0]))
            copies.append(pltpu.make_async_copy(head.at[pl.ds(3 * dim, dim)], up_all.at[second], head_sem.at[buf, index, 1]))
        return copies

    def rows_of(slot):
        return pl.ds(slot * slab, slab)

    def seq_loads(seq, src, src_slot, slot):
        return [pltpu.make_async_copy(src.at[src_slot, which], u_all.at[2 * seq + which, rows_of(slot)], seq_sem.at[2 * seq + which, slot]) for which in (0, 1)]

    seq_own = [copy for slot in range(8) for copy in seq_loads(0, uc_seq, slot, slot)]
    seq_two = [copy for slot in range(4) for copy in seq_loads(1, uc_two, slot, slot)]
    uc_to_t = [
        ring.copy(u_all.at[which, rows_of(slot)], u_all.at[2 + which, rows_of(4 + index)], far_sem.at[0, 2 * index + which], far_sem.at[1, 2 * index + which], SAME_T)
        for which in (0, 1)
        for index, slot in enumerate((0, 1, 4, 5))
    ]
    core_copies = [ring.copy(spare.at[index, pl.ds(0, 4)], acc.at[0, pl.ds(0, 4)], core_send.at[index], core_recv.at[index], PARTNER) for index in (0, 1)]
    f_copy = ring.copy(part_keep.at[0], acc.at[0, pl.ds(4, 4)], f_sem.at[0], f_sem.at[1], SAME_F)

    o_src = c_all.at[0]
    o_out = [
        ring.copy(o_src.at[rows_of(SAME_O)], o_relay.at[0], o_send.at[6], o_relay_recv.at[0], SAME_T),
        ring.copy(o_src.at[rows_of(OTHER_O)], o_relay.at[1], o_send.at[7], o_relay_recv.at[1], SAME_F),
    ] + [ring.copy(o_src.at[rows_of(slot)], o_pos.at[ring.me], o_send.at[slot], o_recv.at[slot], slot) for slot in (5, 4, 3, 2, 1)]
    o_pass = [
        ring.copy(o_relay.at[0], o_pos.at[ring.at(SAME_T)], o_send.at[8], o_recv.at[SAME_O], SAME_F),
        ring.copy(o_relay.at[1], o_pos.at[ring.at(SAME_F)], o_send.at[9], o_recv.at[OTHER_O], OTHER_T),
    ]
    o_keep = pltpu.make_async_copy(o_src.at[rows_of(0)], o_pos.at[ring.me], o_send.at[0])

    late = slab - LATE_ROWS
    early = {slot: late if slot == SAME_F else slab for slot in range(1, 6)}
    du_out = [
        ring.copy(acc.at[1, SAME_O], to_f.at[pl.ds(0, slab)], du_send.at[6], du_relay_recv.at[0], SAME_T),
        ring.copy(acc.at[1, OTHER_O], du_relay, du_send.at[7], du_relay_recv.at[1], SAME_F),
    ] + [ring.copy(acc.at[1, slot, pl.ds(0, early[slot])], du_pos.at[ring.me, pl.ds(0, early[slot])], du_send.at[slot], du_recv.at[slot], slot) for slot in (5, 4, 3, 2, 1)]
    du_keep = pltpu.make_async_copy(acc.at[1, 0], du_pos.at[ring.me], du_send.at[0])
    du_late = pltpu.make_async_copy(acc.at[1, SAME_F, pl.ds(late, slab - late)], to_f.at[pl.ds(slab, slab - late)], du_send.at[8])
    du_pass = ring.copy(du_relay, du_pos.at[ring.at(SAME_F)], du_send.at[9], du_recv.at[OTHER_O], OTHER_T)

    att_f_core.wait_recv()
    att_out[1].wait_recv()
    start(head_loads(2, 0))
    start(head_loads(0, 1))

    def arrive(slots):
        for slot in slots:
            if slot:
                ring.copy(uc_own.at[slot], uc_seq.at[slot], a2a_send.at[0], a2a_recv.at[slot], PARTNER).wait_recv()
            start(seq_own[2 * slot : 2 * slot + 2])

    def project(first, count):
        rows = pl.ds(first, count)
        for buf in (0, 1):
            c_all[2 + buf, rows, pl.ds(0, 6 * dim)] = dot_nt(u_all[0, rows, :], up_all[qkv_rows(buf), :]).astype(BF16)
            c_all[2 + buf, rows, pl.ds(6 * dim, 2 * dim)] = dot_nt(u_all[1, rows, :], up_all[wo_rows(buf), :]).astype(BF16)

    uc_keep.wait()
    arrive((0, 1, 4, 5, 2, 3))
    two_out.wait_recv()
    two_keep.wait()
    start(seq_two)
    out_own.wait()
    acc[1] = jnp.zeros(acc.shape[1:], F32)
    for copy in seq_own[:12] + head_loads(2, 0) + head_loads(0, 1):
        copy.wait()
    pl.semaphore_wait(free_slot.at[2], 1)
    start(uc_to_t)
    project(0, 6 * slab)
    arrive((6, 7))
    for copy in seq_own[12:]:
        copy.wait()
    project(6 * slab, 2 * slab)

    def chip_step(step, carry):
        buf = step % 2
        seq = step // 4
        relation = relation_of(step)

        @pl.when(step == 4)
        def _():
            near.wait_send()
            say_free(3, SAME_F)
            say_free(4, PARTNER)
            for copy in seq_two:
                copy.wait()
            for copy in uc_to_t[:4]:
                copy.wait_recv()

        @pl.when(step >= 2)
        def _():
            for copy in head_loads(0, buf):
                copy.wait()

        @pl.when((step == 3) | (step == 4))
        def _():
            start(head_loads(relation_of(step + 1), 1 - buf))

        kept = pl.ds(pl.multiple_of(jnp.where(step < 2, step, 2) * seq_len, seq_len), seq_len)
        heads = [ring.at_traced(relation * 2 + other) for other in (1, 0)]
        wo_copies = [
            pltpu.make_async_copy(up_all.at[pl.ds(pl.multiple_of(12 * dim + (2 * buf + index) * dim, dim), dim)], wo_full.at[head], wo_sem.at[index])
            for index, head in enumerate(heads)
        ]
        start(wo_copies)

        @pl.when(step >= 2)
        def _():
            c_all[2 + buf, :, pl.ds(0, 6 * dim)] = dot_nt(u_all[2 * seq], up_all[qkv_rows(buf), :]).astype(BF16)

        for index, head in enumerate(heads):
            columns = pl.ds(pl.multiple_of(head * dim, dim), dim)
            own = pl.ds(index * 3 * dim, 3 * dim)
            query, key, value = (c_all[2 + buf, :, pl.ds((index * 3 + part) * dim, dim)] for part in range(3))
            scores = dot_nt(query, key) * (scale * LOG2_E)
            grown = jnp.exp2(scores - jnp.max(scores, axis=-1, keepdims=True))
            prob = grown * (1.0 / jnp.sum(grown, axis=-1, keepdims=True))
            prob_b = prob.astype(BF16)
            c_all[seq, :, columns] = dot_nn(prob_b, value).astype(BF16)
            if index == 0:
                @pl.when(step == 4)
                def _():
                    for copy in uc_to_t[4:]:
                        copy.wait_recv()

                @pl.when(step >= 2)
                def _():
                    c_all[2 + buf, :, pl.ds(6 * dim, 2 * dim)] = dot_nt(u_all[2 * seq + 1], up_all[wo_rows(buf), :]).astype(BF16)

            d_out = c_all[2 + buf, :, pl.ds((6 + index) * dim, dim)]
            d_prob = dot_nt(d_out, value)
            d_score = (prob * (d_prob - jnp.sum(d_prob * prob, axis=-1, keepdims=True)) * scale).astype(BF16)
            down_all[kept, pl.ds(index * 3 * dim, dim)] = dot_nn(d_score, key).astype(BF16)
            down_all[kept, pl.ds((index * 3 + 1) * dim, dim)] = dot_nn(query.T, d_score).T.astype(BF16)
            down_all[kept, pl.ds((index * 3 + 2) * dim, dim)] = dot_nn(d_out.T, prob_b).T.astype(BF16)
            @pl.when(step >= 4)
            def _():
                dst = (spare, part_keep)[index].at[buf]
                dst[pl.ds(0, 3)] += dot_tn(down_all[kept, own], u_all[2]).reshape(3, dim, hidden)
                dst[3] += dot_tn(c_all[1, :, columns], u_all[3])

            if index == 0:
                @pl.when(step == 1)
                def _():
                    att_t.wait_recv()
                    att_t_core.start()

                @pl.when(step == 4)
                def _():
                    pl.semaphore_wait(free_slot.at[4], 1)
                    core_copies[0].start()

                @pl.when(step == 5)
                def _():
                    pl.semaphore_wait(free_slot.at[4], 1)
                    core_copies[1].start()

        @pl.when(step == 1)
        def _():
            att_t_core.wait_recv()
            start(head_loads(1, 0))

        @pl.when(step == 2)
        def _():
            att_o.wait_recv()
            att_o_core.start()

        @pl.when(step < 4)
        def _():
            def du_tile(part, carry):
                rows = pl.ds(pl.multiple_of(jnp.where(step < 2, step, 2) * seq_len + part * half, half), half)
                acc[1, pl.ds(part * fours, fours)] += dot_nn(down_all[rows, pl.ds(0, 6 * dim)], up_all[qkv_rows(buf), :]).reshape(fours, slab, hidden)
                return carry

            lax.fori_loop(0, 2, du_tile, 0)

        @pl.when(step == 2)
        def _():
            att_o_core.wait_recv()
            start(head_loads(3, 1))

        @pl.when(step == 3)
        def _():
            start(o_out)
            start(du_out)
            du_late.start()
            o_keep.start()
            du_keep.start()

            def own_gradients(pair, carry):
                own_rows = pl.ds(pl.multiple_of(pair * seq_len, seq_len), seq_len)
                for index, other in enumerate((1, 0)):
                    columns = pl.ds(pl.multiple_of(ring.at_traced(relation_of(pair) * 2 + other) * dim, dim), dim)
                    dst = (spare, part_keep)[index].at[pair]
                    dst[pl.ds(0, 3)] = dot_tn(down_all[own_rows, pl.ds(index * 3 * dim, 3 * dim)], u_all[0]).reshape(3, dim, hidden)
                    dst[3] = dot_tn(c_all[0, :, columns], u_all[1])
                return carry

            lax.fori_loop(0, 2, own_gradients, 0)

        @pl.when(step == 4)
        def _():
            core_copies[0].wait_recv()
            part_keep[0] += acc[0, pl.ds(0, 4)]
            say_free(4, PARTNER)
            pl.semaphore_wait(free_slot.at[3], 1)
            f_copy.start()

        for copy in wo_copies:
            copy.wait()
        return carry

    lax.fori_loop(0, 6, chip_step, 0)
    for copy in o_out[:2]:
        copy.wait_recv()
    start(o_pass)
    du_out[1].wait_recv()
    du_pass.start()
    core_copies[1].wait_recv()
    part_keep[1] += acc[0, pl.ds(0, 4)]
    for copy in du_out[2:]:
        copy.wait_recv()
    for slot in range(1, 8):
        ring.copy(o_pos.at[0], o_pos.at[ring.at(slot)], near_sem.at[0], o_recv.at[slot], PARTNER).wait_recv()
    du_out[0].wait_recv()
    du_pass.wait_recv()
    near.wait_recv()
    f_copy.wait_recv()
    part_keep[1] += acc[0, pl.ds(4, 4)]
    d_att_copy = pltpu.make_async_copy(part_keep.at[1], d_att, load_sem.at[0])
    d_att_copy.start()

    sends = att_out + [att_t, att_o, att_f_core, att_t_core, att_o_core] + list(a2a_out.values()) + a2a_pass + [two_out]
    for copy in sends + o_out + du_out + o_pass + uc_to_t + core_copies + [du_pass, f_copy]:
        copy.wait_send()
    du_late.wait()
    o_keep.wait()
    du_keep.wait()
    d_att_copy.wait()


def block_call(y_one, y_two, dy_one, dy_two, w_up, w_down, w_qkv, w_out):
    slabs, slab, hidden = y_one.shape
    tokens = slabs * slab
    ffn = w_down.shape[0]
    dim = w_out.shape[0]
    any_spec = pl.BlockSpec(memory_space=pl.ANY)
    dma, vmem, wide, narrow = pltpu.SemaphoreType.DMA, pltpu.VMEM, F32, BF16
    results = [
        ((slabs, slab, hidden), wide), ((slabs, slab, hidden), wide), ((slabs, slab, hidden), wide), ((slabs, slab, hidden), wide),
        ((4, dim, hidden), wide), ((slabs, slab, hidden), narrow), ((slabs, slab, hidden), wide), ((8, dim, hidden), narrow),
        ((slab + LATE_ROWS, hidden), wide),
    ]
    landing = [
        ((8, 2, slab, hidden), narrow), ((4, 2, slab, hidden), narrow), ((8, 4 * dim, hidden), narrow), ((2, slab, hidden), narrow), ((slab, hidden), wide),
    ]
    scratch = [
        vmem((4, tokens, hidden), BF16), vmem((4, tokens, hidden), BF16), vmem((6 * ffn, hidden), BF16), vmem((6 * ffn, hidden), BF16),
        vmem((2, slabs, slab, hidden), F32), vmem((2, 5, slab, hidden), F32), vmem((2, 4, dim, hidden), F32),
        vmem((8, 2, slab, hidden), BF16),
        dma((8,)), dma((2, 3)), dma((2, 2)), dma((16,)), dma((8, 2)), dma((6,)), dma((4, 2)), dma((7,)), dma((8,)), dma((11,)), dma((8,)), dma((3,)), dma((2,)), dma((2,)),
        dma((4, 8)), dma((2, 2, 2)), dma((2,)), dma((2,)), dma((2,)), dma((2,)), dma((2, 8)), dma((10,)), dma((8,)), dma((10,)), dma((8,)), dma((2,)), dma((2,)), dma((2,)),
        pltpu.SemaphoreType.REGULAR((6,)),
    ]
    return pl.pallas_call(
        functools.partial(block_kernel, dim ** -0.5),
        out_shape=[jax.ShapeDtypeStruct(shape, dtype) for shape, dtype in results + landing],
        in_specs=[any_spec] * 8,
        out_specs=[any_spec] * (len(results) + len(landing)),
        scratch_shapes=scratch,
        compiler_params=pltpu.CompilerParams(collective_id=0, has_side_effects=True, vmem_limit_bytes=VMEM_LIMIT),
        cost_estimate=pl.CostEstimate(flops=120 * 10**9, bytes_accessed=128 * 2**20, transcendentals=0),
        name="block",
    )(y_one, y_two, dy_one, dy_two, w_up.reshape(8, hidden // 8, ffn), w_down, w_qkv.reshape(3, 8, hidden // 8, dim), w_out)[: len(results)]


def finish_kernel(
    y_one, o_pos, wo_full, x_two, dx_one, dy_two, du_pos, part_own, near_recv, d_att,
    x_one_out, x_two_out, dx_one_out, dx_two_out, dw_up, dw_down, dw_qkv, dw_out,
    y_buf, o_buf, wo_buf, x_buf, dx_buf, dy_buf, du_buf, own_buf, near_buf, att_buf, up_out, qkv_out, load_sem, store_sem,
):
    tokens = y_buf.shape[0]
    dim = wo_buf.shape[0] // 8
    chunk = 256
    chunks = [pl.ds(index * chunk, chunk) for index in range(tokens // chunk)]

    def pieces(src, dst, sem, row):
        return [pltpu.make_async_copy(src.at[rows], dst.at[rows], sem.at[row, index]) for index, rows in enumerate(chunks)]

    def whole(src, dst, sem, row):
        return pltpu.make_async_copy(src, dst, sem.at[row, 0])

    ring = Ring()
    slab = tokens // 8
    sizes = {0: slab, PARTNER: slab, SAME_T: slab, OTHER_T: slab, SAME_F: slab - LATE_ROWS, OTHER_F: slab, OTHER_O: slab}
    slots = [pl.ds(pl.multiple_of(ring.at(slot) * slab, slab), size) for slot, size in sizes.items()]

    def slabs(src, dst, sem, row):
        return [pltpu.make_async_copy(src.at[rows], dst.at[rows], sem.at[row, index]) for index, rows in enumerate(slots)]

    x_in, dy_in, du_in = pieces(x_two, x_buf, load_sem, 0), slabs(dy_two, dy_buf, load_sem, 1), slabs(du_pos, du_buf, load_sem, 2)
    y_in, o_in = pieces(y_one, y_buf, load_sem, 3), pieces(o_pos, o_buf, load_sem, 4)
    wo_in, dx_in = whole(wo_full, wo_buf, load_sem, 5), pieces(dx_one, dx_buf, load_sem, 6)
    own_in, near_in, att_in = whole(part_own, own_buf, load_sem, 7), whole(near_recv, near_buf, load_sem, 8), whole(d_att, att_buf, load_sem, 9)
    order = [own_in, near_in, att_in, wo_in, *(copy for group in zip(y_in, o_in) for copy in group), *x_in, *(copy for group in zip(dy_in, du_in) for copy in group), *dx_in]
    for copy in order:
        copy.start()

    x_store, dx2_store, x1_store = pieces(x_buf, x_two_out, store_sem, 0), slabs(dy_buf, dx_two_out, store_sem, 1), pieces(y_buf, x_one_out, store_sem, 2)
    dx_store = pieces(dx_buf, dx_one_out, store_sem, 3)
    own_in.wait()
    near_in.wait()
    ffn = up_out.shape[1]
    own_buf[pl.ds(ffn, ffn), :] += near_buf[pl.ds(ffn, ffn), :]
    down_store = whole(own_buf.at[pl.ds(ffn, ffn)], dw_down, store_sem, 7)
    down_store.start()
    for part in range(up_out.shape[0] // ffn):
        columns = pl.ds(part * ffn, ffn)
        up_out[columns, :] = (own_buf[pl.ds(0, ffn), columns] + near_buf[pl.ds(0, ffn), columns]).T
    up_store = whole(up_out, dw_up, store_sem, 4)
    up_store.start()
    att_in.wait()
    for part in range(3):
        qkv_out[pl.ds(part, tokens, stride=3), 0, :] = att_buf[pl.ds(part * dim, dim), :].T
    qkv_store = whole(qkv_out, dw_qkv, store_sem, 5)
    qkv_store.start()
    out_store = whole(att_buf.at[pl.ds(3 * dim, dim)], dw_out, store_sem, 6)
    out_store.start()
    wo_in.wait()
    for index, rows in enumerate(chunks):
        y_in[index].wait()
        o_in[index].wait()
        y_buf[rows, :] -= dot_nn(o_buf[rows, :], wo_buf[...])
        x1_store[index].start()
    for index in range(len(chunks)):
        x_in[index].wait()
        x_store[index].start()
    for index, rows in enumerate(slots):
        dy_in[index].wait()
        du_in[index].wait()
        dy_buf[rows, :] += rms_back(x_buf[rows, :], du_buf[rows, :])
        dx2_store[index].start()
    for index in range(len(chunks)):
        dx_in[index].wait()
        dx_store[index].start()
    for copy in x_store + dx2_store + x1_store + dx_store + [up_store, qkv_store, out_store, down_store]:
        copy.wait()


def finish_call(y_one, o_pos, wo_full, x_two, dx_one, dy_two, du_pos, part_own, near_recv, d_att):
    tokens, hidden = y_one.shape
    ffn = part_own.shape[0] // 2
    dim = d_att.shape[0] // 4
    any_spec = pl.BlockSpec(memory_space=pl.ANY)
    dma, vmem = pltpu.SemaphoreType.DMA, pltpu.VMEM
    state = (tokens, hidden)
    out_shape = [jax.ShapeDtypeStruct(shape, F32) for shape in (state, state, state, state, (hidden, ffn), (ffn, hidden), (3 * hidden, 1, dim), (dim, hidden))]
    scratch = [
        vmem(state, F32), vmem(state, BF16), vmem((hidden, hidden), BF16), vmem(state, F32), vmem(state, F32), vmem(state, F32), vmem(state, F32),
        vmem(part_own.shape, F32), vmem(part_own.shape, F32), vmem(d_att.shape, F32), vmem((hidden, ffn), F32), vmem((3 * hidden, 1, dim), F32),
        dma((10, 7)), dma((8, 7)),
    ]
    return pl.pallas_call(
        finish_kernel,
        out_shape=out_shape,
        in_specs=[any_spec] * 10,
        out_specs=[any_spec] * 8,
        scratch_shapes=scratch,
        compiler_params=pltpu.CompilerParams(vmem_limit_bytes=VMEM_LIMIT),
        cost_estimate=pl.CostEstimate(flops=2 * 10**9, bytes_accessed=52 * 2**20, transcendentals=0),
        name="finish",
    )(y_one, o_pos, wo_full, x_two, dx_one, dy_two, du_pos, part_own, near_recv, d_att)


def last_kernel(x_two, dy_two, du_far, dx_two_in, dx_two_out, x_buf, dy_buf, du_buf, load_sem, store_sem):
    ring = Ring()
    slab = x_buf.shape[1]
    loads, stores, sizes = [], [], (slab, LATE_ROWS)
    for index, (slot, skip) in enumerate(((SAME_O, 0), (SAME_F, slab - LATE_ROWS))):
        size = sizes[index]
        rows = pl.ds(pl.multiple_of(ring.at(slot) * slab + skip, 16), size)
        sources = ((x_two.at[rows], x_buf), (dy_two.at[rows], dy_buf), (du_far.at[pl.ds(index * slab, size)], du_buf))
        loads.append([pltpu.make_async_copy(src, dst.at[index, pl.ds(0, size)], load_sem.at[index, which]) for which, (src, dst) in enumerate(sources)])
        stores.append(pltpu.make_async_copy(dy_buf.at[index, pl.ds(0, size)], dx_two_out.at[rows], store_sem.at[index]))
    for copies in loads:
        for copy in copies:
            copy.start()
    for index, copies in enumerate(loads):
        for copy in copies:
            copy.wait()
        rows = pl.ds(0, sizes[index])
        dy_buf[index, rows, :] += rms_back(x_buf[index, rows, :], du_buf[index, rows, :])
        stores[index].start()
    for copy in stores:
        copy.wait()


def last_call(x_two, dy_two, du_far, dx_two):
    tokens, hidden = x_two.shape
    any_spec = pl.BlockSpec(memory_space=pl.ANY)
    buf = pltpu.VMEM((2, tokens // 8, hidden), F32)
    return pl.pallas_call(
        last_kernel,
        out_shape=jax.ShapeDtypeStruct(dx_two.shape, F32),
        in_specs=[any_spec] * 4,
        out_specs=any_spec,
        input_output_aliases={3: 0},
        scratch_shapes=[buf, buf, buf, pltpu.SemaphoreType.DMA((2, 3)), pltpu.SemaphoreType.DMA((2,))],
        cost_estimate=pl.CostEstimate(flops=10**6, bytes_accessed=4 * 2**20, transcendentals=0),
        name="last",
    )(x_two, dy_two, du_far, dx_two)


def local_backward(y_one, y_two, dy_one, dy_two, w_qkv, w_out, w_up, w_down):
    hidden = y_one.shape[2]
    _, _, _, parts, dim = w_qkv.shape
    qkv_parts = jnp.swapaxes(w_qkv[0, :, 0], 0, 1)
    results = block_call(y_one, y_two, dy_one, dy_two, w_up[0], w_down[0], qkv_parts, w_out[0, 0])
    x_two, dx_one, part_own, near_recv, d_att, o_pos, du_pos, wo_full = (tensor.reshape(-1, hidden) for tensor in results[:8])
    devices = range(lax.axis_size("tp"))
    to_f = [(device, (3 - device // 2) * 2 + device % 2) for device in devices]
    du_far = lax.ppermute(results[8], "tp", to_f)
    y_flat, dy_flat = y_one.reshape(-1, hidden), dy_two.reshape(-1, hidden)
    *states, dw_up, dw_down, dw_qkv, dw_out = finish_call(y_flat, o_pos, wo_full, x_two, dx_one, dy_flat, du_pos, part_own, near_recv, d_att)
    states[3] = last_call(x_two, dy_flat, du_far, states[3])
    states = [tensor.reshape(y_one.shape) for tensor in states]
    return (*states, dw_qkv.reshape(1, hidden, 1, parts, dim), dw_out[None, None], dw_up[None], dw_down[None])


def solution(mesh):
    state_spec = P("dp", "tp", None)
    in_specs = (state_spec, state_spec, state_spec, state_spec, P(None, None, "tp", None, None), P(None, "tp", None, None), P(None, None, "tp"), P(None, "tp", None))
    out_specs = (state_spec, state_spec, state_spec, state_spec, P("dp", None, "tp", None, None), P("dp", "tp", None, None), P("dp", None, "tp"), P("dp", "tp", None))
    return jax.shard_map(local_backward, mesh=mesh, in_specs=in_specs, out_specs=out_specs, check_vma=False)
```

```python
import functools

import jax
import jax.numpy as jnp
from jax import lax
from jax.experimental import pallas as pl
from jax.experimental.pallas import tpu as pltpu
from jax.sharding import PartitionSpec as P

RMS_EPS = 1e-6
LOG2_E = 1.4426950408889634
LATE_ROWS = 96
MESH = pl.DeviceIdType.MESH
BF16, F32 = jnp.bfloat16, jnp.float32
VMEM_LIMIT = 64 * 1024 * 1024 - 65536


def inv_rms(tensor):
    return lax.rsqrt(jnp.mean(tensor * tensor, axis=-1, keepdims=True) + RMS_EPS)


def rms_norm(tensor):
    return tensor * inv_rms(tensor)


def rms_back(tensor, grad_in):
    scale = inv_rms(tensor)
    return scale * grad_in - tensor * (scale * scale * scale) * jnp.mean(grad_in * tensor, axis=-1, keepdims=True)


def gelu_and_slope(tensor):
    root = (2.0 / jnp.pi) ** 0.5
    squared = tensor * tensor
    tanh = jnp.tanh(root * (tensor + 0.044715 * (tensor * squared)))
    cdf = 0.5 * (1.0 + tanh)
    slope = cdf + (0.5 * root) * tensor * ((1.0 - tanh * tanh) * (1.0 + (3 * 0.044715) * squared))
    return tensor * cdf, slope


def dot_nn(left, right):
    return lax.dot_general(left, right, (((1,), (0,)), ((), ())), preferred_element_type=F32)


def dot_nt(left, right):
    return lax.dot_general(left, right, (((1,), (1,)), ((), ())), preferred_element_type=F32)


def dot_tn(left, right):
    return lax.dot_general(left, right, (((0,), (0,)), ((), ())), preferred_element_type=F32)


class Ring:
    def __init__(self):
        me = lax.axis_index("tp")
        chip, core = me // 2, me % 2
        self.me, self.chip, self.core = me, chip, core
        self.chips = (chip, chip + 1 - 2 * (chip % 2), 3 - chip, (chip + 2) % 4)

    def at(self, slot):
        core = self.core if slot % 2 == 0 else 1 - self.core
        return self.chips[slot // 2] * 2 + core

    def at_traced(self, slot):
        relation, other = slot // 2, slot % 2
        own, near_t, near_f, opposite = self.chips
        chip = jnp.where(relation == 0, own, jnp.where(relation == 1, near_t, jnp.where(relation == 2, near_f, opposite)))
        return chip * 2 + (self.core + other) % 2

    def arrive(self):
        for slot in (1, 2, 3, 4, 5):
            pl.semaphore_signal(pltpu.get_barrier_semaphore(), inc=1, device_id={"tp": self.at(slot)}, device_id_type=MESH)

    def meet(self):
        pl.semaphore_wait(pltpu.get_barrier_semaphore(), 5)

    def copy(self, src, dst, send_sem, recv_sem, slot):
        return pltpu.make_async_remote_copy(src_ref=src, dst_ref=dst, send_sem=send_sem, recv_sem=recv_sem, device_id={"tp": self.at(slot)}, device_id_type=MESH)


PARTNER, SAME_T, OTHER_T, SAME_F, OTHER_F, SAME_O, OTHER_O = 1, 2, 3, 4, 5, 6, 7


def block_kernel(
    scale,
    y_one, y_two, dy_one, dy_two, w_up, w_down, w_qkv, w_out,
    x_two, dx_one, part_own, near_recv, d_att, o_pos, du_pos, wo_full, to_f,
    uc_seq, uc_two, att_full, o_relay, du_relay,
    u_all, c_all, up_all, down_all, acc, spare, part_keep, uc_own,
    load_sem, y_sem, x_sem, w_send, w_recv, uc_send, uc_recv, att_send, att_recv, a2a_send, a2a_recv, relay_recv, near_sem, two_sem,
    seq_sem, head_sem, wo_sem, core_send, core_recv, f_sem, far_sem, o_send, o_recv, du_send, du_recv, o_relay_recv, du_relay_recv, free_slot,
):
    ring = Ring()
    slabs, slab, hidden = acc.shape[1:]
    seq_len = slabs * slab
    half = seq_len // 2
    dim = w_out.shape[0]
    fours = slabs // 2

    def start(copies):
        for copy in copies:
            copy.start()

    def say_free(index, to):
        pl.semaphore_signal(free_slot.at[index], inc=1, device_id={"tp": ring.at(to)}, device_id_type=MESH)

    rooms = (0, 1, 2, 3, 4, 5, 1, 3)

    def room(slot):
        return pl.ds(rooms[slot] * half, half)

    def weight_pair(src_slot, dst_slot, to, index):
        return [
            ring.copy(buf.at[room(src_slot)], buf.at[room(dst_slot)], w_send.at[index + which], w_recv.at[dst_slot, which], to)
            for which, buf in enumerate((up_all, down_all))
        ]

    w_own = weight_pair(0, 1, PARTNER, 0) + weight_pair(0, 2, SAME_T, 2) + weight_pair(0, 4, SAME_F, 4)
    w_near_t = weight_pair(2, 6, SAME_F, 6)
    w_near_t_core = weight_pair(2, 3, PARTNER, 8)
    w_near_f = weight_pair(4, 5, PARTNER, 10)
    w_far = weight_pair(6, 7, PARTNER, 12)

    def uc_pair(src_slot, dst_slot, to, index):
        return [ring.copy(buf.at[src_slot], buf.at[dst_slot], uc_send.at[index + which], uc_recv.at[dst_slot, which], to) for which, buf in enumerate((u_all, c_all))]

    u_to_t, c_to_t = uc_pair(0, 2, SAME_T, 0)
    uc_core = uc_pair(0, 1, PARTNER, 2)
    uc_pass = uc_pair(2, 3, PARTNER, 4)

    def att(src, dst_slot, to, index):
        return ring.copy(src, att_full.at[dst_slot], att_send.at[index], att_recv.at[dst_slot], to)

    att_keep = [pltpu.make_async_copy(uc_own.at[part, 0], att_full.at[0, pl.ds(part * dim, dim)], x_sem.at[part // 2, part % 2]) for part in range(4)]
    att_out = [att(att_full.at[0], 4, SAME_F, 0), att(att_full.at[0], 1, PARTNER, 1)]
    att_t, att_o = att(att_full.at[0], 2, SAME_T, 2), att(att_full.at[4], 6, SAME_T, 3)
    att_f_core, att_t_core, att_o_core = att(att_full.at[4], 5, PARTNER, 4), att(att_full.at[2], 3, PARTNER, 5), att(att_full.at[6], 7, PARTNER, 6)

    a2a_out = {slot: ring.copy(uc_own.at[slot], uc_seq.at[slot], a2a_send.at[slot], a2a_recv.at[slot], slot) for slot in (1, 2, 3, 4, 5)}
    a2a_out[SAME_O] = ring.copy(uc_own.at[SAME_O], uc_two.at[2], a2a_send.at[SAME_O], relay_recv.at[0], SAME_F)
    a2a_out[OTHER_O] = ring.copy(uc_own.at[OTHER_O], uc_two.at[3], a2a_send.at[OTHER_O], relay_recv.at[1], OTHER_F)
    a2a_pass = [ring.copy(uc_two.at[2 + index], uc_seq.at[SAME_O + index], a2a_send.at[8 + index], a2a_recv.at[SAME_O + index], SAME_T) for index in (0, 1)]
    uc_keep = pltpu.make_async_copy(uc_own.at[0], uc_seq.at[0], load_sem.at[4])
    two_out = ring.copy(uc_own.at[OTHER_T], uc_two.at[1], a2a_send.at[10], relay_recv.at[2], PARTNER)
    two_keep = pltpu.make_async_copy(uc_own.at[SAME_T], uc_two.at[0], two_sem.at[0])
    near = ring.copy(acc.at[0], near_recv, near_sem.at[0], near_sem.at[1], SAME_F)

    loads = [
        pltpu.make_async_copy(w_down, down_all.at[room(0)], load_sem.at[0]),
        pltpu.make_async_copy(w_up, uc_own.at[:, 0, :, pl.ds(0, half)], load_sem.at[1]),
        pltpu.make_async_copy(y_one, acc.at[0], load_sem.at[2]),
        pltpu.make_async_copy(dy_two, acc.at[1], load_sem.at[3]),
    ]
    qkv_loads = [pltpu.make_async_copy(w_qkv.at[part], uc_own.at[:, 1, :, pl.ds(part * dim, dim)], y_sem.at[0, part]) for part in range(3)]
    ring.arrive()
    start(loads)
    start(qkv_loads)
    ring.meet()
    loads[0].wait()
    start(w_own[1::2])
    loads[1].wait()
    for part in range(half // dim):
        up_all[pl.ds(part * dim, dim), :] = uc_own[:, 0, :, pl.ds(part * dim, dim)].reshape(hidden, dim).T
    start(w_own[0::2])
    out_load = pltpu.make_async_copy(w_out, uc_own.at[3, 0], load_sem.at[7])
    out_load.start()
    loads[2].wait()
    loads[3].wait()

    def normalize(step, carry):
        rows = pl.ds(pl.multiple_of(step * slab, slab), slab)
        u_all[0, rows, :] = rms_norm(acc[0, step]).astype(BF16)
        c_all[0, rows, :] = acc[1, step].astype(BF16)
        acc[0, step] = jnp.zeros((slab, hidden), F32)
        acc[1, step] = jnp.zeros((slab, hidden), F32)
        return carry

    lax.fori_loop(0, slabs, normalize, 0)
    u_to_t.start()
    start(uc_core)
    for part in range(3):
        qkv_loads[part].wait()
        uc_own[part, 0] = uc_own[:, 1, :, pl.ds(part * dim, dim)].reshape(hidden, dim).T
    out_load.wait()
    start(att_keep)

    def y_loads(step, buf):
        seq = ring.at_traced(7 - step)
        return [pltpu.make_async_copy(src.at[seq], spare.at[buf, which], y_sem.at[buf, which]) for which, src in enumerate((y_one, y_two, dy_one))]

    def x_stores(step, buf):
        seq = ring.at_traced(7 - step)
        return [pltpu.make_async_copy(spare.at[buf, 3 + which], dst.at[seq], x_sem.at[buf, which]) for which, dst in enumerate((x_two, dx_one))]

    def feed_forward(step, carry):
        slot = jnp.where(step == 3, 4, jnp.where(step == 4, 3, step))
        place = pl.ds(pl.multiple_of(jnp.where(step == 6, 1, jnp.where(step == 7, 3, slot)) * half, half), half)

        @pl.when((step == 1) | ((step >= 3) & (step != 6)))
        def _():
            for which, buf in enumerate((up_all, down_all)):
                ring.copy(buf.at[place], buf.at[place], w_send.at[0], w_recv.at[slot, which], PARTNER).wait_recv()

        @pl.when(step == 6)
        def _():
            for copy in w_near_t:
                copy.wait_recv()

        @pl.when(step == 2)
        def _():
            pl.semaphore_wait(free_slot.at[0], 1)
            for which, buf in ((1, down_all), (0, up_all)):
                ring.copy(buf.at[room(2)], buf.at[room(2)], w_send.at[0], w_recv.at[2, which], PARTNER).wait_recv()
                w_near_t[which].start()
                w_near_t_core[which].start()
            for copy in att_keep:
                copy.wait()
            start(att_out)

        @pl.when(step == 3)
        def _():
            c_to_t.start()
            start(w_near_f)

        @pl.when(step == 6)
        def _():
            pl.semaphore_wait(free_slot.at[1], 1)
            start(w_far)

        @pl.when(step == 7)
        def _():
            start(y_loads(0, 0))

        def rows_step(part, carry):
            rows = pl.ds(pl.multiple_of(part * half, half), half)
            quarter = pl.ds(part * fours, fours)
            hidden_act, slope = gelu_and_slope(dot_nt(u_all[0, rows, :], up_all[place, :]))
            d_pre = (slope * dot_nt(c_all[0, rows, :], down_all[place, :])).astype(BF16)
            acc[0, quarter] += dot_nn(hidden_act.astype(BF16), down_all[place, :]).reshape(fours, slab, hidden)
            acc[1, quarter] += dot_nn(d_pre, up_all[place, :]).reshape(fours, slab, hidden)
            return carry

        lax.fori_loop(0, 2, rows_step, 0)

        @pl.when(step == 1)
        def _():
            say_free(0, SAME_F)

        @pl.when(step == 4)
        def _():
            say_free(1, PARTNER)

        return carry

    lax.fori_loop(0, 8, feed_forward, 0)

    def finish(step, carry):
        slot = 7 - step
        buf = step % 2
        seq = ring.at_traced(slot)
        for copy in y_loads(step, buf):
            copy.wait()

        @pl.when(step < 7)
        def _():
            start(y_loads(step + 1, 1 - buf))

        @pl.when(step >= 2)
        def _():
            for copy in x_stores(step - 2, buf):
                copy.wait()

        y_first = spare[buf, 0]
        x_second = spare[buf, 1] - acc[0, seq]
        dy_first = spare[buf, 2] + rms_back(y_first, acc[1, seq])
        spare[buf, 3] = x_second
        spare[buf, 4] = dy_first
        uc_own[slot, 0] = rms_norm(x_second).astype(BF16)
        uc_own[slot, 1] = dy_first.astype(BF16)
        acc[0, seq] = jnp.zeros((slab, hidden), F32)
        acc[1, seq] = jnp.zeros((slab, hidden), F32)
        start(x_stores(step, buf))
        return carry

    lax.fori_loop(0, 8, finish, 0)
    for slot in (7, 6, 5, 4, 3, 2, 1):
        a2a_out[slot].start()
    uc_keep.start()
    two_out.start()
    two_keep.start()
    for step in (6, 7):
        for copy in x_stores(step, step % 2):
            copy.wait()

    def gradients(step, carry):
        first = step // 8
        tokens = (step % 8) // 2
        place = pl.ds(pl.multiple_of((4 - 4 * first) * half, half), half)

        @pl.when(step == 0)
        def _():
            u_to_t.wait_recv()
            uc_pass[0].start()

        @pl.when((step == 2) | (step == 6))
        def _():
            for which, buf in enumerate((u_all, c_all)):
                ring.copy(buf.at[tokens], buf.at[tokens], uc_send.at[0], uc_recv.at[tokens, which], PARTNER).wait_recv()

        @pl.when(step == 4)
        def _():
            c_to_t.wait_recv()
            uc_pass[1].start()
            for index in (0, 1):
                a2a_out[SAME_O + index].wait_recv()
            start(a2a_pass)

        @pl.when(step == 8)
        def _():
            near.start()
            att_out[0].wait_recv()
            att_f_core.start()
            att_t.start()
            att_o.start()

        rows = pl.ds(pl.multiple_of((step % 2) * half, half), half)
        u_part, c_part = u_all[tokens, rows, :], c_all[tokens, rows, :]
        hidden_act, slope = gelu_and_slope(dot_nt(up_all[place, :], u_part))
        d_pre = (slope * dot_nt(down_all[place, :], c_part)).astype(BF16)
        acc[first, pl.ds(0, fours)] += dot_nn(d_pre, u_part).reshape(fours, slab, hidden)
        acc[first, pl.ds(fours, fours)] += dot_nn(hidden_act.astype(BF16), c_part).reshape(fours, slab, hidden)
        return carry

    lax.fori_loop(0, 16, gradients, 0)
    out_own = pltpu.make_async_copy(acc.at[1], part_own, load_sem.at[1])
    out_own.start()
    for copy in w_own + w_near_t + w_near_t_core + w_near_f + w_far + [u_to_t, c_to_t] + uc_core + uc_pass:
        copy.wait_send()
    say_free(2, SAME_T)

    def relation_of(step):
        base = step % 4
        return jnp.where(base == 0, 2, jnp.where(base == 3, 3, base - 1))

    def qkv_rows(buf):
        return pl.ds(pl.multiple_of(buf * 6 * dim, 2 * dim), 6 * dim)

    def wo_rows(buf):
        return pl.ds(pl.multiple_of(12 * dim + buf * 2 * dim, 2 * dim), 2 * dim)

    def head_loads(relation, buf):
        copies = []
        for index in (0, 1):
            head = att_full.at[relation * 2 + 1 - index]
            first, second = (pl.ds(pl.multiple_of(base + index * size, dim), size) for base, size in ((buf * 6 * dim, 3 * dim), (12 * dim + buf * 2 * dim, dim)))
            copies.append(pltpu.make_async_copy(head.at[pl.ds(0, 3 * dim)], up_all.at[first], head_sem.at[buf, index, 0]))
            copies.append(pltpu.make_async_copy(head.at[pl.ds(3 * dim, dim)], up_all.at[second], head_sem.at[buf, index, 1]))
        return copies

    def rows_of(slot):
        return pl.ds(slot * slab, slab)

    def seq_loads(seq, src, src_slot, slot):
        return [pltpu.make_async_copy(src.at[src_slot, which], u_all.at[2 * seq + which, rows_of(slot)], seq_sem.at[2 * seq + which, slot]) for which in (0, 1)]

    seq_own = [copy for slot in range(8) for copy in seq_loads(0, uc_seq, slot, slot)]
    seq_two = [copy for slot in range(4) for copy in seq_loads(1, uc_two, slot, slot)]
    uc_to_t = [
        ring.copy(u_all.at[which, rows_of(slot)], u_all.at[2 + which, rows_of(4 + index)], far_sem.at[0, 2 * index + which], far_sem.at[1, 2 * index + which], SAME_T)
        for which in (0, 1)
        for index, slot in enumerate((0, 1, 4, 5))
    ]
    core_copies = [ring.copy(spare.at[index, pl.ds(0, 4)], acc.at[0, pl.ds(0, 4)], core_send.at[index], core_recv.at[index], PARTNER) for index in (0, 1)]
    f_copy = ring.copy(part_keep.at[0], acc.at[0, pl.ds(4, 4)], f_sem.at[0], f_sem.at[1], SAME_F)

    o_src = c_all.at[0]
    o_out = [
        ring.copy(o_src.at[rows_of(SAME_O)], o_relay.at[0], o_send.at[6], o_relay_recv.at[0], SAME_T),
        ring.copy(o_src.at[rows_of(OTHER_O)], o_relay.at[1], o_send.at[7], o_relay_recv.at[1], SAME_F),
    ] + [ring.copy(o_src.at[rows_of(slot)], o_pos.at[ring.me], o_send.at[slot], o_recv.at[slot], slot) for slot in (5, 4, 3, 2, 1)]
    o_pass = [
        ring.copy(o_relay.at[0], o_pos.at[ring.at(SAME_T)], o_send.at[8], o_recv.at[SAME_O], SAME_F),
        ring.copy(o_relay.at[1], o_pos.at[ring.at(SAME_F)], o_send.at[9], o_recv.at[OTHER_O], OTHER_T),
    ]
    o_keep = pltpu.make_async_copy(o_src.at[rows_of(0)], o_pos.at[ring.me], o_send.at[0])

    late = slab - LATE_ROWS
    early = {slot: late if slot == SAME_F else slab for slot in range(1, 6)}
    du_out = [
        ring.copy(acc.at[1, SAME_O], to_f.at[pl.ds(0, slab)], du_send.at[6], du_relay_recv.at[0], SAME_T),
        ring.copy(acc.at[1, OTHER_O], du_relay, du_send.at[7], du_relay_recv.at[1], SAME_F),
    ] + [ring.copy(acc.at[1, slot, pl.ds(0, early[slot])], du_pos.at[ring.me, pl.ds(0, early[slot])], du_send.at[slot], du_recv.at[slot], slot) for slot in (5, 4, 3, 2, 1)]
    du_keep = pltpu.make_async_copy(acc.at[1, 0], du_pos.at[ring.me], du_send.at[0])
    du_late = pltpu.make_async_copy(acc.at[1, SAME_F, pl.ds(late, slab - late)], to_f.at[pl.ds(slab, slab - late)], du_send.at[8])
    du_pass = ring.copy(du_relay, du_pos.at[ring.at(SAME_F)], du_send.at[9], du_recv.at[OTHER_O], OTHER_T)

    att_f_core.wait_recv()
    att_out[1].wait_recv()
    start(head_loads(2, 0))
    start(head_loads(0, 1))

    def arrive(slots):
        for slot in slots:
            if slot:
                ring.copy(uc_own.at[slot], uc_seq.at[slot], a2a_send.at[0], a2a_recv.at[slot], PARTNER).wait_recv()
            start(seq_own[2 * slot : 2 * slot + 2])

    def project(first, count):
        rows = pl.ds(first, count)
        for buf in (0, 1):
            c_all[2 + buf, rows, pl.ds(0, 6 * dim)] = dot_nt(u_all[0, rows, :], up_all[qkv_rows(buf), :]).astype(BF16)
            c_all[2 + buf, rows, pl.ds(6 * dim, 2 * dim)] = dot_nt(u_all[1, rows, :], up_all[wo_rows(buf), :]).astype(BF16)

    uc_keep.wait()
    arrive((0, 1, 4, 5, 2, 3))
    two_out.wait_recv()
    two_keep.wait()
    start(seq_two)
    out_own.wait()
    acc[1] = jnp.zeros(acc.shape[1:], F32)
    for copy in seq_own[:12] + head_loads(2, 0) + head_loads(0, 1):
        copy.wait()
    pl.semaphore_wait(free_slot.at[2], 1)
    start(uc_to_t)
    project(0, 6 * slab)
    arrive((6, 7))
    for copy in seq_own[12:]:
        copy.wait()
    project(6 * slab, 2 * slab)

    def chip_step(step, carry):
        buf = step % 2
        seq = step // 4
        relation = relation_of(step)

        @pl.when(step == 4)
        def _():
            near.wait_send()
            say_free(3, SAME_F)
            say_free(4, PARTNER)
            for copy in seq_two:
                copy.wait()
            for copy in uc_to_t[:4]:
                copy.wait_recv()

        @pl.when(step >= 2)
        def _():
            for copy in head_loads(0, buf):
                copy.wait()

        @pl.when((step == 3) | (step == 4))
        def _():
            start(head_loads(relation_of(step + 1), 1 - buf))

        kept = pl.ds(pl.multiple_of(jnp.where(step < 2, step, 2) * seq_len, seq_len), seq_len)
        heads = [ring.at_traced(relation * 2 + other) for other in (1, 0)]
        wo_copies = [
            pltpu.make_async_copy(up_all.at[pl.ds(pl.multiple_of(12 * dim + (2 * buf + index) * dim, dim), dim)], wo_full.at[head], wo_sem.at[index])
            for index, head in enumerate(heads)
        ]
        start(wo_copies)

        @pl.when(step >= 2)
        def _():
            c_all[2 + buf, :, pl.ds(0, 6 * dim)] = dot_nt(u_all[2 * seq], up_all[qkv_rows(buf), :]).astype(BF16)

        for index, head in enumerate(heads):
            columns = pl.ds(pl.multiple_of(head * dim, dim), dim)
            own = pl.ds(index * 3 * dim, 3 * dim)
            query, key, value = (c_all[2 + buf, :, pl.ds((index * 3 + part) * dim, dim)] for part in range(3))
            scores = dot_nt(query, key) * (scale * LOG2_E)
            grown = jnp.exp2(scores - jnp.max(scores, axis=-1, keepdims=True))
            prob = grown * (1.0 / jnp.sum(grown, axis=-1, keepdims=True))
            prob_b = prob.astype(BF16)
            c_all[seq, :, columns] = dot_nn(prob_b, value).astype(BF16)
            if index == 0:
                @pl.when(step == 4)
                def _():
                    for copy in uc_to_t[4:]:
                        copy.wait_recv()

                @pl.when(step >= 2)
                def _():
                    c_all[2 + buf, :, pl.ds(6 * dim, 2 * dim)] = dot_nt(u_all[2 * seq + 1], up_all[wo_rows(buf), :]).astype(BF16)

            d_out = c_all[2 + buf, :, pl.ds((6 + index) * dim, dim)]
            d_prob = dot_nt(d_out, value)
            d_score = (prob * (d_prob - jnp.sum(d_prob * prob, axis=-1, keepdims=True)) * scale).astype(BF16)
            down_all[kept, pl.ds(index * 3 * dim, dim)] = dot_nn(d_score, key).astype(BF16)
            down_all[kept, pl.ds((index * 3 + 1) * dim, dim)] = dot_nn(query.T, d_score).T.astype(BF16)
            down_all[kept, pl.ds((index * 3 + 2) * dim, dim)] = dot_nn(d_out.T, prob_b).T.astype(BF16)
            @pl.when(step >= 4)
            def _():
                dst = (spare, part_keep)[index].at[buf]
                dst[pl.ds(0, 3)] += dot_tn(down_all[kept, own], u_all[2]).reshape(3, dim, hidden)
                dst[3] += dot_tn(c_all[1, :, columns], u_all[3])

            if index == 0:
                @pl.when(step == 1)
                def _():
                    att_t.wait_recv()
                    att_t_core.start()

                @pl.when(step == 4)
                def _():
                    pl.semaphore_wait(free_slot.at[4], 1)
                    core_copies[0].start()

                @pl.when(step == 5)
                def _():
                    pl.semaphore_wait(free_slot.at[4], 1)
                    core_copies[1].start()

        @pl.when(step == 1)
        def _():
            att_t_core.wait_recv()
            start(head_loads(1, 0))

        @pl.when(step == 2)
        def _():
            att_o.wait_recv()
            att_o_core.start()

        @pl.when(step < 4)
        def _():
            def du_tile(part, carry):
                rows = pl.ds(pl.multiple_of(jnp.where(step < 2, step, 2) * seq_len + part * half, half), half)
                acc[1, pl.ds(part * fours, fours)] += dot_nn(down_all[rows, pl.ds(0, 6 * dim)], up_all[qkv_rows(buf), :]).reshape(fours, slab, hidden)
                return carry

            lax.fori_loop(0, 2, du_tile, 0)

        @pl.when(step == 2)
        def _():
            att_o_core.wait_recv()
            start(head_loads(3, 1))

        @pl.when(step == 3)
        def _():
            start(o_out)
            start(du_out)
            du_late.start()
            o_keep.start()
            du_keep.start()

            def own_gradients(pair, carry):
                own_rows = pl.ds(pl.multiple_of(pair * seq_len, seq_len), seq_len)
                for index, other in enumerate((1, 0)):
                    columns = pl.ds(pl.multiple_of(ring.at_traced(relation_of(pair) * 2 + other) * dim, dim), dim)
                    dst = (spare, part_keep)[index].at[pair]
                    dst[pl.ds(0, 3)] = dot_tn(down_all[own_rows, pl.ds(index * 3 * dim, 3 * dim)], u_all[0]).reshape(3, dim, hidden)
                    dst[3] = dot_tn(c_all[0, :, columns], u_all[1])
                return carry

            lax.fori_loop(0, 2, own_gradients, 0)

        @pl.when(step == 4)
        def _():
            core_copies[0].wait_recv()
            part_keep[0] += acc[0, pl.ds(0, 4)]
            say_free(4, PARTNER)
            pl.semaphore_wait(free_slot.at[3], 1)
            f_copy.start()

        for copy in wo_copies:
            copy.wait()
        return carry

    lax.fori_loop(0, 6, chip_step, 0)
    for copy in o_out[:2]:
        copy.wait_recv()
    start(o_pass)
    du_out[1].wait_recv()
    du_pass.start()
    core_copies[1].wait_recv()
    part_keep[1] += acc[0, pl.ds(0, 4)]
    for copy in du_out[2:]:
        copy.wait_recv()
    for slot in range(1, 8):
        ring.copy(o_pos.at[0], o_pos.at[ring.at(slot)], near_sem.at[0], o_recv.at[slot], PARTNER).wait_recv()
    du_out[0].wait_recv()
    du_pass.wait_recv()
    near.wait_recv()
    f_copy.wait_recv()
    part_keep[1] += acc[0, pl.ds(4, 4)]
    d_att_copy = pltpu.make_async_copy(part_keep.at[1], d_att, load_sem.at[0])
    d_att_copy.start()

    sends = att_out + [att_t, att_o, att_f_core, att_t_core, att_o_core] + list(a2a_out.values()) + a2a_pass + [two_out]
    for copy in sends + o_out + du_out + o_pass + uc_to_t + core_copies + [du_pass, f_copy]:
        copy.wait_send()
    du_late.wait()
    o_keep.wait()
    du_keep.wait()
    d_att_copy.wait()


def block_call(y_one, y_two, dy_one, dy_two, w_up, w_down, w_qkv, w_out):
    slabs, slab, hidden = y_one.shape
    tokens = slabs * slab
    ffn = w_down.shape[0]
    dim = w_out.shape[0]
    any_spec = pl.BlockSpec(memory_space=pl.ANY)
    dma, vmem, wide, narrow = pltpu.SemaphoreType.DMA, pltpu.VMEM, F32, BF16
    results = [
        ((slabs, slab, hidden), wide), ((slabs, slab, hidden), wide), ((slabs, slab, hidden), wide), ((slabs, slab, hidden), wide),
        ((4, dim, hidden), wide), ((slabs, slab, hidden), narrow), ((slabs, slab, hidden), wide), ((8, dim, hidden), narrow),
        ((slab + LATE_ROWS, hidden), wide),
    ]
    landing = [
        ((8, 2, slab, hidden), narrow), ((4, 2, slab, hidden), narrow), ((8, 4 * dim, hidden), narrow), ((2, slab, hidden), narrow), ((slab, hidden), wide),
    ]
    scratch = [
        vmem((4, tokens, hidden), BF16), vmem((4, tokens, hidden), BF16), vmem((6 * ffn, hidden), BF16), vmem((6 * ffn, hidden), BF16),
        vmem((2, slabs, slab, hidden), F32), vmem((2, 5, slab, hidden), F32), vmem((2, 4, dim, hidden), F32),
        vmem((8, 2, slab, hidden), BF16),
        dma((8,)), dma((2, 3)), dma((2, 2)), dma((14,)), dma((8, 2)), dma((6,)), dma((4, 2)), dma((7,)), dma((8,)), dma((11,)), dma((8,)), dma((3,)), dma((2,)), dma((2,)),
        dma((4, 8)), dma((2, 2, 2)), dma((2,)), dma((2,)), dma((2,)), dma((2,)), dma((2, 8)), dma((10,)), dma((8,)), dma((10,)), dma((8,)), dma((2,)), dma((2,)),
        pltpu.SemaphoreType.REGULAR((5,)),
    ]
    return pl.pallas_call(
        functools.partial(block_kernel, dim ** -0.5),
        out_shape=[jax.ShapeDtypeStruct(shape, dtype) for shape, dtype in results + landing],
        in_specs=[any_spec] * 8,
        out_specs=[any_spec] * (len(results) + len(landing)),
        scratch_shapes=scratch,
        compiler_params=pltpu.CompilerParams(collective_id=0, has_side_effects=True, vmem_limit_bytes=VMEM_LIMIT),
        cost_estimate=pl.CostEstimate(flops=120 * 10**9, bytes_accessed=128 * 2**20, transcendentals=0),
        name="block",
    )(y_one, y_two, dy_one, dy_two, w_up.reshape(8, hidden // 8, ffn), w_down, w_qkv.reshape(3, 8, hidden // 8, dim), w_out)[: len(results)]


def finish_kernel(
    y_one, o_pos, wo_full, x_two, dx_one, dy_two, du_pos, part_own, near_recv, d_att,
    x_one_out, x_two_out, dx_one_out, dx_two_out, dw_up, dw_down, dw_qkv, dw_out,
    y_buf, o_buf, wo_buf, x_buf, dx_buf, dy_buf, du_buf, own_buf, near_buf, att_buf, up_out, qkv_out, load_sem, store_sem,
):
    tokens = y_buf.shape[0]
    dim = wo_buf.shape[0] // 8
    chunk = 256
    chunks = [pl.ds(index * chunk, chunk) for index in range(tokens // chunk)]

    def pieces(src, dst, sem, row):
        return [pltpu.make_async_copy(src.at[rows], dst.at[rows], sem.at[row, index]) for index, rows in enumerate(chunks)]

    def whole(src, dst, sem, row):
        return pltpu.make_async_copy(src, dst, sem.at[row, 0])

    ring = Ring()
    slab = tokens // 8
    sizes = {0: slab, PARTNER: slab, SAME_T: slab, OTHER_T: slab, SAME_F: slab - LATE_ROWS, OTHER_F: slab, OTHER_O: slab}
    slots = [pl.ds(pl.multiple_of(ring.at(slot) * slab, slab), size) for slot, size in sizes.items()]

    def slabs(src, dst, sem, row):
        return [pltpu.make_async_copy(src.at[rows], dst.at[rows], sem.at[row, index]) for index, rows in enumerate(slots)]

    x_in, dy_in, du_in = pieces(x_two, x_buf, load_sem, 0), slabs(dy_two, dy_buf, load_sem, 1), slabs(du_pos, du_buf, load_sem, 2)
    y_in, o_in = pieces(y_one, y_buf, load_sem, 3), pieces(o_pos, o_buf, load_sem, 4)
    wo_in, dx_in = whole(wo_full, wo_buf, load_sem, 5), pieces(dx_one, dx_buf, load_sem, 6)
    own_in, near_in, att_in = whole(part_own, own_buf, load_sem, 7), whole(near_recv, near_buf, load_sem, 8), whole(d_att, att_buf, load_sem, 9)
    order = [own_in, near_in, att_in, wo_in, *(copy for group in zip(y_in, o_in) for copy in group), *x_in, *(copy for group in zip(dy_in, du_in) for copy in group), *dx_in]
    for copy in order:
        copy.start()

    x_store, dx2_store, x1_store = pieces(x_buf, x_two_out, store_sem, 0), slabs(dy_buf, dx_two_out, store_sem, 1), pieces(y_buf, x_one_out, store_sem, 2)
    dx_store = pieces(dx_buf, dx_one_out, store_sem, 3)
    own_in.wait()
    near_in.wait()
    ffn = up_out.shape[1]
    own_buf[pl.ds(ffn, ffn), :] += near_buf[pl.ds(ffn, ffn), :]
    down_store = whole(own_buf.at[pl.ds(ffn, ffn)], dw_down, store_sem, 7)
    down_store.start()
    for part in range(up_out.shape[0] // ffn):
        columns = pl.ds(part * ffn, ffn)
        up_out[columns, :] = (own_buf[pl.ds(0, ffn), columns] + near_buf[pl.ds(0, ffn), columns]).T
    up_store = whole(up_out, dw_up, store_sem, 4)
    up_store.start()
    att_in.wait()
    for part in range(3):
        qkv_out[pl.ds(part, tokens, stride=3), 0, :] = att_buf[pl.ds(part * dim, dim), :].T
    qkv_store = whole(qkv_out, dw_qkv, store_sem, 5)
    qkv_store.start()
    out_store = whole(att_buf.at[pl.ds(3 * dim, dim)], dw_out, store_sem, 6)
    out_store.start()
    wo_in.wait()
    for index, rows in enumerate(chunks):
        y_in[index].wait()
        o_in[index].wait()
        y_buf[rows, :] -= dot_nn(o_buf[rows, :], wo_buf[...])
        x1_store[index].start()
    for index in range(len(chunks)):
        x_in[index].wait()
        x_store[index].start()
    for index, rows in enumerate(slots):
        dy_in[index].wait()
        du_in[index].wait()
        dy_buf[rows, :] += rms_back(x_buf[rows, :], du_buf[rows, :])
        dx2_store[index].start()
    for index in range(len(chunks)):
        dx_in[index].wait()
        dx_store[index].start()
    for copy in x_store + dx2_store + x1_store + dx_store + [up_store, qkv_store, out_store, down_store]:
        copy.wait()


def finish_call(y_one, o_pos, wo_full, x_two, dx_one, dy_two, du_pos, part_own, near_recv, d_att):
    tokens, hidden = y_one.shape
    ffn = part_own.shape[0] // 2
    dim = d_att.shape[0] // 4
    any_spec = pl.BlockSpec(memory_space=pl.ANY)
    dma, vmem = pltpu.SemaphoreType.DMA, pltpu.VMEM
    state = (tokens, hidden)
    out_shape = [jax.ShapeDtypeStruct(shape, F32) for shape in (state, state, state, state, (hidden, ffn), (ffn, hidden), (3 * hidden, 1, dim), (dim, hidden))]
    scratch = [
        vmem(state, F32), vmem(state, BF16), vmem((hidden, hidden), BF16), vmem(state, F32), vmem(state, F32), vmem(state, F32), vmem(state, F32),
        vmem(part_own.shape, F32), vmem(part_own.shape, F32), vmem(d_att.shape, F32), vmem((hidden, ffn), F32), vmem((3 * hidden, 1, dim), F32),
        dma((10, 7)), dma((8, 7)),
    ]
    return pl.pallas_call(
        finish_kernel,
        out_shape=out_shape,
        in_specs=[any_spec] * 10,
        out_specs=[any_spec] * 8,
        scratch_shapes=scratch,
        compiler_params=pltpu.CompilerParams(vmem_limit_bytes=VMEM_LIMIT),
        cost_estimate=pl.CostEstimate(flops=2 * 10**9, bytes_accessed=52 * 2**20, transcendentals=0),
        name="finish",
    )(y_one, o_pos, wo_full, x_two, dx_one, dy_two, du_pos, part_own, near_recv, d_att)


def last_kernel(x_two, dy_two, du_far, dx_two_in, dx_two_out, x_buf, dy_buf, du_buf, load_sem, store_sem):
    ring = Ring()
    slab = x_buf.shape[1]
    loads, stores, sizes = [], [], (slab, LATE_ROWS)
    for index, (slot, skip) in enumerate(((SAME_O, 0), (SAME_F, slab - LATE_ROWS))):
        size = sizes[index]
        rows = pl.ds(pl.multiple_of(ring.at(slot) * slab + skip, 16), size)
        sources = ((x_two.at[rows], x_buf), (dy_two.at[rows], dy_buf), (du_far.at[pl.ds(index * slab, size)], du_buf))
        loads.append([pltpu.make_async_copy(src, dst.at[index, pl.ds(0, size)], load_sem.at[index, which]) for which, (src, dst) in enumerate(sources)])
        stores.append(pltpu.make_async_copy(dy_buf.at[index, pl.ds(0, size)], dx_two_out.at[rows], store_sem.at[index]))
    for copies in loads:
        for copy in copies:
            copy.start()
    for index, copies in enumerate(loads):
        for copy in copies:
            copy.wait()
        rows = pl.ds(0, sizes[index])
        dy_buf[index, rows, :] += rms_back(x_buf[index, rows, :], du_buf[index, rows, :])
        stores[index].start()
    for copy in stores:
        copy.wait()


def last_call(x_two, dy_two, du_far, dx_two):
    tokens, hidden = x_two.shape
    any_spec = pl.BlockSpec(memory_space=pl.ANY)
    buf = pltpu.VMEM((2, tokens // 8, hidden), F32)
    return pl.pallas_call(
        last_kernel,
        out_shape=jax.ShapeDtypeStruct(dx_two.shape, F32),
        in_specs=[any_spec] * 4,
        out_specs=any_spec,
        input_output_aliases={3: 0},
        scratch_shapes=[buf, buf, buf, pltpu.SemaphoreType.DMA((2, 3)), pltpu.SemaphoreType.DMA((2,))],
        cost_estimate=pl.CostEstimate(flops=10**6, bytes_accessed=4 * 2**20, transcendentals=0),
        name="last",
    )(x_two, dy_two, du_far, dx_two)


def local_backward(y_one, y_two, dy_one, dy_two, w_qkv, w_out, w_up, w_down):
    hidden = y_one.shape[2]
    _, _, _, parts, dim = w_qkv.shape
    qkv_parts = jnp.swapaxes(w_qkv[0, :, 0], 0, 1)
    results = block_call(y_one, y_two, dy_one, dy_two, w_up[0], w_down[0], qkv_parts, w_out[0, 0])
    x_two, dx_one, part_own, near_recv, d_att, o_pos, du_pos, wo_full = (tensor.reshape(-1, hidden) for tensor in results[:8])
    devices = range(lax.axis_size("tp"))
    to_f = [(device, (3 - device // 2) * 2 + device % 2) for device in devices]
    du_far = lax.ppermute(results[8], "tp", to_f)
    y_flat, dy_flat = y_one.reshape(-1, hidden), dy_two.reshape(-1, hidden)
    *states, dw_up, dw_down, dw_qkv, dw_out = finish_call(y_flat, o_pos, wo_full, x_two, dx_one, dy_flat, du_pos, part_own, near_recv, d_att)
    states[3] = last_call(x_two, dy_flat, du_far, states[3])
    states = [tensor.reshape(y_one.shape) for tensor in states]
    return (*states, dw_qkv.reshape(1, hidden, 1, parts, dim), dw_out[None, None], dw_up[None], dw_down[None])


def solution(mesh):
    state_spec = P("dp", "tp", None)
    in_specs = (state_spec, state_spec, state_spec, state_spec, P(None, None, "tp", None, None), P(None, "tp", None, None), P(None, None, "tp"), P(None, "tp", None))
    out_specs = (state_spec, state_spec, state_spec, state_spec, P("dp", None, "tp", None, None), P("dp", "tp", None, None), P("dp", None, "tp"), P("dp", "tp", None))
    return jax.shard_map(local_backward, mesh=mesh, in_specs=in_specs, out_specs=out_specs, check_vma=False)
```

```python
import functools

import jax
import jax.numpy as jnp
from jax import lax
from jax.experimental import pallas as pl
from jax.experimental.pallas import tpu as pltpu
from jax.sharding import PartitionSpec as P

RMS_EPS = 1e-6
LOG2_E = 1.4426950408889634
LATE_ROWS = 96
MESH = pl.DeviceIdType.MESH
BF16, F32 = jnp.bfloat16, jnp.float32
VMEM_LIMIT = 64 * 1024 * 1024 - 65536


def inv_rms(tensor):
    return lax.rsqrt(jnp.mean(tensor * tensor, axis=-1, keepdims=True) + RMS_EPS)


def rms_norm(tensor):
    return tensor * inv_rms(tensor)


def rms_back(tensor, grad_in):
    scale = inv_rms(tensor)
    return scale * grad_in - tensor * (scale * scale * scale) * jnp.mean(grad_in * tensor, axis=-1, keepdims=True)


def gelu_and_slope(tensor):
    root = (2.0 / jnp.pi) ** 0.5
    squared = tensor * tensor
    tanh = jnp.tanh(root * (tensor + 0.044715 * (tensor * squared)))
    cdf = 0.5 * (1.0 + tanh)
    slope = cdf + (0.5 * root) * tensor * ((1.0 - tanh * tanh) * (1.0 + (3 * 0.044715) * squared))
    return tensor * cdf, slope


def dot_nn(left, right):
    return lax.dot_general(left, right, (((1,), (0,)), ((), ())), preferred_element_type=F32)


def dot_nt(left, right):
    return lax.dot_general(left, right, (((1,), (1,)), ((), ())), preferred_element_type=F32)


def dot_tn(left, right):
    return lax.dot_general(left, right, (((0,), (0,)), ((), ())), preferred_element_type=F32)


class Ring:
    def __init__(self):
        me = lax.axis_index("tp")
        chip, core = me // 2, me % 2
        self.me, self.chip, self.core = me, chip, core
        self.chips = (chip, chip + 1 - 2 * (chip % 2), 3 - chip, (chip + 2) % 4)

    def at(self, slot):
        core = self.core if slot % 2 == 0 else 1 - self.core
        return self.chips[slot // 2] * 2 + core

    def at_traced(self, slot):
        relation, other = slot // 2, slot % 2
        own, near_t, near_f, opposite = self.chips
        chip = jnp.where(relation == 0, own, jnp.where(relation == 1, near_t, jnp.where(relation == 2, near_f, opposite)))
        return chip * 2 + (self.core + other) % 2

    def arrive(self):
        for slot in (1, 2, 3, 4, 5):
            pl.semaphore_signal(pltpu.get_barrier_semaphore(), inc=1, device_id={"tp": self.at(slot)}, device_id_type=MESH)

    def meet(self):
        pl.semaphore_wait(pltpu.get_barrier_semaphore(), 5)

    def copy(self, src, dst, send_sem, recv_sem, slot):
        return pltpu.make_async_remote_copy(src_ref=src, dst_ref=dst, send_sem=send_sem, recv_sem=recv_sem, device_id={"tp": self.at(slot)}, device_id_type=MESH)


PARTNER, SAME_T, OTHER_T, SAME_F, OTHER_F, SAME_O, OTHER_O = 1, 2, 3, 4, 5, 6, 7


def block_kernel(
    scale,
    y_one, y_two, dy_one, dy_two, w_up, w_down, w_qkv, w_out,
    x_two, dx_one, part_own, near_recv, d_att, o_pos, du_pos, wo_full, to_f,
    uc_seq, uc_two, att_full, o_relay, du_relay,
    u_all, c_all, up_all, down_all, acc, spare, part_keep, uc_own,
    load_sem, y_sem, x_sem, w_send, w_recv, uc_send, uc_recv, att_send, att_recv, a2a_send, a2a_recv, relay_recv, near_sem, two_sem,
    seq_sem, head_sem, wo_sem, core_send, core_recv, f_sem, far_sem, o_send, o_recv, du_send, du_recv, o_relay_recv, du_relay_recv, free_slot,
):
    ring = Ring()
    slabs, slab, hidden = acc.shape[1:]
    seq_len = slabs * slab
    half = seq_len // 2
    dim = w_out.shape[0]
    fours = slabs // 2

    def start(copies):
        for copy in copies:
            copy.start()

    def say_free(index, to):
        pl.semaphore_signal(free_slot.at[index], inc=1, device_id={"tp": ring.at(to)}, device_id_type=MESH)

    rooms = (0, 1, 2, 3, 4, 5, 1, 3)

    def room(slot):
        return pl.ds(rooms[slot] * half, half)

    def weight_pair(src_slot, dst_slot, to, index):
        return [
            ring.copy(buf.at[room(src_slot)], buf.at[room(dst_slot)], w_send.at[index + which], w_recv.at[dst_slot, which], to)
            for which, buf in enumerate((up_all, down_all))
        ]

    w_own = weight_pair(0, 1, PARTNER, 0) + weight_pair(0, 2, SAME_T, 2) + weight_pair(0, 4, SAME_F, 4)
    w_near_t = weight_pair(2, 6, SAME_F, 6)
    w_near_t_core = weight_pair(2, 3, PARTNER, 8)
    w_near_f = weight_pair(4, 5, PARTNER, 10)
    w_far = weight_pair(6, 7, PARTNER, 12)

    def uc_pair(src_slot, dst_slot, to, index):
        return [ring.copy(buf.at[src_slot], buf.at[dst_slot], uc_send.at[index + which], uc_recv.at[dst_slot, which], to) for which, buf in enumerate((u_all, c_all))]

    u_to_t, c_to_t = uc_pair(0, 2, SAME_T, 0)
    uc_core = uc_pair(0, 1, PARTNER, 2)
    uc_pass = uc_pair(2, 3, PARTNER, 4)

    def att(src, dst_slot, to, index):
        return ring.copy(src, att_full.at[dst_slot], att_send.at[index], att_recv.at[dst_slot], to)

    att_keep = [pltpu.make_async_copy(uc_own.at[part, 0], att_full.at[0, pl.ds(part * dim, dim)], x_sem.at[part // 2, part % 2]) for part in range(4)]
    att_out = [att(att_full.at[0], 4, SAME_F, 0), att(att_full.at[0], 1, PARTNER, 1)]
    att_t, att_o = att(att_full.at[0], 2, SAME_T, 2), att(att_full.at[4], 6, SAME_T, 3)
    att_f_core, att_t_core, att_o_core = att(att_full.at[4], 5, PARTNER, 4), att(att_full.at[2], 3, PARTNER, 5), att(att_full.at[6], 7, PARTNER, 6)

    a2a_out = {slot: ring.copy(uc_own.at[slot], uc_seq.at[slot], a2a_send.at[slot], a2a_recv.at[slot], slot) for slot in (1, 2, 3, 4, 5)}
    a2a_out[SAME_O] = ring.copy(uc_own.at[SAME_O], uc_two.at[2], a2a_send.at[SAME_O], relay_recv.at[0], SAME_F)
    a2a_out[OTHER_O] = ring.copy(uc_own.at[OTHER_O], uc_two.at[3], a2a_send.at[OTHER_O], relay_recv.at[1], OTHER_F)
    a2a_pass = [ring.copy(uc_two.at[2 + index], uc_seq.at[SAME_O + index], a2a_send.at[8 + index], a2a_recv.at[SAME_O + index], SAME_T) for index in (0, 1)]
    uc_keep = pltpu.make_async_copy(uc_own.at[0], uc_seq.at[0], load_sem.at[4])
    two_out = ring.copy(uc_own.at[OTHER_T], uc_two.at[1], a2a_send.at[10], relay_recv.at[2], PARTNER)
    two_keep = pltpu.make_async_copy(uc_own.at[SAME_T], uc_two.at[0], two_sem.at[0])
    near = ring.copy(acc.at[0], near_recv, near_sem.at[0], near_sem.at[1], SAME_F)

    loads = [
        pltpu.make_async_copy(w_down, down_all.at[room(0)], load_sem.at[0]),
        pltpu.make_async_copy(w_up, uc_own.at[:, 0, :, pl.ds(0, half)], load_sem.at[1]),
        pltpu.make_async_copy(y_one, acc.at[0], load_sem.at[2]),
        pltpu.make_async_copy(dy_two, acc.at[1], load_sem.at[3]),
    ]
    qkv_loads = [pltpu.make_async_copy(w_qkv.at[part], uc_own.at[:, 1, :, pl.ds(part * dim, dim)], y_sem.at[0, part]) for part in range(3)]
    ring.arrive()
    start(loads)
    start(qkv_loads)
    ring.meet()
    loads[0].wait()
    start(w_own[1::2])
    loads[1].wait()
    for part in range(half // dim):
        up_all[pl.ds(part * dim, dim), :] = uc_own[:, 0, :, pl.ds(part * dim, dim)].reshape(hidden, dim).T
    start(w_own[0::2])
    out_load = pltpu.make_async_copy(w_out, uc_own.at[3, 0], load_sem.at[7])
    out_load.start()
    loads[2].wait()
    loads[3].wait()

    def normalize(step, carry):
        rows = pl.ds(pl.multiple_of(step * slab, slab), slab)
        u_all[0, rows, :] = rms_norm(acc[0, step]).astype(BF16)
        c_all[0, rows, :] = acc[1, step].astype(BF16)
        acc[0, step] = jnp.zeros((slab, hidden), F32)
        acc[1, step] = jnp.zeros((slab, hidden), F32)
        return carry

    lax.fori_loop(0, slabs, normalize, 0)
    u_to_t.start()
    start(uc_core)
    for part in range(3):
        qkv_loads[part].wait()
        uc_own[part, 0] = uc_own[:, 1, :, pl.ds(part * dim, dim)].reshape(hidden, dim).T
    out_load.wait()
    start(att_keep)

    def y_loads(step, buf):
        seq = ring.at_traced(7 - step)
        return [pltpu.make_async_copy(src.at[seq], spare.at[buf, which], y_sem.at[buf, which]) for which, src in enumerate((y_one, y_two, dy_one))]

    def x_stores(step, buf):
        seq = ring.at_traced(7 - step)
        return [pltpu.make_async_copy(spare.at[buf, 3 + which], dst.at[seq], x_sem.at[buf, which]) for which, dst in enumerate((x_two, dx_one))]

    def feed_forward(step, carry):
        slot = jnp.where(step == 3, 4, jnp.where(step == 4, 3, step))
        place = pl.ds(pl.multiple_of(jnp.where(step == 6, 1, jnp.where(step == 7, 3, slot)) * half, half), half)

        @pl.when((step == 1) | ((step >= 3) & (step != 6)))
        def _():
            for which, buf in enumerate((up_all, down_all)):
                ring.copy(buf.at[place], buf.at[place], w_send.at[0], w_recv.at[slot, which], PARTNER).wait_recv()

        @pl.when(step == 6)
        def _():
            for copy in w_near_t:
                copy.wait_recv()

        @pl.when(step == 2)
        def _():
            pl.semaphore_wait(free_slot.at[0], 1)
            for which, buf in ((1, down_all), (0, up_all)):
                ring.copy(buf.at[room(2)], buf.at[room(2)], w_send.at[0], w_recv.at[2, which], PARTNER).wait_recv()
                w_near_t[which].start()
                w_near_t_core[which].start()
            for copy in att_keep:
                copy.wait()
            start(att_out)

        @pl.when(step == 3)
        def _():
            c_to_t.start()
            start(w_near_f)

        @pl.when(step == 6)
        def _():
            pl.semaphore_wait(free_slot.at[1], 1)
            start(w_far)

        @pl.when(step == 7)
        def _():
            start(y_loads(0, 0))

        def rows_step(part, carry):
            rows = pl.ds(pl.multiple_of(part * half, half), half)
            quarter = pl.ds(part * fours, fours)
            hidden_act, slope = gelu_and_slope(dot_nt(u_all[0, rows, :], up_all[place, :]))
            d_pre = (slope * dot_nt(c_all[0, rows, :], down_all[place, :])).astype(BF16)
            acc[0, quarter] += dot_nn(hidden_act.astype(BF16), down_all[place, :]).reshape(fours, slab, hidden)
            acc[1, quarter] += dot_nn(d_pre, up_all[place, :]).reshape(fours, slab, hidden)
            return carry

        lax.fori_loop(0, 2, rows_step, 0)

        @pl.when(step == 1)
        def _():
            say_free(0, SAME_F)

        @pl.when(step == 4)
        def _():
            say_free(1, PARTNER)

        return carry

    lax.fori_loop(0, 8, feed_forward, 0)

    def finish(step, carry):
        slot = 7 - step
        buf = step % 2
        seq = ring.at_traced(slot)
        for copy in y_loads(step, buf):
            copy.wait()

        @pl.when(step < 7)
        def _():
            start(y_loads(step + 1, 1 - buf))

        @pl.when(step >= 2)
        def _():
            for copy in x_stores(step - 2, buf):
                copy.wait()

        y_first = spare[buf, 0]
        x_second = spare[buf, 1] - acc[0, seq]
        dy_first = spare[buf, 2] + rms_back(y_first, acc[1, seq])
        spare[buf, 3] = x_second
        spare[buf, 4] = dy_first
        uc_own[slot, 0] = rms_norm(x_second).astype(BF16)
        uc_own[slot, 1] = dy_first.astype(BF16)
        acc[0, seq] = jnp.zeros((slab, hidden), F32)
        acc[1, seq] = jnp.zeros((slab, hidden), F32)
        start(x_stores(step, buf))
        return carry

    lax.fori_loop(0, 8, finish, 0)
    for slot in (7, 6, 5, 4, 3, 2, 1):
        a2a_out[slot].start()
    uc_keep.start()
    two_out.start()
    two_keep.start()
    for step in (6, 7):
        for copy in x_stores(step, step % 2):
            copy.wait()

    def gradients(step, carry):
        first = step // 8
        tokens = (step % 8) // 2
        place = pl.ds(pl.multiple_of((4 - 4 * first) * half, half), half)

        @pl.when(step == 0)
        def _():
            u_to_t.wait_recv()
            uc_pass[0].start()

        @pl.when((step == 2) | (step == 6))
        def _():
            for which, buf in enumerate((u_all, c_all)):
                ring.copy(buf.at[tokens], buf.at[tokens], uc_send.at[0], uc_recv.at[tokens, which], PARTNER).wait_recv()

        @pl.when(step == 4)
        def _():
            c_to_t.wait_recv()
            uc_pass[1].start()
            for index in (0, 1):
                a2a_out[SAME_O + index].wait_recv()
            start(a2a_pass)

        @pl.when(step == 8)
        def _():
            near.start()
            att_out[0].wait_recv()
            att_f_core.start()
            att_t.start()
            att_o.start()

        rows = pl.ds(pl.multiple_of((step % 2) * half, half), half)
        u_part, c_part = u_all[tokens, rows, :], c_all[tokens, rows, :]
        hidden_act, slope = gelu_and_slope(dot_nt(up_all[place, :], u_part))
        d_pre = (slope * dot_nt(down_all[place, :], c_part)).astype(BF16)
        acc[first, pl.ds(0, fours)] += dot_nn(d_pre, u_part).reshape(fours, slab, hidden)
        acc[first, pl.ds(fours, fours)] += dot_nn(hidden_act.astype(BF16), c_part).reshape(fours, slab, hidden)
        return carry

    lax.fori_loop(0, 16, gradients, 0)
    out_own = pltpu.make_async_copy(acc.at[1], part_own, load_sem.at[1])
    out_own.start()
    for copy in w_own + w_near_t + w_near_t_core + w_near_f + w_far + [u_to_t, c_to_t] + uc_core + uc_pass:
        copy.wait_send()
    say_free(2, SAME_T)

    def relation_of(step):
        base = step % 4
        return jnp.where(base == 0, 2, jnp.where(base == 3, 3, base - 1))

    def qkv_rows(buf):
        return pl.ds(pl.multiple_of(buf * 6 * dim, 2 * dim), 6 * dim)

    def wo_rows(buf):
        return pl.ds(pl.multiple_of(12 * dim + buf * 2 * dim, 2 * dim), 2 * dim)

    def head_loads(relation, buf):
        copies = []
        for index in (0, 1):
            head = att_full.at[relation * 2 + 1 - index]
            first, second = (pl.ds(pl.multiple_of(base + index * size, dim), size) for base, size in ((buf * 6 * dim, 3 * dim), (12 * dim + buf * 2 * dim, dim)))
            copies.append(pltpu.make_async_copy(head.at[pl.ds(0, 3 * dim)], up_all.at[first], head_sem.at[buf, index, 0]))
            copies.append(pltpu.make_async_copy(head.at[pl.ds(3 * dim, dim)], up_all.at[second], head_sem.at[buf, index, 1]))
        return copies

    def rows_of(slot):
        return pl.ds(slot * slab, slab)

    def seq_loads(seq, src, src_slot, slot):
        return [pltpu.make_async_copy(src.at[src_slot, which], u_all.at[2 * seq + which, rows_of(slot)], seq_sem.at[2 * seq + which, slot]) for which in (0, 1)]

    seq_own = [copy for slot in range(8) for copy in seq_loads(0, uc_seq, slot, slot)]
    seq_two = [copy for slot in range(4) for copy in seq_loads(1, uc_two, slot, slot)]
    uc_to_t = [
        ring.copy(u_all.at[which, rows_of(slot)], u_all.at[2 + which, rows_of(4 + index)], far_sem.at[0, 2 * index + which], far_sem.at[1, 2 * index + which], SAME_T)
        for which in (0, 1)
        for index, slot in enumerate((0, 1, 4, 5))
    ]
    core_copies = [ring.copy(spare.at[index, pl.ds(0, 4)], acc.at[0, pl.ds(0, 4)], core_send.at[index], core_recv.at[index], PARTNER) for index in (0, 1)]
    f_copy = ring.copy(part_keep.at[0], acc.at[0, pl.ds(4, 4)], f_sem.at[0], f_sem.at[1], SAME_F)

    o_src = c_all.at[0]
    o_out = [
        ring.copy(o_src.at[rows_of(SAME_O)], o_relay.at[0], o_send.at[6], o_relay_recv.at[0], SAME_T),
        ring.copy(o_src.at[rows_of(OTHER_O)], o_relay.at[1], o_send.at[7], o_relay_recv.at[1], SAME_F),
    ] + [ring.copy(o_src.at[rows_of(slot)], o_pos.at[ring.me], o_send.at[slot], o_recv.at[slot], slot) for slot in (5, 4, 3, 2, 1)]
    o_pass = [
        ring.copy(o_relay.at[0], o_pos.at[ring.at(SAME_T)], o_send.at[8], o_recv.at[SAME_O], SAME_F),
        ring.copy(o_relay.at[1], o_pos.at[ring.at(SAME_F)], o_send.at[9], o_recv.at[OTHER_O], OTHER_T),
    ]
    o_keep = pltpu.make_async_copy(o_src.at[rows_of(0)], o_pos.at[ring.me], o_send.at[0])

    late = slab - LATE_ROWS
    early = {slot: late if slot == SAME_F else slab for slot in range(1, 6)}
    du_out = [
        ring.copy(acc.at[1, SAME_O], to_f.at[pl.ds(0, slab)], du_send.at[6], du_relay_recv.at[0], SAME_T),
        ring.copy(acc.at[1, OTHER_O], du_relay, du_send.at[7], du_relay_recv.at[1], SAME_F),
    ] + [ring.copy(acc.at[1, slot, pl.ds(0, early[slot])], du_pos.at[ring.me, pl.ds(0, early[slot])], du_send.at[slot], du_recv.at[slot], slot) for slot in (5, 4, 3, 2, 1)]
    du_keep = pltpu.make_async_copy(acc.at[1, 0], du_pos.at[ring.me], du_send.at[0])
    du_late = pltpu.make_async_copy(acc.at[1, SAME_F, pl.ds(late, slab - late)], to_f.at[pl.ds(slab, slab - late)], du_send.at[8])
    du_pass = ring.copy(du_relay, du_pos.at[ring.at(SAME_F)], du_send.at[9], du_recv.at[OTHER_O], OTHER_T)

    att_f_core.wait_recv()
    att_out[1].wait_recv()
    start(head_loads(2, 0))
    start(head_loads(0, 1))

    def arrive(slots):
        for slot in slots:
            if slot:
                ring.copy(uc_own.at[slot], uc_seq.at[slot], a2a_send.at[0], a2a_recv.at[slot], PARTNER).wait_recv()
            start(seq_own[2 * slot : 2 * slot + 2])

    def project(first, count):
        rows = pl.ds(first, count)
        for buf in (0, 1):
            c_all[2 + buf, rows, pl.ds(0, 6 * dim)] = dot_nt(u_all[0, rows, :], up_all[qkv_rows(buf), :]).astype(BF16)
            c_all[2 + buf, rows, pl.ds(6 * dim, 2 * dim)] = dot_nt(u_all[1, rows, :], up_all[wo_rows(buf), :]).astype(BF16)

    uc_keep.wait()
    arrive((0, 1, 4, 5, 2, 3))
    two_out.wait_recv()
    two_keep.wait()
    start(seq_two)
    out_own.wait()
    acc[1] = jnp.zeros(acc.shape[1:], F32)
    for copy in seq_own[:12] + head_loads(2, 0) + head_loads(0, 1):
        copy.wait()
    pl.semaphore_wait(free_slot.at[2], 1)
    start(uc_to_t)
    project(0, 6 * slab)
    arrive((6, 7))
    for copy in seq_own[12:]:
        copy.wait()
    project(6 * slab, 2 * slab)

    def chip_step(step, carry):
        buf = step % 2
        seq = step // 4
        relation = relation_of(step)

        @pl.when(step == 4)
        def _():
            near.wait_send()
            say_free(3, SAME_F)
            say_free(4, PARTNER)
            for copy in seq_two:
                copy.wait()
            for copy in uc_to_t[:4]:
                copy.wait_recv()

        @pl.when(step >= 2)
        def _():
            for copy in head_loads(0, buf):
                copy.wait()

        @pl.when((step == 3) | (step == 4))
        def _():
            start(head_loads(relation_of(step + 1), 1 - buf))

        kept = pl.ds(pl.multiple_of(jnp.where(step < 2, step, 2) * seq_len, seq_len), seq_len)
        heads = [ring.at_traced(relation * 2 + other) for other in (1, 0)]
        wo_copies = [
            pltpu.make_async_copy(up_all.at[pl.ds(pl.multiple_of(12 * dim + (2 * buf + index) * dim, dim), dim)], wo_full.at[head], wo_sem.at[index])
            for index, head in enumerate(heads)
        ]
        start(wo_copies)

        @pl.when(step >= 2)
        def _():
            c_all[2 + buf, :, pl.ds(0, 6 * dim)] = dot_nt(u_all[2 * seq], up_all[qkv_rows(buf), :]).astype(BF16)

        for index, head in enumerate(heads):
            columns = pl.ds(pl.multiple_of(head * dim, dim), dim)
            own = pl.ds(index * 3 * dim, 3 * dim)
            query, key, value = (c_all[2 + buf, :, pl.ds((index * 3 + part) * dim, dim)] for part in range(3))
            scores = dot_nt(query, key) * (scale * LOG2_E)
            grown = jnp.exp2(scores - jnp.max(scores, axis=-1, keepdims=True))
            prob = grown * (1.0 / jnp.sum(grown, axis=-1, keepdims=True))
            prob_b = prob.astype(BF16)
            c_all[seq, :, columns] = dot_nn(prob_b, value).astype(BF16)
            if index == 0:
                @pl.when(step == 4)
                def _():
                    for copy in uc_to_t[4:]:
                        copy.wait_recv()

                @pl.when(step >= 2)
                def _():
                    c_all[2 + buf, :, pl.ds(6 * dim, 2 * dim)] = dot_nt(u_all[2 * seq + 1], up_all[wo_rows(buf), :]).astype(BF16)

            d_out = c_all[2 + buf, :, pl.ds((6 + index) * dim, dim)]
            d_prob = dot_nt(d_out, value)
            d_score = (prob * (d_prob - jnp.sum(d_prob * prob, axis=-1, keepdims=True)) * scale).astype(BF16)
            down_all[kept, pl.ds(index * 3 * dim, dim)] = dot_nn(d_score, key).astype(BF16)
            down_all[kept, pl.ds((index * 3 + 1) * dim, dim)] = dot_nn(query.T, d_score).T.astype(BF16)
            down_all[kept, pl.ds((index * 3 + 2) * dim, dim)] = dot_nn(d_out.T, prob_b).T.astype(BF16)
            @pl.when(step >= 4)
            def _():
                dst = (spare, part_keep)[index].at[buf]
                dst[pl.ds(0, 3)] += dot_tn(down_all[kept, own], u_all[2]).reshape(3, dim, hidden)
                dst[3] += dot_tn(c_all[1, :, columns], u_all[3])

            if index == 0:
                @pl.when(step == 1)
                def _():
                    att_t.wait_recv()
                    att_t_core.start()

                @pl.when(step == 4)
                def _():
                    pl.semaphore_wait(free_slot.at[4], 1)
                    core_copies[0].start()

                @pl.when(step == 5)
                def _():
                    pl.semaphore_wait(free_slot.at[4], 1)
                    core_copies[1].start()

        @pl.when(step == 1)
        def _():
            att_t_core.wait_recv()
            start(head_loads(1, 0))

        @pl.when(step == 2)
        def _():
            att_o.wait_recv()
            att_o_core.start()
            start(head_loads(3, 1)[2:])

        @pl.when(step < 4)
        def _():
            def du_tile(part, carry):
                rows = pl.ds(pl.multiple_of(jnp.where(step < 2, step, 2) * seq_len + part * half, half), half)
                acc[1, pl.ds(part * fours, fours)] += dot_nn(down_all[rows, pl.ds(0, 6 * dim)], up_all[qkv_rows(buf), :]).reshape(fours, slab, hidden)
                return carry

            lax.fori_loop(0, 2, du_tile, 0)

        @pl.when(step == 2)
        def _():
            att_o_core.wait_recv()
            start(head_loads(3, 1)[:2])

        @pl.when(step == 3)
        def _():
            start(o_out)
            start(du_out)
            du_late.start()
            o_keep.start()
            du_keep.start()

            def own_gradients(pair, carry):
                own_rows = pl.ds(pl.multiple_of(pair * seq_len, seq_len), seq_len)
                for index, other in enumerate((1, 0)):
                    columns = pl.ds(pl.multiple_of(ring.at_traced(relation_of(pair) * 2 + other) * dim, dim), dim)
                    dst = (spare, part_keep)[index].at[pair]
                    dst[pl.ds(0, 3)] = dot_tn(down_all[own_rows, pl.ds(index * 3 * dim, 3 * dim)], u_all[0]).reshape(3, dim, hidden)
                    dst[3] = dot_tn(c_all[0, :, columns], u_all[1])
                return carry

            lax.fori_loop(0, 2, own_gradients, 0)

        @pl.when(step == 4)
        def _():
            core_copies[0].wait_recv()
            part_keep[0] += acc[0, pl.ds(0, 4)]
            say_free(4, PARTNER)
            pl.semaphore_wait(free_slot.at[3], 1)
            f_copy.start()

        for copy in wo_copies:
            copy.wait()
        return carry

    lax.fori_loop(0, 6, chip_step, 0)
    for copy in o_out[:2]:
        copy.wait_recv()
    start(o_pass)
    du_out[1].wait_recv()
    du_pass.start()
    core_copies[1].wait_recv()
    part_keep[1] += acc[0, pl.ds(0, 4)]
    for copy in du_out[2:]:
        copy.wait_recv()
    for slot in range(1, 8):
        ring.copy(o_pos.at[0], o_pos.at[ring.at(slot)], near_sem.at[0], o_recv.at[slot], PARTNER).wait_recv()
    du_out[0].wait_recv()
    du_pass.wait_recv()
    near.wait_recv()
    f_copy.wait_recv()
    part_keep[1] += acc[0, pl.ds(4, 4)]
    d_att_copy = pltpu.make_async_copy(part_keep.at[1], d_att, load_sem.at[0])
    d_att_copy.start()

    sends = att_out + [att_t, att_o, att_f_core, att_t_core, att_o_core] + list(a2a_out.values()) + a2a_pass + [two_out]
    for copy in sends + o_out + du_out + o_pass + uc_to_t + core_copies + [du_pass, f_copy]:
        copy.wait_send()
    du_late.wait()
    o_keep.wait()
    du_keep.wait()
    d_att_copy.wait()


def block_call(y_one, y_two, dy_one, dy_two, w_up, w_down, w_qkv, w_out):
    slabs, slab, hidden = y_one.shape
    tokens = slabs * slab
    ffn = w_down.shape[0]
    dim = w_out.shape[0]
    any_spec = pl.BlockSpec(memory_space=pl.ANY)
    dma, vmem, wide, narrow = pltpu.SemaphoreType.DMA, pltpu.VMEM, F32, BF16
    results = [
        ((slabs, slab, hidden), wide), ((slabs, slab, hidden), wide), ((slabs, slab, hidden), wide), ((slabs, slab, hidden), wide),
        ((4, dim, hidden), wide), ((slabs, slab, hidden), narrow), ((slabs, slab, hidden), wide), ((8, dim, hidden), narrow),
        ((slab + LATE_ROWS, hidden), wide),
    ]
    landing = [
        ((8, 2, slab, hidden), narrow), ((4, 2, slab, hidden), narrow), ((8, 4 * dim, hidden), narrow), ((2, slab, hidden), narrow), ((slab, hidden), wide),
    ]
    scratch = [
        vmem((4, tokens, hidden), BF16), vmem((4, tokens, hidden), BF16), vmem((6 * ffn, hidden), BF16), vmem((6 * ffn, hidden), BF16),
        vmem((2, slabs, slab, hidden), F32), vmem((2, 5, slab, hidden), F32), vmem((2, 4, dim, hidden), F32),
        vmem((8, 2, slab, hidden), BF16),
        dma((8,)), dma((2, 3)), dma((2, 2)), dma((14,)), dma((8, 2)), dma((6,)), dma((4, 2)), dma((7,)), dma((8,)), dma((11,)), dma((8,)), dma((3,)), dma((2,)), dma((2,)),
        dma((4, 8)), dma((2, 2, 2)), dma((2,)), dma((2,)), dma((2,)), dma((2,)), dma((2, 8)), dma((10,)), dma((8,)), dma((10,)), dma((8,)), dma((2,)), dma((2,)),
        pltpu.SemaphoreType.REGULAR((5,)),
    ]
    return pl.pallas_call(
        functools.partial(block_kernel, dim ** -0.5),
        out_shape=[jax.ShapeDtypeStruct(shape, dtype) for shape, dtype in results + landing],
        in_specs=[any_spec] * 8,
        out_specs=[any_spec] * (len(results) + len(landing)),
        scratch_shapes=scratch,
        compiler_params=pltpu.CompilerParams(collective_id=0, has_side_effects=True, vmem_limit_bytes=VMEM_LIMIT),
        cost_estimate=pl.CostEstimate(flops=120 * 10**9, bytes_accessed=128 * 2**20, transcendentals=0),
        name="block",
    )(y_one, y_two, dy_one, dy_two, w_up.reshape(8, hidden // 8, ffn), w_down, w_qkv.reshape(3, 8, hidden // 8, dim), w_out)[: len(results)]


def finish_kernel(
    y_one, o_pos, wo_full, x_two, dx_one, dy_two, du_pos, part_own, near_recv, d_att,
    x_one_out, x_two_out, dx_one_out, dx_two_out, dw_up, dw_down, dw_qkv, dw_out,
    y_buf, o_buf, wo_buf, x_buf, dx_buf, dy_buf, du_buf, own_buf, near_buf, att_buf, up_out, qkv_out, load_sem, store_sem,
):
    tokens = y_buf.shape[0]
    dim = wo_buf.shape[0] // 8
    chunk = 256
    chunks = [pl.ds(index * chunk, chunk) for index in range(tokens // chunk)]

    def pieces(src, dst, sem, row):
        return [pltpu.make_async_copy(src.at[rows], dst.at[rows], sem.at[row, index]) for index, rows in enumerate(chunks)]

    def whole(src, dst, sem, row):
        return pltpu.make_async_copy(src, dst, sem.at[row, 0])

    ring = Ring()
    slab = tokens // 8
    sizes = {0: slab, PARTNER: slab, SAME_T: slab, OTHER_T: slab, SAME_F: slab - LATE_ROWS, OTHER_F: slab, OTHER_O: slab}
    slots = [pl.ds(pl.multiple_of(ring.at(slot) * slab, slab), size) for slot, size in sizes.items()]

    def slabs(src, dst, sem, row):
        return [pltpu.make_async_copy(src.at[rows], dst.at[rows], sem.at[row, index]) for index, rows in enumerate(slots)]

    x_in, dy_in, du_in = pieces(x_two, x_buf, load_sem, 0), slabs(dy_two, dy_buf, load_sem, 1), slabs(du_pos, du_buf, load_sem, 2)
    y_in, o_in = pieces(y_one, y_buf, load_sem, 3), pieces(o_pos, o_buf, load_sem, 4)
    wo_in, dx_in = whole(wo_full, wo_buf, load_sem, 5), pieces(dx_one, dx_buf, load_sem, 6)
    own_in, near_in, att_in = whole(part_own, own_buf, load_sem, 7), whole(near_recv, near_buf, load_sem, 8), whole(d_att, att_buf, load_sem, 9)
    order = [own_in, near_in, att_in, wo_in, *(copy for group in zip(y_in, o_in) for copy in group), *x_in, *(copy for group in zip(dy_in, du_in) for copy in group), *dx_in]
    for copy in order:
        copy.start()

    x_store, dx2_store, x1_store = pieces(x_buf, x_two_out, store_sem, 0), slabs(dy_buf, dx_two_out, store_sem, 1), pieces(y_buf, x_one_out, store_sem, 2)
    dx_store = pieces(dx_buf, dx_one_out, store_sem, 3)
    own_in.wait()
    near_in.wait()
    ffn = up_out.shape[1]
    own_buf[pl.ds(ffn, ffn), :] += near_buf[pl.ds(ffn, ffn), :]
    down_store = whole(own_buf.at[pl.ds(ffn, ffn)], dw_down, store_sem, 7)
    down_store.start()
    for part in range(up_out.shape[0] // ffn):
        columns = pl.ds(part * ffn, ffn)
        up_out[columns, :] = (own_buf[pl.ds(0, ffn), columns] + near_buf[pl.ds(0, ffn), columns]).T
    up_store = whole(up_out, dw_up, store_sem, 4)
    up_store.start()
    att_in.wait()
    for part in range(3):
        qkv_out[pl.ds(part, tokens, stride=3), 0, :] = att_buf[pl.ds(part * dim, dim), :].T
    qkv_store = whole(qkv_out, dw_qkv, store_sem, 5)
    qkv_store.start()
    out_store = whole(att_buf.at[pl.ds(3 * dim, dim)], dw_out, store_sem, 6)
    out_store.start()
    wo_in.wait()
    for index, rows in enumerate(chunks):
        y_in[index].wait()
        o_in[index].wait()
        y_buf[rows, :] -= dot_nn(o_buf[rows, :], wo_buf[...])
        x1_store[index].start()
    for index in range(len(chunks)):
        x_in[index].wait()
        x_store[index].start()
    for index, rows in enumerate(slots):
        dy_in[index].wait()
        du_in[index].wait()
        dy_buf[rows, :] += rms_back(x_buf[rows, :], du_buf[rows, :])
        dx2_store[index].start()
    for index in range(len(chunks)):
        dx_in[index].wait()
        dx_store[index].start()
    for copy in x_store + dx2_store + x1_store + dx_store + [up_store, qkv_store, out_store, down_store]:
        copy.wait()


def finish_call(y_one, o_pos, wo_full, x_two, dx_one, dy_two, du_pos, part_own, near_recv, d_att):
    tokens, hidden = y_one.shape
    ffn = part_own.shape[0] // 2
    dim = d_att.shape[0] // 4
    any_spec = pl.BlockSpec(memory_space=pl.ANY)
    dma, vmem = pltpu.SemaphoreType.DMA, pltpu.VMEM
    state = (tokens, hidden)
    out_shape = [jax.ShapeDtypeStruct(shape, F32) for shape in (state, state, state, state, (hidden, ffn), (ffn, hidden), (3 * hidden, 1, dim), (dim, hidden))]
    scratch = [
        vmem(state, F32), vmem(state, BF16), vmem((hidden, hidden), BF16), vmem(state, F32), vmem(state, F32), vmem(state, F32), vmem(state, F32),
        vmem(part_own.shape, F32), vmem(part_own.shape, F32), vmem(d_att.shape, F32), vmem((hidden, ffn), F32), vmem((3 * hidden, 1, dim), F32),
        dma((10, 7)), dma((8, 7)),
    ]
    return pl.pallas_call(
        finish_kernel,
        out_shape=out_shape,
        in_specs=[any_spec] * 10,
        out_specs=[any_spec] * 8,
        scratch_shapes=scratch,
        compiler_params=pltpu.CompilerParams(vmem_limit_bytes=VMEM_LIMIT),
        cost_estimate=pl.CostEstimate(flops=2 * 10**9, bytes_accessed=52 * 2**20, transcendentals=0),
        name="finish",
    )(y_one, o_pos, wo_full, x_two, dx_one, dy_two, du_pos, part_own, near_recv, d_att)


def last_kernel(x_two, dy_two, du_far, dx_two_in, dx_two_out, x_buf, dy_buf, du_buf, load_sem, store_sem):
    ring = Ring()
    slab = x_buf.shape[1]
    loads, stores, sizes = [], [], (slab, LATE_ROWS)
    for index, (slot, skip) in enumerate(((SAME_O, 0), (SAME_F, slab - LATE_ROWS))):
        size = sizes[index]
        rows = pl.ds(pl.multiple_of(ring.at(slot) * slab + skip, 16), size)
        sources = ((x_two.at[rows], x_buf), (dy_two.at[rows], dy_buf), (du_far.at[pl.ds(index * slab, size)], du_buf))
        loads.append([pltpu.make_async_copy(src, dst.at[index, pl.ds(0, size)], load_sem.at[index, which]) for which, (src, dst) in enumerate(sources)])
        stores.append(pltpu.make_async_copy(dy_buf.at[index, pl.ds(0, size)], dx_two_out.at[rows], store_sem.at[index]))
    for copies in loads:
        for copy in copies:
            copy.start()
    for index, copies in enumerate(loads):
        for copy in copies:
            copy.wait()
        rows = pl.ds(0, sizes[index])
        dy_buf[index, rows, :] += rms_back(x_buf[index, rows, :], du_buf[index, rows, :])
        stores[index].start()
    for copy in stores:
        copy.wait()


def last_call(x_two, dy_two, du_far, dx_two):
    tokens, hidden = x_two.shape
    any_spec = pl.BlockSpec(memory_space=pl.ANY)
    buf = pltpu.VMEM((2, tokens // 8, hidden), F32)
    return pl.pallas_call(
        last_kernel,
        out_shape=jax.ShapeDtypeStruct(dx_two.shape, F32),
        in_specs=[any_spec] * 4,
        out_specs=any_spec,
        input_output_aliases={3: 0},
        scratch_shapes=[buf, buf, buf, pltpu.SemaphoreType.DMA((2, 3)), pltpu.SemaphoreType.DMA((2,))],
        cost_estimate=pl.CostEstimate(flops=10**6, bytes_accessed=4 * 2**20, transcendentals=0),
        name="last",
    )(x_two, dy_two, du_far, dx_two)


def local_backward(y_one, y_two, dy_one, dy_two, w_qkv, w_out, w_up, w_down):
    hidden = y_one.shape[2]
    _, _, _, parts, dim = w_qkv.shape
    qkv_parts = jnp.swapaxes(w_qkv[0, :, 0], 0, 1)
    results = block_call(y_one, y_two, dy_one, dy_two, w_up[0], w_down[0], qkv_parts, w_out[0, 0])
    x_two, dx_one, part_own, near_recv, d_att, o_pos, du_pos, wo_full = (tensor.reshape(-1, hidden) for tensor in results[:8])
    devices = range(lax.axis_size("tp"))
    to_f = [(device, (3 - device // 2) * 2 + device % 2) for device in devices]
    du_far = lax.ppermute(results[8], "tp", to_f)
    y_flat, dy_flat = y_one.reshape(-1, hidden), dy_two.reshape(-1, hidden)
    *states, dw_up, dw_down, dw_qkv, dw_out = finish_call(y_flat, o_pos, wo_full, x_two, dx_one, dy_flat, du_pos, part_own, near_recv, d_att)
    states[3] = last_call(x_two, dy_flat, du_far, states[3])
    states = [tensor.reshape(y_one.shape) for tensor in states]
    return (*states, dw_qkv.reshape(1, hidden, 1, parts, dim), dw_out[None, None], dw_up[None], dw_down[None])


def solution(mesh):
    state_spec = P("dp", "tp", None)
    in_specs = (state_spec, state_spec, state_spec, state_spec, P(None, None, "tp", None, None), P(None, "tp", None, None), P(None, None, "tp"), P(None, "tp", None))
    out_specs = (state_spec, state_spec, state_spec, state_spec, P("dp", None, "tp", None, None), P("dp", "tp", None, None), P("dp", None, "tp"), P("dp", "tp", None))
    return jax.shard_map(local_backward, mesh=mesh, in_specs=in_specs, out_specs=out_specs, check_vma=False)
```
